32 devices in a mesh: data: 2 (over x), model: 4 (over z), stage: 4 (over y, core).
Axes of the slice: x: 2, y: 2, z: 4, core: 2. Of those that a mesh axis runs over, the one named last changes fastest.
Arguments:
- inputs: bfloat16 [12, 256, 2048], P('data'), parts along dimension 0
- targets: bfloat16 [12, 256, 2048], P('data'), parts along dimension 0
- w_in: bfloat16 [4, 1, 2048, 8192], P('stage', None, None, 'model')
- w_out: bfloat16 [4, 1, 8192, 2048], P('stage', None, 'model')
Outputs:
- output 1: float32 [8, 1, 2048, 8192], P(('data', 'stage'), None, None, 'model'), parts along dimension 0
- output 2: float32 [8, 1, 8192, 2048], P(('data', 'stage'), None, 'model'), parts along dimension 0
- output 3: float32 [2], P('data'), parts along dimension 0
There are 2 independent parts. The reference program is written for one: setup_inputs(seed, part) draws one part's arguments, and reference() takes and returns one part's arrays. A program takes and returns all parts, laid end to end along the dimension named above; an argument that names none is the same for every part.
All inputs are finite; a program needn't handle non-finite values.
Results may differ from the reference program's by a relative error of at most 0.00873894.
Values are sent between devices in bfloat16 or wider.
A program may use at most 1 GiB of HBM per device.

```python
import jax
import jax.numpy as jnp
from jax import lax

STAGES = 4
LAYERS_PER_STAGE = 1
MODEL_DIM = 2048
HIDDEN_DIM = 8192
MICRO_BATCHES = 6
MICRO_TOKENS = 256

TOTAL_LAYERS = STAGES * LAYERS_PER_STAGE
GELU_COEF = 0.7978845608028654
CUBIC_COEF = 0.044715


def gelu_tanh(values):
    inner_arg = GELU_COEF * (values + CUBIC_COEF * values * values * values)
    return 0.5 * values * (1.0 + jnp.tanh(inner_arg))


def gelu_slope(values):
    tanh_val = jnp.tanh(GELU_COEF * (values + CUBIC_COEF * values * values * values))
    return 0.5 * (1.0 + tanh_val) + 0.5 * values * (1.0 - tanh_val * tanh_val) * GELU_COEF * (1.0 + 3.0 * CUBIC_COEF * values * values)


def setup_inputs(seed: int = 0, part: int = 0) -> dict:
    part_key = jax.random.fold_in(jax.random.key(seed), part)
    key_in, key_tgt = jax.random.split(part_key, 2)
    key_w1, key_w2 = jax.random.split(jax.random.key(seed + 1), 2)
    act_shape = (MICRO_BATCHES, MICRO_TOKENS, MODEL_DIM)
    inputs = jax.random.normal(key_in, act_shape, jnp.float32).astype(jnp.bfloat16)
    targets = jax.random.normal(key_tgt, act_shape, jnp.float32).astype(jnp.bfloat16)
    in_scale = MODEL_DIM ** -0.5
    out_scale = (HIDDEN_DIM ** -0.5) * (2.0 / TOTAL_LAYERS) ** 0.5
    w_in = (jax.random.normal(key_w1, (STAGES, LAYERS_PER_STAGE, MODEL_DIM, HIDDEN_DIM), jnp.float32) * in_scale).astype(jnp.bfloat16)
    w_out = (jax.random.normal(key_w2, (STAGES, LAYERS_PER_STAGE, HIDDEN_DIM, MODEL_DIM), jnp.float32) * out_scale).astype(jnp.bfloat16)
    return {"inputs": inputs, "targets": targets, "w_in": w_in, "w_out": w_out}


def layer_forward(hidden, w_in_l, w_out_l):
    pre_act = jnp.dot(hidden, w_in_l, preferred_element_type=jnp.float32).astype(jnp.bfloat16)
    act_out = gelu_tanh(pre_act.astype(jnp.float32)).astype(jnp.bfloat16)
    branch = jnp.dot(act_out, w_out_l, preferred_element_type=jnp.float32)
    return (hidden.astype(jnp.float32) + branch).astype(jnp.bfloat16)


def layer_backward(grad_h, hidden, w_in_l, w_out_l):
    pre_act = jnp.dot(hidden, w_in_l, preferred_element_type=jnp.float32).astype(jnp.bfloat16)
    act_out = gelu_tanh(pre_act.astype(jnp.float32)).astype(jnp.bfloat16)
    grad_act = jnp.dot(grad_h, w_out_l.T, preferred_element_type=jnp.float32).astype(jnp.bfloat16)
    grad_pre = (gelu_slope(pre_act.astype(jnp.float32)) * grad_act.astype(jnp.float32)).astype(jnp.bfloat16)
    grad_prev = (grad_h.astype(jnp.float32) + jnp.dot(grad_pre, w_in_l.T, preferred_element_type=jnp.float32)).astype(jnp.bfloat16)
    part_in = jnp.dot(hidden.T, grad_pre, preferred_element_type=jnp.float32)
    part_out = jnp.dot(act_out.T, grad_h, preferred_element_type=jnp.float32)
    return grad_prev, part_in, part_out


def reference(inputs, targets, w_in, w_out):
    w_in_flat = w_in.reshape(TOTAL_LAYERS, MODEL_DIM, HIDDEN_DIM)
    w_out_flat = w_out.reshape(TOTAL_LAYERS, HIDDEN_DIM, MODEL_DIM)
    grad_scale = 1.0 / (MICRO_BATCHES * MICRO_TOKENS * MODEL_DIM)

    def fwd_step(hidden, layer_w):
        return layer_forward(hidden, layer_w[0], layer_w[1]), hidden

    def bwd_step(grad_h, layer_data):
        w_in_l, w_out_l, saved_in, acc_in, acc_out = layer_data
        grad_prev, part_in, part_out = layer_backward(grad_h, saved_in, w_in_l, w_out_l)
        return grad_prev, (acc_in + part_in, acc_out + part_out)

    def micro_step(state_in, micro_pair):
        acc_in, acc_out, loss_sum = state_in
        final_out, saved_in = lax.scan(fwd_step, micro_pair[0], (w_in_flat, w_out_flat))
        out_err = final_out.astype(jnp.float32) - micro_pair[1].astype(jnp.float32)
        start_grad = (out_err * grad_scale).astype(jnp.bfloat16)
        input_grad, (acc_in, acc_out) = lax.scan(bwd_step, start_grad, (w_in_flat, w_out_flat, saved_in, acc_in, acc_out), reverse=True)
        return (acc_in, acc_out, loss_sum + 0.5 * jnp.sum(out_err * out_err)), None

    init_state = (jnp.zeros((TOTAL_LAYERS, MODEL_DIM, HIDDEN_DIM), jnp.float32), jnp.zeros((TOTAL_LAYERS, HIDDEN_DIM, MODEL_DIM), jnp.float32), jnp.zeros((), jnp.float32))
    (acc_in, acc_out, loss_sum), unused_ys = lax.scan(micro_step, init_state, (inputs, targets))
    grad_in = acc_in.reshape(STAGES, LAYERS_PER_STAGE, MODEL_DIM, HIDDEN_DIM)
    grad_out = acc_out.reshape(STAGES, LAYERS_PER_STAGE, HIDDEN_DIM, MODEL_DIM)
    return grad_in, grad_out, jnp.reshape(loss_sum * grad_scale, (1,))
```

```python
import functools

import jax
import jax.numpy as jnp
from jax import lax
from jax.experimental import pallas as pl
from jax.experimental.pallas import tpu as pltpu
from jax.sharding import PartitionSpec as P

GELU_COEF = 0.7978845608028654
CUBIC_COEF = 0.044715

CHUNK_TOKENS = 128
PIECE_COLS = 256
HIDDEN_COLS = 512
HOP_LAG = 2
SEND_SLOTS = 4
RECV_SLOTS = 8
GATHER_SLOTS = 16

BF16 = jnp.bfloat16
F32 = jnp.float32
MESH = pl.DeviceIdType.MESH


def gelu_tanh(values):
    inner_arg = GELU_COEF * (values + CUBIC_COEF * values * values * values)
    return 0.5 * values * (1.0 + jnp.tanh(inner_arg))


def gelu_slope(values):
    tanh_val = jnp.tanh(GELU_COEF * (values + CUBIC_COEF * values * values * values))
    return 0.5 * (1.0 + tanh_val) + 0.5 * values * (1.0 - tanh_val * tanh_val) * GELU_COEF * (1.0 + 3.0 * CUBIC_COEF * values * values)


def dot_nn(left, right):
    return jnp.dot(left, right, preferred_element_type=F32)


def dot_nt(left, right):
    return lax.dot_general(left, right, (((1,), (1,)), ((), ())), preferred_element_type=F32)


def stage_kernel(
    n_stage, n_model, n_chunk, half_pieces, piece, hid_cols, hop, grad_scale,
    inputs_hbm, targets_hbm, w1_hbm, w2_hbm,
    x_out, e_out, a_out, g_out, loss_out,
    w1, w2, acts, hid, send_buf, recv_buf, loss_acc, loss_in,
    w_sem, in_sem, tgt_sem, sum_send, sum_recv, gat_send, gat_recv, fwd_send, out_sem, loss_send, loss_recv, spent_sem,
):
    pos = lax.axis_index("model")
    stage = lax.axis_index("stage")
    last_pos = n_model - 1
    last_stage = n_stage - 1
    total = n_chunk * half_pieces
    half = half_pieces * piece
    drain = 6 * hop + SEND_SLOTS
    gap = jnp.where(stage == last_stage, max(0, 6 * hop + half_pieces - total), drain)
    hid_steps = w1.shape[1] // hid_cols

    barrier = pltpu.get_barrier_semaphore()
    for to_stage in range(n_stage):
        for to_pos in range(n_model):

            @pl.when((to_stage != stage) | (to_pos != pos))
            def _():
                pl.semaphore_signal(barrier, inc=1, device_id={"stage": to_stage, "model": to_pos}, device_id_type=MESH)

    copy_w1 = pltpu.make_async_copy(w1_hbm, w1, w_sem.at[0])
    copy_w2 = pltpu.make_async_copy(w2_hbm, w2, w_sem.at[1])

    def copy_in(chunk):
        return pltpu.make_async_copy(inputs_hbm.at[chunk], acts.at[0, chunk], in_sem.at[chunk])

    def grad_in(chunk):
        return pltpu.make_async_copy(inputs_hbm.at[chunk], acts.at[1, chunk], in_sem.at[n_chunk + chunk])

    def copy_targets(side):
        cols = pl.ds(side * half, half)
        return pltpu.make_async_copy(targets_hbm.at[:, :, cols], acts.at[1, :, :, cols], tgt_sem)

    def copy_out(kind, chunk):
        src, dst = ((acts.at[0], x_out), (acts.at[1], e_out), (hid.at[0], a_out), (hid.at[1], g_out))[kind]
        return pltpu.make_async_copy(src.at[chunk], dst.at[chunk], out_sem.at[kind, chunk])

    @pl.when(stage == 0)
    def _():
        copy_in(0).start()

    copy_w1.start()
    copy_w2.start()

    @pl.when(stage == 0)
    def _():
        for chunk in range(1, n_chunk):
            copy_in(chunk).start()

    @pl.when((stage == last_stage) & (pos == last_pos))
    def _():
        copy_targets(0).start()

    @pl.when((stage == last_stage) & (pos == 0))
    def _():
        copy_targets(1).start()

    loss_acc[...] = jnp.zeros_like(loss_acc)
    pl.semaphore_wait(barrier, n_stage * n_model - 1)

    def first_product(step):
        back = step - total - gap

        @pl.when((step < total) & (step % half_pieces == 0))
        def _():
            chunk = step // half_pieces
            copy_in(chunk).wait()
            copy_out(0, chunk).start()

            @pl.when(step == 0)
            def _():
                copy_w1.wait()

            def hid_step(index, carry):
                cols = pl.ds(pl.multiple_of(index * hid_cols, hid_cols), hid_cols)
                pre = dot_nn(acts[0, chunk], w1[:, cols]).astype(BF16)
                hid[1, chunk, :, cols] = pre
                hid[0, chunk, :, cols] = gelu_tanh(pre.astype(F32)).astype(BF16)
                return carry

            lax.fori_loop(0, hid_steps, hid_step, 0)
            copy_out(2, chunk).start()

            @pl.when(step == 0)
            def _():
                copy_w2.wait()

        @pl.when((back >= 0) & (back < total) & (back % half_pieces == 0))
        def _():
            chunk = back // half_pieces

            @pl.when(stage < last_stage)
            def _():
                @pl.when(back == 0)
                def _():
                    for side in (0, 1):
                        pl.semaphore_signal(spent_sem.at[side], inc=1, device_id={"stage": stage + 1}, device_id_type=MESH)

                grad_in(chunk).wait()

            copy_out(1, chunk).start()

            @pl.when(back == 0)
            def _():
                for done in range(n_chunk):
                    copy_out(0, done).wait()

            def hid_step(index, carry):
                cols = pl.ds(pl.multiple_of(index * hid_cols, hid_cols), hid_cols)
                grad_act = dot_nt(acts[1, chunk], w2[cols, :]).astype(BF16)
                slope = gelu_slope(hid[1, chunk, :, cols].astype(F32))
                hid[1, chunk, :, cols] = (slope * grad_act.astype(F32)).astype(BF16)
                return carry

            lax.fori_loop(0, hid_steps, hid_step, 0)
            copy_out(3, chunk).start()

    def send_loss(side):
        loss_in[side] = loss_acc[...]
        for to_stage in range(n_stage):
            for to_pos in range(n_model):

                @pl.when((to_stage != stage) | (to_pos != pos))
                def _():
                    loss_copy(side, to_stage, to_pos).start()

    def loss_copy(side, to_stage, to_pos):
        return pltpu.make_async_remote_copy(
            src_ref=loss_acc,
            dst_ref=loss_in.at[side],
            send_sem=loss_send.at[to_stage * n_model + to_pos],
            recv_sem=loss_recv.at[side],
            device_id={"stage": to_stage, "model": to_pos},
            device_id_type=MESH,
        )

    def turn(place):
        back = place - total - gap
        fwd = (place >= 0) & (place < total)
        bwd = (back >= 0) & (back < total) & (stage > 0)
        old = (place >= SEND_SLOTS) & (place < total + SEND_SLOTS)
        old_b = (back >= SEND_SLOTS) & (back < total + SEND_SLOTS) & (stage > 0)
        is_back = (back >= 0).astype(jnp.int32)
        return fwd, bwd, old, old_b, is_back, place - is_back * (total + gap)

    def piece_at(side, index):
        col = side * half + (index % half_pieces) * piece
        return index // half_pieces, pl.ds(pl.multiple_of(col, piece), piece)

    def sum_step(side, step):
        rank = pos if side == 0 else last_pos - pos
        nxt = pos + 1 if side == 0 else pos - 1
        place = step - hop * rank
        fwd, bwd, old, old_b, is_back, index = turn(place)
        out = lax.rem(place + 8 * SEND_SLOTS, SEND_SLOTS)
        inn = lax.rem(place + 8 * RECV_SLOTS, RECV_SLOTS)
        chunk, cols = piece_at(side, index)

        def hand_on():
            return pltpu.make_async_remote_copy(
                src_ref=send_buf.at[side, out],
                dst_ref=recv_buf.at[side, inn],
                send_sem=sum_send.at[side, out],
                recv_sem=sum_recv.at[side, inn],
                device_id={"model": nxt},
                device_id_type=MESH,
            )

        @pl.when((old | old_b) & (rank < last_pos))
        def _():
            hand_on().wait_send()

        @pl.when(fwd)
        def _():
            send_buf[side, out] = dot_nn(hid[0, chunk], w2[:, cols])

        @pl.when(bwd)
        def _():
            send_buf[side, out] = dot_nt(hid[1, chunk], w1[cols, :])

        @pl.when(fwd | bwd)
        def _():
            @pl.when(rank > 0)
            def _():
                hand_on().wait_recv()
                send_buf[side, out] = send_buf[side, out] + recv_buf[side, inn]

            @pl.when(rank < last_pos)
            def _():
                hand_on().start()

            @pl.when(rank == last_pos)
            def _():
                whole = acts[is_back, chunk, :, cols].astype(F32) + send_buf[side, out]
                scored = fwd & (stage == last_stage)

                @pl.when(scored)
                def _():
                    @pl.when(index == 0)
                    def _():
                        copy_targets(side).wait()

                    err = whole.astype(BF16).astype(F32) - acts[1, chunk, :, cols].astype(F32)
                    acts[1, chunk, :, cols] = (err * grad_scale).astype(BF16)
                    square = jnp.sum((err * err).reshape(err.shape[0] // 8, 8, piece), axis=0)
                    part = square[:, :128]
                    for lane in range(1, piece // 128):
                        part = part + square[:, lane * 128 : (lane + 1) * 128]
                    loss_acc[...] = loss_acc[...] + part

                    @pl.when(index == total - 1)
                    def _():
                        send_loss(side)

                @pl.when(jnp.logical_not(scored))
                def _():
                    acts[1 - is_back, chunk, :, cols] = whole.astype(BF16)

    def gather_step(side, step):
        rank = pos if side == 0 else last_pos - pos
        nxt = pos - 1 if side == 0 else pos + 1
        place = step - 3 * hop - hop * (last_pos - rank)
        fwd, bwd, old, old_b, is_back, index = turn(place)
        out = lax.rem(place + 8 * SEND_SLOTS, SEND_SLOTS)
        inn = lax.rem(place + 8 * GATHER_SLOTS, GATHER_SLOTS)
        chunk, cols = piece_at(side, index)

        def hand_on():
            return pltpu.make_async_remote_copy(
                src_ref=acts.at[1 - is_back, chunk, :, cols],
                dst_ref=acts.at[1 - is_back, chunk, :, cols],
                send_sem=gat_send.at[side, out],
                recv_sem=gat_recv.at[side, inn],
                device_id={"model": nxt},
                device_id_type=MESH,
            )

        def hand_over():
            return pltpu.make_async_remote_copy(
                src_ref=acts.at[1 - is_back, chunk, :, cols],
                dst_ref=acts.at[is_back, chunk, :, cols],
                send_sem=fwd_send.at[side, out],
                recv_sem=in_sem.at[is_back * n_chunk + chunk],
                device_id={"stage": stage + 1 - 2 * is_back},
                device_id_type=MESH,
            )

        def spent():
            return pltpu.make_async_remote_copy(
                src_ref=acts.at[0, 0, :, pl.ds(0, piece)],
                dst_ref=acts.at[0, 0, :, pl.ds(0, piece)],
                send_sem=gat_send.at[side, out],
                recv_sem=gat_recv.at[side, inn],
                device_id={"model": nxt},
                device_id_type=MESH,
            )

        def spent_over():
            return pltpu.make_async_remote_copy(
                src_ref=acts.at[0, 0, :, pl.ds(0, piece)],
                dst_ref=acts.at[0, 0, :, pl.ds(0, piece)],
                send_sem=fwd_send.at[side, out],
                recv_sem=gat_recv.at[side, inn],
                device_id={"model": nxt},
                device_id_type=MESH,
            )

        @pl.when((old | old_b) & (rank > 0))
        def _():
            spent().wait_send()

        @pl.when((old & (stage < last_stage)) | old_b)
        def _():
            spent_over().wait_send()

        @pl.when(fwd | bwd)
        def _():
            @pl.when(rank < last_pos)
            def _():
                hand_on().wait_recv()

            @pl.when(rank > 0)
            def _():
                hand_on().start()

            @pl.when(bwd & (index == total - half_pieces))
            def _():
                pl.semaphore_wait(spent_sem.at[side], 1)

            @pl.when(bwd | (stage < last_stage))
            def _():
                hand_over().start()

    def loop_step(step, carry):
        first_product(step)
        sum_step(0, step)
        sum_step(1, step)
        gather_step(0, step)
        gather_step(1, step)
        return carry

    lax.fori_loop(0, 2 * total + 2 * drain, loop_step, 0)

    for side, owner in ((0, last_pos), (1, 0)):
        owns = (stage == last_stage) & (pos == owner)

        @pl.when(jnp.logical_not(owns))
        def _():
            loss_copy(side, 0, 0).wait_recv()

        @pl.when(owns)
        def _():
            for to_stage in range(n_stage):
                for to_pos in range(n_model):

                    @pl.when((to_stage != stage) | (to_pos != pos))
                    def _():
                        loss_copy(side, to_stage, to_pos).wait_send()

    loss_out[...] = jnp.full(loss_out.shape, jnp.sum(loss_in[0] + loss_in[1]) * (0.5 * grad_scale), F32)
    for chunk in range(n_chunk):
        for kind in (1, 2, 3):
            copy_out(kind, chunk).wait()


def solution(mesh):
    n_stage = mesh.shape["stage"]
    n_model = mesh.shape["model"]

    def stage_step(inputs, targets, w_in, w_out):
        num_micro, num_tokens, model_dim = inputs.shape
        hid_dim = w_in.shape[3]
        rows = num_micro * num_tokens
        chunk = min(CHUNK_TOKENS, num_tokens)
        n_chunk = rows // chunk
        piece = min(PIECE_COLS, model_dim // 2)
        half_pieces = model_dim // 2 // piece
        hid_cols = min(HIDDEN_COLS, hid_dim)
        grad_scale = 1.0 / (rows * model_dim)
        kernel = functools.partial(
            stage_kernel, n_stage, n_model, n_chunk, half_pieces, piece, hid_cols, HOP_LAG, grad_scale
        )
        any_space = pl.BlockSpec(memory_space=pl.ANY)
        dma = pltpu.SemaphoreType.DMA
        layer_in, layer_grad, layer_act, layer_pre, loss = pl.pallas_call(
            kernel,
            out_shape=(
                jax.ShapeDtypeStruct((n_chunk, chunk, model_dim), BF16),
                jax.ShapeDtypeStruct((n_chunk, chunk, model_dim), BF16),
                jax.ShapeDtypeStruct((n_chunk, chunk, hid_dim), BF16),
                jax.ShapeDtypeStruct((n_chunk, chunk, hid_dim), BF16),
                jax.ShapeDtypeStruct((8, 128), F32),
            ),
            in_specs=[any_space] * 4,
            out_specs=(any_space, any_space, any_space, any_space, pl.BlockSpec(memory_space=pltpu.VMEM)),
            scratch_shapes=[
                pltpu.VMEM((model_dim, hid_dim), BF16),
                pltpu.VMEM((hid_dim, model_dim), BF16),
                pltpu.VMEM((2, n_chunk, chunk, model_dim), BF16),
                pltpu.VMEM((2, n_chunk, chunk, hid_dim), BF16),
                pltpu.VMEM((2, SEND_SLOTS, chunk, piece), F32),
                pltpu.VMEM((2, RECV_SLOTS, chunk, piece), F32),
                pltpu.VMEM((8, 128), F32),
                pltpu.VMEM((2, 8, 128), F32),
                dma((2,)),
                dma((2 * n_chunk,)),
                dma,
                dma((2, SEND_SLOTS)),
                dma((2, RECV_SLOTS)),
                dma((2, SEND_SLOTS)),
                dma((2, GATHER_SLOTS)),
                dma((2, SEND_SLOTS)),
                dma((4, n_chunk)),
                dma((n_stage * n_model,)),
                dma((2,)),
                pltpu.SemaphoreType.REGULAR((2,)),
            ],
            compiler_params=pltpu.CompilerParams(collective_id=0, has_side_effects=True, vmem_limit_bytes=62 * 1024 * 1024),
            name="stage_kernel",
        )(
            inputs.reshape(n_chunk, chunk, model_dim),
            targets.reshape(n_chunk, chunk, model_dim),
            w_in.reshape(model_dim, hid_dim),
            w_out.reshape(hid_dim, model_dim),
        )

        def over_rows(left, right):
            left = left.reshape(rows, left.shape[2])
            right = right.reshape(rows, right.shape[2])
            return lax.dot_general(left, right, (((0,), (0,)), ((), ())), preferred_element_type=F32)

        grad_in = over_rows(layer_in, layer_pre)
        grad_out = over_rows(layer_act, layer_grad)
        return grad_in[None, None], grad_out[None, None], loss[0, :1]

    return jax.shard_map(
        stage_step,
        mesh=mesh,
        in_specs=(P("data", None, None), P("data", None, None), P("stage", None, None, "model"), P("stage", None, "model", None)),
        out_specs=(P(("data", "stage"), None, None, "model"), P(("data", "stage"), None, "model", None), P("data")),
        check_vma=False,
    )
```

```python
import functools

import jax
import jax.numpy as jnp
from jax import lax
from jax.experimental import pallas as pl
from jax.experimental.pallas import tpu as pltpu
from jax.sharding import PartitionSpec as P

GELU_COEF = 0.7978845608028654
CUBIC_COEF = 0.044715

CHUNK_TOKENS = 64
PIECE_COLS = 256
HIDDEN_COLS = 512
PARTS = 2
HOP_LAG = 2
RECV_SLOTS = 8
LAST_LEAD = 5
PREV_LEAD = 16
FIRST_IDLE = 11
NEXT_IDLE = 7

BF16 = jnp.bfloat16
F32 = jnp.float32
MESH = pl.DeviceIdType.MESH


def gelu_tanh(values):
    inner_arg = GELU_COEF * (values + CUBIC_COEF * values * values * values)
    return 0.5 * values * (1.0 + jnp.tanh(inner_arg))


def gelu_slope(values):
    tanh_val = jnp.tanh(GELU_COEF * (values + CUBIC_COEF * values * values * values))
    return 0.5 * (1.0 + tanh_val) + 0.5 * values * (1.0 - tanh_val * tanh_val) * GELU_COEF * (1.0 + 3.0 * CUBIC_COEF * values * values)


def dot_nn(left, right):
    return jnp.dot(left, right, preferred_element_type=F32)


def dot_nt(left, right):
    return lax.dot_general(left, right, (((1,), (1,)), ((), ())), preferred_element_type=F32)


def stage_kernel(
    n_stage, n_model, n_chunk, half_pieces, piece, hop, lead, idle, grad_scale,
    inputs_hbm, targets_hbm, w1_hbm, w2_hbm,
    x_out, e_out, a_out, g_out, loss_out,
    wts, acts, hid, send_buf, recv_buf, loss_acc, loss_in,
    w_sem, in_sem, tgt_sem, sum_send, sum_recv, gat_send, gat_recv, over_send, back_send, back_recv, down_send, out_sem,
    loss_send, loss_recv, spent_sem,
):
    pos = lax.axis_index("model")
    stage = lax.axis_index("stage")
    last_pos = n_model - 1
    last_stage = n_stage - 1
    slots = half_pieces
    total = n_chunk * half_pieces
    half = half_pieces * piece
    hid_dim = wts.shape[2]
    hid_part = hid_dim // PARTS
    hid_cols = min(HIDDEN_COLS, hid_part)
    n_lead, n_idle = jnp.int32(n_chunk), jnp.int32(0)
    for at in range(n_stage):
        n_lead = jnp.where(stage == at, lead[at], n_lead)
        n_idle = jnp.where(stage == at, idle[at], n_idle)
    turns = 2 * n_chunk + n_idle
    early = half_pieces + 3 * hop

    barrier = pltpu.get_barrier_semaphore()
    for to_stage in range(n_stage):
        for to_pos in range(n_model):

            @pl.when((to_stage != stage) | (to_pos != pos))
            def _():
                pl.semaphore_signal(barrier, inc=1, device_id={"stage": to_stage, "model": to_pos}, device_id_type=MESH)

    copy_w1 = pltpu.make_async_copy(w1_hbm, wts.at[0], w_sem.at[0])
    copy_w2 = pltpu.make_async_copy(w2_hbm, wts.at[1], w_sem.at[1])

    def copy_in(chunk):
        return pltpu.make_async_copy(inputs_hbm.at[chunk], acts.at[0, chunk], in_sem.at[chunk])

    def copy_targets(side):
        cols = pl.ds(side * half, half)
        return pltpu.make_async_copy(targets_hbm.at[:, :, cols], acts.at[1, :, :, cols], tgt_sem)

    def copy_out(kind, chunk):
        src, dst = ((acts.at[0], x_out), (acts.at[1], e_out), (hid.at[0], a_out), (hid.at[1], g_out))[kind]
        return pltpu.make_async_copy(src.at[chunk], dst.at[chunk], out_sem.at[kind, chunk])

    @pl.when(stage == 0)
    def _():
        copy_in(0).start()

    copy_w1.start()
    copy_w2.start()

    @pl.when(stage == 0)
    def _():
        def start_in(chunk, carry):
            copy_in(chunk).start()
            return carry

        lax.fori_loop(1, n_chunk, start_in, 0)

    @pl.when((stage == last_stage) & (pos == last_pos))
    def _():
        copy_targets(0).start()

    @pl.when((stage == last_stage) & (pos == 0))
    def _():
        copy_targets(1).start()

    def transpose_weights():
        tile = min(256, hid_dim)
        count = hid_dim // tile

        def one(index, carry):
            rows = pl.ds(pl.multiple_of((index // count) * tile, tile), tile)
            cols = pl.ds(pl.multiple_of((index % count) * tile, tile), tile)
            wts[2, cols, rows] = jnp.swapaxes(wts[1, rows, cols], 0, 1)
            wts[3, cols, rows] = jnp.swapaxes(wts[0, rows, cols], 0, 1)
            return carry

        lax.fori_loop(0, count * count, one, 0)

    loss_acc[...] = jnp.zeros_like(loss_acc)
    copy_w1.wait()

    @pl.when(stage > 0)
    def _():
        copy_w2.wait()
        transpose_weights()

    pl.semaphore_wait(barrier, n_stage * n_model - 1)

    def turn_at(place):
        inside = (place >= 0) & (place < turns * half_pieces)
        place = jnp.clip(place, 0, turns * half_pieces - 1)
        turn = place // half_pieces
        after = turn - n_lead - n_idle
        mixed = after < 2 * (n_chunk - n_lead)
        pair = jnp.maximum(after, 0) // 2
        odd = jnp.maximum(after, 0) - 2 * pair
        leads = turn < n_lead
        fwd = leads | ((after >= 0) & mixed & (odd == 1))
        bwd = (after >= 0) & jnp.logical_not(mixed & (odd == 1))
        chunk = jnp.where(leads, turn, jnp.where(mixed, pair + odd * n_lead, after - (n_chunk - n_lead)))
        chunk = jnp.clip(chunk, 0, n_chunk - 1)
        return inside & fwd, inside & bwd, chunk, chunk * half_pieces + place % half_pieces

    def piece_at(side, index):
        col = side * half + (index % half_pieces) * piece
        return pl.ds(pl.multiple_of(col, piece), piece)

    def remote(src, dst, send_sem, recv_sem, device):
        return pltpu.make_async_remote_copy(
            src_ref=src, dst_ref=dst, send_sem=send_sem, recv_sem=recv_sem, device_id=device, device_id_type=MESH
        )

    def left(send_sem, like):
        remote(like, like, send_sem, loss_recv.at[0], {"model": pos}).wait_send()

    any_piece = acts.at[0, 0, :, pl.ds(0, piece)]
    any_sum = send_buf.at[0, 0]

    def rank_of(side):
        return pos if side == 0 else last_pos - pos

    def up(side):
        return {"model": pos + 1 if side == 0 else pos - 1}

    def down(side):
        return {"model": pos - 1 if side == 0 else pos + 1}

    def first_product(step, part):
        place = step + PARTS - 1 - part
        fwd, bwd, chunk, index = turn_at(place)
        starts = (place >= 0) & (place % half_pieces == 0)

        @pl.when(starts & fwd)
        def _():
            if part == 0:
                copy_in(chunk).wait()
                copy_out(0, chunk).start()
            for col in range(part * hid_part, (part + 1) * hid_part, hid_cols):
                cols = pl.ds(col, hid_cols)
                pre = dot_nn(acts[0, chunk], wts[0, :, cols]).astype(BF16)
                hid[1, chunk, :, cols] = pre
                hid[0, chunk, :, cols] = gelu_tanh(pre.astype(F32)).astype(BF16)
            if part == PARTS - 1:
                copy_out(2, chunk).start()

                @pl.when((stage == 0) & (index == 0))
                def _():
                    copy_w2.wait()

        @pl.when(starts & bwd)
        def _():
            if part == 0:
                copy_out(1, chunk).start()
                copy_out(0, chunk).wait()
            for col in range(part * hid_part, (part + 1) * hid_part, hid_cols):
                cols = pl.ds(col, hid_cols)
                grad_act = dot_nn(acts[1, chunk], wts[2, :, cols]).astype(BF16)
                slope = gelu_slope(hid[1, chunk, :, cols].astype(F32))
                hid[1, chunk, :, cols] = (slope * grad_act.astype(F32)).astype(BF16)
            if part == PARTS - 1:
                copy_out(3, chunk).start()

        if part == 0:

            @pl.when((stage == 0) & (place == n_lead * half_pieces))
            def _():
                transpose_weights()

    def loss_copy(side, to_stage, to_pos):
        return remote(
            loss_acc, loss_in.at[side], loss_send.at[to_stage * n_model + to_pos], loss_recv.at[side],
            {"stage": to_stage, "model": to_pos},
        )

    def send_loss(side):
        loss_in[side] = loss_acc[...]
        for to_stage in range(n_stage):
            for to_pos in range(n_model):

                @pl.when((to_stage != stage) | (to_pos != pos))
                def _():
                    loss_copy(side, to_stage, to_pos).start()

    def sum_steps(step):
        now = []
        for side in (0, 1):
            rank = rank_of(side)
            place = step - hop * rank
            fwd, bwd, chunk, index = turn_at(place)
            old_fwd, old_bwd, _, _ = turn_at(place - slots)
            out = jnp.maximum(place, 0) % slots
            inn = jnp.maximum(place, 0) % RECV_SLOTS
            is_back = bwd.astype(jnp.int32)
            sums = fwd | (bwd & (stage > 0))
            now.append((rank, fwd, bwd, sums, is_back, chunk, index, out, inn, piece_at(side, index)))

            @pl.when((old_fwd | (old_bwd & (stage > 0))) & (rank < last_pos))
            def _():
                left(sum_send.at[side, out], any_sum)

            @pl.when(old_bwd & (stage > 0) & (rank == last_pos))
            def _():
                left(down_send.at[side, out], any_piece)

        @pl.when(now[0][3] | now[1][3])
        def _():
            for side in (0, 1):
                _, _, _, _, is_back, chunk, _, out, _, cols = now[side]
                send_buf[side, out] = dot_nn(hid[is_back, chunk], wts[1 + 2 * is_back, :, cols])

        for side in (0, 1):
            rank, fwd, bwd, sums, is_back, chunk, index, out, inn, cols = now[side]
            hand_on = remote(
                send_buf.at[side, out], recv_buf.at[side, inn], sum_send.at[side, out], sum_recv.at[side, inn], up(side)
            )

            @pl.when(sums & (rank > 0))
            def _():
                hand_on.wait_recv()
                send_buf[side, out] = send_buf[side, out] + recv_buf[side, inn]

            @pl.when(sums & (rank < last_pos))
            def _():
                hand_on.start()

            @pl.when(sums & (rank == last_pos))
            def _():
                whole = acts[is_back, chunk, :, cols].astype(F32) + send_buf[side, out]
                scored = fwd & (stage == last_stage)

                @pl.when(scored)
                def _():
                    @pl.when(index == 0)
                    def _():
                        copy_targets(side).wait()

                    err = whole.astype(BF16).astype(F32) - acts[1, chunk, :, cols].astype(F32)
                    acts[1, chunk, :, cols] = (err * grad_scale).astype(BF16)
                    square = jnp.sum((err * err).reshape(err.shape[0] // 8, 8, piece), axis=0)
                    part = square[:, :128]
                    for lane in range(1, piece // 128):
                        part = part + square[:, lane * 128 : (lane + 1) * 128]
                    loss_acc[...] = loss_acc[...] + part

                    @pl.when(index == total - 1)
                    def _():
                        send_loss(side)

                @pl.when(jnp.logical_not(scored))
                def _():
                    acts[1 - is_back, chunk, :, cols] = whole.astype(BF16)

                @pl.when(bwd & (index == total - half_pieces))
                def _():
                    pl.semaphore_wait(spent_sem.at[side], 1)

                @pl.when(bwd)
                def _():
                    remote(
                        acts.at[0, chunk, :, cols], acts.at[1, chunk, :, cols], down_send.at[side, out],
                        back_recv.at[side, index], {"stage": stage - 1},
                    ).start()

    def gather_step(side, step):
        rank = rank_of(side)
        place = step - 3 * hop - hop * (last_pos - rank)
        fwd, _, chunk, index = turn_at(place)
        old, _, _, old_index = turn_at(place - slots)
        out = jnp.maximum(place, 0) % slots
        cols = piece_at(side, index)
        here = acts.at[1, chunk, :, cols]
        hand_on = remote(here, here, gat_send.at[side, out], gat_recv.at[side, index], down(side))

        @pl.when(old & (rank > 0))
        def _():
            left(gat_send.at[side, out], any_piece)

        @pl.when(old & (stage < last_stage))
        def _():
            left(over_send.at[side, out], any_piece)

            @pl.when((old_index == total - 1) & (rank == last_pos))
            def _():
                pl.semaphore_signal(spent_sem.at[side], inc=1, device_id={"stage": stage + 1}, device_id_type=MESH)

        @pl.when(fwd & (rank < last_pos))
        def _():
            hand_on.wait_recv()

        @pl.when(fwd & (rank > 0))
        def _():
            hand_on.start()

        @pl.when(fwd & (stage < last_stage))
        def _():
            remote(here, acts.at[0, chunk, :, cols], over_send.at[side, out], in_sem.at[chunk], {"stage": stage + 1}).start()

    def back_step(side, step):
        rank = rank_of(side)
        place = step + early - hop * (last_pos - rank)
        _, bwd, chunk, index = turn_at(place)
        _, old, _, _ = turn_at(place - slots)
        out = jnp.maximum(place, 0) % slots
        here = acts.at[1, chunk, :, piece_at(side, index)]
        hand_on = remote(here, here, back_send.at[side, out], back_recv.at[side, index], down(side))

        @pl.when(old & (rank > 0) & (stage < last_stage))
        def _():
            left(back_send.at[side, out], any_piece)

        @pl.when(bwd & (stage < last_stage))
        def _():
            hand_on.wait_recv()

            @pl.when(rank > 0)
            def _():
                hand_on.start()

    def loop_step(step, carry):
        back_step(0, step)
        back_step(1, step)
        for part in range(PARTS):
            first_product(step, part)
        sum_steps(step)
        gather_step(0, step)
        gather_step(1, step)
        return carry

    lax.fori_loop(1 - PARTS, (2 * n_chunk + max(idle)) * half_pieces + 6 * hop + slots, loop_step, 0)

    for side, owner in ((0, last_pos), (1, 0)):
        owns = (stage == last_stage) & (pos == owner)

        @pl.when(jnp.logical_not(owns))
        def _():
            loss_copy(side, 0, 0).wait_recv()

        @pl.when(owns)
        def _():
            for to_stage in range(n_stage):
                for to_pos in range(n_model):

                    @pl.when((to_stage != stage) | (to_pos != pos))
                    def _():
                        loss_copy(side, to_stage, to_pos).wait_send()

    loss_out[...] = jnp.full(loss_out.shape, jnp.sum(loss_in[0] + loss_in[1]) * (0.5 * grad_scale), F32)

    def end_out(chunk, carry):
        for kind in (1, 2, 3):
            copy_out(kind, chunk).wait()
        return carry

    lax.fori_loop(0, n_chunk, end_out, 0)


def solution(mesh):
    n_stage = mesh.shape["stage"]
    n_model = mesh.shape["model"]

    def stage_step(inputs, targets, w_in, w_out):
        num_micro, num_tokens, model_dim = inputs.shape
        hid_dim = w_in.shape[3]
        rows = num_micro * num_tokens
        chunk = min(CHUNK_TOKENS, num_tokens)
        n_chunk = rows // chunk
        piece = min(PIECE_COLS, model_dim // 2)
        half_pieces = model_dim // 2 // piece
        grad_scale = 1.0 / (rows * model_dim)
        lead = [n_chunk] * (n_stage - 2) + [min(PREV_LEAD, n_chunk), min(LAST_LEAD, n_chunk)]
        idle = [FIRST_IDLE] + [NEXT_IDLE] * (n_stage - 3) + [0, 0]
        kernel = functools.partial(stage_kernel, n_stage, n_model, n_chunk, half_pieces, piece, HOP_LAG, lead, idle, grad_scale)
        any_space = pl.BlockSpec(memory_space=pl.ANY)
        dma = pltpu.SemaphoreType.DMA
        layer_in, layer_grad, layer_act, layer_pre, loss = pl.pallas_call(
            kernel,
            out_shape=(
                jax.ShapeDtypeStruct((n_chunk, chunk, model_dim), BF16),
                jax.ShapeDtypeStruct((n_chunk, chunk, model_dim), BF16),
                jax.ShapeDtypeStruct((n_chunk, chunk, hid_dim), BF16),
                jax.ShapeDtypeStruct((n_chunk, chunk, hid_dim), BF16),
                jax.ShapeDtypeStruct((8, 128), F32),
            ),
            in_specs=[any_space] * 4,
            out_specs=(any_space, any_space, any_space, any_space, pl.BlockSpec(memory_space=pltpu.VMEM)),
            scratch_shapes=[
                pltpu.VMEM((4, model_dim, hid_dim), BF16),
                pltpu.VMEM((2, n_chunk, chunk, model_dim), BF16),
                pltpu.VMEM((2, n_chunk, chunk, hid_dim), BF16),
                pltpu.VMEM((2, half_pieces, chunk, piece), F32),
                pltpu.VMEM((2, RECV_SLOTS, chunk, piece), F32),
                pltpu.VMEM((8, 128), F32),
                pltpu.VMEM((2, 8, 128), F32),
                dma((2,)),
                dma((n_chunk,)),
                dma,
                dma((2, half_pieces)),
                dma((2, RECV_SLOTS)),
                dma((2, half_pieces)),
                dma((2, n_chunk * half_pieces)),
                dma((2, half_pieces)),
                dma((2, half_pieces)),
                dma((2, n_chunk * half_pieces)),
                dma((2, half_pieces)),
                dma((4, n_chunk)),
                dma((n_stage * n_model,)),
                dma((2,)),
                pltpu.SemaphoreType.REGULAR((2,)),
            ],
            compiler_params=pltpu.CompilerParams(collective_id=0, has_side_effects=True, vmem_limit_bytes=63 * 1024 * 1024),
            name="stage_kernel",
        )(
            inputs.reshape(n_chunk, chunk, model_dim),
            targets.reshape(n_chunk, chunk, model_dim),
            w_in.reshape(model_dim, hid_dim),
            w_out.reshape(hid_dim, model_dim),
        )

        def over_rows(left, right):
            left = left.reshape(rows, left.shape[2])
            right = right.reshape(rows, right.shape[2])
            return lax.dot_general(left, right, (((0,), (0,)), ((), ())), preferred_element_type=F32)

        grad_in = over_rows(layer_in, layer_pre)
        grad_out = over_rows(layer_act, layer_grad)
        return grad_in[None, None], grad_out[None, None], loss[0, :1]

    return jax.shard_map(
        stage_step,
        mesh=mesh,
        in_specs=(P("data", None, None), P("data", None, None), P("stage", None, None, "model"), P("stage", None, "model", None)),
        out_specs=(P(("data", "stage"), None, None, "model"), P(("data", "stage"), None, "model", None), P("data")),
        check_vma=False,
    )
```

```python
import functools

import jax
import jax.numpy as jnp
from jax import lax
from jax.experimental import pallas as pl
from jax.experimental.pallas import tpu as pltpu
from jax.sharding import PartitionSpec as P

GELU_COEF = 0.7978845608028654
CUBIC_COEF = 0.044715

CHUNK_TOKENS = 64
PIECE_COLS = 256
HIDDEN_COLS = 512
PARTS = 2
HOP_LAG = 2
RECV_SLOTS = 8
LAST_LEAD = 5
PREV_LEAD = 16
FIRST_IDLE = 11
NEXT_IDLE = 7

BF16 = jnp.bfloat16
F32 = jnp.float32
MESH = pl.DeviceIdType.MESH


def gelu_tanh(values):
    inner_arg = GELU_COEF * (values + CUBIC_COEF * values * values * values)
    return 0.5 * values * (1.0 + jnp.tanh(inner_arg))


def gelu_slope(values):
    tanh_val = jnp.tanh(GELU_COEF * (values + CUBIC_COEF * values * values * values))
    return 0.5 * (1.0 + tanh_val) + 0.5 * values * (1.0 - tanh_val * tanh_val) * GELU_COEF * (1.0 + 3.0 * CUBIC_COEF * values * values)


def dot_nn(left, right):
    return jnp.dot(left, right, preferred_element_type=F32)


def dot_nt(left, right):
    return lax.dot_general(left, right, (((1,), (1,)), ((), ())), preferred_element_type=F32)


def stage_kernel(
    n_stage, n_model, n_chunk, half_pieces, piece, hop, lead, idle, grad_scale,
    inputs_hbm, targets_hbm, w1_hbm, w2_hbm,
    x_out, e_out, a_out, g_out, loss_out,
    wts, acts, hid, send_buf, recv_buf, loss_acc, loss_in,
    w_sem, in_sem, tgt_sem, sum_send, sum_recv, gat_send, gat_recv, over_send, back_send, back_recv, down_send, out_sem,
    loss_send, loss_recv, spent_sem,
):
    pos = lax.axis_index("model")
    stage = lax.axis_index("stage")
    last_pos = n_model - 1
    last_stage = n_stage - 1
    slots = half_pieces
    total = n_chunk * half_pieces
    half = half_pieces * piece
    hid_dim = wts.shape[2]
    chunk_rows = acts.shape[2]
    hid_part = hid_dim // PARTS
    hid_cols = min(HIDDEN_COLS, hid_part)
    n_lead, n_idle = jnp.int32(n_chunk), jnp.int32(0)
    for at in range(n_stage):
        n_lead = jnp.where(stage == at, lead[at], n_lead)
        n_idle = jnp.where(stage == at, idle[at], n_idle)
    turns = 2 * n_chunk + n_idle
    n_steps = turns * half_pieces + jnp.where(stage == 0, max(1 - half_pieces, -hop), 6 * hop + slots)
    early = half_pieces + 3 * hop

    barrier = pltpu.get_barrier_semaphore()
    for to_stage in range(n_stage):
        for to_pos in range(n_model):

            @pl.when((to_stage != stage) | (to_pos != pos))
            def _():
                pl.semaphore_signal(barrier, inc=1, device_id={"stage": to_stage, "model": to_pos}, device_id_type=MESH)

    copy_w1 = pltpu.make_async_copy(w1_hbm, wts.at[0], w_sem.at[0])
    copy_w2 = pltpu.make_async_copy(w2_hbm, wts.at[1], w_sem.at[1])

    def copy_in(chunk):
        return pltpu.make_async_copy(inputs_hbm.at[chunk], acts.at[0, chunk], in_sem.at[chunk])

    def copy_targets(side):
        cols = pl.ds(side * half, half)
        return pltpu.make_async_copy(targets_hbm.at[:, :, cols], acts.at[1, :, :, cols], tgt_sem)

    def copy_out(kind, chunk):
        src, dst = ((acts.at[0], x_out), (acts.at[1], e_out), (hid.at[0], a_out), (hid.at[1], g_out))[kind]
        rows = pl.ds(pl.multiple_of(chunk * chunk_rows, chunk_rows), chunk_rows)
        return pltpu.make_async_copy(src.at[chunk], dst.at[rows, :], out_sem.at[kind, chunk])

    @pl.when(stage == 0)
    def _():
        copy_in(0).start()

    copy_w1.start()
    copy_w2.start()

    @pl.when(stage == 0)
    def _():
        def start_in(chunk, carry):
            copy_in(chunk).start()
            return carry

        lax.fori_loop(1, n_chunk, start_in, 0)

    @pl.when((stage == last_stage) & (pos == last_pos))
    def _():
        copy_targets(0).start()

    @pl.when((stage == last_stage) & (pos == 0))
    def _():
        copy_targets(1).start()

    def transpose_weights():
        tile = min(256, hid_dim)
        count = hid_dim // tile

        def one(index, carry):
            rows = pl.ds(pl.multiple_of((index // count) * tile, tile), tile)
            cols = pl.ds(pl.multiple_of((index % count) * tile, tile), tile)
            wts[2, cols, rows] = jnp.swapaxes(wts[1, rows, cols], 0, 1)
            wts[3, cols, rows] = jnp.swapaxes(wts[0, rows, cols], 0, 1)
            return carry

        lax.fori_loop(0, count * count, one, 0)

    loss_acc[...] = jnp.zeros_like(loss_acc)
    copy_w1.wait()

    @pl.when(stage > 0)
    def _():
        copy_w2.wait()
        transpose_weights()

    pl.semaphore_wait(barrier, n_stage * n_model - 1)

    n_mixed = 2 * (n_chunk - n_lead)
    n_after = 2 * n_chunk - n_lead
    n_first = n_lead + n_idle

    def turn_of(place):
        return lax.div(place + 64 * half_pieces, half_pieces) - 64

    def is_fwd(turn):
        after = turn - n_first
        odd = lax.rem(after + 1024, 2) == 1
        return ((turn >= 0) & (turn < n_lead)) | ((after >= 0) & (after < n_mixed) & odd)

    def is_bwd(turn):
        after = turn - n_first
        odd = lax.rem(after + 1024, 2) == 1
        return (after >= 0) & (after < n_after) & jnp.logical_not((after < n_mixed) & odd)

    def fwd_chunk(turn):
        return jnp.where(turn < n_lead, turn, n_lead + lax.div(turn - n_first + 1024, 2) - 512)

    def bwd_chunk(turn):
        after = turn - n_first
        return jnp.where(after < n_mixed, lax.div(after + 1024, 2) - 512, after - (n_chunk - n_lead))

    def piece_of(place):
        return lax.rem(place + 64 * half_pieces, half_pieces)

    def any_chunk(turn, bwd):
        return jnp.clip(jnp.where(bwd, bwd_chunk(turn), fwd_chunk(turn)), 0, n_chunk - 1)

    def piece_at(side, index):
        col = side * half + index * piece
        return pl.ds(pl.multiple_of(col, piece), piece)

    def remote(src, dst, send_sem, recv_sem, device):
        return pltpu.make_async_remote_copy(
            src_ref=src, dst_ref=dst, send_sem=send_sem, recv_sem=recv_sem, device_id=device, device_id_type=MESH
        )

    def left(send_sem, like):
        remote(like, like, send_sem, loss_recv.at[0], {"model": pos}).wait_send()

    any_piece = acts.at[0, 0, :, pl.ds(0, piece)]
    any_sum = send_buf.at[0, 0]

    def rank_of(side):
        return pos if side == 0 else last_pos - pos

    def up(side):
        return {"model": pos + 1 if side == 0 else pos - 1}

    def down(side):
        return {"model": pos - 1 if side == 0 else pos + 1}

    def first_product(step, part):
        place = step + PARTS - 1 - part
        turn = turn_of(place)
        starts = piece_of(place) == 0

        @pl.when(starts & is_fwd(turn))
        def _():
            chunk = fwd_chunk(turn)
            if part == 0:
                copy_in(chunk).wait()
                copy_out(0, chunk).start()
            for col in range(part * hid_part, (part + 1) * hid_part, hid_cols):
                cols = pl.ds(col, hid_cols)
                pre = dot_nn(acts[0, chunk], wts[0, :, cols]).astype(BF16)
                hid[1, chunk, :, cols] = pre
                hid[0, chunk, :, cols] = gelu_tanh(pre.astype(F32)).astype(BF16)
            if part == PARTS - 1:
                copy_out(2, chunk).start()

                @pl.when((stage == 0) & (turn == 0))
                def _():
                    copy_w2.wait()

        @pl.when(starts & is_bwd(turn))
        def _():
            chunk = bwd_chunk(turn)
            if part == 0:
                copy_out(1, chunk).start()
                copy_out(0, chunk).wait()
            for col in range(part * hid_part, (part + 1) * hid_part, hid_cols):
                cols = pl.ds(col, hid_cols)
                grad_act = dot_nn(acts[1, chunk], wts[2, :, cols]).astype(BF16)
                slope = gelu_slope(hid[1, chunk, :, cols].astype(F32))
                hid[1, chunk, :, cols] = (slope * grad_act.astype(F32)).astype(BF16)
            if part == PARTS - 1:
                copy_out(3, chunk).start()

        if part == 0:

            @pl.when((stage == 0) & (place == n_lead * half_pieces))
            def _():
                transpose_weights()

    def loss_copy(side, to_stage, to_pos):
        return remote(
            loss_acc, loss_in.at[side], loss_send.at[to_stage * n_model + to_pos], loss_recv.at[side],
            {"stage": to_stage, "model": to_pos},
        )

    def send_loss(side):
        loss_in[side] = loss_acc[...]
        for to_stage in range(n_stage):
            for to_pos in range(n_model):

                @pl.when((to_stage != stage) | (to_pos != pos))
                def _():
                    loss_copy(side, to_stage, to_pos).start()

    def sum_steps(step):
        now = []
        for side in (0, 1):
            rank = rank_of(side)
            place = step - hop * rank
            turn = turn_of(place)
            fwd, bwd = is_fwd(turn), is_bwd(turn)
            old_fwd, old_bwd = is_fwd(turn - 1), is_bwd(turn - 1)
            out = piece_of(place)
            inn = lax.rem(place + 64 * RECV_SLOTS, RECV_SLOTS)
            is_back = bwd.astype(jnp.int32)
            sums = fwd | (bwd & (stage > 0))
            now.append((rank, fwd, bwd, sums, is_back, any_chunk(turn, bwd), out, inn, piece_at(side, out)))

            @pl.when((old_fwd | (old_bwd & (stage > 0))) & (rank < last_pos))
            def _():
                left(sum_send.at[side, out], any_sum)

            @pl.when(old_bwd & (stage > 0) & (rank == last_pos))
            def _():
                left(down_send.at[side, out], any_piece)

        @pl.when(now[0][3] | now[1][3])
        def _():
            for side in (0, 1):
                _, _, _, _, is_back, chunk, out, _, cols = now[side]
                send_buf[side, out] = dot_nn(hid[is_back, chunk], wts[1 + 2 * is_back, :, cols])

        for side in (0, 1):
            rank, fwd, bwd, sums, is_back, chunk, out, inn, cols = now[side]
            index = chunk * half_pieces + out
            hand_on = remote(
                send_buf.at[side, out], recv_buf.at[side, inn], sum_send.at[side, out], sum_recv.at[side, inn], up(side)
            )

            @pl.when(sums & (rank > 0))
            def _():
                hand_on.wait_recv()
                send_buf[side, out] = send_buf[side, out] + recv_buf[side, inn]

            @pl.when(sums & (rank < last_pos))
            def _():
                hand_on.start()

            @pl.when(sums & (rank == last_pos))
            def _():
                whole = acts[is_back, chunk, :, cols].astype(F32) + send_buf[side, out]
                scored = fwd & (stage == last_stage)

                @pl.when(scored)
                def _():
                    @pl.when(index == 0)
                    def _():
                        copy_targets(side).wait()

                    err = whole.astype(BF16).astype(F32) - acts[1, chunk, :, cols].astype(F32)
                    acts[1, chunk, :, cols] = (err * grad_scale).astype(BF16)
                    square = jnp.sum((err * err).reshape(err.shape[0] // 8, 8, piece), axis=0)
                    part = square[:, :128]
                    for lane in range(1, piece // 128):
                        part = part + square[:, lane * 128 : (lane + 1) * 128]
                    loss_acc[...] = loss_acc[...] + part

                    @pl.when(index == total - 1)
                    def _():
                        send_loss(side)

                @pl.when(jnp.logical_not(scored))
                def _():
                    acts[1 - is_back, chunk, :, cols] = whole.astype(BF16)

                @pl.when(bwd & (index == total - half_pieces))
                def _():
                    pl.semaphore_wait(spent_sem.at[side], 1)

                @pl.when(bwd)
                def _():
                    remote(
                        acts.at[0, chunk, :, cols], acts.at[1, chunk, :, cols], down_send.at[side, out],
                        back_recv.at[side, index], {"stage": stage - 1},
                    ).start()

    def gather_step(side, step):
        rank = rank_of(side)
        place = step - 3 * hop - hop * (last_pos - rank)
        turn = turn_of(place)
        fwd, old = is_fwd(turn), is_fwd(turn - 1)
        out = piece_of(place)
        chunk = jnp.clip(fwd_chunk(turn), 0, n_chunk - 1)
        index = chunk * half_pieces + out
        cols = piece_at(side, out)
        here = acts.at[1, chunk, :, cols]
        hand_on = remote(here, here, gat_send.at[side, out], gat_recv.at[side, index], down(side))

        @pl.when(old & (rank > 0))
        def _():
            left(gat_send.at[side, out], any_piece)

        @pl.when(old & (stage < last_stage))
        def _():
            left(over_send.at[side, out], any_piece)

            @pl.when((fwd_chunk(turn - 1) == n_chunk - 1) & (out == half_pieces - 1) & (rank == last_pos))
            def _():
                pl.semaphore_signal(spent_sem.at[side], inc=1, device_id={"stage": stage + 1}, device_id_type=MESH)

        @pl.when(fwd & (rank < last_pos))
        def _():
            hand_on.wait_recv()

        @pl.when(fwd & (rank > 0))
        def _():
            hand_on.start()

        @pl.when(fwd & (stage < last_stage))
        def _():
            remote(here, acts.at[0, chunk, :, cols], over_send.at[side, out], in_sem.at[chunk], {"stage": stage + 1}).start()

    def back_step(side, step):
        rank = rank_of(side)
        place = step + early - hop * (last_pos - rank)
        turn = turn_of(place)
        bwd, old = is_bwd(turn), is_bwd(turn - 1)
        out = piece_of(place)
        chunk = jnp.clip(bwd_chunk(turn), 0, n_chunk - 1)
        index = chunk * half_pieces + out
        here = acts.at[1, chunk, :, piece_at(side, out)]
        hand_on = remote(here, here, back_send.at[side, out], back_recv.at[side, index], down(side))

        @pl.when(old & (rank > 0) & (stage < last_stage))
        def _():
            left(back_send.at[side, out], any_piece)

        @pl.when(bwd & (stage < last_stage))
        def _():
            hand_on.wait_recv()

            @pl.when(rank > 0)
            def _():
                hand_on.start()

    def loop_step(step, carry):
        back_step(0, step)
        back_step(1, step)
        for part in range(PARTS):
            first_product(step, part)
        sum_steps(step)
        gather_step(0, step)
        gather_step(1, step)
        return carry

    lax.fori_loop(1 - PARTS, n_steps, loop_step, 0)

    for side, owner in ((0, last_pos), (1, 0)):
        owns = (stage == last_stage) & (pos == owner)

        @pl.when(jnp.logical_not(owns))
        def _():
            loss_copy(side, 0, 0).wait_recv()

        @pl.when(owns)
        def _():
            for to_stage in range(n_stage):
                for to_pos in range(n_model):

                    @pl.when((to_stage != stage) | (to_pos != pos))
                    def _():
                        loss_copy(side, to_stage, to_pos).wait_send()

    loss_out[...] = jnp.full(loss_out.shape, jnp.sum(loss_in[0] + loss_in[1]) * (0.5 * grad_scale), F32)

    def end_out(chunk, carry):
        for kind in (1, 2, 3):
            copy_out(kind, chunk).wait()
        return carry

    lax.fori_loop(0, n_chunk, end_out, 0)


def solution(mesh):
    n_stage = mesh.shape["stage"]
    n_model = mesh.shape["model"]

    def stage_step(inputs, targets, w_in, w_out):
        num_micro, num_tokens, model_dim = inputs.shape
        hid_dim = w_in.shape[3]
        rows = num_micro * num_tokens
        chunk = min(CHUNK_TOKENS, num_tokens)
        n_chunk = rows // chunk
        piece = min(PIECE_COLS, model_dim // 2)
        half_pieces = model_dim // 2 // piece
        grad_scale = 1.0 / (rows * model_dim)
        lead = [n_chunk] * (n_stage - 2) + [min(PREV_LEAD, n_chunk), min(LAST_LEAD, n_chunk)]
        idle = [FIRST_IDLE] + [NEXT_IDLE] * (n_stage - 3) + [0, 0]
        kernel = functools.partial(stage_kernel, n_stage, n_model, n_chunk, half_pieces, piece, HOP_LAG, lead, idle, grad_scale)
        any_space = pl.BlockSpec(memory_space=pl.ANY)
        dma = pltpu.SemaphoreType.DMA
        layer_in, layer_grad, layer_act, layer_pre, loss = pl.pallas_call(
            kernel,
            out_shape=(
                jax.ShapeDtypeStruct((rows, model_dim), BF16),
                jax.ShapeDtypeStruct((rows, model_dim), BF16),
                jax.ShapeDtypeStruct((rows, hid_dim), BF16),
                jax.ShapeDtypeStruct((rows, hid_dim), BF16),
                jax.ShapeDtypeStruct((8, 128), F32),
            ),
            in_specs=[any_space] * 4,
            out_specs=(any_space, any_space, any_space, any_space, pl.BlockSpec(memory_space=pltpu.VMEM)),
            scratch_shapes=[
                pltpu.VMEM((4, model_dim, hid_dim), BF16),
                pltpu.VMEM((2, n_chunk, chunk, model_dim), BF16),
                pltpu.VMEM((2, n_chunk, chunk, hid_dim), BF16),
                pltpu.VMEM((2, half_pieces, chunk, piece), F32),
                pltpu.VMEM((2, RECV_SLOTS, chunk, piece), F32),
                pltpu.VMEM((8, 128), F32),
                pltpu.VMEM((2, 8, 128), F32),
                dma((2,)),
                dma((n_chunk,)),
                dma,
                dma((2, half_pieces)),
                dma((2, RECV_SLOTS)),
                dma((2, half_pieces)),
                dma((2, n_chunk * half_pieces)),
                dma((2, half_pieces)),
                dma((2, half_pieces)),
                dma((2, n_chunk * half_pieces)),
                dma((2, half_pieces)),
                dma((4, n_chunk)),
                dma((n_stage * n_model,)),
                dma((2,)),
                pltpu.SemaphoreType.REGULAR((2,)),
            ],
            compiler_params=pltpu.CompilerParams(collective_id=0, has_side_effects=True, vmem_limit_bytes=63 * 1024 * 1024),
            name="stage_kernel",
        )(
            inputs.reshape(n_chunk, chunk, model_dim),
            targets.reshape(n_chunk, chunk, model_dim),
            w_in.reshape(model_dim, hid_dim),
            w_out.reshape(hid_dim, model_dim),
        )

        def over_rows(left, right):
            return lax.dot_general(left, right, (((0,), (0,)), ((), ())), preferred_element_type=F32)

        grad_in = over_rows(layer_in, layer_pre)
        grad_out = over_rows(layer_act, layer_grad)
        return grad_in[None, None], grad_out[None, None], loss[0, :1]

    return jax.shard_map(
        stage_step,
        mesh=mesh,
        in_specs=(P("data", None, None), P("data", None, None), P("stage", None, None, "model"), P("stage", None, "model", None)),
        out_specs=(P(("data", "stage"), None, None, "model"), P(("data", "stage"), None, "model", None), P("data")),
        check_vma=False,
    )
```

```python
import functools

import jax
import jax.numpy as jnp
from jax import lax
from jax.experimental import pallas as pl
from jax.experimental.pallas import tpu as pltpu
from jax.sharding import PartitionSpec as P

GELU_COEF = 0.7978845608028654
CUBIC_COEF = 0.044715

CHUNK_TOKENS = 64
PIECE_COLS = 256
HIDDEN_COLS = 512
PARTS = 2
HOP_LAG = 2
RECV_SLOTS = 8
GRAD_ROWS = 512
GRAD_COLS = 1024
LAST_LEAD = 5
PREV_LEAD = 16
FIRST_IDLE = 11
NEXT_IDLE = 7

BF16 = jnp.bfloat16
F32 = jnp.float32
MESH = pl.DeviceIdType.MESH


def gelu_tanh(values):
    inner_arg = GELU_COEF * (values + CUBIC_COEF * values * values * values)
    return 0.5 * values * (1.0 + jnp.tanh(inner_arg))


def gelu_slope(values):
    tanh_val = jnp.tanh(GELU_COEF * (values + CUBIC_COEF * values * values * values))
    return 0.5 * (1.0 + tanh_val) + 0.5 * values * (1.0 - tanh_val * tanh_val) * GELU_COEF * (1.0 + 3.0 * CUBIC_COEF * values * values)


def dot_nn(left, right):
    return jnp.dot(left, right, preferred_element_type=F32)


def dot_nt(left, right):
    return lax.dot_general(left, right, (((1,), (1,)), ((), ())), preferred_element_type=F32)


def stage_kernel(
    n_stage, n_model, n_chunk, half_pieces, piece, hop, lead, idle, grad_scale,
    inputs_hbm, targets_hbm, w1_hbm, w2_hbm,
    x_out, e_out, a_out, g_out, loss_out,
    wts, acts, hid, send_buf, recv_buf, loss_acc, loss_in,
    w_sem, in_sem, tgt_sem, sum_send, sum_recv, gat_send, gat_recv, over_send, back_send, back_recv, down_send, out_sem,
    loss_send, loss_recv, spent_sem,
):
    pos = lax.axis_index("model")
    stage = lax.axis_index("stage")
    last_pos = n_model - 1
    last_stage = n_stage - 1
    slots = half_pieces
    total = n_chunk * half_pieces
    half = half_pieces * piece
    hid_dim = wts.shape[2]
    chunk_rows = acts.shape[2]
    hid_part = hid_dim // PARTS
    hid_cols = min(HIDDEN_COLS, hid_part)
    n_lead, n_idle = jnp.int32(n_chunk), jnp.int32(0)
    for at in range(n_stage):
        n_lead = jnp.where(stage == at, lead[at], n_lead)
        n_idle = jnp.where(stage == at, idle[at], n_idle)
    turns = 2 * n_chunk + n_idle
    n_steps = turns * half_pieces + jnp.where(stage == 0, max(1 - half_pieces, -hop), 6 * hop + slots)
    early = half_pieces + 3 * hop

    barrier = pltpu.get_barrier_semaphore()
    for to_stage in range(n_stage):
        for to_pos in range(n_model):

            @pl.when((to_stage != stage) | (to_pos != pos))
            def _():
                pl.semaphore_signal(barrier, inc=1, device_id={"stage": to_stage, "model": to_pos}, device_id_type=MESH)

    copy_w1 = pltpu.make_async_copy(w1_hbm, wts.at[0], w_sem.at[0])
    copy_w2 = pltpu.make_async_copy(w2_hbm, wts.at[1], w_sem.at[1])

    def copy_in(chunk):
        return pltpu.make_async_copy(inputs_hbm.at[chunk], acts.at[0, chunk], in_sem.at[chunk])

    def copy_targets(side):
        cols = pl.ds(side * half, half)
        return pltpu.make_async_copy(targets_hbm.at[:, :, cols], acts.at[1, :, :, cols], tgt_sem)

    def copy_out(kind, chunk):
        src, dst = ((acts.at[0], x_out), (acts.at[1], e_out), (hid.at[0], a_out), (hid.at[1], g_out))[kind]
        rows = pl.ds(pl.multiple_of(chunk * chunk_rows, chunk_rows), chunk_rows)
        return pltpu.make_async_copy(src.at[chunk], dst.at[rows, :], out_sem.at[kind, chunk])

    @pl.when(stage == 0)
    def _():
        copy_in(0).start()

    copy_w1.start()
    copy_w2.start()

    @pl.when(stage == 0)
    def _():
        def start_in(chunk, carry):
            copy_in(chunk).start()
            return carry

        lax.fori_loop(1, n_chunk, start_in, 0)

    @pl.when((stage == last_stage) & (pos == last_pos))
    def _():
        copy_targets(0).start()

    @pl.when((stage == last_stage) & (pos == 0))
    def _():
        copy_targets(1).start()

    def transpose_weights():
        tile = min(256, hid_dim)
        count = hid_dim // tile

        def one(index, carry):
            rows = pl.ds(pl.multiple_of((index // count) * tile, tile), tile)
            cols = pl.ds(pl.multiple_of((index % count) * tile, tile), tile)
            wts[2, cols, rows] = jnp.swapaxes(wts[1, rows, cols], 0, 1)
            wts[3, cols, rows] = jnp.swapaxes(wts[0, rows, cols], 0, 1)
            return carry

        lax.fori_loop(0, count * count, one, 0)

    loss_acc[...] = jnp.zeros_like(loss_acc)
    copy_w1.wait()

    @pl.when(stage > 0)
    def _():
        copy_w2.wait()
        transpose_weights()

    pl.semaphore_wait(barrier, n_stage * n_model - 1)

    n_mixed = 2 * (n_chunk - n_lead)
    n_after = 2 * n_chunk - n_lead
    n_first = n_lead + n_idle

    def turn_of(place):
        return lax.div(place + 64 * half_pieces, half_pieces) - 64

    def is_fwd(turn):
        after = turn - n_first
        odd = lax.rem(after + 1024, 2) == 1
        return ((turn >= 0) & (turn < n_lead)) | ((after >= 0) & (after < n_mixed) & odd)

    def is_bwd(turn):
        after = turn - n_first
        odd = lax.rem(after + 1024, 2) == 1
        return (after >= 0) & (after < n_after) & jnp.logical_not((after < n_mixed) & odd)

    def fwd_chunk(turn):
        return jnp.where(turn < n_lead, turn, n_lead + lax.div(turn - n_first + 1024, 2) - 512)

    def bwd_chunk(turn):
        after = turn - n_first
        return jnp.where(after < n_mixed, lax.div(after + 1024, 2) - 512, after - (n_chunk - n_lead))

    def piece_of(place):
        return lax.rem(place + 64 * half_pieces, half_pieces)

    def any_chunk(turn, bwd):
        return jnp.clip(jnp.where(bwd, bwd_chunk(turn), fwd_chunk(turn)), 0, n_chunk - 1)

    def piece_at(side, index):
        col = side * half + index * piece
        return pl.ds(pl.multiple_of(col, piece), piece)

    def remote(src, dst, send_sem, recv_sem, device):
        return pltpu.make_async_remote_copy(
            src_ref=src, dst_ref=dst, send_sem=send_sem, recv_sem=recv_sem, device_id=device, device_id_type=MESH
        )

    def left(send_sem, like):
        remote(like, like, send_sem, loss_recv.at[0], {"model": pos}).wait_send()

    any_piece = acts.at[0, 0, :, pl.ds(0, piece)]
    any_sum = send_buf.at[0, 0]

    def rank_of(side):
        return pos if side == 0 else last_pos - pos

    def up(side):
        return {"model": pos + 1 if side == 0 else pos - 1}

    def down(side):
        return {"model": pos - 1 if side == 0 else pos + 1}

    def first_product(step, part):
        place = step + PARTS - 1 - part
        turn = turn_of(place)
        starts = piece_of(place) == 0

        @pl.when(starts & is_fwd(turn))
        def _():
            chunk = fwd_chunk(turn)
            if part == 0:
                copy_in(chunk).wait()
                copy_out(0, chunk).start()
            for col in range(part * hid_part, (part + 1) * hid_part, hid_cols):
                cols = pl.ds(col, hid_cols)
                pre = dot_nn(acts[0, chunk], wts[0, :, cols]).astype(BF16)
                hid[1, chunk, :, cols] = pre
                hid[0, chunk, :, cols] = gelu_tanh(pre.astype(F32)).astype(BF16)
            if part == PARTS - 1:
                copy_out(2, chunk).start()

                @pl.when((stage == 0) & (turn == 0))
                def _():
                    copy_w2.wait()

        @pl.when(starts & is_bwd(turn))
        def _():
            chunk = bwd_chunk(turn)
            if part == 0:
                copy_out(1, chunk).start()
                copy_out(0, chunk).wait()
            for col in range(part * hid_part, (part + 1) * hid_part, hid_cols):
                cols = pl.ds(col, hid_cols)
                grad_act = dot_nn(acts[1, chunk], wts[2, :, cols]).astype(BF16)
                slope = gelu_slope(hid[1, chunk, :, cols].astype(F32))
                hid[1, chunk, :, cols] = (slope * grad_act.astype(F32)).astype(BF16)
            if part == PARTS - 1:
                copy_out(3, chunk).start()

        if part == 0:

            @pl.when((stage == 0) & (place == n_lead * half_pieces))
            def _():
                transpose_weights()

    def loss_copy(side, to_stage, to_pos):
        return remote(
            loss_acc, loss_in.at[side], loss_send.at[to_stage * n_model + to_pos], loss_recv.at[side],
            {"stage": to_stage, "model": to_pos},
        )

    def send_loss(side):
        loss_in[side] = loss_acc[...]
        for to_stage in range(n_stage):
            for to_pos in range(n_model):

                @pl.when((to_stage != stage) | (to_pos != pos))
                def _():
                    loss_copy(side, to_stage, to_pos).start()

    def sum_steps(step):
        now = []
        for side in (0, 1):
            rank = rank_of(side)
            place = step - hop * rank
            turn = turn_of(place)
            fwd, bwd = is_fwd(turn), is_bwd(turn)
            old_fwd, old_bwd = is_fwd(turn - 1), is_bwd(turn - 1)
            out = piece_of(place)
            inn = lax.rem(place + 64 * RECV_SLOTS, RECV_SLOTS)
            is_back = bwd.astype(jnp.int32)
            sums = fwd | (bwd & (stage > 0))
            now.append((rank, fwd, bwd, sums, is_back, any_chunk(turn, bwd), out, inn, piece_at(side, out)))

            @pl.when((old_fwd | (old_bwd & (stage > 0))) & (rank < last_pos))
            def _():
                left(sum_send.at[side, out], any_sum)

            @pl.when(old_bwd & (stage > 0) & (rank == last_pos))
            def _():
                left(down_send.at[side, out], any_piece)

        @pl.when(now[0][3] | now[1][3])
        def _():
            for side in (0, 1):
                _, _, _, _, is_back, chunk, out, _, cols = now[side]
                send_buf[side, out] = dot_nn(hid[is_back, chunk], wts[1 + 2 * is_back, :, cols])

        for side in (0, 1):
            rank, fwd, bwd, sums, is_back, chunk, out, inn, cols = now[side]
            index = chunk * half_pieces + out
            hand_on = remote(
                send_buf.at[side, out], recv_buf.at[side, inn], sum_send.at[side, out], sum_recv.at[side, inn], up(side)
            )

            @pl.when(sums & (rank > 0))
            def _():
                hand_on.wait_recv()
                send_buf[side, out] = send_buf[side, out] + recv_buf[side, inn]

            @pl.when(sums & (rank < last_pos))
            def _():
                hand_on.start()

            @pl.when(sums & (rank == last_pos))
            def _():
                whole = acts[is_back, chunk, :, cols].astype(F32) + send_buf[side, out]
                scored = fwd & (stage == last_stage)

                @pl.when(scored)
                def _():
                    @pl.when(index == 0)
                    def _():
                        copy_targets(side).wait()

                    err = whole.astype(BF16).astype(F32) - acts[1, chunk, :, cols].astype(F32)
                    acts[1, chunk, :, cols] = (err * grad_scale).astype(BF16)
                    square = jnp.sum((err * err).reshape(err.shape[0] // 8, 8, piece), axis=0)
                    part = square[:, :128]
                    for lane in range(1, piece // 128):
                        part = part + square[:, lane * 128 : (lane + 1) * 128]
                    loss_acc[...] = loss_acc[...] + part

                    @pl.when(index == total - 1)
                    def _():
                        send_loss(side)

                @pl.when(jnp.logical_not(scored))
                def _():
                    acts[1 - is_back, chunk, :, cols] = whole.astype(BF16)

                @pl.when(bwd & (index == total - half_pieces))
                def _():
                    pl.semaphore_wait(spent_sem.at[side], 1)

                @pl.when(bwd)
                def _():
                    remote(
                        acts.at[0, chunk, :, cols], acts.at[1, chunk, :, cols], down_send.at[side, out],
                        back_recv.at[side, index], {"stage": stage - 1},
                    ).start()

    def gather_step(side, step):
        rank = rank_of(side)
        place = step - 3 * hop - hop * (last_pos - rank)
        turn = turn_of(place)
        fwd, old = is_fwd(turn), is_fwd(turn - 1)
        out = piece_of(place)
        chunk = jnp.clip(fwd_chunk(turn), 0, n_chunk - 1)
        index = chunk * half_pieces + out
        cols = piece_at(side, out)
        here = acts.at[1, chunk, :, cols]
        hand_on = remote(here, here, gat_send.at[side, out], gat_recv.at[side, index], down(side))

        @pl.when(old & (rank > 0))
        def _():
            left(gat_send.at[side, out], any_piece)

        @pl.when(old & (stage < last_stage))
        def _():
            left(over_send.at[side, out], any_piece)

            @pl.when((fwd_chunk(turn - 1) == n_chunk - 1) & (out == half_pieces - 1) & (rank == last_pos))
            def _():
                pl.semaphore_signal(spent_sem.at[side], inc=1, device_id={"stage": stage + 1}, device_id_type=MESH)

        @pl.when(fwd & (rank < last_pos))
        def _():
            hand_on.wait_recv()

        @pl.when(fwd & (rank > 0))
        def _():
            hand_on.start()

        @pl.when(fwd & (stage < last_stage))
        def _():
            remote(here, acts.at[0, chunk, :, cols], over_send.at[side, out], in_sem.at[chunk], {"stage": stage + 1}).start()

    def back_step(side, step):
        rank = rank_of(side)
        place = step + early - hop * (last_pos - rank)
        turn = turn_of(place)
        bwd, old = is_bwd(turn), is_bwd(turn - 1)
        out = piece_of(place)
        chunk = jnp.clip(bwd_chunk(turn), 0, n_chunk - 1)
        index = chunk * half_pieces + out
        here = acts.at[1, chunk, :, piece_at(side, out)]
        hand_on = remote(here, here, back_send.at[side, out], back_recv.at[side, index], down(side))

        @pl.when(old & (rank > 0) & (stage < last_stage))
        def _():
            left(back_send.at[side, out], any_piece)

        @pl.when(bwd & (stage < last_stage))
        def _():
            hand_on.wait_recv()

            @pl.when(rank > 0)
            def _():
                hand_on.start()

    def loop_step(step, carry):
        back_step(0, step)
        back_step(1, step)
        for part in range(PARTS):
            first_product(step, part)
        sum_steps(step)
        gather_step(0, step)
        gather_step(1, step)
        return carry

    lax.fori_loop(1 - PARTS, n_steps, loop_step, 0)

    for side, owner in ((0, last_pos), (1, 0)):
        owns = (stage == last_stage) & (pos == owner)

        @pl.when(jnp.logical_not(owns))
        def _():
            loss_copy(side, 0, 0).wait_recv()

        @pl.when(owns)
        def _():
            for to_stage in range(n_stage):
                for to_pos in range(n_model):

                    @pl.when((to_stage != stage) | (to_pos != pos))
                    def _():
                        loss_copy(side, to_stage, to_pos).wait_send()

    loss_out[...] = jnp.full(loss_out.shape, jnp.sum(loss_in[0] + loss_in[1]) * (0.5 * grad_scale), F32)

    def end_out(chunk, carry):
        for kind in (1, 2, 3):
            copy_out(kind, chunk).wait()
        return carry

    lax.fori_loop(0, n_chunk, end_out, 0)


def grad_kernel(blk, cols, x_hbm, g_hbm, a_hbm, e_hbm, dw1, dw2, lhs, lhs_t, rhs, out, lhs_sem, rhs_sem, out_sem):
    rows = lhs.shape[1]
    n_blk = dw1.shape[0] // blk
    n_col = dw1.shape[1] // cols

    def copy_lhs(which, index, slot):
        src = (x_hbm, a_hbm)[which]
        return pltpu.make_async_copy(src.at[:, pl.ds(pl.multiple_of(index * blk, blk), blk)], lhs.at[slot], lhs_sem.at[slot])

    def copy_rhs(which, index):
        src = (g_hbm, e_hbm)[which]
        part = pl.ds(index * cols, cols)
        return pltpu.make_async_copy(src.at[:, part], rhs.at[which, :, part], rhs_sem.at[which, index])

    def copy_res(which, index, col, slot):
        dst = (dw1, dw2)[which]
        return pltpu.make_async_copy(
            out.at[slot], dst.at[pl.ds(pl.multiple_of(index * blk, blk), blk), pl.ds(col * cols, cols)], out_sem.at[slot]
        )

    copy_lhs(0, 0, 0).start()
    for col in range(n_col):
        copy_rhs(0, col).start()
    copy_lhs(0, 1, 1).start()
    for col in range(n_col):
        copy_rhs(1, col).start()

    def turn(slot, col):
        width = blk // n_col
        part = pl.ds(col * width, width)
        lhs_t[slot, part, :] = jnp.swapaxes(lhs[slot, :, part], 0, 1)

    copy_lhs(0, 0, 0).wait()
    for col in range(n_col):
        turn(0, col)

    for which in (0, 1):

        def pair(step, carry):
            for slot in (0, 1):
                index = 2 * step + slot
                nxt = 1 - slot
                if slot == 0:
                    copy_lhs(which, index + 1, nxt).wait()
                else:

                    @pl.when(index + 1 < n_blk)
                    def _():
                        copy_lhs(which, index + 1, nxt).wait()

                    if which == 0:

                        @pl.when(index + 1 == n_blk)
                        def _():
                            copy_lhs(1, 0, nxt).wait()
                for col in range(n_col):

                    @pl.when(index == 0)
                    def _():
                        copy_rhs(which, col).wait()

                    place = slot * n_col + col
                    if which == 0:

                        @pl.when(step > 0)
                        def _():
                            copy_res(which, index, col, place).wait()
                    else:
                        copy_res(which, index, col, place).wait()
                    out[place] = dot_nn(lhs_t[slot], rhs[which, :, col * cols : (col + 1) * cols])
                    turn(nxt, col)
                    copy_res(which, index, col, place).start()
                @pl.when(index + 2 < n_blk)
                def _():
                    copy_lhs(which, index + 2, slot).start()

                if which == 0:

                    @pl.when(index + 2 >= n_blk)
                    def _():
                        copy_lhs(1, index + 2 - n_blk, slot).start()
            return carry

        lax.fori_loop(0, n_blk // 2, pair, 0)

    for slot in (0, 1):
        for col in range(n_col):
            copy_res(1, 0, col, slot * n_col + col).wait()


def weight_grads(x, g, a, e):
    rows, dim = x.shape
    hid_dim = g.shape[1]
    blk, cols = min(GRAD_ROWS, dim // 2), min(GRAD_COLS, hid_dim)
    any_space = pl.BlockSpec(memory_space=pl.ANY)
    dma = pltpu.SemaphoreType.DMA
    n_col = hid_dim // cols
    return pl.pallas_call(
        functools.partial(grad_kernel, blk, cols),
        out_shape=(jax.ShapeDtypeStruct((dim, hid_dim), F32), jax.ShapeDtypeStruct((hid_dim, dim), F32)),
        in_specs=[any_space] * 4,
        out_specs=(any_space, any_space),
        scratch_shapes=[
            pltpu.VMEM((2, rows, blk), BF16),
            pltpu.VMEM((2, blk, rows), BF16),
            pltpu.VMEM((2, rows, hid_dim), BF16),
            pltpu.VMEM((2 * n_col, blk, cols), F32),
            dma((2,)),
            dma((2, n_col)),
            dma((2 * n_col,)),
        ],
        compiler_params=pltpu.CompilerParams(vmem_limit_bytes=63 * 1024 * 1024),
        name="grad_kernel",
    )(x, g, a, e)


def solution(mesh):
    n_stage = mesh.shape["stage"]
    n_model = mesh.shape["model"]

    def stage_step(inputs, targets, w_in, w_out):
        num_micro, num_tokens, model_dim = inputs.shape
        hid_dim = w_in.shape[3]
        rows = num_micro * num_tokens
        chunk = min(CHUNK_TOKENS, num_tokens)
        n_chunk = rows // chunk
        piece = min(PIECE_COLS, model_dim // 2)
        half_pieces = model_dim // 2 // piece
        grad_scale = 1.0 / (rows * model_dim)
        lead = [n_chunk] * (n_stage - 2) + [min(PREV_LEAD, n_chunk), min(LAST_LEAD, n_chunk)]
        idle = [FIRST_IDLE] + [NEXT_IDLE] * (n_stage - 3) + [0, 0]
        kernel = functools.partial(stage_kernel, n_stage, n_model, n_chunk, half_pieces, piece, HOP_LAG, lead, idle, grad_scale)
        any_space = pl.BlockSpec(memory_space=pl.ANY)
        dma = pltpu.SemaphoreType.DMA
        layer_in, layer_grad, layer_act, layer_pre, loss = pl.pallas_call(
            kernel,
            out_shape=(
                jax.ShapeDtypeStruct((rows, model_dim), BF16),
                jax.ShapeDtypeStruct((rows, model_dim), BF16),
                jax.ShapeDtypeStruct((rows, hid_dim), BF16),
                jax.ShapeDtypeStruct((rows, hid_dim), BF16),
                jax.ShapeDtypeStruct((8, 128), F32),
            ),
            in_specs=[any_space] * 4,
            out_specs=(any_space, any_space, any_space, any_space, pl.BlockSpec(memory_space=pltpu.VMEM)),
            scratch_shapes=[
                pltpu.VMEM((4, model_dim, hid_dim), BF16),
                pltpu.VMEM((2, n_chunk, chunk, model_dim), BF16),
                pltpu.VMEM((2, n_chunk, chunk, hid_dim), BF16),
                pltpu.VMEM((2, half_pieces, chunk, piece), F32),
                pltpu.VMEM((2, RECV_SLOTS, chunk, piece), F32),
                pltpu.VMEM((8, 128), F32),
                pltpu.VMEM((2, 8, 128), F32),
                dma((2,)),
                dma((n_chunk,)),
                dma,
                dma((2, half_pieces)),
                dma((2, RECV_SLOTS)),
                dma((2, half_pieces)),
                dma((2, n_chunk * half_pieces)),
                dma((2, half_pieces)),
                dma((2, half_pieces)),
                dma((2, n_chunk * half_pieces)),
                dma((2, half_pieces)),
                dma((4, n_chunk)),
                dma((n_stage * n_model,)),
                dma((2,)),
                pltpu.SemaphoreType.REGULAR((2,)),
            ],
            compiler_params=pltpu.CompilerParams(collective_id=0, has_side_effects=True, vmem_limit_bytes=63 * 1024 * 1024),
            name="stage_kernel",
        )(
            inputs.reshape(n_chunk, chunk, model_dim),
            targets.reshape(n_chunk, chunk, model_dim),
            w_in.reshape(model_dim, hid_dim),
            w_out.reshape(hid_dim, model_dim),
        )

        grad_in, grad_out = weight_grads(layer_in, layer_pre, layer_act, layer_grad)
        return grad_in[None, None], grad_out[None, None], loss[0, :1]

    return jax.shard_map(
        stage_step,
        mesh=mesh,
        in_specs=(P("data", None, None), P("data", None, None), P("stage", None, None, "model"), P("stage", None, "model", None)),
        out_specs=(P(("data", "stage"), None, None, "model"), P(("data", "stage"), None, "model", None), P("data")),
        check_vma=False,
    )
```

```python
import functools

import jax
import jax.numpy as jnp
from jax import lax
from jax.experimental import pallas as pl
from jax.experimental.pallas import tpu as pltpu
from jax.sharding import PartitionSpec as P

GELU_COEF = 0.7978845608028654
CUBIC_COEF = 0.044715

CHUNK_TOKENS = 64
PIECE_COLS = 256
HIDDEN_COLS = 512
PARTS = 2
HOP_LAG = 2
RECV_SLOTS = 8
LAST_LEAD = 5
PREV_LEAD = 16
FIRST_IDLE = 12
NEXT_IDLE = 7
FORE_CHUNKS = 6
RELAY_CHUNKS = 18
RELAY_START = 0

BF16 = jnp.bfloat16
F32 = jnp.float32
MESH = pl.DeviceIdType.MESH


def gelu_tanh(values):
    inner_arg = GELU_COEF * (values + CUBIC_COEF * values * values * values)
    return 0.5 * values * (1.0 + jnp.tanh(inner_arg))


def gelu_slope(values):
    tanh_val = jnp.tanh(GELU_COEF * (values + CUBIC_COEF * values * values * values))
    return 0.5 * (1.0 + tanh_val) + 0.5 * values * (1.0 - tanh_val * tanh_val) * GELU_COEF * (1.0 + 3.0 * CUBIC_COEF * values * values)


def dot_nn(left, right):
    return jnp.dot(left, right, preferred_element_type=F32)


def dot_nt(left, right):
    return lax.dot_general(left, right, (((1,), (1,)), ((), ())), preferred_element_type=F32)


def stage_kernel(
    n_stage, n_model, n_chunk, half_pieces, piece, hop, lead, idle, n_fore, n_relay, grad_scale,
    inputs_hbm, targets_hbm, w1_hbm, w2_hbm,
    x_out, e_out, a_out, g_out, loss_out,
    wts, acts, hid, send_buf, recv_buf, loss_acc, loss_in,
    w_sem, in_sem, tgt_sem, sum_send, sum_recv, gat_send, gat_recv, over_send, back_send, take_recv, down_send, out_sem,
    loss_send, loss_recv, spent_sem, rel_send, rel_over, rel_recv, rel_in, free_sem,
):
    pos = lax.axis_index("model")
    stage = lax.axis_index("stage")
    last_pos = n_model - 1
    last_stage = n_stage - 1
    fore_stage = n_stage - 2
    slots = half_pieces
    total = n_chunk * half_pieces
    half = half_pieces * piece
    hid_dim = wts.shape[2]
    chunk_rows = acts.shape[2]
    hid_part = hid_dim // PARTS
    hid_cols = min(HIDDEN_COLS, hid_part)
    n_lead, n_idle = jnp.int32(n_chunk), jnp.int32(0)
    for at in range(n_stage):
        n_lead = jnp.where(stage == at, lead[at], n_lead)
        n_idle = jnp.where(stage == at, idle[at], n_idle)
    turns = 2 * n_chunk + n_idle
    n_steps = turns * half_pieces + jnp.where(stage == 0, max(1 - half_pieces, -hop), 6 * hop + slots)
    early = half_pieces + 3 * hop

    barrier = pltpu.get_barrier_semaphore()
    for to_stage in range(n_stage):
        for to_pos in range(n_model):

            @pl.when((to_stage != stage) | (to_pos != pos))
            def _():
                pl.semaphore_signal(barrier, inc=1, device_id={"stage": to_stage, "model": to_pos}, device_id_type=MESH)

    copy_w1 = pltpu.make_async_copy(w1_hbm, wts.at[0], w_sem.at[0])
    copy_w2 = pltpu.make_async_copy(w2_hbm, wts.at[1], w_sem.at[1])

    def copy_in(chunk):
        return pltpu.make_async_copy(inputs_hbm.at[chunk], acts.at[0, chunk], in_sem.at[chunk])

    def grad_in(chunk):
        return pltpu.make_async_copy(inputs_hbm.at[chunk], acts.at[1, chunk], rel_in.at[chunk])

    def copy_targets(side):
        cols = pl.ds(side * half, half)
        return pltpu.make_async_copy(targets_hbm.at[:, :, cols], acts.at[1, :, :, cols], tgt_sem)

    def copy_out(kind, chunk):
        src, dst = ((acts.at[0], x_out), (acts.at[1], e_out), (hid.at[0], a_out), (hid.at[1], g_out))[kind]
        rows = pl.ds(pl.multiple_of(chunk * chunk_rows, chunk_rows), chunk_rows)
        return pltpu.make_async_copy(src.at[chunk], dst.at[rows, :], out_sem.at[kind, chunk])

    @pl.when(stage == 0)
    def _():
        copy_in(0).start()

    copy_w1.start()
    copy_w2.start()

    @pl.when(stage == 0)
    def _():
        def start_in(chunk, carry):
            copy_in(chunk).start()
            return carry

        lax.fori_loop(1, n_chunk, start_in, 0)

    @pl.when((stage == last_stage) & (pos == last_pos))
    def _():
        copy_targets(0).start()

    @pl.when((stage == last_stage) & (pos == 0))
    def _():
        copy_targets(1).start()

    def transpose_weights():
        tile = min(256, hid_dim)
        count = hid_dim // tile

        def one(index, carry):
            rows = pl.ds(pl.multiple_of((index // count) * tile, tile), tile)
            cols = pl.ds(pl.multiple_of((index % count) * tile, tile), tile)
            wts[2, cols, rows] = jnp.swapaxes(wts[1, rows, cols], 0, 1)
            wts[3, cols, rows] = jnp.swapaxes(wts[0, rows, cols], 0, 1)
            return carry

        lax.fori_loop(0, count * count, one, 0)

    loss_acc[...] = jnp.zeros_like(loss_acc)
    copy_w1.wait()

    @pl.when(stage > 0)
    def _():
        copy_w2.wait()
        transpose_weights()

    pl.semaphore_wait(barrier, n_stage * n_model - 1)

    n_mixed = 2 * (n_chunk - n_lead)
    n_after = 2 * n_chunk - n_lead
    n_first = n_lead + n_idle

    def turn_of(place):
        return lax.div(place + 64 * half_pieces, half_pieces) - 64

    def is_fwd(turn):
        after = turn - n_first
        odd = lax.rem(after + 1024, 2) == 1
        return ((turn >= 0) & (turn < n_lead)) | ((after >= 0) & (after < n_mixed) & odd)

    def is_bwd(turn):
        after = turn - n_first
        odd = lax.rem(after + 1024, 2) == 1
        return (after >= 0) & (after < n_after) & jnp.logical_not((after < n_mixed) & odd)

    def fwd_chunk(turn):
        return jnp.where(turn < n_lead, turn, n_lead + lax.div(turn - n_first + 1024, 2) - 512)

    def bwd_chunk(turn):
        after = turn - n_first
        return jnp.where(after < n_mixed, lax.div(after + 1024, 2) - 512, after - (n_chunk - n_lead))

    def piece_of(place):
        return lax.rem(place + 64 * half_pieces, half_pieces)

    def any_chunk(turn, bwd):
        return jnp.clip(jnp.where(bwd, bwd_chunk(turn), fwd_chunk(turn)), 0, n_chunk - 1)

    def piece_at(side, index):
        col = side * half + index * piece
        return pl.ds(pl.multiple_of(col, piece), piece)

    def remote(src, dst, send_sem, recv_sem, device):
        return pltpu.make_async_remote_copy(
            src_ref=src, dst_ref=dst, send_sem=send_sem, recv_sem=recv_sem, device_id=device, device_id_type=MESH
        )

    def left(send_sem, like):
        remote(like, like, send_sem, loss_recv.at[0], {"model": pos}).wait_send()

    any_piece = acts.at[0, 0, :, pl.ds(0, piece)]
    any_sum = send_buf.at[0, 0]

    def rank_of(side):
        return pos if side == 0 else last_pos - pos

    def up(side):
        return {"model": pos + 1 if side == 0 else pos - 1}

    def down(side):
        return {"model": pos - 1 if side == 0 else pos + 1}

    def first_product(step, part):
        place = step + PARTS - 1 - part
        turn = turn_of(place)
        starts = piece_of(place) == 0

        @pl.when(starts & is_fwd(turn))
        def _():
            chunk = fwd_chunk(turn)
            if part == 0:

                @pl.when((stage != fore_stage) | (chunk >= n_fore))
                def _():
                    copy_in(chunk).wait()

                copy_out(0, chunk).start()
            for col in range(part * hid_part, (part + 1) * hid_part, hid_cols):
                cols = pl.ds(col, hid_cols)
                pre = dot_nn(acts[0, chunk], wts[0, :, cols]).astype(BF16)
                hid[1, chunk, :, cols] = pre
                hid[0, chunk, :, cols] = gelu_tanh(pre.astype(F32)).astype(BF16)
            if part == PARTS - 1:
                copy_out(2, chunk).start()

                @pl.when((stage == 0) & (turn == 0))
                def _():
                    copy_w2.wait()

        @pl.when(starts & is_bwd(turn))
        def _():
            chunk = bwd_chunk(turn)
            if part == 0:

                @pl.when((stage == fore_stage) & (chunk < n_relay))
                def _():
                    grad_in(chunk).wait()

                copy_out(1, chunk).start()
                copy_out(0, chunk).wait()
            for col in range(part * hid_part, (part + 1) * hid_part, hid_cols):
                cols = pl.ds(col, hid_cols)
                grad_act = dot_nn(acts[1, chunk], wts[2, :, cols]).astype(BF16)
                slope = gelu_slope(hid[1, chunk, :, cols].astype(F32))
                hid[1, chunk, :, cols] = (slope * grad_act.astype(F32)).astype(BF16)
            if part == PARTS - 1:
                copy_out(3, chunk).start()

        if part == 0:

            @pl.when((stage == 0) & (place == n_lead * half_pieces))
            def _():
                transpose_weights()

    def loss_copy(side, to_stage, to_pos):
        return remote(
            loss_acc, loss_in.at[side], loss_send.at[to_stage * n_model + to_pos], loss_recv.at[side],
            {"stage": to_stage, "model": to_pos},
        )

    def send_loss(side):
        loss_in[side] = loss_acc[...]
        for to_stage in range(n_stage):
            for to_pos in range(n_model):

                @pl.when((to_stage != stage) | (to_pos != pos))
                def _():
                    loss_copy(side, to_stage, to_pos).start()

    def sum_steps(step):
        now = []
        for side in (0, 1):
            rank = rank_of(side)
            place = step - hop * rank
            turn = turn_of(place)
            fwd, bwd = is_fwd(turn), is_bwd(turn)
            old_fwd, old_bwd = is_fwd(turn - 1), is_bwd(turn - 1)
            out = piece_of(place)
            inn = lax.rem(place + 64 * RECV_SLOTS, RECV_SLOTS)
            is_back = bwd.astype(jnp.int32)
            sums = fwd | (bwd & (stage > 0))
            now.append((rank, fwd, bwd, sums, is_back, any_chunk(turn, bwd), out, inn, piece_at(side, out)))

            @pl.when((old_fwd | (old_bwd & (stage > 0))) & (rank < last_pos))
            def _():
                left(sum_send.at[side, out], any_sum)

            @pl.when(old_bwd & (stage > 0) & (rank == last_pos))
            def _():
                left(down_send.at[side, out], any_piece)

        @pl.when(now[0][3] | now[1][3])
        def _():
            for side in (0, 1):
                _, _, _, _, is_back, chunk, out, _, cols = now[side]
                send_buf[side, out] = dot_nn(hid[is_back, chunk], wts[1 + 2 * is_back, :, cols])

        for side in (0, 1):
            rank, fwd, bwd, sums, is_back, chunk, out, inn, cols = now[side]
            index = chunk * half_pieces + out
            hand_on = remote(
                send_buf.at[side, out], recv_buf.at[side, inn], sum_send.at[side, out], sum_recv.at[side, inn], up(side)
            )

            @pl.when(sums & (rank > 0))
            def _():
                hand_on.wait_recv()
                send_buf[side, out] = send_buf[side, out] + recv_buf[side, inn]

            @pl.when(sums & (rank < last_pos))
            def _():
                hand_on.start()

            @pl.when(sums & (rank == last_pos))
            def _():
                whole = acts[is_back, chunk, :, cols].astype(F32) + send_buf[side, out]
                scored = fwd & (stage == last_stage)

                @pl.when(scored)
                def _():
                    @pl.when(index == 0)
                    def _():
                        copy_targets(side).wait()

                    err = whole.astype(BF16).astype(F32) - acts[1, chunk, :, cols].astype(F32)
                    acts[1, chunk, :, cols] = (err * grad_scale).astype(BF16)
                    square = jnp.sum((err * err).reshape(err.shape[0] // 8, 8, piece), axis=0)
                    part = square[:, :128]
                    for lane in range(1, piece // 128):
                        part = part + square[:, lane * 128 : (lane + 1) * 128]
                    loss_acc[...] = loss_acc[...] + part

                    @pl.when(index == total - 1)
                    def _():
                        send_loss(side)

                @pl.when(jnp.logical_not(scored))
                def _():
                    acts[1 - is_back, chunk, :, cols] = whole.astype(BF16)

                @pl.when(bwd & (index == total - half_pieces))
                def _():
                    pl.semaphore_wait(spent_sem.at[side], 1)

                @pl.when(bwd & (stage == 1) & (index == (n_relay - 1) * half_pieces))
                def _():
                    pl.semaphore_wait(free_sem.at[side], 1)

                relayed = (stage == last_stage) & (chunk < n_relay)
                there = acts.at[1, chunk, :, cols]

                @pl.when(bwd & relayed)
                def _():
                    arrived = rel_recv.at[side, jnp.minimum(index, n_relay * half_pieces - 1)]
                    remote(acts.at[0, chunk, :, cols], there, down_send.at[side, out], arrived, {"stage": 0}).start()

                @pl.when(bwd & jnp.logical_not(relayed))
                def _():
                    arrived = take_recv.at[side, index]
                    remote(acts.at[0, chunk, :, cols], there, down_send.at[side, out], arrived, {"stage": stage - 1}).start()

    def gather_step(side, step):
        rank = rank_of(side)
        place = step - 3 * hop - hop * (last_pos - rank)
        turn = turn_of(place)
        fwd, old = is_fwd(turn), is_fwd(turn - 1)
        out = piece_of(place)
        chunk = jnp.clip(fwd_chunk(turn), 0, n_chunk - 1)
        index = chunk * half_pieces + out
        cols = piece_at(side, out)
        here = acts.at[1, chunk, :, cols]
        hand_on = remote(here, here, gat_send.at[side, out], gat_recv.at[side, index], down(side))

        early_one = (stage == fore_stage - 1) & (chunk < n_fore)
        early_old = (stage == fore_stage - 1) & (fwd_chunk(turn - 1) < n_fore)

        @pl.when(old & (rank > 0) & jnp.logical_not(early_old))
        def _():
            left(gat_send.at[side, out], any_piece)

        @pl.when(old & (stage < last_stage) & (jnp.logical_not(early_old) | (rank == last_pos)))
        def _():
            left(over_send.at[side, out], any_piece)

            @pl.when((fwd_chunk(turn - 1) == n_chunk - 1) & (out == half_pieces - 1) & (rank == last_pos))
            def _():
                pl.semaphore_signal(spent_sem.at[side], inc=1, device_id={"stage": stage + 1}, device_id_type=MESH)

        @pl.when(fwd & jnp.logical_not(early_one))
        def _():
            @pl.when(rank < last_pos)
            def _():
                hand_on.wait_recv()

            @pl.when(rank > 0)
            def _():
                hand_on.start()

            @pl.when(stage < last_stage)
            def _():
                arrived = in_sem.at[chunk]
                remote(here, acts.at[0, chunk, :, cols], over_send.at[side, out], arrived, {"stage": stage + 1}).start()

        @pl.when(fwd & early_one & (rank == last_pos))
        def _():
            arrived = take_recv.at[side, jnp.minimum(total + index, total + n_fore * half_pieces - 1)]
            remote(here, acts.at[0, chunk, :, cols], over_send.at[side, out], arrived, {"stage": stage + 1}).start()

    def take_step(side, step):
        rank = rank_of(side)
        place = step + early - hop * (last_pos - rank)
        turn = turn_of(place)
        bwd = is_bwd(turn)

        def takes(turn):
            back = is_bwd(turn) & (stage < last_stage) & ((stage < fore_stage) | (bwd_chunk(turn) >= n_relay))
            return back | (is_fwd(turn) & (stage == fore_stage) & (fwd_chunk(turn) < n_fore))

        out = piece_of(place)
        chunk = any_chunk(turn, bwd)
        is_back = bwd.astype(jnp.int32)
        index = chunk * half_pieces + out + (1 - is_back) * total
        here = acts.at[is_back, chunk, :, piece_at(side, out)]
        arrived = take_recv.at[side, jnp.minimum(index, total + n_fore * half_pieces - 1)]
        hand_on = remote(here, here, back_send.at[side, out], arrived, down(side))

        @pl.when(takes(turn - 1) & (rank > 0))
        def _():
            left(back_send.at[side, out], any_piece)

        @pl.when(takes(turn))
        def _():
            hand_on.wait_recv()

            @pl.when(rank > 0)
            def _():
                hand_on.start()

    def relay_step(side, step):
        rank = rank_of(side)
        place = step - (n_chunk + RELAY_START) * half_pieces - hop * (last_pos - rank)
        turn = turn_of(place)
        out = piece_of(place)
        chunk = jnp.clip(turn, 0, n_relay - 1)
        here = acts.at[1, chunk, :, piece_at(side, out)]
        arrived = rel_recv.at[side, chunk * half_pieces + out]
        hand_on = remote(here, here, rel_send.at[side, out], arrived, down(side))

        @pl.when((turn >= 1) & (turn <= n_relay))
        def _():
            @pl.when(rank > 0)
            def _():
                left(rel_send.at[side, out], any_piece)

            left(rel_over.at[side, out], any_piece)

            @pl.when((turn == n_relay) & (out == half_pieces - 1) & (rank == last_pos))
            def _():
                pl.semaphore_signal(free_sem.at[side], inc=1, device_id={"stage": 1}, device_id_type=MESH)

        @pl.when((turn >= 0) & (turn < n_relay))
        def _():
            hand_on.wait_recv()

            @pl.when(rank > 0)
            def _():
                hand_on.start()

            remote(here, here, rel_over.at[side, out], rel_in.at[chunk], {"stage": fore_stage}).start()

    def loop_step(step, carry):
        take_step(0, step)
        take_step(1, step)
        for part in range(PARTS):
            first_product(step, part)
        sum_steps(step)
        gather_step(0, step)
        gather_step(1, step)

        @pl.when((stage == 0) & (step >= n_chunk * half_pieces))
        def _():
            relay_step(0, step)
            relay_step(1, step)

        return carry

    lax.fori_loop(jnp.where(stage == fore_stage, -early, 1 - PARTS), n_steps, loop_step, 0)

    for side, owner in ((0, last_pos), (1, 0)):
        owns = (stage == last_stage) & (pos == owner)

        @pl.when(jnp.logical_not(owns))
        def _():
            loss_copy(side, 0, 0).wait_recv()

        @pl.when(owns)
        def _():
            for to_stage in range(n_stage):
                for to_pos in range(n_model):

                    @pl.when((to_stage != stage) | (to_pos != pos))
                    def _():
                        loss_copy(side, to_stage, to_pos).wait_send()

    loss_out[...] = jnp.full(loss_out.shape, jnp.sum(loss_in[0] + loss_in[1]) * (0.5 * grad_scale), F32)

    def end_out(chunk, carry):
        for kind in (1, 2, 3):
            copy_out(kind, chunk).wait()
        return carry

    lax.fori_loop(0, n_chunk, end_out, 0)


def solution(mesh):
    n_stage = mesh.shape["stage"]
    n_model = mesh.shape["model"]

    def stage_step(inputs, targets, w_in, w_out):
        num_micro, num_tokens, model_dim = inputs.shape
        hid_dim = w_in.shape[3]
        rows = num_micro * num_tokens
        chunk = min(CHUNK_TOKENS, num_tokens)
        n_chunk = rows // chunk
        piece = min(PIECE_COLS, model_dim // 2)
        half_pieces = model_dim // 2 // piece
        grad_scale = 1.0 / (rows * model_dim)
        lead = [n_chunk] * (n_stage - 2) + [min(PREV_LEAD, n_chunk), min(LAST_LEAD, n_chunk)]
        idle = [FIRST_IDLE] + [NEXT_IDLE] * (n_stage - 3) + [0, 0]
        n_fore, n_relay = min(FORE_CHUNKS, n_chunk - 1), min(RELAY_CHUNKS, n_chunk - 1)
        kernel = functools.partial(
            stage_kernel, n_stage, n_model, n_chunk, half_pieces, piece, HOP_LAG, lead, idle, n_fore, n_relay, grad_scale
        )
        any_space = pl.BlockSpec(memory_space=pl.ANY)
        dma = pltpu.SemaphoreType.DMA
        layer_in, layer_grad, layer_act, layer_pre, loss = pl.pallas_call(
            kernel,
            out_shape=(
                jax.ShapeDtypeStruct((rows, model_dim), BF16),
                jax.ShapeDtypeStruct((rows, model_dim), BF16),
                jax.ShapeDtypeStruct((rows, hid_dim), BF16),
                jax.ShapeDtypeStruct((rows, hid_dim), BF16),
                jax.ShapeDtypeStruct((8, 128), F32),
            ),
            in_specs=[any_space] * 4,
            out_specs=(any_space, any_space, any_space, any_space, pl.BlockSpec(memory_space=pltpu.VMEM)),
            scratch_shapes=[
                pltpu.VMEM((4, model_dim, hid_dim), BF16),
                pltpu.VMEM((2, n_chunk, chunk, model_dim), BF16),
                pltpu.VMEM((2, n_chunk, chunk, hid_dim), BF16),
                pltpu.VMEM((2, half_pieces, chunk, piece), F32),
                pltpu.VMEM((2, RECV_SLOTS, chunk, piece), F32),
                pltpu.VMEM((8, 128), F32),
                pltpu.VMEM((2, 8, 128), F32),
                dma((2,)),
                dma((n_chunk,)),
                dma,
                dma((2, half_pieces)),
                dma((2, RECV_SLOTS)),
                dma((2, half_pieces)),
                dma((2, n_chunk * half_pieces)),
                dma((2, half_pieces)),
                dma((2, half_pieces)),
                dma((2, (n_chunk + n_fore) * half_pieces)),
                dma((2, half_pieces)),
                dma((4, n_chunk)),
                dma((n_stage * n_model,)),
                dma((2,)),
                pltpu.SemaphoreType.REGULAR((2,)),
                dma((2, half_pieces)),
                dma((2, half_pieces)),
                dma((2, n_relay * half_pieces)),
                dma((n_relay,)),
                pltpu.SemaphoreType.REGULAR((2,)),
            ],
            compiler_params=pltpu.CompilerParams(collective_id=0, has_side_effects=True, vmem_limit_bytes=63 * 1024 * 1024),
            name="stage_kernel",
        )(
            inputs.reshape(n_chunk, chunk, model_dim),
            targets.reshape(n_chunk, chunk, model_dim),
            w_in.reshape(model_dim, hid_dim),
            w_out.reshape(hid_dim, model_dim),
        )

        def over_rows(left, right):
            return lax.dot_general(left, right, (((0,), (0,)), ((), ())), preferred_element_type=F32)

        grad_in = over_rows(layer_in, layer_pre)
        grad_out = over_rows(layer_act, layer_grad)
        return grad_in[None, None], grad_out[None, None], loss[0, :1]

    return jax.shard_map(
        stage_step,
        mesh=mesh,
        in_specs=(P("data", None, None), P("data", None, None), P("stage", None, None, "model"), P("stage", None, "model", None)),
        out_specs=(P(("data", "stage"), None, None, "model"), P(("data", "stage"), None, "model", None), P("data")),
        check_vma=False,
    )
```

```python
import functools

import jax
import jax.numpy as jnp
from jax import lax
from jax.experimental import pallas as pl
from jax.experimental.pallas import tpu as pltpu
from jax.sharding import PartitionSpec as P

GELU_COEF = 0.7978845608028654
CUBIC_COEF = 0.044715

CHUNK_TOKENS = 64
PIECE_COLS = 256
HIDDEN_COLS = 512
PARTS = 2
HOP_LAG = 2
RECV_SLOTS = 8
LAST_LEAD = 5
PREV_LEAD = 16
FIRST_IDLE = 12
NEXT_IDLE = 7
FORE_CHUNKS = 6
RELAY_CHUNKS = 18
RELAY_START = 0

SUM, BACK, GATHER, EARLY, TAKE, FWD, BWD = 256, 512, 1024, 2048, 4096, 8192, 16384
MARGIN = 16

BF16 = jnp.bfloat16
F32 = jnp.float32
MESH = pl.DeviceIdType.MESH


def gelu_tanh(values):
    inner_arg = GELU_COEF * (values + CUBIC_COEF * values * values * values)
    return 0.5 * values * (1.0 + jnp.tanh(inner_arg))


def gelu_slope(values):
    tanh_val = jnp.tanh(GELU_COEF * (values + CUBIC_COEF * values * values * values))
    return 0.5 * (1.0 + tanh_val) + 0.5 * values * (1.0 - tanh_val * tanh_val) * GELU_COEF * (1.0 + 3.0 * CUBIC_COEF * values * values)


def dot_nn(left, right):
    return jnp.dot(left, right, preferred_element_type=F32)


def dot_nt(left, right):
    return lax.dot_general(left, right, (((1,), (1,)), ((), ())), preferred_element_type=F32)


def stage_kernel(
    n_stage, n_model, n_chunk, half_pieces, piece, hop, lead, idle, n_fore, n_relay, grad_scale,
    inputs_hbm, targets_hbm, w1_hbm, w2_hbm,
    x_out, e_out, a_out, g_out, loss_out,
    wts, acts, hid, send_buf, recv_buf, loss_acc, loss_in,
    w_sem, in_sem, tgt_sem, sum_send, sum_recv, gat_send, gat_recv, over_send, back_send, take_recv, down_send, out_sem,
    loss_send, loss_recv, spent_sem, rel_send, rel_over, rel_recv, rel_in, free_sem, table,
):
    pos = lax.axis_index("model")
    stage = lax.axis_index("stage")
    last_pos = n_model - 1
    last_stage = n_stage - 1
    fore_stage = n_stage - 2
    bits = half_pieces.bit_length() - 1
    total = n_chunk * half_pieces
    half = half_pieces * piece
    hid_dim = wts.shape[2]
    chunk_rows = acts.shape[2]
    hid_part = hid_dim // PARTS
    hid_cols = min(HIDDEN_COLS, hid_part)
    n_lead, n_idle = jnp.int32(n_chunk), jnp.int32(0)
    for at in range(n_stage):
        n_lead = jnp.where(stage == at, lead[at], n_lead)
        n_idle = jnp.where(stage == at, idle[at], n_idle)
    turns = 2 * n_chunk + n_idle
    n_steps = turns * half_pieces + jnp.where(stage == 0, 1 - hop, half_pieces + hop * last_pos + 1)
    early = half_pieces + 3 * hop

    barrier = pltpu.get_barrier_semaphore()
    for to_stage in range(n_stage):
        for to_pos in range(n_model):

            @pl.when((to_stage != stage) | (to_pos != pos))
            def _():
                pl.semaphore_signal(barrier, inc=1, device_id={"stage": to_stage, "model": to_pos}, device_id_type=MESH)

    copy_w2 = pltpu.make_async_copy(w2_hbm, wts.at[1], w_sem.at[PARTS])

    def copy_w1(part):
        cols = pl.ds(part * hid_part, hid_part)
        return pltpu.make_async_copy(w1_hbm.at[:, cols], wts.at[0, :, cols], w_sem.at[part])


    def copy_in(chunk):
        return pltpu.make_async_copy(inputs_hbm.at[chunk], acts.at[0, chunk], in_sem.at[chunk])

    def grad_in(chunk):
        return pltpu.make_async_copy(inputs_hbm.at[chunk], acts.at[1, chunk], rel_in.at[chunk])

    def copy_targets(side):
        cols = pl.ds(side * half, half)
        return pltpu.make_async_copy(targets_hbm.at[:, :, cols], acts.at[1, :, :, cols], tgt_sem)

    def copy_out(kind, chunk):
        src, dst = ((acts.at[0], x_out), (acts.at[1], e_out), (hid.at[0], a_out), (hid.at[1], g_out))[kind]
        rows = pl.ds(pl.multiple_of(chunk * chunk_rows, chunk_rows), chunk_rows)
        return pltpu.make_async_copy(src.at[chunk], dst.at[rows, :], out_sem.at[kind, chunk])

    @pl.when(stage == 0)
    def _():
        copy_in(0).start()

    for part in range(PARTS):
        copy_w1(part).start()
    copy_w2.start()

    @pl.when(stage == 0)
    def _():
        def start_in(chunk, carry):
            copy_in(chunk).start()
            return carry

        lax.fori_loop(1, n_chunk, start_in, 0)

    @pl.when((stage == last_stage) & (pos == last_pos))
    def _():
        copy_targets(0).start()

    @pl.when((stage == last_stage) & (pos == 0))
    def _():
        copy_targets(1).start()

    def transpose_weights():
        tile = min(256, hid_dim)
        count = hid_dim // tile

        def one(index, carry):
            rows = pl.ds(pl.multiple_of((index // count) * tile, tile), tile)
            cols = pl.ds(pl.multiple_of((index % count) * tile, tile), tile)
            wts[2, cols, rows] = jnp.swapaxes(wts[1, rows, cols], 0, 1)
            wts[3, cols, rows] = jnp.swapaxes(wts[0, rows, cols], 0, 1)
            return carry

        lax.fori_loop(0, count * count, one, 0)

    n_mixed = 2 * (n_chunk - n_lead)
    n_after = 2 * n_chunk - n_lead
    n_first = n_lead + n_idle

    def fill(entry, carry):
        turn = entry - MARGIN
        after = turn - n_first
        pair = (after + 1024) // 2 - 512
        odd = (after + 1024) % 2 == 1
        mixed = (after >= 0) & (after < n_mixed)
        leads = (turn >= 0) & (turn < n_lead)
        fwd = leads | (mixed & odd)
        bwd = (after >= 0) & (after < n_after) & jnp.logical_not(mixed & odd)
        chunk = jnp.where(leads, turn, jnp.where(odd, n_lead + pair, pair))
        chunk = jnp.where(bwd & (after >= n_mixed), after - (n_chunk - n_lead), chunk)
        early_one = fwd & (stage == fore_stage - 1) & (chunk < n_fore)
        back = bwd & (stage < last_stage) & ((stage < fore_stage) | (chunk >= n_relay))
        take = back | (fwd & (stage == fore_stage) & (chunk < n_fore))
        word = jnp.int32(0)
        for flag, bit in (
            (fwd | (bwd & (stage > 0)), SUM),
            (bwd, BACK),
            (fwd & jnp.logical_not(early_one), GATHER),
            (early_one, EARLY),
            (take, TAKE),
            (fwd, FWD),
            (bwd, BWD),
        ):
            word = word + jnp.where(flag, bit, 0)
        table[entry] = word
        return carry

    lax.fori_loop(0, table.shape[0], fill, 0)
    loss_acc[...] = jnp.zeros_like(loss_acc)
    copy_w1(0).wait()

    @pl.when(stage > 0)
    def _():
        for part in range(1, PARTS):
            copy_w1(part).wait()
        copy_w2.wait()
        transpose_weights()

    pl.semaphore_wait(barrier, n_stage * n_model - 1)

    def turn_of(place):
        return lax.shift_right_logical(place + MARGIN * half_pieces, jnp.int32(bits))

    def piece_of(place):
        return lax.bitwise_and(place + MARGIN * half_pieces, jnp.int32(half_pieces - 1))

    def has(word, mask):
        return lax.bitwise_and(word, jnp.int32(mask)) != 0

    def fwd_chunk(turn):
        after = turn - (n_first + MARGIN)
        return jnp.where(turn < n_lead + MARGIN, turn - MARGIN, n_lead + lax.shift_right_arithmetic(after, jnp.int32(1)))

    def bwd_chunk(turn):
        after = turn - (n_first + MARGIN)
        return jnp.where(after < n_mixed, lax.shift_right_arithmetic(after, jnp.int32(1)), after - (n_chunk - n_lead))

    def back_of(turn):
        after = turn - (n_first + MARGIN)
        odd = lax.bitwise_and(after, jnp.int32(1)) == 1
        return ((after >= 0) & jnp.logical_not((after < n_mixed) & odd)).astype(jnp.int32)

    def chunk_of(turn, is_back):
        return jnp.clip(jnp.where(is_back == 1, bwd_chunk(turn), fwd_chunk(turn)), 0, n_chunk - 1)

    def piece_at(side, index):
        col = side * half + index * piece
        return pl.ds(pl.multiple_of(col, piece), piece)

    def remote(src, dst, send_sem, recv_sem, device):
        return pltpu.make_async_remote_copy(
            src_ref=src, dst_ref=dst, send_sem=send_sem, recv_sem=recv_sem, device_id=device, device_id_type=MESH
        )

    def left(send_sem, like):
        remote(like, like, send_sem, loss_recv.at[0], {"model": pos}).wait_send()

    turn_pieces = acts.at[0, 0, :, pl.ds(0, half)]
    turn_sums = send_buf.at[0, 0]

    def rank_of(side):
        return pos if side == 0 else last_pos - pos

    def up(side):
        return {"model": pos + 1 if side == 0 else pos - 1}

    def down(side):
        return {"model": pos - 1 if side == 0 else pos + 1}

    def first_product(step, part):
        place = step + PARTS - 1 - part
        turn = turn_of(place)
        word = table[turn]
        starts = piece_of(place) == 0

        @pl.when(starts & has(word, FWD))
        def _():
            chunk = fwd_chunk(turn)
            if part == 0:

                @pl.when((stage != fore_stage) | (chunk >= n_fore))
                def _():
                    copy_in(chunk).wait()

                copy_out(0, chunk).start()
            else:

                @pl.when((stage == 0) & (place == 0))
                def _():
                    copy_w1(part).wait()

            for col in range(part * hid_part, (part + 1) * hid_part, hid_cols):
                cols = pl.ds(col, hid_cols)
                pre = dot_nn(acts[0, chunk], wts[0, :, cols]).astype(BF16)
                hid[1, chunk, :, cols] = pre
                hid[0, chunk, :, cols] = gelu_tanh(pre.astype(F32)).astype(BF16)
            if part == PARTS - 1:
                copy_out(2, chunk).start()

                @pl.when((stage == 0) & (place == 0))
                def _():
                    copy_w2.wait()

        @pl.when(starts & has(word, BWD))
        def _():
            chunk = bwd_chunk(turn)
            if part == 0:

                @pl.when((stage == fore_stage) & (chunk < n_relay))
                def _():
                    grad_in(chunk).wait()

                copy_out(1, chunk).start()
                copy_out(0, chunk).wait()
            for col in range(part * hid_part, (part + 1) * hid_part, hid_cols):
                cols = pl.ds(col, hid_cols)
                grad_act = dot_nn(acts[1, chunk], wts[2, :, cols]).astype(BF16)
                slope = gelu_slope(hid[1, chunk, :, cols].astype(F32))
                hid[1, chunk, :, cols] = (slope * grad_act.astype(F32)).astype(BF16)
            if part == PARTS - 1:
                copy_out(3, chunk).start()

        if part == 0:

            @pl.when((stage == 0) & (place == n_lead * half_pieces))
            def _():
                transpose_weights()

    def loss_copy(side, to_stage, to_pos):
        return remote(
            loss_acc, loss_in.at[side], loss_send.at[to_stage * n_model + to_pos], loss_recv.at[side],
            {"stage": to_stage, "model": to_pos},
        )

    def send_loss(side):
        loss_in[side] = loss_acc[...]
        for to_stage in range(n_stage):
            for to_pos in range(n_model):

                @pl.when((to_stage != stage) | (to_pos != pos))
                def _():
                    loss_copy(side, to_stage, to_pos).start()

    def sum_steps(step):
        now = []
        for side in (0, 1):
            rank = rank_of(side)
            place = step - hop * rank
            turn = turn_of(place)
            word, old = table[turn], table[turn - 2]
            index = piece_of(place)
            half_turn = lax.bitwise_and(turn, jnp.int32(1))
            inn = lax.bitwise_and(place + MARGIN * half_pieces, jnp.int32(RECV_SLOTS - 1))
            sums = has(word, SUM)
            is_back = back_of(turn)
            now.append((rank, word, sums, is_back, chunk_of(turn, is_back), index, half_turn, inn, piece_at(side, index)))

            @pl.when((index == 0) & has(old, SUM))
            def _():
                @pl.when(rank < last_pos)
                def _():
                    left(sum_send.at[side, half_turn], turn_sums)

                @pl.when((rank == last_pos) & has(old, BACK))
                def _():
                    left(down_send.at[side, half_turn], turn_pieces)

        @pl.when(now[0][2] | now[1][2])
        def _():
            for side in (0, 1):
                _, _, _, is_back, chunk, index, half_turn, _, cols = now[side]
                send_buf[side, half_turn, index] = dot_nn(hid[is_back, chunk], wts[1 + 2 * is_back, :, cols])

        for side in (0, 1):
            rank, word, sums, is_back, chunk, out, half_turn, inn, cols = now[side]
            bwd = has(word, BACK)
            index = chunk * half_pieces + out
            mine = send_buf.at[side, half_turn, out]
            gone = down_send.at[side, half_turn]
            hand_on = remote(mine, recv_buf.at[side, inn], sum_send.at[side, half_turn], sum_recv.at[side, inn], up(side))

            @pl.when(sums & (rank > 0))
            def _():
                hand_on.wait_recv()
                mine[...] = mine[...] + recv_buf[side, inn]

            @pl.when(sums & (rank < last_pos))
            def _():
                hand_on.start()

            @pl.when(sums & (rank == last_pos))
            def _():
                whole = acts[is_back, chunk, :, cols].astype(F32) + mine[...]
                scored = has(word, FWD) & (stage == last_stage)

                @pl.when(scored)
                def _():
                    @pl.when(index == 0)
                    def _():
                        copy_targets(side).wait()

                    err = whole.astype(BF16).astype(F32) - acts[1, chunk, :, cols].astype(F32)
                    acts[1, chunk, :, cols] = (err * grad_scale).astype(BF16)
                    square = jnp.sum((err * err).reshape(err.shape[0] // 8, 8, piece), axis=0)
                    part = square[:, :128]
                    for lane in range(1, piece // 128):
                        part = part + square[:, lane * 128 : (lane + 1) * 128]
                    loss_acc[...] = loss_acc[...] + part

                    @pl.when(index == total - 1)
                    def _():
                        send_loss(side)

                @pl.when(jnp.logical_not(scored))
                def _():
                    acts[1 - is_back, chunk, :, cols] = whole.astype(BF16)

                @pl.when(bwd & (index == total - 2 * half_pieces))
                def _():
                    pl.semaphore_wait(spent_sem.at[side], 1)

                @pl.when(bwd & (stage == 1) & (index == (n_relay - 2) * half_pieces))
                def _():
                    pl.semaphore_wait(free_sem.at[side], 1)

                relayed = (stage == last_stage) & (chunk < n_relay)
                there = acts.at[1, chunk, :, cols]

                @pl.when(bwd & relayed)
                def _():
                    arrived = rel_recv.at[side, jnp.minimum(index, n_relay * half_pieces - 1)]
                    remote(acts.at[0, chunk, :, cols], there, gone, arrived, {"stage": 0}).start()

                @pl.when(bwd & jnp.logical_not(relayed))
                def _():
                    arrived = take_recv.at[side, index]
                    remote(acts.at[0, chunk, :, cols], there, gone, arrived, {"stage": stage - 1}).start()

    def gather_step(side, step):
        rank = rank_of(side)
        place = step - 3 * hop - hop * (last_pos - rank)
        turn = turn_of(place)
        word, old = table[turn], table[turn - 2]
        out = piece_of(place)
        half_turn = lax.bitwise_and(turn, jnp.int32(1))
        chunk = jnp.clip(fwd_chunk(turn), 0, n_chunk - 1)
        index = chunk * half_pieces + out
        cols = piece_at(side, out)
        here = acts.at[1, chunk, :, cols]
        gone = over_send.at[side, half_turn]

        @pl.when((out == 0) & has(old, GATHER | EARLY))
        def _():
            @pl.when(has(old, GATHER) & (rank > 0))
            def _():
                left(gat_send.at[side, half_turn], turn_pieces)

            @pl.when((stage < last_stage) & (has(old, GATHER) | (rank == last_pos)))
            def _():
                left(gone, turn_pieces)

                @pl.when((fwd_chunk(turn - 2) == n_chunk - 1) & (rank == last_pos))
                def _():
                    pl.semaphore_signal(spent_sem.at[side], inc=1, device_id={"stage": stage + 1}, device_id_type=MESH)

        @pl.when(has(word, GATHER))
        def _():
            hand_on = remote(here, here, gat_send.at[side, half_turn], gat_recv.at[side, index], down(side))

            @pl.when(rank < last_pos)
            def _():
                hand_on.wait_recv()

            @pl.when(rank > 0)
            def _():
                hand_on.start()

            @pl.when(stage < last_stage)
            def _():
                remote(here, acts.at[0, chunk, :, cols], gone, in_sem.at[chunk], {"stage": stage + 1}).start()

        @pl.when(has(word, EARLY) & (rank == last_pos))
        def _():
            arrived = take_recv.at[side, jnp.minimum(total + index, total + n_fore * half_pieces - 1)]
            remote(here, acts.at[0, chunk, :, cols], gone, arrived, {"stage": stage + 1}).start()

    def take_step(side, step):
        rank = rank_of(side)
        place = step + early - hop * (last_pos - rank)
        turn = turn_of(place)
        word, old = table[turn], table[turn - 2]
        out = piece_of(place)
        gone = back_send.at[side, lax.bitwise_and(turn, jnp.int32(1))]

        @pl.when((out == 0) & has(old, TAKE) & (rank > 0))
        def _():
            left(gone, turn_pieces)

        @pl.when(has(word, TAKE))
        def _():
            is_back = back_of(turn)
            chunk = chunk_of(turn, is_back)
            index = chunk * half_pieces + out + (1 - is_back) * total
            here = acts.at[is_back, chunk, :, piece_at(side, out)]
            hand_on = remote(here, here, gone, take_recv.at[side, index], down(side))
            hand_on.wait_recv()

            @pl.when(rank > 0)
            def _():
                hand_on.start()

    def relay_step(side, step):
        rank = rank_of(side)
        place = step - (n_chunk + RELAY_START) * half_pieces - hop * (last_pos - rank)
        turn = turn_of(place) - MARGIN
        out = piece_of(place)
        half_turn = lax.bitwise_and(turn, jnp.int32(1))
        chunk = jnp.clip(turn, 0, n_relay - 1)
        here = acts.at[1, chunk, :, piece_at(side, out)]
        gone = rel_over.at[side, half_turn]
        hand_on = remote(here, here, rel_send.at[side, half_turn], rel_recv.at[side, chunk * half_pieces + out], down(side))

        @pl.when((out == 0) & (turn >= 2) & (turn < n_relay + 2))
        def _():
            @pl.when(rank > 0)
            def _():
                left(rel_send.at[side, half_turn], turn_pieces)

            left(gone, turn_pieces)

            @pl.when((turn == n_relay + 1) & (rank == last_pos))
            def _():
                pl.semaphore_signal(free_sem.at[side], inc=1, device_id={"stage": 1}, device_id_type=MESH)

        @pl.when((turn >= 0) & (turn < n_relay))
        def _():
            hand_on.wait_recv()

            @pl.when(rank > 0)
            def _():
                hand_on.start()

            remote(here, here, gone, rel_in.at[chunk], {"stage": fore_stage}).start()

    def loop_step(step, carry):
        take_step(0, step)
        take_step(1, step)
        for part in range(PARTS):
            first_product(step, part)
        sum_steps(step)
        gather_step(0, step)
        gather_step(1, step)

        @pl.when((stage == 0) & (step >= n_chunk * half_pieces))
        def _():
            relay_step(0, step)
            relay_step(1, step)

        return carry

    lax.fori_loop(jnp.where(stage == fore_stage, -early, 1 - PARTS), n_steps, loop_step, 0)

    for side, owner in ((0, last_pos), (1, 0)):
        owns = (stage == last_stage) & (pos == owner)

        @pl.when(jnp.logical_not(owns))
        def _():
            loss_copy(side, 0, 0).wait_recv()

        @pl.when(owns)
        def _():
            for to_stage in range(n_stage):
                for to_pos in range(n_model):

                    @pl.when((to_stage != stage) | (to_pos != pos))
                    def _():
                        loss_copy(side, to_stage, to_pos).wait_send()

    loss_out[...] = jnp.full(loss_out.shape, jnp.sum(loss_in[0] + loss_in[1]) * (0.5 * grad_scale), F32)

    def end_out(chunk, carry):
        for kind in (1, 2, 3):
            copy_out(kind, chunk).wait()
        return carry

    lax.fori_loop(0, n_chunk, end_out, 0)


def solution(mesh):
    n_stage = mesh.shape["stage"]
    n_model = mesh.shape["model"]

    def stage_step(inputs, targets, w_in, w_out):
        num_micro, num_tokens, model_dim = inputs.shape
        hid_dim = w_in.shape[3]
        rows = num_micro * num_tokens
        chunk = min(CHUNK_TOKENS, num_tokens)
        n_chunk = rows // chunk
        piece = min(PIECE_COLS, model_dim // 2)
        half_pieces = model_dim // 2 // piece
        grad_scale = 1.0 / (rows * model_dim)
        lead = [n_chunk] * (n_stage - 2) + [min(PREV_LEAD, n_chunk), min(LAST_LEAD, n_chunk)]
        idle = [FIRST_IDLE] + [NEXT_IDLE] * (n_stage - 3) + [0, 0]
        n_fore, n_relay = min(FORE_CHUNKS, n_chunk - 1), min(RELAY_CHUNKS, n_chunk - 1)
        kernel = functools.partial(
            stage_kernel, n_stage, n_model, n_chunk, half_pieces, piece, HOP_LAG, lead, idle, n_fore, n_relay, grad_scale
        )
        any_space = pl.BlockSpec(memory_space=pl.ANY)
        dma = pltpu.SemaphoreType.DMA
        layer_in, layer_grad, layer_act, layer_pre, loss = pl.pallas_call(
            kernel,
            out_shape=(
                jax.ShapeDtypeStruct((rows, model_dim), BF16),
                jax.ShapeDtypeStruct((rows, model_dim), BF16),
                jax.ShapeDtypeStruct((rows, hid_dim), BF16),
                jax.ShapeDtypeStruct((rows, hid_dim), BF16),
                jax.ShapeDtypeStruct((8, 128), F32),
            ),
            in_specs=[any_space] * 4,
            out_specs=(any_space, any_space, any_space, any_space, pl.BlockSpec(memory_space=pltpu.VMEM)),
            scratch_shapes=[
                pltpu.VMEM((4, model_dim, hid_dim), BF16),
                pltpu.VMEM((2, n_chunk, chunk, model_dim), BF16),
                pltpu.VMEM((2, n_chunk, chunk, hid_dim), BF16),
                pltpu.VMEM((2, 2, half_pieces, chunk, piece), F32),
                pltpu.VMEM((2, RECV_SLOTS, chunk, piece), F32),
                pltpu.VMEM((8, 128), F32),
                pltpu.VMEM((2, 8, 128), F32),
                dma((PARTS + 1,)),
                dma((n_chunk,)),
                dma,
                dma((2, 2)),
                dma((2, RECV_SLOTS)),
                dma((2, 2)),
                dma((2, n_chunk * half_pieces)),
                dma((2, 2)),
                dma((2, 2)),
                dma((2, (n_chunk + n_fore) * half_pieces)),
                dma((2, 2)),
                dma((4, n_chunk)),
                dma((n_stage * n_model,)),
                dma((2,)),
                pltpu.SemaphoreType.REGULAR((2,)),
                dma((2, 2)),
                dma((2, 2)),
                dma((2, n_relay * half_pieces)),
                dma((n_relay,)),
                pltpu.SemaphoreType.REGULAR((2,)),
                pltpu.SMEM((2 * n_chunk + max(idle) + 2 * MARGIN,), jnp.int32),
            ],
            compiler_params=pltpu.CompilerParams(collective_id=0, has_side_effects=True, vmem_limit_bytes=63 * 1024 * 1024),
            name="stage_kernel",
        )(
            inputs.reshape(n_chunk, chunk, model_dim),
            targets.reshape(n_chunk, chunk, model_dim),
            w_in.reshape(model_dim, hid_dim),
            w_out.reshape(hid_dim, model_dim),
        )

        def over_rows(left, right):
            return lax.dot_general(left, right, (((0,), (0,)), ((), ())), preferred_element_type=F32)

        grad_in = over_rows(layer_in, layer_pre)
        grad_out = over_rows(layer_act, layer_grad)
        return grad_in[None, None], grad_out[None, None], loss[0, :1]

    return jax.shard_map(
        stage_step,
        mesh=mesh,
        in_specs=(P("data", None, None), P("data", None, None), P("stage", None, None, "model"), P("stage", None, "model", None)),
        out_specs=(P(("data", "stage"), None, None, "model"), P(("data", "stage"), None, "model", None), P("data")),
        check_vma=False,
    )
```

```python
import functools

import jax
import jax.numpy as jnp
from jax import lax
from jax.experimental import pallas as pl
from jax.experimental.pallas import tpu as pltpu
from jax.sharding import PartitionSpec as P

GELU_COEF = 0.7978845608028654
CUBIC_COEF = 0.044715

CHUNK_TOKENS = 64
PIECE_COLS = 256
HIDDEN_COLS = 512
PARTS = 2
HOP_LAG = 2
RECV_SLOTS = 8
LAST_LEAD = 5
PREV_LEAD = 16
FIRST_IDLE = 12
NEXT_IDLE = 7
FORE_CHUNKS = 6
RELAY_CHUNKS = 18
RELAY_START = 0

SUM, BACK, GATHER, EARLY, TAKE, FWD, BWD = 256, 512, 1024, 2048, 4096, 8192, 16384
MARGIN = 8

BF16 = jnp.bfloat16
F32 = jnp.float32
MESH = pl.DeviceIdType.MESH


def gelu_tanh(values):
    inner_arg = GELU_COEF * (values + CUBIC_COEF * values * values * values)
    return 0.5 * values * (1.0 + jnp.tanh(inner_arg))


def gelu_slope(values):
    tanh_val = jnp.tanh(GELU_COEF * (values + CUBIC_COEF * values * values * values))
    return 0.5 * (1.0 + tanh_val) + 0.5 * values * (1.0 - tanh_val * tanh_val) * GELU_COEF * (1.0 + 3.0 * CUBIC_COEF * values * values)


def dot_nn(left, right):
    return jnp.dot(left, right, preferred_element_type=F32)


def dot_nt(left, right):
    return lax.dot_general(left, right, (((1,), (1,)), ((), ())), preferred_element_type=F32)


def stage_kernel(
    n_stage, n_model, n_chunk, half_pieces, piece, hop, lead, idle, n_fore, n_relay, grad_scale,
    inputs_hbm, targets_hbm, w1_hbm, w2_hbm,
    x_out, e_out, a_out, g_out, loss_out,
    wts, acts, hid, send_buf, recv_buf, loss_acc, loss_in,
    w_sem, in_sem, tgt_sem, sum_send, sum_recv, gat_send, gat_recv, over_send, back_send, take_recv, down_send, out_sem,
    loss_send, loss_recv, spent_sem, rel_send, rel_over, rel_recv, rel_in, free_sem, table,
):
    pos = lax.axis_index("model")
    stage = lax.axis_index("stage")
    last_pos = n_model - 1
    last_stage = n_stage - 1
    fore_stage = n_stage - 2
    bits = half_pieces.bit_length() - 1
    total = n_chunk * half_pieces
    half = half_pieces * piece
    hid_dim = wts.shape[2]
    chunk_rows = acts.shape[2]
    hid_part = hid_dim // PARTS
    hid_cols = min(HIDDEN_COLS, hid_part)
    n_lead, n_idle = jnp.int32(n_chunk), jnp.int32(0)
    for at in range(n_stage):
        n_lead = jnp.where(stage == at, lead[at], n_lead)
        n_idle = jnp.where(stage == at, idle[at], n_idle)
    turns = 2 * n_chunk + n_idle
    n_steps = turns * half_pieces + jnp.where(stage == 0, 1 - hop, half_pieces + hop * last_pos + 1)
    early = half_pieces + 3 * hop + 1

    barrier = pltpu.get_barrier_semaphore()
    for to_stage in range(n_stage):
        for to_pos in range(n_model):

            @pl.when((to_stage != stage) | (to_pos != pos))
            def _():
                pl.semaphore_signal(barrier, inc=1, device_id={"stage": to_stage, "model": to_pos}, device_id_type=MESH)

    copy_w2 = pltpu.make_async_copy(w2_hbm, wts.at[1], w_sem.at[PARTS])

    def copy_w1(part):
        cols = pl.ds(part * hid_part, hid_part)
        return pltpu.make_async_copy(w1_hbm.at[:, cols], wts.at[0, :, cols], w_sem.at[part])


    def copy_in(chunk):
        return pltpu.make_async_copy(inputs_hbm.at[chunk], acts.at[0, chunk], in_sem.at[chunk])

    def grad_in(chunk):
        return pltpu.make_async_copy(inputs_hbm.at[chunk], acts.at[1, chunk], rel_in.at[chunk])

    def copy_targets(side):
        cols = pl.ds(side * half, half)
        return pltpu.make_async_copy(targets_hbm.at[:, :, cols], acts.at[1, :, :, cols], tgt_sem)

    def copy_out(kind, chunk):
        src, dst = ((acts.at[0], x_out), (acts.at[1], e_out), (hid.at[0], a_out), (hid.at[1], g_out))[kind]
        rows = pl.ds(pl.multiple_of(chunk * chunk_rows, chunk_rows), chunk_rows)
        return pltpu.make_async_copy(src.at[chunk], dst.at[rows, :], out_sem.at[kind, chunk])

    @pl.when(stage == 0)
    def _():
        copy_in(0).start()

    for part in range(PARTS):
        copy_w1(part).start()
    copy_w2.start()

    @pl.when(stage == 0)
    def _():
        def start_in(chunk, carry):
            copy_in(chunk).start()
            return carry

        lax.fori_loop(1, n_chunk, start_in, 0)

    @pl.when((stage == last_stage) & (pos == last_pos))
    def _():
        copy_targets(0).start()

    @pl.when((stage == last_stage) & (pos == 0))
    def _():
        copy_targets(1).start()

    def transpose_weights():
        tile = min(256, hid_dim)
        count = hid_dim // tile

        def one(index, carry):
            rows = pl.ds(pl.multiple_of((index // count) * tile, tile), tile)
            cols = pl.ds(pl.multiple_of((index % count) * tile, tile), tile)
            wts[2, cols, rows] = jnp.swapaxes(wts[1, rows, cols], 0, 1)
            wts[3, cols, rows] = jnp.swapaxes(wts[0, rows, cols], 0, 1)
            return carry

        lax.fori_loop(0, count * count, one, 0)

    n_mixed = 2 * (n_chunk - n_lead)
    n_after = 2 * n_chunk - n_lead
    n_first = n_lead + n_idle

    def fill(entry, carry):
        turn = entry - MARGIN
        after = turn - n_first
        pair = (after + 1024) // 2 - 512
        odd = (after + 1024) % 2 == 1
        mixed = (after >= 0) & (after < n_mixed)
        leads = (turn >= 0) & (turn < n_lead)
        fwd = leads | (mixed & odd)
        bwd = (after >= 0) & (after < n_after) & jnp.logical_not(mixed & odd)
        chunk = jnp.where(leads, turn, jnp.where(odd, n_lead + pair, pair))
        chunk = jnp.where(bwd & (after >= n_mixed), after - (n_chunk - n_lead), chunk)
        early_one = fwd & (stage == fore_stage - 1) & (chunk < n_fore)
        back = bwd & (stage < last_stage) & ((stage < fore_stage) | (chunk >= n_relay))
        take = back | (fwd & (stage == fore_stage) & (chunk < n_fore))
        word = jnp.int32(0)
        for flag, bit in (
            (fwd | (bwd & (stage > 0)), SUM),
            (bwd, BACK),
            (fwd & jnp.logical_not(early_one), GATHER),
            (early_one, EARLY),
            (take, TAKE),
            (fwd, FWD),
            (bwd, BWD),
        ):
            word = word + jnp.where(flag, bit, 0)
        table[entry] = word
        return carry

    lax.fori_loop(0, table.shape[0], fill, 0)
    loss_acc[...] = jnp.zeros_like(loss_acc)
    copy_w1(0).wait()

    @pl.when(stage > 0)
    def _():
        for part in range(1, PARTS):
            copy_w1(part).wait()
        copy_w2.wait()
        transpose_weights()

    pl.semaphore_wait(barrier, n_stage * n_model - 1)

    def turn_of(place):
        return lax.shift_right_logical(place + MARGIN * half_pieces, jnp.int32(bits))

    def piece_of(place):
        return lax.bitwise_and(place + MARGIN * half_pieces, jnp.int32(half_pieces - 1))

    def has(word, mask):
        return lax.bitwise_and(word, jnp.int32(mask)) != 0

    def fwd_chunk(turn):
        after = turn - (n_first + MARGIN)
        return jnp.where(turn < n_lead + MARGIN, turn - MARGIN, n_lead + lax.shift_right_arithmetic(after, jnp.int32(1)))

    def bwd_chunk(turn):
        after = turn - (n_first + MARGIN)
        return jnp.where(after < n_mixed, lax.shift_right_arithmetic(after, jnp.int32(1)), after - (n_chunk - n_lead))

    def back_of(turn):
        after = turn - (n_first + MARGIN)
        odd = lax.bitwise_and(after, jnp.int32(1)) == 1
        return ((after >= 0) & jnp.logical_not((after < n_mixed) & odd)).astype(jnp.int32)

    def chunk_of(turn, is_back):
        return jnp.clip(jnp.where(is_back == 1, bwd_chunk(turn), fwd_chunk(turn)), 0, n_chunk - 1)

    def piece_at(side, index):
        col = side * half + index * piece
        return pl.ds(pl.multiple_of(col, piece), piece)

    def remote(src, dst, send_sem, recv_sem, device):
        return pltpu.make_async_remote_copy(
            src_ref=src, dst_ref=dst, send_sem=send_sem, recv_sem=recv_sem, device_id=device, device_id_type=MESH
        )

    def left(send_sem, like):
        remote(like, like, send_sem, loss_recv.at[0], {"model": pos}).wait_send()

    turn_pieces = acts.at[0, 0, :, pl.ds(0, half)]
    turn_sums = send_buf.at[0, 0]

    def rank_of(side):
        return pos if side == 0 else last_pos - pos

    def up(side):
        return {"model": pos + 1 if side == 0 else pos - 1}

    def down(side):
        return {"model": pos - 1 if side == 0 else pos + 1}

    def first_product(step, part):
        place = step + PARTS - 1 - part
        turn = turn_of(place)
        word = table[turn]
        starts = piece_of(place) == 0

        @pl.when(starts & has(word, FWD))
        def _():
            chunk = fwd_chunk(turn)
            if part == 0:

                @pl.when((stage != fore_stage) | (chunk >= n_fore))
                def _():
                    copy_in(chunk).wait()

                copy_out(0, chunk).start()
            else:

                @pl.when((stage == 0) & (place == 0))
                def _():
                    copy_w1(part).wait()

            for col in range(part * hid_part, (part + 1) * hid_part, hid_cols):
                cols = pl.ds(col, hid_cols)
                pre = dot_nn(acts[0, chunk], wts[0, :, cols]).astype(BF16)
                hid[1, chunk, :, cols] = pre
                hid[0, chunk, :, cols] = gelu_tanh(pre.astype(F32)).astype(BF16)
            if part == PARTS - 1:
                copy_out(2, chunk).start()

                @pl.when((stage == 0) & (place == 0))
                def _():
                    copy_w2.wait()

        @pl.when(starts & has(word, BWD))
        def _():
            chunk = bwd_chunk(turn)
            if part == 0:

                @pl.when((stage == fore_stage) & (chunk < n_relay))
                def _():
                    grad_in(chunk).wait()

                copy_out(1, chunk).start()
                copy_out(0, chunk).wait()
            for col in range(part * hid_part, (part + 1) * hid_part, hid_cols):
                cols = pl.ds(col, hid_cols)
                grad_act = dot_nn(acts[1, chunk], wts[2, :, cols]).astype(BF16)
                slope = gelu_slope(hid[1, chunk, :, cols].astype(F32))
                hid[1, chunk, :, cols] = (slope * grad_act.astype(F32)).astype(BF16)
            if part == PARTS - 1:
                copy_out(3, chunk).start()

        if part == 0:

            @pl.when((stage == 0) & (place == n_lead * half_pieces))
            def _():
                transpose_weights()

    def loss_copy(side, to_stage, to_pos):
        return remote(
            loss_acc, loss_in.at[side], loss_send.at[to_stage * n_model + to_pos], loss_recv.at[side],
            {"stage": to_stage, "model": to_pos},
        )

    def send_loss(side):
        loss_in[side] = loss_acc[...]
        for to_stage in range(n_stage):
            for to_pos in range(n_model):

                @pl.when((to_stage != stage) | (to_pos != pos))
                def _():
                    loss_copy(side, to_stage, to_pos).start()

    def sum_steps(step):
        now = []
        for side in (0, 1):
            rank = rank_of(side)
            place = step - hop * rank
            turn = turn_of(place)
            word, old = table[turn], table[turn - 2]
            index = piece_of(place)
            half_turn = lax.bitwise_and(turn, jnp.int32(1))
            inn = lax.bitwise_and(place + MARGIN * half_pieces, jnp.int32(RECV_SLOTS - 1))
            sums = has(word, SUM)
            is_back = back_of(turn)
            now.append((rank, word, sums, is_back, chunk_of(turn, is_back), index, half_turn, inn, piece_at(side, index)))

            @pl.when((index == 0) & has(old, SUM))
            def _():
                @pl.when(rank < last_pos)
                def _():
                    left(sum_send.at[side, half_turn], turn_sums)

                @pl.when((rank == last_pos) & has(old, BACK))
                def _():
                    left(down_send.at[side, half_turn], turn_pieces)

        @pl.when(now[0][2] | now[1][2])
        def _():
            for side in (0, 1):
                _, _, _, is_back, chunk, index, half_turn, _, cols = now[side]
                send_buf[side, half_turn, index] = dot_nn(hid[is_back, chunk], wts[1 + 2 * is_back, :, cols])

        for side in (0, 1):
            rank, word, sums, is_back, chunk, out, half_turn, inn, cols = now[side]
            bwd = has(word, BACK)
            index = chunk * half_pieces + out
            mine = send_buf.at[side, half_turn, out]
            gone = down_send.at[side, half_turn]
            hand_on = remote(mine, recv_buf.at[side, inn], sum_send.at[side, half_turn], sum_recv.at[side, inn], up(side))

            @pl.when(sums & (rank > 0))
            def _():
                hand_on.wait_recv()
                mine[...] = mine[...] + recv_buf[side, inn]

            @pl.when(sums & (rank < last_pos))
            def _():
                hand_on.start()

            @pl.when(sums & (rank == last_pos))
            def _():
                whole = acts[is_back, chunk, :, cols].astype(F32) + mine[...]
                scored = has(word, FWD) & (stage == last_stage)

                @pl.when(scored)
                def _():
                    @pl.when(index == 0)
                    def _():
                        copy_targets(side).wait()

                    err = whole.astype(BF16).astype(F32) - acts[1, chunk, :, cols].astype(F32)
                    acts[1, chunk, :, cols] = (err * grad_scale).astype(BF16)
                    square = jnp.sum((err * err).reshape(err.shape[0] // 8, 8, piece), axis=0)
                    part = square[:, :128]
                    for lane in range(1, piece // 128):
                        part = part + square[:, lane * 128 : (lane + 1) * 128]
                    loss_acc[...] = loss_acc[...] + part

                    @pl.when(index == total - 1)
                    def _():
                        send_loss(side)

                @pl.when(jnp.logical_not(scored))
                def _():
                    acts[1 - is_back, chunk, :, cols] = whole.astype(BF16)

                @pl.when(bwd & (index == total - 2 * half_pieces))
                def _():
                    pl.semaphore_wait(spent_sem.at[side], 1)

                @pl.when(bwd & (stage == 1) & (index == (n_relay - 2) * half_pieces))
                def _():
                    pl.semaphore_wait(free_sem.at[side], 1)

                relayed = (stage == last_stage) & (chunk < n_relay)
                there = acts.at[1, chunk, :, cols]

                @pl.when(bwd & relayed)
                def _():
                    arrived = rel_recv.at[side, jnp.minimum(index, n_relay * half_pieces - 1)]
                    remote(acts.at[0, chunk, :, cols], there, gone, arrived, {"stage": 0}).start()

                @pl.when(bwd & jnp.logical_not(relayed))
                def _():
                    arrived = take_recv.at[side, index]
                    remote(acts.at[0, chunk, :, cols], there, gone, arrived, {"stage": stage - 1}).start()

    def gather_step(side, step):
        rank = rank_of(side)
        place = step - 3 * hop - hop * (last_pos - rank)
        turn = turn_of(place)
        word, old = table[turn], table[turn - 2]
        out = piece_of(place)
        half_turn = lax.bitwise_and(turn, jnp.int32(1))
        chunk = jnp.clip(fwd_chunk(turn), 0, n_chunk - 1)
        index = chunk * half_pieces + out
        cols = piece_at(side, out)
        here = acts.at[1, chunk, :, cols]
        gone = over_send.at[side, half_turn]

        @pl.when((out == 0) & has(old, GATHER | EARLY))
        def _():
            @pl.when(has(old, GATHER) & (rank > 0))
            def _():
                left(gat_send.at[side, half_turn], turn_pieces)

            @pl.when((stage < last_stage) & (has(old, GATHER) | (rank == last_pos)))
            def _():
                left(gone, turn_pieces)

                @pl.when((fwd_chunk(turn - 2) == n_chunk - 1) & (rank == last_pos))
                def _():
                    pl.semaphore_signal(spent_sem.at[side], inc=1, device_id={"stage": stage + 1}, device_id_type=MESH)

        @pl.when(has(word, GATHER))
        def _():
            hand_on = remote(here, here, gat_send.at[side, half_turn], gat_recv.at[side, index], down(side))

            @pl.when(rank < last_pos)
            def _():
                hand_on.wait_recv()

            @pl.when(rank > 0)
            def _():
                hand_on.start()

            @pl.when(stage < last_stage)
            def _():
                remote(here, acts.at[0, chunk, :, cols], gone, in_sem.at[chunk], {"stage": stage + 1}).start()

        @pl.when(has(word, EARLY) & (rank == last_pos))
        def _():
            arrived = take_recv.at[side, jnp.minimum(total + index, total + n_fore * half_pieces - 1)]
            remote(here, acts.at[0, chunk, :, cols], gone, arrived, {"stage": stage + 1}).start()

    def take_step(side, step):
        rank = rank_of(side)
        place = step + early - hop * (last_pos - rank)
        turn = turn_of(place)
        word, old = table[turn], table[turn - 2]
        out = piece_of(place)
        gone = back_send.at[side, lax.bitwise_and(turn, jnp.int32(1))]

        @pl.when((out == 0) & has(old, TAKE) & (rank > 0))
        def _():
            left(gone, turn_pieces)

        @pl.when(has(word, TAKE))
        def _():
            is_back = back_of(turn)
            chunk = chunk_of(turn, is_back)
            index = chunk * half_pieces + out + (1 - is_back) * total
            here = acts.at[is_back, chunk, :, piece_at(side, out)]
            hand_on = remote(here, here, gone, take_recv.at[side, index], down(side))
            hand_on.wait_recv()

            @pl.when(rank > 0)
            def _():
                hand_on.start()

    def relay_step(side, step):
        rank = rank_of(side)
        place = step - (n_chunk + RELAY_START) * half_pieces - hop * (last_pos - rank)
        turn = turn_of(place) - MARGIN
        out = piece_of(place)
        half_turn = lax.bitwise_and(turn, jnp.int32(1))
        chunk = jnp.clip(turn, 0, n_relay - 1)
        here = acts.at[1, chunk, :, piece_at(side, out)]
        gone = rel_over.at[side, half_turn]
        hand_on = remote(here, here, rel_send.at[side, half_turn], rel_recv.at[side, chunk * half_pieces + out], down(side))

        @pl.when((out == 0) & (turn >= 2) & (turn < n_relay + 2))
        def _():
            @pl.when(rank > 0)
            def _():
                left(rel_send.at[side, half_turn], turn_pieces)

            left(gone, turn_pieces)

            @pl.when((turn == n_relay + 1) & (rank == last_pos))
            def _():
                pl.semaphore_signal(free_sem.at[side], inc=1, device_id={"stage": 1}, device_id_type=MESH)

        @pl.when((turn >= 0) & (turn < n_relay))
        def _():
            hand_on.wait_recv()

            @pl.when(rank > 0)
            def _():
                hand_on.start()

            remote(here, here, gone, rel_in.at[chunk], {"stage": fore_stage}).start()

    def loop_step(step, carry):
        for part in range(PARTS):
            first_product(step, part)
        sum_steps(step)
        take_step(0, step)
        take_step(1, step)

        @pl.when((stage == 0) & (step >= n_chunk * half_pieces))
        def _():
            relay_step(0, step)
            relay_step(1, step)

        gather_step(0, step)
        gather_step(1, step)
        return carry

    lax.fori_loop(jnp.where(stage == fore_stage, -early, 1 - PARTS), n_steps, loop_step, 0)

    for side, owner in ((0, last_pos), (1, 0)):
        owns = (stage == last_stage) & (pos == owner)

        @pl.when(jnp.logical_not(owns))
        def _():
            loss_copy(side, 0, 0).wait_recv()

        @pl.when(owns)
        def _():
            for to_stage in range(n_stage):
                for to_pos in range(n_model):

                    @pl.when((to_stage != stage) | (to_pos != pos))
                    def _():
                        loss_copy(side, to_stage, to_pos).wait_send()

    loss_out[...] = jnp.full(loss_out.shape, jnp.sum(loss_in[0] + loss_in[1]) * (0.5 * grad_scale), F32)

    def end_out(chunk, carry):
        for kind in (1, 2, 3):
            copy_out(kind, chunk).wait()
        return carry

    lax.fori_loop(0, n_chunk, end_out, 0)


def solution(mesh):
    n_stage = mesh.shape["stage"]
    n_model = mesh.shape["model"]

    def stage_step(inputs, targets, w_in, w_out):
        num_micro, num_tokens, model_dim = inputs.shape
        hid_dim = w_in.shape[3]
        rows = num_micro * num_tokens
        chunk = min(CHUNK_TOKENS, num_tokens)
        n_chunk = rows // chunk
        piece = min(PIECE_COLS, model_dim // 2)
        half_pieces = model_dim // 2 // piece
        grad_scale = 1.0 / (rows * model_dim)
        lead = [n_chunk] * (n_stage - 2) + [min(PREV_LEAD, n_chunk), min(LAST_LEAD, n_chunk)]
        idle = [FIRST_IDLE] + [NEXT_IDLE] * (n_stage - 3) + [0, 0]
        n_fore, n_relay = min(FORE_CHUNKS, n_chunk - 1), min(RELAY_CHUNKS, n_chunk - 1)
        kernel = functools.partial(
            stage_kernel, n_stage, n_model, n_chunk, half_pieces, piece, HOP_LAG, lead, idle, n_fore, n_relay, grad_scale
        )
        any_space = pl.BlockSpec(memory_space=pl.ANY)
        dma = pltpu.SemaphoreType.DMA
        layer_in, layer_grad, layer_act, layer_pre, loss = pl.pallas_call(
            kernel,
            out_shape=(
                jax.ShapeDtypeStruct((rows, model_dim), BF16),
                jax.ShapeDtypeStruct((rows, model_dim), BF16),
                jax.ShapeDtypeStruct((rows, hid_dim), BF16),
                jax.ShapeDtypeStruct((rows, hid_dim), BF16),
                jax.ShapeDtypeStruct((8, 128), F32),
            ),
            in_specs=[any_space] * 4,
            out_specs=(any_space, any_space, any_space, any_space, pl.BlockSpec(memory_space=pltpu.VMEM)),
            scratch_shapes=[
                pltpu.VMEM((4, model_dim, hid_dim), BF16),
                pltpu.VMEM((2, n_chunk, chunk, model_dim), BF16),
                pltpu.VMEM((2, n_chunk, chunk, hid_dim), BF16),
                pltpu.VMEM((2, 2, half_pieces, chunk, piece), F32),
                pltpu.VMEM((2, RECV_SLOTS, chunk, piece), F32),
                pltpu.VMEM((8, 128), F32),
                pltpu.VMEM((2, 8, 128), F32),
                dma((PARTS + 1,)),
                dma((n_chunk,)),
                dma,
                dma((2, 2)),
                dma((2, RECV_SLOTS)),
                dma((2, 2)),
                dma((2, n_chunk * half_pieces)),
                dma((2, 2)),
                dma((2, 2)),
                dma((2, (n_chunk + n_fore) * half_pieces)),
                dma((2, 2)),
                dma((4, n_chunk)),
                dma((n_stage * n_model,)),
                dma((2,)),
                pltpu.SemaphoreType.REGULAR((2,)),
                dma((2, 2)),
                dma((2, 2)),
                dma((2, n_relay * half_pieces)),
                dma((n_relay,)),
                pltpu.SemaphoreType.REGULAR((2,)),
                pltpu.SMEM((2 * n_chunk + max(idle) + 2 * MARGIN,), jnp.int32),
            ],
            compiler_params=pltpu.CompilerParams(collective_id=0, has_side_effects=True, vmem_limit_bytes=63 * 1024 * 1024),
            name="stage_kernel",
        )(
            inputs.reshape(n_chunk, chunk, model_dim),
            targets.reshape(n_chunk, chunk, model_dim),
            w_in.reshape(model_dim, hid_dim),
            w_out.reshape(hid_dim, model_dim),
        )

        def over_rows(left, right):
            return lax.dot_general(left, right, (((0,), (0,)), ((), ())), preferred_element_type=F32)

        grad_in = over_rows(layer_in, layer_pre)
        grad_out = over_rows(layer_act, layer_grad)
        return grad_in[None, None], grad_out[None, None], loss[0, :1]

    return jax.shard_map(
        stage_step,
        mesh=mesh,
        in_specs=(P("data", None, None), P("data", None, None), P("stage", None, None, "model"), P("stage", None, "model", None)),
        out_specs=(P(("data", "stage"), None, None, "model"), P(("data", "stage"), None, "model", None), P("data")),
        check_vma=False,
    )
```

```python
import functools

import jax
import jax.numpy as jnp
from jax import lax
from jax.experimental import pallas as pl
from jax.experimental.pallas import tpu as pltpu
from jax.sharding import PartitionSpec as P

GELU_COEF = 0.7978845608028654
CUBIC_COEF = 0.044715

CHUNK_TOKENS = 64
PIECE_COLS = 256
HIDDEN_COLS = 512
PARTS = 2
HOP_LAG = 2
RECV_SLOTS = 8
LAST_LEAD = 5
PREV_LEAD = 16
FIRST_IDLE = 12
NEXT_IDLE = 7
FORE_CHUNKS = 6
RELAY_CHUNKS = 18
RELAY_START = 0

SUM, BACK, GATHER, EARLY, TAKE, FWD, BWD = 256, 512, 1024, 2048, 4096, 8192, 16384
MARGIN = 8

BF16 = jnp.bfloat16
F32 = jnp.float32
MESH = pl.DeviceIdType.MESH


def gelu_tanh(values):
    inner_arg = GELU_COEF * (values + CUBIC_COEF * values * values * values)
    return 0.5 * values * (1.0 + jnp.tanh(inner_arg))


def gelu_slope(values):
    tanh_val = jnp.tanh(GELU_COEF * (values + CUBIC_COEF * values * values * values))
    return 0.5 * (1.0 + tanh_val) + 0.5 * values * (1.0 - tanh_val * tanh_val) * GELU_COEF * (1.0 + 3.0 * CUBIC_COEF * values * values)


def dot_nn(left, right):
    return jnp.dot(left, right, preferred_element_type=F32)


def dot_nt(left, right):
    return lax.dot_general(left, right, (((1,), (1,)), ((), ())), preferred_element_type=F32)


def stage_kernel(
    n_stage, n_model, n_chunk, half_pieces, piece, hop, lead, idle, n_fore, n_relay, grad_scale,
    inputs_hbm, targets_hbm, w1_hbm, w2_hbm,
    x_out, e_out, a_out, g_out, loss_out,
    wts, acts, hid, send_buf, recv_buf, loss_acc, loss_in,
    w_sem, in_sem, tgt_sem, sum_send, sum_recv, gat_send, gat_recv, over_send, back_send, take_recv, down_send, out_sem,
    loss_send, loss_recv, spent_sem, rel_send, rel_over, rel_recv, rel_in, free_sem, table,
):
    pos = lax.axis_index("model")
    stage = lax.axis_index("stage")
    last_pos = n_model - 1
    last_stage = n_stage - 1
    fore_stage = n_stage - 2
    bits = half_pieces.bit_length() - 1
    total = n_chunk * half_pieces
    half = half_pieces * piece
    hid_dim = wts.shape[2]
    chunk_rows = acts.shape[2]
    hid_part = hid_dim // PARTS
    hid_cols = min(HIDDEN_COLS, hid_part)
    n_lead, n_idle = jnp.int32(n_chunk), jnp.int32(0)
    for at in range(n_stage):
        n_lead = jnp.where(stage == at, lead[at], n_lead)
        n_idle = jnp.where(stage == at, idle[at], n_idle)
    turns = 2 * n_chunk + n_idle
    n_steps = turns * half_pieces + jnp.where(stage == 0, 1 - hop, half_pieces + hop * last_pos + 1)
    early = half_pieces + 3 * hop + 1

    barrier = pltpu.get_barrier_semaphore()
    for to_stage in range(n_stage):
        for to_pos in range(n_model):

            @pl.when((to_stage != stage) | (to_pos != pos))
            def _():
                pl.semaphore_signal(barrier, inc=1, device_id={"stage": to_stage, "model": to_pos}, device_id_type=MESH)

    copy_w2 = pltpu.make_async_copy(w2_hbm, wts.at[1], w_sem.at[PARTS])

    def copy_w1(part):
        cols = pl.ds(part * hid_part, hid_part)
        return pltpu.make_async_copy(w1_hbm.at[:, cols], wts.at[0, :, cols], w_sem.at[part])


    def copy_in(chunk):
        return pltpu.make_async_copy(inputs_hbm.at[chunk], acts.at[0, chunk], in_sem.at[chunk])

    def grad_in(chunk):
        return pltpu.make_async_copy(inputs_hbm.at[chunk], acts.at[1, chunk], rel_in.at[chunk])

    def copy_targets(side):
        cols = pl.ds(side * half, half)
        return pltpu.make_async_copy(targets_hbm.at[:, :, cols], acts.at[1, :, :, cols], tgt_sem)

    def copy_out(kind, chunk):
        src, dst = ((acts.at[0], x_out), (acts.at[1], e_out), (hid.at[0], a_out), (hid.at[1], g_out))[kind]
        rows = pl.ds(pl.multiple_of(chunk * chunk_rows, chunk_rows), chunk_rows)
        return pltpu.make_async_copy(src.at[chunk], dst.at[rows, :], out_sem.at[kind, chunk])

    @pl.when(stage == 0)
    def _():
        copy_in(0).start()

    for part in range(PARTS):
        copy_w1(part).start()
    copy_w2.start()

    @pl.when(stage == 0)
    def _():
        def start_in(chunk, carry):
            copy_in(chunk).start()
            return carry

        lax.fori_loop(1, n_chunk, start_in, 0)

    @pl.when((stage == last_stage) & (pos == last_pos))
    def _():
        copy_targets(0).start()

    @pl.when((stage == last_stage) & (pos == 0))
    def _():
        copy_targets(1).start()

    def transpose_weights():
        tile = min(256, hid_dim)
        count = hid_dim // tile

        def one(index, carry):
            rows = pl.ds(pl.multiple_of((index // count) * tile, tile), tile)
            cols = pl.ds(pl.multiple_of((index % count) * tile, tile), tile)
            wts[2, cols, rows] = jnp.swapaxes(wts[1, rows, cols], 0, 1)
            wts[3, cols, rows] = jnp.swapaxes(wts[0, rows, cols], 0, 1)
            return carry

        lax.fori_loop(0, count * count, one, 0)

    n_mixed = 2 * (n_chunk - n_lead)
    n_after = 2 * n_chunk - n_lead
    n_first = n_lead + n_idle

    def fill(entry, carry):
        turn = entry - MARGIN
        after = turn - n_first
        pair = (after + 1024) // 2 - 512
        odd = (after + 1024) % 2 == 1
        mixed = (after >= 0) & (after < n_mixed)
        leads = (turn >= 0) & (turn < n_lead)
        fwd = leads | (mixed & odd)
        bwd = (after >= 0) & (after < n_after) & jnp.logical_not(mixed & odd)
        chunk = jnp.where(leads, turn, jnp.where(odd, n_lead + pair, pair))
        chunk = jnp.where(bwd & (after >= n_mixed), after - (n_chunk - n_lead), chunk)
        early_one = fwd & (stage == fore_stage - 1) & (chunk < n_fore)
        back = bwd & (stage < last_stage) & ((stage < fore_stage) | (chunk >= n_relay))
        take = back | (fwd & (stage == fore_stage) & (chunk < n_fore))
        word = jnp.int32(0)
        for flag, bit in (
            (fwd | (bwd & (stage > 0)), SUM),
            (bwd, BACK),
            (fwd & jnp.logical_not(early_one), GATHER),
            (early_one, EARLY),
            (take, TAKE),
            (fwd, FWD),
            (bwd, BWD),
        ):
            word = word + jnp.where(flag, bit, 0)
        table[entry] = word
        return carry

    lax.fori_loop(0, table.shape[0], fill, 0)
    loss_acc[...] = jnp.zeros_like(loss_acc)
    copy_w1(0).wait()

    @pl.when(stage > 0)
    def _():
        for part in range(1, PARTS):
            copy_w1(part).wait()
        copy_w2.wait()
        transpose_weights()

    def meet():
        pl.semaphore_wait(barrier, n_stage * n_model - 1)

    @pl.when(stage == fore_stage)
    def _():
        meet()


    def turn_of(place):
        return lax.shift_right_logical(place + MARGIN * half_pieces, jnp.int32(bits))

    def piece_of(place):
        return lax.bitwise_and(place + MARGIN * half_pieces, jnp.int32(half_pieces - 1))

    def has(word, mask):
        return lax.bitwise_and(word, jnp.int32(mask)) != 0

    def fwd_chunk(turn):
        after = turn - (n_first + MARGIN)
        return jnp.where(turn < n_lead + MARGIN, turn - MARGIN, n_lead + lax.shift_right_arithmetic(after, jnp.int32(1)))

    def bwd_chunk(turn):
        after = turn - (n_first + MARGIN)
        return jnp.where(after < n_mixed, lax.shift_right_arithmetic(after, jnp.int32(1)), after - (n_chunk - n_lead))

    def back_of(turn):
        after = turn - (n_first + MARGIN)
        odd = lax.bitwise_and(after, jnp.int32(1)) == 1
        return ((after >= 0) & jnp.logical_not((after < n_mixed) & odd)).astype(jnp.int32)

    def chunk_of(turn, is_back):
        return jnp.clip(jnp.where(is_back == 1, bwd_chunk(turn), fwd_chunk(turn)), 0, n_chunk - 1)

    def piece_at(side, index):
        col = side * half + index * piece
        return pl.ds(pl.multiple_of(col, piece), piece)

    def remote(src, dst, send_sem, recv_sem, device):
        return pltpu.make_async_remote_copy(
            src_ref=src, dst_ref=dst, send_sem=send_sem, recv_sem=recv_sem, device_id=device, device_id_type=MESH
        )

    def left(send_sem, like):
        remote(like, like, send_sem, loss_recv.at[0], {"model": pos}).wait_send()

    turn_pieces = acts.at[0, 0, :, pl.ds(0, half)]
    turn_sums = send_buf.at[0, 0]

    def rank_of(side):
        return pos if side == 0 else last_pos - pos

    def up(side):
        return {"model": pos + 1 if side == 0 else pos - 1}

    def down(side):
        return {"model": pos - 1 if side == 0 else pos + 1}

    def first_product(step, part):
        place = step + PARTS - 1 - part
        turn = turn_of(place)
        word = table[turn]
        starts = piece_of(place) == 0

        @pl.when(starts & has(word, FWD))
        def _():
            chunk = fwd_chunk(turn)
            if part == 0:

                @pl.when((stage != fore_stage) | (chunk >= n_fore))
                def _():
                    copy_in(chunk).wait()

                copy_out(0, chunk).start()
            else:

                @pl.when((stage == 0) & (place == 0))
                def _():
                    copy_w1(part).wait()

            for col in range(part * hid_part, (part + 1) * hid_part, hid_cols):
                cols = pl.ds(col, hid_cols)
                pre = dot_nn(acts[0, chunk], wts[0, :, cols]).astype(BF16)
                hid[1, chunk, :, cols] = pre
                hid[0, chunk, :, cols] = gelu_tanh(pre.astype(F32)).astype(BF16)
            if part == PARTS - 1:
                copy_out(2, chunk).start()

                @pl.when((stage == 0) & (place == 0))
                def _():
                    copy_w2.wait()

        @pl.when(starts & has(word, BWD))
        def _():
            chunk = bwd_chunk(turn)
            if part == 0:

                @pl.when((stage == fore_stage) & (chunk < n_relay))
                def _():
                    grad_in(chunk).wait()

                copy_out(1, chunk).start()
                copy_out(0, chunk).wait()
            for col in range(part * hid_part, (part + 1) * hid_part, hid_cols):
                cols = pl.ds(col, hid_cols)
                grad_act = dot_nn(acts[1, chunk], wts[2, :, cols]).astype(BF16)
                slope = gelu_slope(hid[1, chunk, :, cols].astype(F32))
                hid[1, chunk, :, cols] = (slope * grad_act.astype(F32)).astype(BF16)
            if part == PARTS - 1:
                copy_out(3, chunk).start()

        if part == 0:

            @pl.when((stage == 0) & (place == n_lead * half_pieces))
            def _():
                transpose_weights()

    def loss_copy(side, to_stage, to_pos):
        return remote(
            loss_acc, loss_in.at[side], loss_send.at[to_stage * n_model + to_pos], loss_recv.at[side],
            {"stage": to_stage, "model": to_pos},
        )

    def send_loss(side):
        loss_in[side] = loss_acc[...]
        for to_stage in range(n_stage):
            for to_pos in range(n_model):

                @pl.when((to_stage != stage) | (to_pos != pos))
                def _():
                    loss_copy(side, to_stage, to_pos).start()

    def sum_steps(step):
        now = []
        for side in (0, 1):
            rank = rank_of(side)
            place = step - hop * rank
            turn = turn_of(place)
            word, old = table[turn], table[turn - 2]
            index = piece_of(place)
            half_turn = lax.bitwise_and(turn, jnp.int32(1))
            inn = lax.bitwise_and(place + MARGIN * half_pieces, jnp.int32(RECV_SLOTS - 1))
            sums = has(word, SUM)
            is_back = back_of(turn)
            now.append((rank, word, sums, is_back, chunk_of(turn, is_back), index, half_turn, inn, piece_at(side, index)))

            @pl.when((index == 0) & has(old, SUM))
            def _():
                @pl.when(rank < last_pos)
                def _():
                    left(sum_send.at[side, half_turn], turn_sums)

                @pl.when((rank == last_pos) & has(old, BACK))
                def _():
                    left(down_send.at[side, half_turn], turn_pieces)

        @pl.when(now[0][2] | now[1][2])
        def _():
            for side in (0, 1):
                _, _, _, is_back, chunk, index, half_turn, _, cols = now[side]
                send_buf[side, half_turn, index] = dot_nn(hid[is_back, chunk], wts[1 + 2 * is_back, :, cols])

        for side in (0, 1):
            rank, word, sums, is_back, chunk, out, half_turn, inn, cols = now[side]
            bwd = has(word, BACK)
            index = chunk * half_pieces + out
            mine = send_buf.at[side, half_turn, out]
            gone = down_send.at[side, half_turn]
            hand_on = remote(mine, recv_buf.at[side, inn], sum_send.at[side, half_turn], sum_recv.at[side, inn], up(side))

            @pl.when(sums & (rank > 0))
            def _():
                hand_on.wait_recv()
                mine[...] = mine[...] + recv_buf[side, inn]

            @pl.when(sums & (rank < last_pos))
            def _():
                hand_on.start()

            @pl.when(sums & (rank == last_pos))
            def _():
                whole = acts[is_back, chunk, :, cols].astype(F32) + mine[...]
                scored = has(word, FWD) & (stage == last_stage)

                @pl.when(scored)
                def _():
                    @pl.when(index == 0)
                    def _():
                        copy_targets(side).wait()

                    err = whole.astype(BF16).astype(F32) - acts[1, chunk, :, cols].astype(F32)
                    acts[1, chunk, :, cols] = (err * grad_scale).astype(BF16)
                    square = jnp.sum((err * err).reshape(err.shape[0] // 8, 8, piece), axis=0)
                    part = square[:, :128]
                    for lane in range(1, piece // 128):
                        part = part + square[:, lane * 128 : (lane + 1) * 128]
                    loss_acc[...] = loss_acc[...] + part

                    @pl.when(index == total - 1)
                    def _():
                        send_loss(side)

                @pl.when(jnp.logical_not(scored))
                def _():
                    acts[1 - is_back, chunk, :, cols] = whole.astype(BF16)

                @pl.when(bwd & (index == total - 2 * half_pieces))
                def _():
                    pl.semaphore_wait(spent_sem.at[side], 1)

                @pl.when(bwd & (stage == 1) & (index == (n_relay - 2) * half_pieces))
                def _():
                    pl.semaphore_wait(free_sem.at[side], 1)

                relayed = (stage == last_stage) & (chunk < n_relay)
                there = acts.at[1, chunk, :, cols]

                @pl.when(bwd & relayed)
                def _():
                    arrived = rel_recv.at[side, jnp.minimum(index, n_relay * half_pieces - 1)]
                    remote(acts.at[0, chunk, :, cols], there, gone, arrived, {"stage": 0}).start()

                @pl.when(bwd & jnp.logical_not(relayed))
                def _():
                    arrived = take_recv.at[side, index]
                    remote(acts.at[0, chunk, :, cols], there, gone, arrived, {"stage": stage - 1}).start()

    def gather_step(side, step):
        rank = rank_of(side)
        place = step - 1 - 3 * hop - hop * (last_pos - rank)
        turn = turn_of(place)
        word, old = table[turn], table[turn - 2]
        out = piece_of(place)
        half_turn = lax.bitwise_and(turn, jnp.int32(1))
        chunk = jnp.clip(fwd_chunk(turn), 0, n_chunk - 1)
        index = chunk * half_pieces + out
        cols = piece_at(side, out)
        here = acts.at[1, chunk, :, cols]
        gone = over_send.at[side, half_turn]

        @pl.when((out == 0) & has(old, GATHER | EARLY))
        def _():
            @pl.when(has(old, GATHER) & (rank > 0))
            def _():
                left(gat_send.at[side, half_turn], turn_pieces)

            @pl.when((stage < last_stage) & (has(old, GATHER) | (rank == last_pos)))
            def _():
                left(gone, turn_pieces)

                @pl.when((fwd_chunk(turn - 2) == n_chunk - 1) & (rank == last_pos))
                def _():
                    pl.semaphore_signal(spent_sem.at[side], inc=1, device_id={"stage": stage + 1}, device_id_type=MESH)

        @pl.when(has(word, GATHER))
        def _():
            hand_on = remote(here, here, gat_send.at[side, half_turn], gat_recv.at[side, index], down(side))

            @pl.when(rank < last_pos)
            def _():
                hand_on.wait_recv()

            @pl.when(rank > 0)
            def _():
                hand_on.start()

            @pl.when(stage < last_stage)
            def _():
                remote(here, acts.at[0, chunk, :, cols], gone, in_sem.at[chunk], {"stage": stage + 1}).start()

        @pl.when(has(word, EARLY) & (rank == last_pos))
        def _():
            arrived = take_recv.at[side, jnp.minimum(total + index, total + n_fore * half_pieces - 1)]
            remote(here, acts.at[0, chunk, :, cols], gone, arrived, {"stage": stage + 1}).start()

    def take_step(side, step):
        rank = rank_of(side)
        place = step + early - hop * (last_pos - rank)
        turn = turn_of(place)
        word, old = table[turn], table[turn - 2]
        out = piece_of(place)
        gone = back_send.at[side, lax.bitwise_and(turn, jnp.int32(1))]

        @pl.when((out == 0) & has(old, TAKE) & (rank > 0))
        def _():
            left(gone, turn_pieces)

        @pl.when(has(word, TAKE))
        def _():
            is_back = back_of(turn)
            chunk = chunk_of(turn, is_back)
            index = chunk * half_pieces + out + (1 - is_back) * total
            here = acts.at[is_back, chunk, :, piece_at(side, out)]
            hand_on = remote(here, here, gone, take_recv.at[side, index], down(side))
            hand_on.wait_recv()

            @pl.when(rank > 0)
            def _():
                hand_on.start()

    def relay_step(side, step):
        rank = rank_of(side)
        place = step - (n_chunk + RELAY_START) * half_pieces - hop * (last_pos - rank)
        turn = turn_of(place) - MARGIN
        out = piece_of(place)
        half_turn = lax.bitwise_and(turn, jnp.int32(1))
        chunk = jnp.clip(turn, 0, n_relay - 1)
        here = acts.at[1, chunk, :, piece_at(side, out)]
        gone = rel_over.at[side, half_turn]
        hand_on = remote(here, here, rel_send.at[side, half_turn], rel_recv.at[side, chunk * half_pieces + out], down(side))

        @pl.when((out == 0) & (turn >= 2) & (turn < n_relay + 2))
        def _():
            @pl.when(rank > 0)
            def _():
                left(rel_send.at[side, half_turn], turn_pieces)

            left(gone, turn_pieces)

            @pl.when((turn == n_relay + 1) & (rank == last_pos))
            def _():
                pl.semaphore_signal(free_sem.at[side], inc=1, device_id={"stage": 1}, device_id_type=MESH)

        @pl.when((turn >= 0) & (turn < n_relay))
        def _():
            hand_on.wait_recv()

            @pl.when(rank > 0)
            def _():
                hand_on.start()

            remote(here, here, gone, rel_in.at[chunk], {"stage": fore_stage}).start()

    def loop_step(step, carry):
        for part in range(PARTS):
            first_product(step, part)

        @pl.when((step == 0) & (stage != fore_stage))
        def _():
            meet()

        gather_step(0, step)
        gather_step(1, step)
        sum_steps(step)

        @pl.when((stage == 0) & (step >= n_chunk * half_pieces))
        def _():
            relay_step(0, step)
            relay_step(1, step)

        take_step(0, step)
        take_step(1, step)
        return carry

    lax.fori_loop(jnp.where(stage == fore_stage, -early, 1 - PARTS), n_steps, loop_step, 0)

    for side, owner in ((0, last_pos), (1, 0)):
        owns = (stage == last_stage) & (pos == owner)

        @pl.when(jnp.logical_not(owns))
        def _():
            loss_copy(side, 0, 0).wait_recv()

        @pl.when(owns)
        def _():
            for to_stage in range(n_stage):
                for to_pos in range(n_model):

                    @pl.when((to_stage != stage) | (to_pos != pos))
                    def _():
                        loss_copy(side, to_stage, to_pos).wait_send()

    loss_out[...] = jnp.full(loss_out.shape, jnp.sum(loss_in[0] + loss_in[1]) * (0.5 * grad_scale), F32)

    def end_out(chunk, carry):
        for kind in (1, 2, 3):
            copy_out(kind, chunk).wait()
        return carry

    lax.fori_loop(0, n_chunk, end_out, 0)


def solution(mesh):
    n_stage = mesh.shape["stage"]
    n_model = mesh.shape["model"]

    def stage_step(inputs, targets, w_in, w_out):
        num_micro, num_tokens, model_dim = inputs.shape
        hid_dim = w_in.shape[3]
        rows = num_micro * num_tokens
        chunk = min(CHUNK_TOKENS, num_tokens)
        n_chunk = rows // chunk
        piece = min(PIECE_COLS, model_dim // 2)
        half_pieces = model_dim // 2 // piece
        grad_scale = 1.0 / (rows * model_dim)
        lead = [n_chunk] * (n_stage - 2) + [min(PREV_LEAD, n_chunk), min(LAST_LEAD, n_chunk)]
        idle = [FIRST_IDLE] + [NEXT_IDLE] * (n_stage - 3) + [0, 0]
        n_fore, n_relay = min(FORE_CHUNKS, n_chunk - 1), min(RELAY_CHUNKS, n_chunk - 1)
        kernel = functools.partial(
            stage_kernel, n_stage, n_model, n_chunk, half_pieces, piece, HOP_LAG, lead, idle, n_fore, n_relay, grad_scale
        )
        any_space = pl.BlockSpec(memory_space=pl.ANY)
        dma = pltpu.SemaphoreType.DMA
        layer_in, layer_grad, layer_act, layer_pre, loss = pl.pallas_call(
            kernel,
            out_shape=(
                jax.ShapeDtypeStruct((rows, model_dim), BF16),
                jax.ShapeDtypeStruct((rows, model_dim), BF16),
                jax.ShapeDtypeStruct((rows, hid_dim), BF16),
                jax.ShapeDtypeStruct((rows, hid_dim), BF16),
                jax.ShapeDtypeStruct((8, 128), F32),
            ),
            in_specs=[any_space] * 4,
            out_specs=(any_space, any_space, any_space, any_space, pl.BlockSpec(memory_space=pltpu.VMEM)),
            scratch_shapes=[
                pltpu.VMEM((4, model_dim, hid_dim), BF16),
                pltpu.VMEM((2, n_chunk, chunk, model_dim), BF16),
                pltpu.VMEM((2, n_chunk, chunk, hid_dim), BF16),
                pltpu.VMEM((2, 2, half_pieces, chunk, piece), F32),
                pltpu.VMEM((2, RECV_SLOTS, chunk, piece), F32),
                pltpu.VMEM((8, 128), F32),
                pltpu.VMEM((2, 8, 128), F32),
                dma((PARTS + 1,)),
                dma((n_chunk,)),
                dma,
                dma((2, 2)),
                dma((2, RECV_SLOTS)),
                dma((2, 2)),
                dma((2, n_chunk * half_pieces)),
                dma((2, 2)),
                dma((2, 2)),
                dma((2, (n_chunk + n_fore) * half_pieces)),
                dma((2, 2)),
                dma((4, n_chunk)),
                dma((n_stage * n_model,)),
                dma((2,)),
                pltpu.SemaphoreType.REGULAR((2,)),
                dma((2, 2)),
                dma((2, 2)),
                dma((2, n_relay * half_pieces)),
                dma((n_relay,)),
                pltpu.SemaphoreType.REGULAR((2,)),
                pltpu.SMEM((2 * n_chunk + max(idle) + 2 * MARGIN,), jnp.int32),
            ],
            compiler_params=pltpu.CompilerParams(collective_id=0, has_side_effects=True, vmem_limit_bytes=63 * 1024 * 1024),
            name="stage_kernel",
        )(
            inputs.reshape(n_chunk, chunk, model_dim),
            targets.reshape(n_chunk, chunk, model_dim),
            w_in.reshape(model_dim, hid_dim),
            w_out.reshape(hid_dim, model_dim),
        )

        def over_rows(left, right):
            return lax.dot_general(left, right, (((0,), (0,)), ((), ())), preferred_element_type=F32)

        grad_in = over_rows(layer_in, layer_pre)
        grad_out = over_rows(layer_act, layer_grad)
        return grad_in[None, None], grad_out[None, None], loss[0, :1]

    return jax.shard_map(
        stage_step,
        mesh=mesh,
        in_specs=(P("data", None, None), P("data", None, None), P("stage", None, None, "model"), P("stage", None, "model", None)),
        out_specs=(P(("data", "stage"), None, None, "model"), P(("data", "stage"), None, "model", None), P("data")),
        check_vma=False,
    )
```

```python
import functools

import jax
import jax.numpy as jnp
from jax import lax
from jax.experimental import pallas as pl
from jax.experimental.pallas import tpu as pltpu
from jax.sharding import PartitionSpec as P

GELU_COEF = 0.7978845608028654
CUBIC_COEF = 0.044715

CHUNK_TOKENS = 64
PIECE_COLS = 256
HIDDEN_COLS = 512
PARTS = 2
HOP_LAG = 2
RECV_SLOTS = 8
LAST_LEAD = 5
PREV_LEAD = 16
FIRST_IDLE = 12
NEXT_IDLE = 7
FORE_CHUNKS = 6
RELAY_CHUNKS = 18
RELAY_START = 0

FIRST_GRADS = 12
TILE_ROWS = 256
TILE_COLS = 1024
TILE_STEPS = 2

SUM, BACK, GATHER, EARLY, TAKE, FWD, BWD = 256, 512, 1024, 2048, 4096, 8192, 16384
MARGIN = 8

BF16 = jnp.bfloat16
F32 = jnp.float32
MESH = pl.DeviceIdType.MESH


def gelu_tanh(values):
    inner_arg = GELU_COEF * (values + CUBIC_COEF * values * values * values)
    return 0.5 * values * (1.0 + jnp.tanh(inner_arg))


def gelu_slope(values):
    tanh_val = jnp.tanh(GELU_COEF * (values + CUBIC_COEF * values * values * values))
    return 0.5 * (1.0 + tanh_val) + 0.5 * values * (1.0 - tanh_val * tanh_val) * GELU_COEF * (1.0 + 3.0 * CUBIC_COEF * values * values)


def dot_nn(left, right):
    return jnp.dot(left, right, preferred_element_type=F32)


def dot_nt(left, right):
    return lax.dot_general(left, right, (((1,), (1,)), ((), ())), preferred_element_type=F32)


def stage_kernel(
    n_stage, n_model, n_chunk, half_pieces, piece, hop, lead, idle, n_fore, n_relay, n_grad, grad_scale,
    inputs_hbm, targets_hbm, w1_hbm, w2_hbm,
    x_out, e_out, a_out, g_out, grad_hbm, loss_out,
    wts, acts, hid, send_buf, recv_buf, loss_acc, loss_in,
    w_sem, in_sem, tgt_sem, sum_send, sum_recv, gat_send, gat_recv, over_send, back_send, take_recv, down_send, out_sem,
    loss_send, loss_recv, spent_sem, rel_send, rel_over, rel_recv, rel_in, free_sem, table, tile_buf, tile_sem,
):
    pos = lax.axis_index("model")
    stage = lax.axis_index("stage")
    last_pos = n_model - 1
    last_stage = n_stage - 1
    fore_stage = n_stage - 2
    bits = half_pieces.bit_length() - 1
    total = n_chunk * half_pieces
    half = half_pieces * piece
    hid_dim = wts.shape[2]
    chunk_rows = acts.shape[2]
    hid_part = hid_dim // PARTS
    hid_cols = min(HIDDEN_COLS, hid_part)
    n_lead, n_idle = jnp.int32(n_chunk), jnp.int32(0)
    for at in range(n_stage):
        n_lead = jnp.where(stage == at, lead[at], n_lead)
        n_idle = jnp.where(stage == at, idle[at], n_idle)
    turns = 2 * n_chunk + n_idle
    n_steps = turns * half_pieces + jnp.where(stage == 0, 1 - hop, half_pieces + hop * last_pos + 1)
    early = half_pieces + 3 * hop + 1

    barrier = pltpu.get_barrier_semaphore()
    for to_stage in range(n_stage):
        for to_pos in range(n_model):

            @pl.when((to_stage != stage) | (to_pos != pos))
            def _():
                pl.semaphore_signal(barrier, inc=1, device_id={"stage": to_stage, "model": to_pos}, device_id_type=MESH)

    copy_w2 = pltpu.make_async_copy(w2_hbm, wts.at[1], w_sem.at[PARTS])

    def copy_w1(part):
        cols = pl.ds(part * hid_part, hid_part)
        return pltpu.make_async_copy(w1_hbm.at[:, cols], wts.at[0, :, cols], w_sem.at[part])


    def copy_in(chunk):
        return pltpu.make_async_copy(inputs_hbm.at[chunk], acts.at[0, chunk], in_sem.at[chunk])

    def grad_in(chunk):
        return pltpu.make_async_copy(inputs_hbm.at[chunk], acts.at[1, chunk], rel_in.at[chunk])

    def copy_targets(side):
        cols = pl.ds(side * half, half)
        return pltpu.make_async_copy(targets_hbm.at[:, :, cols], acts.at[1, :, :, cols], tgt_sem)

    def copy_out(kind, chunk):
        src, dst = ((acts.at[0], x_out), (acts.at[1], e_out), (hid.at[0], a_out), (hid.at[1], g_out))[kind]
        first = n_grad if kind in (1, 2) else 0
        rows = pl.ds(pl.multiple_of((chunk - first) * chunk_rows, chunk_rows), chunk_rows)
        return pltpu.make_async_copy(src.at[chunk], dst.at[rows, :], out_sem.at[kind, chunk])

    @pl.when(stage == 0)
    def _():
        copy_in(0).start()

    for part in range(PARTS):
        copy_w1(part).start()
    copy_w2.start()

    @pl.when(stage == 0)
    def _():
        def start_in(chunk, carry):
            copy_in(chunk).start()
            return carry

        lax.fori_loop(1, n_chunk, start_in, 0)

    @pl.when((stage == last_stage) & (pos == last_pos))
    def _():
        copy_targets(0).start()

    @pl.when((stage == last_stage) & (pos == 0))
    def _():
        copy_targets(1).start()

    def transpose_weights():
        tile = min(256, hid_dim)
        count = hid_dim // tile

        def one(index, carry):
            rows = pl.ds(pl.multiple_of((index // count) * tile, tile), tile)
            cols = pl.ds(pl.multiple_of((index % count) * tile, tile), tile)
            wts[2, cols, rows] = jnp.swapaxes(wts[1, rows, cols], 0, 1)
            wts[3, cols, rows] = jnp.swapaxes(wts[0, rows, cols], 0, 1)
            return carry

        lax.fori_loop(0, count * count, one, 0)

    n_mixed = 2 * (n_chunk - n_lead)
    n_after = 2 * n_chunk - n_lead
    n_first = n_lead + n_idle

    def fill(entry, carry):
        turn = entry - MARGIN
        after = turn - n_first
        pair = (after + 1024) // 2 - 512
        odd = (after + 1024) % 2 == 1
        mixed = (after >= 0) & (after < n_mixed)
        leads = (turn >= 0) & (turn < n_lead)
        fwd = leads | (mixed & odd)
        bwd = (after >= 0) & (after < n_after) & jnp.logical_not(mixed & odd)
        chunk = jnp.where(leads, turn, jnp.where(odd, n_lead + pair, pair))
        chunk = jnp.where(bwd & (after >= n_mixed), after - (n_chunk - n_lead), chunk)
        early_one = fwd & (stage == fore_stage - 1) & (chunk < n_fore)
        back = bwd & (stage < last_stage) & ((stage < fore_stage) | (chunk >= n_relay))
        take = back | (fwd & (stage == fore_stage) & (chunk < n_fore))
        word = jnp.int32(0)
        for flag, bit in (
            (fwd | (bwd & (stage > 0)), SUM),
            (bwd, BACK),
            (fwd & jnp.logical_not(early_one), GATHER),
            (early_one, EARLY),
            (take, TAKE),
            (fwd, FWD),
            (bwd, BWD),
        ):
            word = word + jnp.where(flag, bit, 0)
        table[entry] = word
        return carry

    lax.fori_loop(0, table.shape[0], fill, 0)
    loss_acc[...] = jnp.zeros_like(loss_acc)
    copy_w1(0).wait()

    @pl.when(stage > 0)
    def _():
        for part in range(1, PARTS):
            copy_w1(part).wait()
        copy_w2.wait()
        transpose_weights()

    def meet():
        pl.semaphore_wait(barrier, n_stage * n_model - 1)

    @pl.when(stage == fore_stage)
    def _():
        meet()


    def turn_of(place):
        return lax.shift_right_logical(place + MARGIN * half_pieces, jnp.int32(bits))

    def piece_of(place):
        return lax.bitwise_and(place + MARGIN * half_pieces, jnp.int32(half_pieces - 1))

    def has(word, mask):
        return lax.bitwise_and(word, jnp.int32(mask)) != 0

    def fwd_chunk(turn):
        after = turn - (n_first + MARGIN)
        return jnp.where(turn < n_lead + MARGIN, turn - MARGIN, n_lead + lax.shift_right_arithmetic(after, jnp.int32(1)))

    def bwd_chunk(turn):
        after = turn - (n_first + MARGIN)
        return jnp.where(after < n_mixed, lax.shift_right_arithmetic(after, jnp.int32(1)), after - (n_chunk - n_lead))

    def back_of(turn):
        after = turn - (n_first + MARGIN)
        odd = lax.bitwise_and(after, jnp.int32(1)) == 1
        return ((after >= 0) & jnp.logical_not((after < n_mixed) & odd)).astype(jnp.int32)

    def chunk_of(turn, is_back):
        return jnp.clip(jnp.where(is_back == 1, bwd_chunk(turn), fwd_chunk(turn)), 0, n_chunk - 1)

    def piece_at(side, index):
        col = side * half + index * piece
        return pl.ds(pl.multiple_of(col, piece), piece)

    def remote(src, dst, send_sem, recv_sem, device):
        return pltpu.make_async_remote_copy(
            src_ref=src, dst_ref=dst, send_sem=send_sem, recv_sem=recv_sem, device_id=device, device_id_type=MESH
        )

    def left(send_sem, like):
        remote(like, like, send_sem, loss_recv.at[0], {"model": pos}).wait_send()

    turn_pieces = acts.at[0, 0, :, pl.ds(0, half)]
    turn_sums = send_buf.at[0, 0]

    def rank_of(side):
        return pos if side == 0 else last_pos - pos

    def up(side):
        return {"model": pos + 1 if side == 0 else pos - 1}

    def down(side):
        return {"model": pos - 1 if side == 0 else pos + 1}

    def first_product(step, part):
        place = step + PARTS - 1 - part
        turn = turn_of(place)
        word = table[turn]
        starts = piece_of(place) == 0

        @pl.when(starts & has(word, FWD))
        def _():
            chunk = fwd_chunk(turn)
            if part == 0:

                @pl.when((stage != fore_stage) | (chunk >= n_fore))
                def _():
                    copy_in(chunk).wait()

                copy_out(0, chunk).start()
            else:

                @pl.when((stage == 0) & (place == 0))
                def _():
                    copy_w1(part).wait()

            for col in range(part * hid_part, (part + 1) * hid_part, hid_cols):
                cols = pl.ds(col, hid_cols)
                pre = dot_nn(acts[0, chunk], wts[0, :, cols]).astype(BF16)
                hid[1, chunk, :, cols] = pre
                hid[0, chunk, :, cols] = gelu_tanh(pre.astype(F32)).astype(BF16)
            if part == PARTS - 1:

                @pl.when(chunk >= n_grad)
                def _():
                    copy_out(2, chunk).start()

                @pl.when((stage == 0) & (place == 0))
                def _():
                    copy_w2.wait()

        @pl.when(starts & has(word, BWD))
        def _():
            chunk = bwd_chunk(turn)
            if part == 0:

                @pl.when((stage == fore_stage) & (chunk < n_relay))
                def _():
                    grad_in(chunk).wait()

                @pl.when(chunk >= n_grad)
                def _():
                    copy_out(1, chunk).start()

                copy_out(0, chunk).wait()
            for col in range(part * hid_part, (part + 1) * hid_part, hid_cols):
                cols = pl.ds(col, hid_cols)
                grad_act = dot_nn(acts[1, chunk], wts[2, :, cols]).astype(BF16)
                slope = gelu_slope(hid[1, chunk, :, cols].astype(F32))
                hid[1, chunk, :, cols] = (slope * grad_act.astype(F32)).astype(BF16)
            if part == PARTS - 1:
                copy_out(3, chunk).start()

        if part == 0:

            @pl.when((stage == 0) & (place == n_lead * half_pieces))
            def _():
                transpose_weights()

    def loss_copy(side, to_stage, to_pos):
        return remote(
            loss_acc, loss_in.at[side], loss_send.at[to_stage * n_model + to_pos], loss_recv.at[side],
            {"stage": to_stage, "model": to_pos},
        )

    def send_loss(side):
        loss_in[side] = loss_acc[...]
        for to_stage in range(n_stage):
            for to_pos in range(n_model):

                @pl.when((to_stage != stage) | (to_pos != pos))
                def _():
                    loss_copy(side, to_stage, to_pos).start()

    def sum_steps(step):
        now = []
        for side in (0, 1):
            rank = rank_of(side)
            place = step - hop * rank
            turn = turn_of(place)
            word, old = table[turn], table[turn - 2]
            index = piece_of(place)
            half_turn = lax.bitwise_and(turn, jnp.int32(1))
            inn = lax.bitwise_and(place + MARGIN * half_pieces, jnp.int32(RECV_SLOTS - 1))
            sums = has(word, SUM)
            is_back = back_of(turn)
            now.append((rank, word, sums, is_back, chunk_of(turn, is_back), index, half_turn, inn, piece_at(side, index)))

            @pl.when((index == 0) & has(old, SUM))
            def _():
                @pl.when(rank < last_pos)
                def _():
                    left(sum_send.at[side, half_turn], turn_sums)

                @pl.when((rank == last_pos) & has(old, BACK))
                def _():
                    left(down_send.at[side, half_turn], turn_pieces)

        @pl.when(now[0][2] | now[1][2])
        def _():
            for side in (0, 1):
                _, _, _, is_back, chunk, index, half_turn, _, cols = now[side]
                send_buf[side, half_turn, index] = dot_nn(hid[is_back, chunk], wts[1 + 2 * is_back, :, cols])

        for side in (0, 1):
            rank, word, sums, is_back, chunk, out, half_turn, inn, cols = now[side]
            bwd = has(word, BACK)
            index = chunk * half_pieces + out
            mine = send_buf.at[side, half_turn, out]
            gone = down_send.at[side, half_turn]
            hand_on = remote(mine, recv_buf.at[side, inn], sum_send.at[side, half_turn], sum_recv.at[side, inn], up(side))

            @pl.when(sums & (rank > 0))
            def _():
                hand_on.wait_recv()
                mine[...] = mine[...] + recv_buf[side, inn]

            @pl.when(sums & (rank < last_pos))
            def _():
                hand_on.start()

            @pl.when(sums & (rank == last_pos))
            def _():
                whole = acts[is_back, chunk, :, cols].astype(F32) + mine[...]
                scored = has(word, FWD) & (stage == last_stage)

                @pl.when(scored)
                def _():
                    @pl.when(index == 0)
                    def _():
                        copy_targets(side).wait()

                    err = whole.astype(BF16).astype(F32) - acts[1, chunk, :, cols].astype(F32)
                    acts[1, chunk, :, cols] = (err * grad_scale).astype(BF16)
                    square = jnp.sum((err * err).reshape(err.shape[0] // 8, 8, piece), axis=0)
                    part = square[:, :128]
                    for lane in range(1, piece // 128):
                        part = part + square[:, lane * 128 : (lane + 1) * 128]
                    loss_acc[...] = loss_acc[...] + part

                    @pl.when(index == total - 1)
                    def _():
                        send_loss(side)

                @pl.when(jnp.logical_not(scored))
                def _():
                    acts[1 - is_back, chunk, :, cols] = whole.astype(BF16)

                @pl.when(bwd & (index == total - 2 * half_pieces))
                def _():
                    pl.semaphore_wait(spent_sem.at[side], 1)

                @pl.when(bwd & (stage == 1) & (index == (n_relay - 2) * half_pieces))
                def _():
                    pl.semaphore_wait(free_sem.at[side], 1)

                relayed = (stage == last_stage) & (chunk < n_relay)
                there = acts.at[1, chunk, :, cols]

                @pl.when(bwd & relayed)
                def _():
                    arrived = rel_recv.at[side, jnp.minimum(index, n_relay * half_pieces - 1)]
                    remote(acts.at[0, chunk, :, cols], there, gone, arrived, {"stage": 0}).start()

                @pl.when(bwd & jnp.logical_not(relayed))
                def _():
                    arrived = take_recv.at[side, index]
                    remote(acts.at[0, chunk, :, cols], there, gone, arrived, {"stage": stage - 1}).start()

    def gather_step(side, step):
        rank = rank_of(side)
        place = step - 1 - 3 * hop - hop * (last_pos - rank)
        turn = turn_of(place)
        word, old = table[turn], table[turn - 2]
        out = piece_of(place)
        half_turn = lax.bitwise_and(turn, jnp.int32(1))
        chunk = jnp.clip(fwd_chunk(turn), 0, n_chunk - 1)
        index = chunk * half_pieces + out
        cols = piece_at(side, out)
        here = acts.at[1, chunk, :, cols]
        gone = over_send.at[side, half_turn]

        @pl.when((out == 0) & has(old, GATHER | EARLY))
        def _():
            @pl.when(has(old, GATHER) & (rank > 0))
            def _():
                left(gat_send.at[side, half_turn], turn_pieces)

            @pl.when((stage < last_stage) & (has(old, GATHER) | (rank == last_pos)))
            def _():
                left(gone, turn_pieces)

                @pl.when((fwd_chunk(turn - 2) == n_chunk - 1) & (rank == last_pos))
                def _():
                    pl.semaphore_signal(spent_sem.at[side], inc=1, device_id={"stage": stage + 1}, device_id_type=MESH)

        @pl.when(has(word, GATHER))
        def _():
            hand_on = remote(here, here, gat_send.at[side, half_turn], gat_recv.at[side, index], down(side))

            @pl.when(rank < last_pos)
            def _():
                hand_on.wait_recv()

            @pl.when(rank > 0)
            def _():
                hand_on.start()

            @pl.when(stage < last_stage)
            def _():
                remote(here, acts.at[0, chunk, :, cols], gone, in_sem.at[chunk], {"stage": stage + 1}).start()

        @pl.when(has(word, EARLY) & (rank == last_pos))
        def _():
            arrived = take_recv.at[side, jnp.minimum(total + index, total + n_fore * half_pieces - 1)]
            remote(here, acts.at[0, chunk, :, cols], gone, arrived, {"stage": stage + 1}).start()

    def take_step(side, step):
        rank = rank_of(side)
        place = step + early - hop * (last_pos - rank)
        turn = turn_of(place)
        word, old = table[turn], table[turn - 2]
        out = piece_of(place)
        gone = back_send.at[side, lax.bitwise_and(turn, jnp.int32(1))]

        @pl.when((out == 0) & has(old, TAKE) & (rank > 0))
        def _():
            left(gone, turn_pieces)

        @pl.when(has(word, TAKE))
        def _():
            is_back = back_of(turn)
            chunk = chunk_of(turn, is_back)
            index = chunk * half_pieces + out + (1 - is_back) * total
            here = acts.at[is_back, chunk, :, piece_at(side, out)]
            hand_on = remote(here, here, gone, take_recv.at[side, index], down(side))
            hand_on.wait_recv()

            @pl.when(rank > 0)
            def _():
                hand_on.start()

    def relay_step(side, step):
        rank = rank_of(side)
        place = step - (n_chunk + RELAY_START) * half_pieces - hop * (last_pos - rank)
        turn = turn_of(place) - MARGIN
        out = piece_of(place)
        half_turn = lax.bitwise_and(turn, jnp.int32(1))
        chunk = jnp.clip(turn, 0, n_relay - 1)
        here = acts.at[1, chunk, :, piece_at(side, out)]
        gone = rel_over.at[side, half_turn]
        hand_on = remote(here, here, rel_send.at[side, half_turn], rel_recv.at[side, chunk * half_pieces + out], down(side))

        @pl.when((out == 0) & (turn >= 2) & (turn < n_relay + 2))
        def _():
            @pl.when(rank > 0)
            def _():
                left(rel_send.at[side, half_turn], turn_pieces)

            left(gone, turn_pieces)

            @pl.when((turn == n_relay + 1) & (rank == last_pos))
            def _():
                pl.semaphore_signal(free_sem.at[side], inc=1, device_id={"stage": 1}, device_id_type=MESH)

        @pl.when((turn >= 0) & (turn < n_relay))
        def _():
            hand_on.wait_recv()

            @pl.when(rank > 0)
            def _():
                hand_on.start()

            remote(here, here, gone, rel_in.at[chunk], {"stage": fore_stage}).start()

    tile_rows, tile_cols = tile_buf.shape[1], tile_buf.shape[2]
    per_row = wts.shape[1] // tile_cols
    n_tiles = hid_dim // tile_rows * per_row
    first_tile = (lead[0] + idle[0] + n_grad) * half_pieces

    def copy_tile(index):
        rows = pl.ds(pl.multiple_of(index // per_row * tile_rows, tile_rows), tile_rows)
        cols = pl.ds(pl.multiple_of(index % per_row * tile_cols, tile_cols), tile_cols)
        return pltpu.make_async_copy(tile_buf.at[index % 2], grad_hbm.at[rows, cols], tile_sem.at[index % 2])

    def grad_tile(index):
        rows = pl.ds(pl.multiple_of(index // per_row * tile_rows, tile_rows), tile_rows)
        cols = pl.ds(pl.multiple_of(index % per_row * tile_cols, tile_cols), tile_cols)

        @pl.when(index >= 2)
        def _():
            copy_tile(index).wait()

        act = hid[0, 0:n_grad, :, rows].reshape(n_grad * chunk_rows, tile_rows)
        grad = acts[1, 0:n_grad, :, cols].reshape(n_grad * chunk_rows, tile_cols)
        tile_buf[index % 2] = lax.dot_general(act, grad, (((0,), (0,)), ((), ())), preferred_element_type=F32)
        copy_tile(index).start()

    def loop_step(step, carry):
        for part in range(PARTS):
            first_product(step, part)

        @pl.when((step == 0) & (stage != fore_stage))
        def _():
            meet()

        gather_step(0, step)
        gather_step(1, step)
        sum_steps(step)

        @pl.when((stage == 0) & (step >= n_chunk * half_pieces))
        def _():
            relay_step(0, step)
            relay_step(1, step)

        take_step(0, step)
        take_step(1, step)
        since = step - first_tile

        @pl.when((stage == 0) & (since >= 0) & (since < n_tiles * TILE_STEPS) & (since % TILE_STEPS == 0))
        def _():
            grad_tile(since // TILE_STEPS)

        return carry

    lax.fori_loop(jnp.where(stage == fore_stage, -early, 1 - PARTS), n_steps, loop_step, 0)

    @pl.when(stage > 0)
    def _():
        def next_tile(index, carry):
            grad_tile(index)
            return carry

        lax.fori_loop(0, n_tiles, next_tile, 0)

    for side, owner in ((0, last_pos), (1, 0)):
        owns = (stage == last_stage) & (pos == owner)

        @pl.when(jnp.logical_not(owns))
        def _():
            loss_copy(side, 0, 0).wait_recv()

        @pl.when(owns)
        def _():
            for to_stage in range(n_stage):
                for to_pos in range(n_model):

                    @pl.when((to_stage != stage) | (to_pos != pos))
                    def _():
                        loss_copy(side, to_stage, to_pos).wait_send()

    loss_out[...] = jnp.full(loss_out.shape, jnp.sum(loss_in[0] + loss_in[1]) * (0.5 * grad_scale), F32)

    for index in (0, 1):
        copy_tile(index).wait()

    def end_out(chunk, carry):
        copy_out(3, chunk).wait()

        @pl.when(chunk >= n_grad)
        def _():
            for kind in (1, 2):
                copy_out(kind, chunk).wait()

        return carry

    lax.fori_loop(0, n_chunk, end_out, 0)


def finish_kernel(first, act, grad, total):
    total[...] = first[...] + lax.dot_general(act[...], grad[...], (((0,), (0,)), ((), ())), preferred_element_type=F32)


def finish_grads(first, act, grad):
    rows, hid_dim = act.shape
    model_dim = grad.shape[1]
    block = min(TILE_ROWS, hid_dim)
    return pl.pallas_call(
        finish_kernel,
        out_shape=jax.ShapeDtypeStruct((hid_dim, model_dim), F32),
        grid=(hid_dim // block,),
        in_specs=[
            pl.BlockSpec((block, model_dim), lambda i: (i, 0)),
            pl.BlockSpec((rows, block), lambda i: (0, i)),
            pl.BlockSpec((rows, model_dim), lambda i: (0, 0)),
        ],
        out_specs=pl.BlockSpec((block, model_dim), lambda i: (i, 0)),
        compiler_params=pltpu.CompilerParams(vmem_limit_bytes=51 * 1024 * 1024),
        cost_estimate=pl.CostEstimate(
            flops=2 * rows * hid_dim * model_dim, bytes_accessed=8 * hid_dim * model_dim, transcendentals=0
        ),
        name="finish_kernel",
    )(first, act, grad)


def solution(mesh):
    n_stage = mesh.shape["stage"]
    n_model = mesh.shape["model"]

    def stage_step(inputs, targets, w_in, w_out):
        num_micro, num_tokens, model_dim = inputs.shape
        hid_dim = w_in.shape[3]
        rows = num_micro * num_tokens
        chunk = min(CHUNK_TOKENS, num_tokens)
        n_chunk = rows // chunk
        piece = min(PIECE_COLS, model_dim // 2)
        half_pieces = model_dim // 2 // piece
        grad_scale = 1.0 / (rows * model_dim)
        lead = [n_chunk] * (n_stage - 2) + [min(PREV_LEAD, n_chunk), min(LAST_LEAD, n_chunk)]
        idle = [FIRST_IDLE] + [NEXT_IDLE] * (n_stage - 3) + [0, 0]
        n_fore, n_relay = min(FORE_CHUNKS, n_chunk - 1), min(RELAY_CHUNKS, n_chunk - 1)
        n_grad = min(FIRST_GRADS, n_chunk // 2)
        rest = rows - n_grad * chunk
        tile_rows, tile_cols = min(TILE_ROWS, hid_dim), min(TILE_COLS, model_dim)
        kernel = functools.partial(
            stage_kernel, n_stage, n_model, n_chunk, half_pieces, piece, HOP_LAG, lead, idle, n_fore, n_relay, n_grad, grad_scale
        )
        any_space = pl.BlockSpec(memory_space=pl.ANY)
        dma = pltpu.SemaphoreType.DMA
        layer_in, layer_grad, layer_act, layer_pre, first_grads, loss = pl.pallas_call(
            kernel,
            out_shape=(
                jax.ShapeDtypeStruct((rows, model_dim), BF16),
                jax.ShapeDtypeStruct((rest, model_dim), BF16),
                jax.ShapeDtypeStruct((rest, hid_dim), BF16),
                jax.ShapeDtypeStruct((rows, hid_dim), BF16),
                jax.ShapeDtypeStruct((hid_dim, model_dim), F32),
                jax.ShapeDtypeStruct((8, 128), F32),
            ),
            in_specs=[any_space] * 4,
            out_specs=(any_space, any_space, any_space, any_space, any_space, pl.BlockSpec(memory_space=pltpu.VMEM)),
            scratch_shapes=[
                pltpu.VMEM((4, model_dim, hid_dim), BF16),
                pltpu.VMEM((2, n_chunk, chunk, model_dim), BF16),
                pltpu.VMEM((2, n_chunk, chunk, hid_dim), BF16),
                pltpu.VMEM((2, 2, half_pieces, chunk, piece), F32),
                pltpu.VMEM((2, RECV_SLOTS, chunk, piece), F32),
                pltpu.VMEM((8, 128), F32),
                pltpu.VMEM((2, 8, 128), F32),
                dma((PARTS + 1,)),
                dma((n_chunk,)),
                dma,
                dma((2, 2)),
                dma((2, RECV_SLOTS)),
                dma((2, 2)),
                dma((2, n_chunk * half_pieces)),
                dma((2, 2)),
                dma((2, 2)),
                dma((2, (n_chunk + n_fore) * half_pieces)),
                dma((2, 2)),
                dma((4, n_chunk)),
                dma((n_stage * n_model,)),
                dma((2,)),
                pltpu.SemaphoreType.REGULAR((2,)),
                dma((2, 2)),
                dma((2, 2)),
                dma((2, n_relay * half_pieces)),
                dma((n_relay,)),
                pltpu.SemaphoreType.REGULAR((2,)),
                pltpu.SMEM((2 * n_chunk + max(idle) + 2 * MARGIN,), jnp.int32),
                pltpu.VMEM((2, tile_rows, tile_cols), F32),
                dma((2,)),
            ],
            compiler_params=pltpu.CompilerParams(collective_id=0, has_side_effects=True, vmem_limit_bytes=63 * 1024 * 1024),
            name="stage_kernel",
        )(
            inputs.reshape(n_chunk, chunk, model_dim),
            targets.reshape(n_chunk, chunk, model_dim),
            w_in.reshape(model_dim, hid_dim),
            w_out.reshape(hid_dim, model_dim),
        )

        def over_rows(left, right):
            return lax.dot_general(left, right, (((0,), (0,)), ((), ())), preferred_element_type=F32)

        grad_in = over_rows(layer_in, layer_pre)
        grad_out = finish_grads(first_grads, layer_act, layer_grad)
        return grad_in[None, None], grad_out[None, None], loss[0, :1]

    return jax.shard_map(
        stage_step,
        mesh=mesh,
        in_specs=(P("data", None, None), P("data", None, None), P("stage", None, None, "model"), P("stage", None, "model", None)),
        out_specs=(P(("data", "stage"), None, None, "model"), P(("data", "stage"), None, "model", None), P("data")),
        check_vma=False,
    )
```

```python
import functools

import jax
import jax.numpy as jnp
from jax import lax
from jax.experimental import pallas as pl
from jax.experimental.pallas import tpu as pltpu
from jax.sharding import PartitionSpec as P

GELU_COEF = 0.7978845608028654
CUBIC_COEF = 0.044715

CHUNK_TOKENS = 64
PIECE_COLS = 256
HIDDEN_COLS = 512
PARTS = 2
HOP_LAG = 2
RECV_SLOTS = 8
LAST_LEAD = 5
PREV_LEAD = 16
FIRST_IDLE = 12
NEXT_IDLE = 7
FORE_CHUNKS = 6
RELAY_CHUNKS = 18
RELAY_START = 0

FIRST_GRADS = 12
TILE_ROWS = 256
TILE_COLS = 1024
FIRST_TILES = (32, 1)
NEXT_TILES = (16, 2)

SUM, BACK, GATHER, EARLY, TAKE, FWD, BWD = 256, 512, 1024, 2048, 4096, 8192, 16384
MARGIN = 8

BF16 = jnp.bfloat16
F32 = jnp.float32
MESH = pl.DeviceIdType.MESH


def gelu_tanh(values):
    inner_arg = GELU_COEF * (values + CUBIC_COEF * values * values * values)
    return 0.5 * values * (1.0 + jnp.tanh(inner_arg))


def gelu_slope(values):
    tanh_val = jnp.tanh(GELU_COEF * (values + CUBIC_COEF * values * values * values))
    return 0.5 * (1.0 + tanh_val) + 0.5 * values * (1.0 - tanh_val * tanh_val) * GELU_COEF * (1.0 + 3.0 * CUBIC_COEF * values * values)


def dot_nn(left, right):
    return jnp.dot(left, right, preferred_element_type=F32)


def dot_nt(left, right):
    return lax.dot_general(left, right, (((1,), (1,)), ((), ())), preferred_element_type=F32)


def stage_kernel(
    n_stage, n_model, n_chunk, half_pieces, piece, hop, lead, idle, n_fore, n_relay, n_grad, grad_scale,
    inputs_hbm, targets_hbm, w1_hbm, w2_hbm,
    left_out, right_out, grad_hbm, loss_out,
    wts, acts, hid, send_buf, recv_buf, loss_acc, loss_in,
    w_sem, in_sem, tgt_sem, sum_send, sum_recv, gat_send, gat_recv, over_send, back_send, take_recv, down_send, out_sem,
    loss_send, loss_recv, spent_sem, rel_send, rel_over, rel_recv, rel_in, free_sem, table, tile_buf, tile_sem, end_buf,
):
    pos = lax.axis_index("model")
    stage = lax.axis_index("stage")
    last_pos = n_model - 1
    last_stage = n_stage - 1
    fore_stage = n_stage - 2
    bits = half_pieces.bit_length() - 1
    total = n_chunk * half_pieces
    half = half_pieces * piece
    hid_dim = wts.shape[2]
    chunk_rows = acts.shape[2]
    hid_part = hid_dim // PARTS
    hid_cols = min(HIDDEN_COLS, hid_part)
    n_lead, n_idle = jnp.int32(n_chunk), jnp.int32(0)
    for at in range(n_stage):
        n_lead = jnp.where(stage == at, lead[at], n_lead)
        n_idle = jnp.where(stage == at, idle[at], n_idle)
    turns = 2 * n_chunk + n_idle
    n_steps = turns * half_pieces + jnp.where(stage == 0, 1 - hop, half_pieces + hop * last_pos + 1)
    early = half_pieces + 3 * hop + 1

    barrier = pltpu.get_barrier_semaphore()
    for to_stage in range(n_stage):
        for to_pos in range(n_model):

            @pl.when((to_stage != stage) | (to_pos != pos))
            def _():
                pl.semaphore_signal(barrier, inc=1, device_id={"stage": to_stage, "model": to_pos}, device_id_type=MESH)

    copy_w2 = pltpu.make_async_copy(w2_hbm, wts.at[1], w_sem.at[PARTS])

    def copy_w1(part):
        cols = pl.ds(part * hid_part, hid_part)
        return pltpu.make_async_copy(w1_hbm.at[:, cols], wts.at[0, :, cols], w_sem.at[part])


    def copy_in(chunk):
        return pltpu.make_async_copy(inputs_hbm.at[chunk], acts.at[0, chunk], in_sem.at[chunk])

    def grad_in(chunk):
        return pltpu.make_async_copy(inputs_hbm.at[chunk], acts.at[1, chunk], rel_in.at[chunk])

    def copy_targets(side):
        cols = pl.ds(side * half, half)
        return pltpu.make_async_copy(targets_hbm.at[:, :, cols], acts.at[1, :, :, cols], tgt_sem)

    def copy_out(kind, chunk):
        src = (acts.at[0], hid.at[0], hid.at[1], acts.at[1])[kind]
        dst = (left_out.at[0], left_out.at[1], right_out.at[0], right_out.at[1])[kind]
        rows = pl.ds(pl.multiple_of((chunk - n_grad) * chunk_rows, chunk_rows), chunk_rows)
        return pltpu.make_async_copy(src.at[chunk], dst.at[rows, :], out_sem.at[kind, chunk])

    @pl.when(stage == 0)
    def _():
        copy_in(0).start()

    for part in range(PARTS):
        copy_w1(part).start()
    copy_w2.start()

    @pl.when(stage == 0)
    def _():
        def start_in(chunk, carry):
            copy_in(chunk).start()
            return carry

        lax.fori_loop(1, n_chunk, start_in, 0)

    @pl.when((stage == last_stage) & (pos == last_pos))
    def _():
        copy_targets(0).start()

    @pl.when((stage == last_stage) & (pos == 0))
    def _():
        copy_targets(1).start()

    def transpose_weights():
        tile = min(256, hid_dim)
        count = hid_dim // tile

        def one(index, carry):
            rows = pl.ds(pl.multiple_of((index // count) * tile, tile), tile)
            cols = pl.ds(pl.multiple_of((index % count) * tile, tile), tile)
            wts[2, cols, rows] = jnp.swapaxes(wts[1, rows, cols], 0, 1)
            wts[3, cols, rows] = jnp.swapaxes(wts[0, rows, cols], 0, 1)
            return carry

        lax.fori_loop(0, count * count, one, 0)

    n_mixed = 2 * (n_chunk - n_lead)
    n_after = 2 * n_chunk - n_lead
    n_first = n_lead + n_idle

    def fill(entry, carry):
        turn = entry - MARGIN
        after = turn - n_first
        pair = (after + 1024) // 2 - 512
        odd = (after + 1024) % 2 == 1
        mixed = (after >= 0) & (after < n_mixed)
        leads = (turn >= 0) & (turn < n_lead)
        fwd = leads | (mixed & odd)
        bwd = (after >= 0) & (after < n_after) & jnp.logical_not(mixed & odd)
        chunk = jnp.where(leads, turn, jnp.where(odd, n_lead + pair, pair))
        chunk = jnp.where(bwd & (after >= n_mixed), after - (n_chunk - n_lead), chunk)
        early_one = fwd & (stage == fore_stage - 1) & (chunk < n_fore)
        back = bwd & (stage < last_stage) & ((stage < fore_stage) | (chunk >= n_relay))
        take = back | (fwd & (stage == fore_stage) & (chunk < n_fore))
        word = jnp.int32(0)
        for flag, bit in (
            (fwd | (bwd & (stage > 0)), SUM),
            (bwd, BACK),
            (fwd & jnp.logical_not(early_one), GATHER),
            (early_one, EARLY),
            (take, TAKE),
            (fwd, FWD),
            (bwd, BWD),
        ):
            word = word + jnp.where(flag, bit, 0)
        table[entry] = word
        return carry

    lax.fori_loop(0, table.shape[0], fill, 0)
    loss_acc[...] = jnp.zeros_like(loss_acc)
    copy_w1(0).wait()

    @pl.when(stage > 0)
    def _():
        for part in range(1, PARTS):
            copy_w1(part).wait()
        copy_w2.wait()
        transpose_weights()

    def meet():
        pl.semaphore_wait(barrier, n_stage * n_model - 1)

    @pl.when(stage == fore_stage)
    def _():
        meet()


    def turn_of(place):
        return lax.shift_right_logical(place + MARGIN * half_pieces, jnp.int32(bits))

    def piece_of(place):
        return lax.bitwise_and(place + MARGIN * half_pieces, jnp.int32(half_pieces - 1))

    def has(word, mask):
        return lax.bitwise_and(word, jnp.int32(mask)) != 0

    def fwd_chunk(turn):
        after = turn - (n_first + MARGIN)
        return jnp.where(turn < n_lead + MARGIN, turn - MARGIN, n_lead + lax.shift_right_arithmetic(after, jnp.int32(1)))

    def bwd_chunk(turn):
        after = turn - (n_first + MARGIN)
        return jnp.where(after < n_mixed, lax.shift_right_arithmetic(after, jnp.int32(1)), after - (n_chunk - n_lead))

    def back_of(turn):
        after = turn - (n_first + MARGIN)
        odd = lax.bitwise_and(after, jnp.int32(1)) == 1
        return ((after >= 0) & jnp.logical_not((after < n_mixed) & odd)).astype(jnp.int32)

    def chunk_of(turn, is_back):
        return jnp.clip(jnp.where(is_back == 1, bwd_chunk(turn), fwd_chunk(turn)), 0, n_chunk - 1)

    def piece_at(side, index):
        col = side * half + index * piece
        return pl.ds(pl.multiple_of(col, piece), piece)

    def remote(src, dst, send_sem, recv_sem, device):
        return pltpu.make_async_remote_copy(
            src_ref=src, dst_ref=dst, send_sem=send_sem, recv_sem=recv_sem, device_id=device, device_id_type=MESH
        )

    def left(send_sem, like):
        remote(like, like, send_sem, loss_recv.at[0], {"model": pos}).wait_send()

    turn_pieces = acts.at[0, 0, :, pl.ds(0, half)]
    turn_sums = send_buf.at[0, 0]

    def rank_of(side):
        return pos if side == 0 else last_pos - pos

    def up(side):
        return {"model": pos + 1 if side == 0 else pos - 1}

    def down(side):
        return {"model": pos - 1 if side == 0 else pos + 1}

    def first_product(step, part):
        place = step + PARTS - 1 - part
        turn = turn_of(place)
        word = table[turn]
        starts = piece_of(place) == 0

        @pl.when(starts & has(word, FWD))
        def _():
            chunk = fwd_chunk(turn)
            if part == 0:

                @pl.when((stage != fore_stage) | (chunk >= n_fore))
                def _():
                    copy_in(chunk).wait()

                @pl.when(chunk >= n_grad)
                def _():
                    copy_out(0, chunk).start()

            else:

                @pl.when((stage == 0) & (place == 0))
                def _():
                    copy_w1(part).wait()

            for col in range(part * hid_part, (part + 1) * hid_part, hid_cols):
                cols = pl.ds(col, hid_cols)
                pre = dot_nn(acts[0, chunk], wts[0, :, cols]).astype(BF16)
                hid[1, chunk, :, cols] = pre
                hid[0, chunk, :, cols] = gelu_tanh(pre.astype(F32)).astype(BF16)
            if part == PARTS - 1:

                @pl.when(chunk >= n_grad)
                def _():
                    copy_out(1, chunk).start()

                @pl.when((stage == 0) & (place == 0))
                def _():
                    copy_w2.wait()

        @pl.when(starts & has(word, BWD))
        def _():
            chunk = bwd_chunk(turn)
            if part == 0:

                @pl.when((stage == fore_stage) & (chunk < n_relay))
                def _():
                    grad_in(chunk).wait()

                @pl.when(chunk >= n_grad)
                def _():
                    copy_out(3, chunk).start()

            for col in range(part * hid_part, (part + 1) * hid_part, hid_cols):
                cols = pl.ds(col, hid_cols)
                grad_act = dot_nn(acts[1, chunk], wts[2, :, cols]).astype(BF16)
                slope = gelu_slope(hid[1, chunk, :, cols].astype(F32))
                hid[1, chunk, :, cols] = (slope * grad_act.astype(F32)).astype(BF16)
            if part == PARTS - 1:

                @pl.when(chunk >= n_grad)
                def _():
                    copy_out(2, chunk).start()

        if part == 0:

            @pl.when((stage == 0) & (place == n_lead * half_pieces))
            def _():
                transpose_weights()

    def loss_copy(side, to_stage, to_pos):
        return remote(
            loss_acc, loss_in.at[side], loss_send.at[to_stage * n_model + to_pos], loss_recv.at[side],
            {"stage": to_stage, "model": to_pos},
        )

    def send_loss(side):
        loss_in[side] = loss_acc[...]
        for to_stage in range(n_stage):
            for to_pos in range(n_model):

                @pl.when((to_stage != stage) | (to_pos != pos))
                def _():
                    loss_copy(side, to_stage, to_pos).start()

    def sum_steps(step):
        now = []
        for side in (0, 1):
            rank = rank_of(side)
            place = step - hop * rank
            turn = turn_of(place)
            word, old = table[turn], table[turn - 2]
            index = piece_of(place)
            half_turn = lax.bitwise_and(turn, jnp.int32(1))
            inn = lax.bitwise_and(place + MARGIN * half_pieces, jnp.int32(RECV_SLOTS - 1))
            sums = has(word, SUM)
            is_back = back_of(turn)
            now.append((rank, word, sums, is_back, chunk_of(turn, is_back), index, half_turn, inn, piece_at(side, index)))

            @pl.when((index == 0) & has(old, SUM))
            def _():
                @pl.when(rank < last_pos)
                def _():
                    left(sum_send.at[side, half_turn], turn_sums)

                @pl.when((rank == last_pos) & has(old, BACK))
                def _():
                    left(down_send.at[side, half_turn], turn_pieces)

        @pl.when(now[0][2] | now[1][2])
        def _():
            for side in (0, 1):
                _, _, _, is_back, chunk, index, half_turn, _, cols = now[side]
                send_buf[side, half_turn, index] = dot_nn(hid[is_back, chunk], wts[1 + 2 * is_back, :, cols])

        for side in (0, 1):
            rank, word, sums, is_back, chunk, out, half_turn, inn, cols = now[side]
            bwd = has(word, BACK)
            index = chunk * half_pieces + out
            mine = send_buf.at[side, half_turn, out]
            gone = down_send.at[side, half_turn]
            hand_on = remote(mine, recv_buf.at[side, inn], sum_send.at[side, half_turn], sum_recv.at[side, inn], up(side))

            @pl.when(sums & (rank > 0))
            def _():
                hand_on.wait_recv()
                mine[...] = mine[...] + recv_buf[side, inn]

            @pl.when(sums & (rank < last_pos))
            def _():
                hand_on.start()

            @pl.when(sums & (rank == last_pos))
            def _():
                whole = acts[is_back, chunk, :, cols].astype(F32) + mine[...]
                scored = has(word, FWD) & (stage == last_stage)

                @pl.when(scored)
                def _():
                    @pl.when(index == 0)
                    def _():
                        copy_targets(side).wait()

                    err = whole.astype(BF16).astype(F32) - acts[1, chunk, :, cols].astype(F32)
                    acts[1, chunk, :, cols] = (err * grad_scale).astype(BF16)
                    square = jnp.sum((err * err).reshape(err.shape[0] // 8, 8, piece), axis=0)
                    part = square[:, :128]
                    for lane in range(1, piece // 128):
                        part = part + square[:, lane * 128 : (lane + 1) * 128]
                    loss_acc[...] = loss_acc[...] + part

                    @pl.when(index == total - 1)
                    def _():
                        send_loss(side)

                @pl.when(has(word, FWD) & (stage < last_stage))
                def _():
                    acts[1, chunk, :, cols] = whole.astype(BF16)

                ended = end_buf.at[side, half_turn, out]

                @pl.when(bwd)
                def _():
                    ended[...] = whole.astype(BF16)

                @pl.when(bwd & (index == total - 2 * half_pieces))
                def _():
                    pl.semaphore_wait(spent_sem.at[side], 1)

                @pl.when(bwd & (stage == 1) & (index == (n_relay - 2) * half_pieces))
                def _():
                    pl.semaphore_wait(free_sem.at[side], 1)

                relayed = (stage == last_stage) & (chunk < n_relay)
                there = acts.at[1, chunk, :, cols]

                @pl.when(bwd & relayed)
                def _():
                    arrived = rel_recv.at[side, jnp.minimum(index, n_relay * half_pieces - 1)]
                    remote(ended, there, gone, arrived, {"stage": 0}).start()

                @pl.when(bwd & jnp.logical_not(relayed))
                def _():
                    arrived = take_recv.at[side, index]
                    remote(ended, there, gone, arrived, {"stage": stage - 1}).start()

    def gather_step(side, step):
        rank = rank_of(side)
        place = step - 1 - 3 * hop - hop * (last_pos - rank)
        turn = turn_of(place)
        word, old = table[turn], table[turn - 2]
        out = piece_of(place)
        half_turn = lax.bitwise_and(turn, jnp.int32(1))
        chunk = jnp.clip(fwd_chunk(turn), 0, n_chunk - 1)
        index = chunk * half_pieces + out
        cols = piece_at(side, out)
        here = acts.at[1, chunk, :, cols]
        gone = over_send.at[side, half_turn]

        @pl.when((out == 0) & has(old, GATHER | EARLY))
        def _():
            @pl.when(has(old, GATHER) & (rank > 0))
            def _():
                left(gat_send.at[side, half_turn], turn_pieces)

            @pl.when((stage < last_stage) & (has(old, GATHER) | (rank == last_pos)))
            def _():
                left(gone, turn_pieces)

                @pl.when((fwd_chunk(turn - 2) == n_chunk - 1) & (rank == last_pos))
                def _():
                    pl.semaphore_signal(spent_sem.at[side], inc=1, device_id={"stage": stage + 1}, device_id_type=MESH)

        @pl.when(has(word, GATHER))
        def _():
            hand_on = remote(here, here, gat_send.at[side, half_turn], gat_recv.at[side, index], down(side))

            @pl.when(rank < last_pos)
            def _():
                hand_on.wait_recv()

            @pl.when(rank > 0)
            def _():
                hand_on.start()

            @pl.when(stage < last_stage)
            def _():
                remote(here, acts.at[0, chunk, :, cols], gone, in_sem.at[chunk], {"stage": stage + 1}).start()

        @pl.when(has(word, EARLY) & (rank == last_pos))
        def _():
            arrived = take_recv.at[side, jnp.minimum(total + index, total + n_fore * half_pieces - 1)]
            remote(here, acts.at[0, chunk, :, cols], gone, arrived, {"stage": stage + 1}).start()

    def take_step(side, step):
        rank = rank_of(side)
        place = step + early - hop * (last_pos - rank)
        turn = turn_of(place)
        word, old = table[turn], table[turn - 2]
        out = piece_of(place)
        gone = back_send.at[side, lax.bitwise_and(turn, jnp.int32(1))]

        @pl.when((out == 0) & has(old, TAKE) & (rank > 0))
        def _():
            left(gone, turn_pieces)

        @pl.when(has(word, TAKE))
        def _():
            is_back = back_of(turn)
            chunk = chunk_of(turn, is_back)
            index = chunk * half_pieces + out + (1 - is_back) * total
            here = acts.at[is_back, chunk, :, piece_at(side, out)]
            hand_on = remote(here, here, gone, take_recv.at[side, index], down(side))
            hand_on.wait_recv()

            @pl.when(rank > 0)
            def _():
                hand_on.start()

    def relay_step(side, step):
        rank = rank_of(side)
        place = step - (n_chunk + RELAY_START) * half_pieces - hop * (last_pos - rank)
        turn = turn_of(place) - MARGIN
        out = piece_of(place)
        half_turn = lax.bitwise_and(turn, jnp.int32(1))
        chunk = jnp.clip(turn, 0, n_relay - 1)
        here = acts.at[1, chunk, :, piece_at(side, out)]
        gone = rel_over.at[side, half_turn]
        hand_on = remote(here, here, rel_send.at[side, half_turn], rel_recv.at[side, chunk * half_pieces + out], down(side))

        @pl.when((out == 0) & (turn >= 2) & (turn < n_relay + 2))
        def _():
            @pl.when(rank > 0)
            def _():
                left(rel_send.at[side, half_turn], turn_pieces)

            left(gone, turn_pieces)

            @pl.when((turn == n_relay + 1) & (rank == last_pos))
            def _():
                pl.semaphore_signal(free_sem.at[side], inc=1, device_id={"stage": 1}, device_id_type=MESH)

        @pl.when((turn >= 0) & (turn < n_relay))
        def _():
            hand_on.wait_recv()

            @pl.when(rank > 0)
            def _():
                hand_on.start()

            remote(here, here, gone, rel_in.at[chunk], {"stage": fore_stage}).start()

    tile_rows, tile_cols = tile_buf.shape[1], tile_buf.shape[2]
    per_row = wts.shape[1] // tile_cols
    n_tiles = hid_dim // tile_rows * per_row

    def copy_tile(which, index):
        rows = pl.ds(pl.multiple_of(index // per_row * tile_rows, tile_rows), tile_rows)
        cols = pl.ds(pl.multiple_of(index % per_row * tile_cols, tile_cols), tile_cols)
        return pltpu.make_async_copy(tile_buf.at[index % 2], grad_hbm.at[which, rows, cols], tile_sem.at[index % 2])

    def grad_tile(number):
        for which, index in ((1, number), (0, number - n_tiles)):

            @pl.when((index >= 0) & (index < n_tiles))
            def _():
                rows = pl.ds(pl.multiple_of(index // per_row * tile_rows, tile_rows), tile_rows)
                cols = pl.ds(pl.multiple_of(index % per_row * tile_cols, tile_cols), tile_cols)

                @pl.when(number >= 2)
                def _():
                    copy_tile(which, index).wait()

                inputs, grads = (acts.at[0], hid.at[1]) if which == 0 else (hid.at[0], acts.at[1])
                lefts = inputs[0:n_grad, :, rows].reshape(n_grad * chunk_rows, tile_rows)
                rights = grads[0:n_grad, :, cols].reshape(n_grad * chunk_rows, tile_cols)
                tile_buf[index % 2] = lax.dot_general(lefts, rights, (((0,), (0,)), ((), ())), preferred_element_type=F32)
                copy_tile(which, index).start()

    in_loop = jnp.where(stage == 0, FIRST_TILES[0], jnp.where(stage == 1, NEXT_TILES[0], 0))
    pitch = jnp.where(stage == 0, FIRST_TILES[1], NEXT_TILES[1])
    first_tile = (n_first + n_grad) * half_pieces

    def loop_step(step, carry):
        for part in range(PARTS):
            first_product(step, part)

        @pl.when((step == 0) & (stage != fore_stage))
        def _():
            meet()

        gather_step(0, step)
        gather_step(1, step)
        sum_steps(step)

        @pl.when((stage == 0) & (step >= n_chunk * half_pieces))
        def _():
            relay_step(0, step)
            relay_step(1, step)

        take_step(0, step)
        take_step(1, step)
        since = step - first_tile

        @pl.when((since >= 0) & (since < in_loop * pitch) & (since % pitch == 0))
        def _():
            grad_tile(since // pitch)

        return carry

    lax.fori_loop(jnp.where(stage == fore_stage, -early, 1 - PARTS), n_steps, loop_step, 0)

    def next_tile(number, carry):
        grad_tile(number)
        return carry

    lax.fori_loop(in_loop, 2 * n_tiles, next_tile, 0)

    for side, owner in ((0, last_pos), (1, 0)):
        owns = (stage == last_stage) & (pos == owner)

        @pl.when(jnp.logical_not(owns))
        def _():
            loss_copy(side, 0, 0).wait_recv()

        @pl.when(owns)
        def _():
            for to_stage in range(n_stage):
                for to_pos in range(n_model):

                    @pl.when((to_stage != stage) | (to_pos != pos))
                    def _():
                        loss_copy(side, to_stage, to_pos).wait_send()

    loss_out[...] = jnp.full(loss_out.shape, jnp.sum(loss_in[0] + loss_in[1]) * (0.5 * grad_scale), F32)

    for index in (0, 1):
        copy_tile(0, index).wait()

    def end_out(chunk, carry):
        for kind in range(4):
            copy_out(kind, chunk).wait()
        return carry

    lax.fori_loop(n_grad, n_chunk, end_out, 0)


def finish_kernel(first, lefts, rights, grad_in, grad_out):
    def whole():
        return first[0] + lax.dot_general(lefts[0], rights[0], (((0,), (0,)), ((), ())), preferred_element_type=F32)

    @pl.when(pl.program_id(0) == 0)
    def _():
        grad_in[...] = whole()

    @pl.when(pl.program_id(0) == 1)
    def _():
        grad_out[...] = whole()


def finish_grads(first, lefts, rights):
    rows, dim = lefts.shape[1:]
    block = min(TILE_ROWS, dim)
    blocks = dim // block
    shape = jax.ShapeDtypeStruct((dim, dim), F32)
    return pl.pallas_call(
        finish_kernel,
        out_shape=(shape, shape),
        grid=(2, blocks),
        in_specs=[
            pl.BlockSpec((1, block, dim), lambda which, i: (which, i, 0)),
            pl.BlockSpec((1, rows, block), lambda which, i: (which, 0, i)),
            pl.BlockSpec((1, rows, dim), lambda which, i: (which, 0, 0)),
        ],
        out_specs=(
            pl.BlockSpec((block, dim), lambda which, i: (i * (1 - which) + (blocks - 1) * which, 0)),
            pl.BlockSpec((block, dim), lambda which, i: (i * which, 0)),
        ),
        compiler_params=pltpu.CompilerParams(vmem_limit_bytes=60 * 1024 * 1024),
        cost_estimate=pl.CostEstimate(flops=4 * rows * dim * dim, bytes_accessed=16 * dim * dim, transcendentals=0),
        name="finish_kernel",
    )(first, lefts, rights)


def solution(mesh):
    n_stage = mesh.shape["stage"]
    n_model = mesh.shape["model"]

    def stage_step(inputs, targets, w_in, w_out):
        num_micro, num_tokens, model_dim = inputs.shape
        hid_dim = w_in.shape[3]
        rows = num_micro * num_tokens
        chunk = min(CHUNK_TOKENS, num_tokens)
        n_chunk = rows // chunk
        piece = min(PIECE_COLS, model_dim // 2)
        half_pieces = model_dim // 2 // piece
        grad_scale = 1.0 / (rows * model_dim)
        lead = [n_chunk] * (n_stage - 2) + [min(PREV_LEAD, n_chunk), min(LAST_LEAD, n_chunk)]
        idle = [FIRST_IDLE] + [NEXT_IDLE] * (n_stage - 3) + [0, 0]
        n_fore, n_relay = min(FORE_CHUNKS, n_chunk - 1), min(RELAY_CHUNKS, n_chunk - 1)
        n_grad = min(FIRST_GRADS, n_chunk // 2)
        rest = rows - n_grad * chunk
        tile_rows, tile_cols = min(TILE_ROWS, hid_dim), min(TILE_COLS, model_dim)
        kernel = functools.partial(
            stage_kernel, n_stage, n_model, n_chunk, half_pieces, piece, HOP_LAG, lead, idle, n_fore, n_relay, n_grad, grad_scale
        )
        any_space = pl.BlockSpec(memory_space=pl.ANY)
        dma = pltpu.SemaphoreType.DMA
        lefts, rights, first_grads, loss = pl.pallas_call(
            kernel,
            out_shape=(
                jax.ShapeDtypeStruct((2, rest, model_dim), BF16),
                jax.ShapeDtypeStruct((2, rest, model_dim), BF16),
                jax.ShapeDtypeStruct((2, hid_dim, model_dim), F32),
                jax.ShapeDtypeStruct((8, 128), F32),
            ),
            in_specs=[any_space] * 4,
            out_specs=(any_space, any_space, any_space, pl.BlockSpec(memory_space=pltpu.VMEM)),
            scratch_shapes=[
                pltpu.VMEM((4, model_dim, hid_dim), BF16),
                pltpu.VMEM((2, n_chunk, chunk, model_dim), BF16),
                pltpu.VMEM((2, n_chunk, chunk, hid_dim), BF16),
                pltpu.VMEM((2, 2, half_pieces, chunk, piece), F32),
                pltpu.VMEM((2, RECV_SLOTS, chunk, piece), F32),
                pltpu.VMEM((8, 128), F32),
                pltpu.VMEM((2, 8, 128), F32),
                dma((PARTS + 1,)),
                dma((n_chunk,)),
                dma,
                dma((2, 2)),
                dma((2, RECV_SLOTS)),
                dma((2, 2)),
                dma((2, n_chunk * half_pieces)),
                dma((2, 2)),
                dma((2, 2)),
                dma((2, (n_chunk + n_fore) * half_pieces)),
                dma((2, 2)),
                dma((4, n_chunk)),
                dma((n_stage * n_model,)),
                dma((2,)),
                pltpu.SemaphoreType.REGULAR((2,)),
                dma((2, 2)),
                dma((2, 2)),
                dma((2, n_relay * half_pieces)),
                dma((n_relay,)),
                pltpu.SemaphoreType.REGULAR((2,)),
                pltpu.SMEM((2 * n_chunk + max(idle) + 2 * MARGIN,), jnp.int32),
                pltpu.VMEM((2, tile_rows, tile_cols), F32),
                dma((2,)),
                pltpu.VMEM((2, 2, half_pieces, chunk, piece), BF16),
            ],
            compiler_params=pltpu.CompilerParams(collective_id=0, has_side_effects=True, vmem_limit_bytes=63 * 1024 * 1024),
            name="stage_kernel",
        )(
            inputs.reshape(n_chunk, chunk, model_dim),
            targets.reshape(n_chunk, chunk, model_dim),
            w_in.reshape(model_dim, hid_dim),
            w_out.reshape(hid_dim, model_dim),
        )

        grad_in, grad_out = finish_grads(first_grads, lefts, rights)
        return grad_in[None, None], grad_out[None, None], loss[0, :1]

    return jax.shard_map(
        stage_step,
        mesh=mesh,
        in_specs=(P("data", None, None), P("data", None, None), P("stage", None, None, "model"), P("stage", None, "model", None)),
        out_specs=(P(("data", "stage"), None, None, "model"), P(("data", "stage"), None, "model", None), P("data")),
        check_vma=False,
    )
```

```python
import functools

import jax
import jax.numpy as jnp
from jax import lax
from jax.experimental import pallas as pl
from jax.experimental.pallas import tpu as pltpu
from jax.sharding import PartitionSpec as P

GELU_COEF = 0.7978845608028654
CUBIC_COEF = 0.044715

CHUNK_TOKENS = 64
PIECE_COLS = 256
HIDDEN_COLS = 512
PARTS = 2
HOP_LAG = 2
RECV_SLOTS = 8
LAST_LEAD = 5
PREV_LEAD = 16
FIRST_IDLE = 12
NEXT_IDLE = 7
FORE_CHUNKS = 6
RELAY_CHUNKS = 18
RELAY_START = 0

FIRST_GRADS = 14
TILE_ROWS = 256
TILE_COLS = 1024
IN_FLIGHT = 5
FIRST_TILES = (32, 1)
NEXT_TILES = (16, 2)

SUM, BACK, GATHER, EARLY, TAKE, FWD, BWD = 256, 512, 1024, 2048, 4096, 8192, 16384
MARGIN = 8

BF16 = jnp.bfloat16
F32 = jnp.float32
MESH = pl.DeviceIdType.MESH


def gelu_tanh(values):
    inner_arg = GELU_COEF * (values + CUBIC_COEF * values * values * values)
    return 0.5 * values * (1.0 + jnp.tanh(inner_arg))


def gelu_slope(values):
    tanh_val = jnp.tanh(GELU_COEF * (values + CUBIC_COEF * values * values * values))
    return 0.5 * (1.0 + tanh_val) + 0.5 * values * (1.0 - tanh_val * tanh_val) * GELU_COEF * (1.0 + 3.0 * CUBIC_COEF * values * values)


def dot_nn(left, right):
    return jnp.dot(left, right, preferred_element_type=F32)


def dot_nt(left, right):
    return lax.dot_general(left, right, (((1,), (1,)), ((), ())), preferred_element_type=F32)


def stage_kernel(
    n_stage, n_model, n_chunk, half_pieces, piece, hop, lead, idle, n_fore, n_relay, n_grad, grad_scale,
    inputs_hbm, targets_hbm, w1_hbm, w2_hbm,
    left_out, right_out, grad_hbm, loss_out,
    wts, acts, hid, send_buf, recv_buf, loss_acc, loss_in,
    w_sem, in_sem, tgt_sem, sum_send, sum_recv, gat_send, gat_recv, over_send, back_send, take_recv, down_send, out_sem,
    loss_send, loss_recv, spent_sem, rel_send, rel_over, rel_recv, rel_in, free_sem, table, tile_buf, tile_sem, end_buf,
):
    pos = lax.axis_index("model")
    stage = lax.axis_index("stage")
    last_pos = n_model - 1
    last_stage = n_stage - 1
    fore_stage = n_stage - 2
    bits = half_pieces.bit_length() - 1
    total = n_chunk * half_pieces
    half = half_pieces * piece
    hid_dim = wts.shape[2]
    chunk_rows = acts.shape[2]
    hid_part = hid_dim // PARTS
    hid_cols = min(HIDDEN_COLS, hid_part)
    n_lead, n_idle = jnp.int32(n_chunk), jnp.int32(0)
    for at in range(n_stage):
        n_lead = jnp.where(stage == at, lead[at], n_lead)
        n_idle = jnp.where(stage == at, idle[at], n_idle)
    turns = 2 * n_chunk + n_idle
    n_steps = turns * half_pieces + jnp.where(stage == 0, 1 - hop, half_pieces + hop * last_pos + 1)
    early = half_pieces + 3 * hop + 1

    barrier = pltpu.get_barrier_semaphore()
    for to_stage in range(n_stage):
        for to_pos in range(n_model):

            @pl.when((to_stage != stage) | (to_pos != pos))
            def _():
                pl.semaphore_signal(barrier, inc=1, device_id={"stage": to_stage, "model": to_pos}, device_id_type=MESH)

    copy_w2 = pltpu.make_async_copy(w2_hbm, wts.at[1], w_sem.at[PARTS])

    def copy_w1(part):
        cols = pl.ds(part * hid_part, hid_part)
        return pltpu.make_async_copy(w1_hbm.at[:, cols], wts.at[0, :, cols], w_sem.at[part])


    def copy_in(chunk):
        return pltpu.make_async_copy(inputs_hbm.at[chunk], acts.at[0, chunk], in_sem.at[chunk])

    def grad_in(chunk):
        return pltpu.make_async_copy(inputs_hbm.at[chunk], acts.at[1, chunk], rel_in.at[chunk])

    def copy_targets(side):
        cols = pl.ds(side * half, half)
        return pltpu.make_async_copy(targets_hbm.at[:, :, cols], acts.at[1, :, :, cols], tgt_sem)

    def copy_out(kind, chunk):
        src = (acts.at[0], hid.at[0], hid.at[1], acts.at[1])[kind]
        dst = (left_out.at[0], left_out.at[1], right_out.at[0], right_out.at[1])[kind]
        rows = pl.ds(pl.multiple_of((chunk - n_grad) * chunk_rows, chunk_rows), chunk_rows)
        return pltpu.make_async_copy(src.at[chunk], dst.at[rows, :], out_sem.at[kind, chunk])

    @pl.when(stage == 0)
    def _():
        copy_in(0).start()

    for part in range(PARTS):
        copy_w1(part).start()
    copy_w2.start()

    @pl.when(stage == 0)
    def _():
        def start_in(chunk, carry):
            copy_in(chunk).start()
            return carry

        lax.fori_loop(1, n_chunk, start_in, 0)

    @pl.when((stage == last_stage) & (pos == last_pos))
    def _():
        copy_targets(0).start()

    @pl.when((stage == last_stage) & (pos == 0))
    def _():
        copy_targets(1).start()

    def transpose_weights():
        tile = min(256, hid_dim)
        count = hid_dim // tile

        def one(index, carry):
            rows = pl.ds(pl.multiple_of((index // count) * tile, tile), tile)
            cols = pl.ds(pl.multiple_of((index % count) * tile, tile), tile)
            wts[2, cols, rows] = jnp.swapaxes(wts[1, rows, cols], 0, 1)
            wts[3, cols, rows] = jnp.swapaxes(wts[0, rows, cols], 0, 1)
            return carry

        lax.fori_loop(0, count * count, one, 0)

    n_mixed = 2 * (n_chunk - n_lead)
    n_after = 2 * n_chunk - n_lead
    n_first = n_lead + n_idle

    def fill(entry, carry):
        turn = entry - MARGIN
        after = turn - n_first
        pair = (after + 1024) // 2 - 512
        odd = (after + 1024) % 2 == 1
        mixed = (after >= 0) & (after < n_mixed)
        leads = (turn >= 0) & (turn < n_lead)
        fwd = leads | (mixed & odd)
        bwd = (after >= 0) & (after < n_after) & jnp.logical_not(mixed & odd)
        chunk = jnp.where(leads, turn, jnp.where(odd, n_lead + pair, pair))
        chunk = jnp.where(bwd & (after >= n_mixed), after - (n_chunk - n_lead), chunk)
        early_one = fwd & (stage == fore_stage - 1) & (chunk < n_fore)
        back = bwd & (stage < last_stage) & ((stage < fore_stage) | (chunk >= n_relay))
        take = back | (fwd & (stage == fore_stage) & (chunk < n_fore))
        word = jnp.int32(0)
        for flag, bit in (
            (fwd | (bwd & (stage > 0)), SUM),
            (bwd, BACK),
            (fwd & jnp.logical_not(early_one), GATHER),
            (early_one, EARLY),
            (take, TAKE),
            (fwd, FWD),
            (bwd, BWD),
        ):
            word = word + jnp.where(flag, bit, 0)
        table[entry] = word
        return carry

    lax.fori_loop(0, table.shape[0], fill, 0)
    loss_acc[...] = jnp.zeros_like(loss_acc)
    copy_w1(0).wait()

    @pl.when(stage > 0)
    def _():
        for part in range(1, PARTS):
            copy_w1(part).wait()
        copy_w2.wait()
        transpose_weights()

    def meet():
        pl.semaphore_wait(barrier, n_stage * n_model - 1)

    @pl.when(stage == fore_stage)
    def _():
        meet()


    def turn_of(place):
        return lax.shift_right_logical(place + MARGIN * half_pieces, jnp.int32(bits))

    def piece_of(place):
        return lax.bitwise_and(place + MARGIN * half_pieces, jnp.int32(half_pieces - 1))

    def has(word, mask):
        return lax.bitwise_and(word, jnp.int32(mask)) != 0

    def fwd_chunk(turn):
        after = turn - (n_first + MARGIN)
        return jnp.where(turn < n_lead + MARGIN, turn - MARGIN, n_lead + lax.shift_right_arithmetic(after, jnp.int32(1)))

    def bwd_chunk(turn):
        after = turn - (n_first + MARGIN)
        return jnp.where(after < n_mixed, lax.shift_right_arithmetic(after, jnp.int32(1)), after - (n_chunk - n_lead))

    def back_of(turn):
        after = turn - (n_first + MARGIN)
        odd = lax.bitwise_and(after, jnp.int32(1)) == 1
        return ((after >= 0) & jnp.logical_not((after < n_mixed) & odd)).astype(jnp.int32)

    def chunk_of(turn, is_back):
        return jnp.clip(jnp.where(is_back == 1, bwd_chunk(turn), fwd_chunk(turn)), 0, n_chunk - 1)

    def piece_at(side, index):
        col = side * half + index * piece
        return pl.ds(pl.multiple_of(col, piece), piece)

    def remote(src, dst, send_sem, recv_sem, device):
        return pltpu.make_async_remote_copy(
            src_ref=src, dst_ref=dst, send_sem=send_sem, recv_sem=recv_sem, device_id=device, device_id_type=MESH
        )

    def left(send_sem, like):
        remote(like, like, send_sem, loss_recv.at[0], {"model": pos}).wait_send()

    turn_pieces = acts.at[0, 0, :, pl.ds(0, half)]
    turn_sums = send_buf.at[0, 0]

    def rank_of(side):
        return pos if side == 0 else last_pos - pos

    def up(side):
        return {"model": pos + 1 if side == 0 else pos - 1}

    def down(side):
        return {"model": pos - 1 if side == 0 else pos + 1}

    def first_product(step, part):
        place = step + PARTS - 1 - part
        turn = turn_of(place)
        word = table[turn]
        starts = piece_of(place) == 0

        @pl.when(starts & has(word, FWD))
        def _():
            chunk = fwd_chunk(turn)
            if part == 0:

                @pl.when((stage != fore_stage) | (chunk >= n_fore))
                def _():
                    copy_in(chunk).wait()

                @pl.when(chunk >= n_grad)
                def _():
                    copy_out(0, chunk).start()

            else:

                @pl.when((stage == 0) & (place == 0))
                def _():
                    copy_w1(part).wait()

            for col in range(part * hid_part, (part + 1) * hid_part, hid_cols):
                cols = pl.ds(col, hid_cols)
                pre = dot_nn(acts[0, chunk], wts[0, :, cols]).astype(BF16)
                hid[1, chunk, :, cols] = pre
                hid[0, chunk, :, cols] = gelu_tanh(pre.astype(F32)).astype(BF16)
            if part == PARTS - 1:

                @pl.when(chunk >= n_grad)
                def _():
                    copy_out(1, chunk).start()

                @pl.when((stage == 0) & (place == 0))
                def _():
                    copy_w2.wait()

        @pl.when(starts & has(word, BWD))
        def _():
            chunk = bwd_chunk(turn)
            if part == 0:

                @pl.when((stage == fore_stage) & (chunk < n_relay))
                def _():
                    grad_in(chunk).wait()

                @pl.when(chunk >= n_grad)
                def _():
                    copy_out(3, chunk).start()

            for col in range(part * hid_part, (part + 1) * hid_part, hid_cols):
                cols = pl.ds(col, hid_cols)
                grad_act = dot_nn(acts[1, chunk], wts[2, :, cols]).astype(BF16)
                slope = gelu_slope(hid[1, chunk, :, cols].astype(F32))
                hid[1, chunk, :, cols] = (slope * grad_act.astype(F32)).astype(BF16)
            if part == PARTS - 1:

                @pl.when(chunk >= n_grad)
                def _():
                    copy_out(2, chunk).start()

        if part == 0:

            @pl.when((stage == 0) & (place == n_lead * half_pieces))
            def _():
                transpose_weights()

    def loss_copy(side, to_stage, to_pos):
        return remote(
            loss_acc, loss_in.at[side], loss_send.at[to_stage * n_model + to_pos], loss_recv.at[side],
            {"stage": to_stage, "model": to_pos},
        )

    def send_loss(side):
        loss_in[side] = loss_acc[...]
        for to_stage in range(n_stage):
            for to_pos in range(n_model):

                @pl.when((to_stage != stage) | (to_pos != pos))
                def _():
                    loss_copy(side, to_stage, to_pos).start()

    def sum_steps(step):
        now = []
        for side in (0, 1):
            rank = rank_of(side)
            place = step - hop * rank
            turn = turn_of(place)
            word, old = table[turn], table[turn - 2]
            index = piece_of(place)
            half_turn = lax.bitwise_and(turn, jnp.int32(1))
            inn = lax.bitwise_and(place + MARGIN * half_pieces, jnp.int32(RECV_SLOTS - 1))
            sums = has(word, SUM)
            is_back = back_of(turn)
            now.append((rank, word, sums, is_back, chunk_of(turn, is_back), index, half_turn, inn, piece_at(side, index)))

            @pl.when((index == 0) & has(old, SUM))
            def _():
                @pl.when(rank < last_pos)
                def _():
                    left(sum_send.at[side, half_turn], turn_sums)

                @pl.when((rank == last_pos) & has(old, BACK))
                def _():
                    left(down_send.at[side, half_turn], turn_pieces)

        @pl.when(now[0][2] | now[1][2])
        def _():
            for side in (0, 1):
                _, _, _, is_back, chunk, index, half_turn, _, cols = now[side]
                send_buf[side, half_turn, index] = dot_nn(hid[is_back, chunk], wts[1 + 2 * is_back, :, cols])

        for side in (0, 1):
            rank, word, sums, is_back, chunk, out, half_turn, inn, cols = now[side]
            bwd = has(word, BACK)
            index = chunk * half_pieces + out
            mine = send_buf.at[side, half_turn, out]
            gone = down_send.at[side, half_turn]
            hand_on = remote(mine, recv_buf.at[side, inn], sum_send.at[side, half_turn], sum_recv.at[side, inn], up(side))

            @pl.when(sums & (rank > 0))
            def _():
                hand_on.wait_recv()
                mine[...] = mine[...] + recv_buf[side, inn]

            @pl.when(sums & (rank < last_pos))
            def _():
                hand_on.start()

            @pl.when(sums & (rank == last_pos))
            def _():
                whole = acts[is_back, chunk, :, cols].astype(F32) + mine[...]
                scored = has(word, FWD) & (stage == last_stage)

                @pl.when(scored)
                def _():
                    @pl.when(index == 0)
                    def _():
                        copy_targets(side).wait()

                    err = whole.astype(BF16).astype(F32) - acts[1, chunk, :, cols].astype(F32)
                    acts[1, chunk, :, cols] = (err * grad_scale).astype(BF16)
                    square = jnp.sum((err * err).reshape(err.shape[0] // 8, 8, piece), axis=0)
                    part = square[:, :128]
                    for lane in range(1, piece // 128):
                        part = part + square[:, lane * 128 : (lane + 1) * 128]
                    loss_acc[...] = loss_acc[...] + part

                    @pl.when(index == total - 1)
                    def _():
                        send_loss(side)

                @pl.when(has(word, FWD) & (stage < last_stage))
                def _():
                    acts[1, chunk, :, cols] = whole.astype(BF16)

                ended = end_buf.at[side, half_turn, out]

                @pl.when(bwd)
                def _():
                    ended[...] = whole.astype(BF16)

                @pl.when(bwd & (index == total - 2 * half_pieces))
                def _():
                    pl.semaphore_wait(spent_sem.at[side], 1)

                @pl.when(bwd & (stage == 1) & (index == (n_relay - 2) * half_pieces))
                def _():
                    pl.semaphore_wait(free_sem.at[side], 1)

                relayed = (stage == last_stage) & (chunk < n_relay)
                there = acts.at[1, chunk, :, cols]

                @pl.when(bwd & relayed)
                def _():
                    arrived = rel_recv.at[side, jnp.minimum(index, n_relay * half_pieces - 1)]
                    remote(ended, there, gone, arrived, {"stage": 0}).start()

                @pl.when(bwd & jnp.logical_not(relayed))
                def _():
                    arrived = take_recv.at[side, index]
                    remote(ended, there, gone, arrived, {"stage": stage - 1}).start()

    def gather_step(side, step):
        rank = rank_of(side)
        place = step - 1 - 3 * hop - hop * (last_pos - rank)
        turn = turn_of(place)
        word, old = table[turn], table[turn - 2]
        out = piece_of(place)
        half_turn = lax.bitwise_and(turn, jnp.int32(1))
        chunk = jnp.clip(fwd_chunk(turn), 0, n_chunk - 1)
        index = chunk * half_pieces + out
        cols = piece_at(side, out)
        here = acts.at[1, chunk, :, cols]
        gone = over_send.at[side, half_turn]

        @pl.when((out == 0) & has(old, GATHER | EARLY))
        def _():
            @pl.when(has(old, GATHER) & (rank > 0))
            def _():
                left(gat_send.at[side, half_turn], turn_pieces)

            @pl.when((stage < last_stage) & (has(old, GATHER) | (rank == last_pos)))
            def _():
                left(gone, turn_pieces)

                @pl.when((fwd_chunk(turn - 2) == n_chunk - 1) & (rank == last_pos))
                def _():
                    pl.semaphore_signal(spent_sem.at[side], inc=1, device_id={"stage": stage + 1}, device_id_type=MESH)

        @pl.when(has(word, GATHER))
        def _():
            hand_on = remote(here, here, gat_send.at[side, half_turn], gat_recv.at[side, index], down(side))

            @pl.when(rank < last_pos)
            def _():
                hand_on.wait_recv()

            @pl.when(rank > 0)
            def _():
                hand_on.start()

            @pl.when(stage < last_stage)
            def _():
                remote(here, acts.at[0, chunk, :, cols], gone, in_sem.at[chunk], {"stage": stage + 1}).start()

        @pl.when(has(word, EARLY) & (rank == last_pos))
        def _():
            arrived = take_recv.at[side, jnp.minimum(total + index, total + n_fore * half_pieces - 1)]
            remote(here, acts.at[0, chunk, :, cols], gone, arrived, {"stage": stage + 1}).start()

    def take_step(side, step):
        rank = rank_of(side)
        place = step + early - hop * (last_pos - rank)
        turn = turn_of(place)
        word, old = table[turn], table[turn - 2]
        out = piece_of(place)
        gone = back_send.at[side, lax.bitwise_and(turn, jnp.int32(1))]

        @pl.when((out == 0) & has(old, TAKE) & (rank > 0))
        def _():
            left(gone, turn_pieces)

        @pl.when(has(word, TAKE))
        def _():
            is_back = back_of(turn)
            chunk = chunk_of(turn, is_back)
            index = chunk * half_pieces + out + (1 - is_back) * total
            here = acts.at[is_back, chunk, :, piece_at(side, out)]
            hand_on = remote(here, here, gone, take_recv.at[side, index], down(side))
            hand_on.wait_recv()

            @pl.when(rank > 0)
            def _():
                hand_on.start()

    def relay_step(side, step):
        rank = rank_of(side)
        place = step - (n_chunk + RELAY_START) * half_pieces - hop * (last_pos - rank)
        turn = turn_of(place) - MARGIN
        out = piece_of(place)
        half_turn = lax.bitwise_and(turn, jnp.int32(1))
        chunk = jnp.clip(turn, 0, n_relay - 1)
        here = acts.at[1, chunk, :, piece_at(side, out)]
        gone = rel_over.at[side, half_turn]
        hand_on = remote(here, here, rel_send.at[side, half_turn], rel_recv.at[side, chunk * half_pieces + out], down(side))

        @pl.when((out == 0) & (turn >= 2) & (turn < n_relay + 2))
        def _():
            @pl.when(rank > 0)
            def _():
                left(rel_send.at[side, half_turn], turn_pieces)

            left(gone, turn_pieces)

            @pl.when((turn == n_relay + 1) & (rank == last_pos))
            def _():
                pl.semaphore_signal(free_sem.at[side], inc=1, device_id={"stage": 1}, device_id_type=MESH)

        @pl.when((turn >= 0) & (turn < n_relay))
        def _():
            hand_on.wait_recv()

            @pl.when(rank > 0)
            def _():
                hand_on.start()

            remote(here, here, gone, rel_in.at[chunk], {"stage": fore_stage}).start()

    tile_rows, tile_cols = tile_buf.shape[1], tile_buf.shape[2]
    per_row = wts.shape[1] // tile_cols
    n_tiles = hid_dim // tile_rows * per_row

    def copy_tile(which, index):
        rows = pl.ds(pl.multiple_of(index // per_row * tile_rows, tile_rows), tile_rows)
        cols = pl.ds(pl.multiple_of(index % per_row * tile_cols, tile_cols), tile_cols)
        return pltpu.make_async_copy(tile_buf.at[index % 2], grad_hbm.at[which, rows, cols], tile_sem.at[index % 2])

    def grad_tile(number):
        for which, index in ((1, number), (0, number - n_tiles)):

            @pl.when((index >= 0) & (index < n_tiles))
            def _():
                rows = pl.ds(pl.multiple_of(index // per_row * tile_rows, tile_rows), tile_rows)
                cols = pl.ds(pl.multiple_of(index % per_row * tile_cols, tile_cols), tile_cols)

                @pl.when(number >= 2)
                def _():
                    copy_tile(which, index).wait()

                inputs, grads = (acts.at[0], hid.at[1]) if which == 0 else (hid.at[0], acts.at[1])
                lefts = inputs[0:n_grad, :, rows].reshape(n_grad * chunk_rows, tile_rows)
                rights = grads[0:n_grad, :, cols].reshape(n_grad * chunk_rows, tile_cols)
                tile_buf[index % 2] = lax.dot_general(lefts, rights, (((0,), (0,)), ((), ())), preferred_element_type=F32)
                copy_tile(which, index).start()

    in_loop = jnp.where(stage == 0, FIRST_TILES[0], jnp.where(stage == 1, NEXT_TILES[0], 0))
    pitch = jnp.where(stage == 0, FIRST_TILES[1], NEXT_TILES[1])
    first_tile = (n_first + n_grad) * half_pieces

    def loop_step(step, carry):
        for part in range(PARTS):
            first_product(step, part)

        @pl.when((step == 0) & (stage != fore_stage))
        def _():
            meet()

        gather_step(0, step)
        gather_step(1, step)
        sum_steps(step)

        @pl.when((stage == 0) & (step >= n_chunk * half_pieces))
        def _():
            relay_step(0, step)
            relay_step(1, step)

        take_step(0, step)
        take_step(1, step)
        since = step - first_tile

        @pl.when((since >= 0) & (since < in_loop * pitch) & (since % pitch == 0))
        def _():
            grad_tile(since // pitch)

        return carry

    lax.fori_loop(jnp.where(stage == fore_stage, -early, 1 - PARTS), n_steps, loop_step, 0)

    def next_tile(number, carry):
        grad_tile(number)
        return carry

    lax.fori_loop(in_loop, 2 * n_tiles, next_tile, 0)

    for side, owner in ((0, last_pos), (1, 0)):
        owns = (stage == last_stage) & (pos == owner)

        @pl.when(jnp.logical_not(owns))
        def _():
            loss_copy(side, 0, 0).wait_recv()

        @pl.when(owns)
        def _():
            for to_stage in range(n_stage):
                for to_pos in range(n_model):

                    @pl.when((to_stage != stage) | (to_pos != pos))
                    def _():
                        loss_copy(side, to_stage, to_pos).wait_send()

    loss_out[...] = jnp.full(loss_out.shape, jnp.sum(loss_in[0] + loss_in[1]) * (0.5 * grad_scale), F32)

    for index in (0, 1):
        copy_tile(0, index).wait()

    def end_out(chunk, carry):
        for kind in range(4):
            copy_out(kind, chunk).wait()
        return carry

    lax.fori_loop(n_grad, n_chunk, end_out, 0)


def finish_kernel(first_hbm, lefts_hbm, rights_hbm, grad_in, grad_out, sums, lefts, rights, sum_in, sum_out, operand_in):
    block = sums.shape[1]
    blocks = grad_in.shape[0] // block
    half = lefts.shape[1] // 2

    def copy_operands(which):
        pairs = ((rights_hbm, rights, 0), (lefts_hbm, lefts, 1))
        return [
            pltpu.make_async_copy(
                src.at[which, pl.ds(part * half, half), :], dst.at[which, pl.ds(part * half, half), :], operand_in.at[which, kind, part]
            )
            for src, dst, kind in pairs
            for part in (0, 1)
        ]

    def rows_of(number):
        return pl.ds(pl.multiple_of(number % blocks * block, block), block)

    def copy_first(number):
        return pltpu.make_async_copy(first_hbm.at[number // blocks, rows_of(number), :], sums.at[number], sum_in.at[number])

    def copy_result(number, which):
        return pltpu.make_async_copy(sums.at[number], (grad_in, grad_out)[which].at[rows_of(number), :], sum_out.at[number])

    for copy in copy_operands(0):
        copy.start()
    for number in range(IN_FLIGHT):
        copy_first(number).start()

    def one(number, carry):
        for which in (0, 1):

            @pl.when(number == which * blocks)
            def _():
                for copy in copy_operands(which):
                    copy.wait()

        @pl.when(number == 1)
        def _():
            for copy in copy_operands(1):
                copy.start()

        copy_first(number).wait()

        @pl.when(number + IN_FLIGHT < 2 * blocks)
        def _():
            copy_first(number + IN_FLIGHT).start()

        which = number // blocks
        part = lax.dot_general(
            lefts[which, :, rows_of(number)], rights[which], (((0,), (0,)), ((), ())), preferred_element_type=F32
        )
        sums[number] = sums[number] + part

        for kind in (0, 1):

            @pl.when(which == kind)
            def _():
                copy_result(number, kind).start()

        return carry

    lax.fori_loop(0, 2 * blocks, one, 0)

    def end(number, carry):
        copy_result(number, 0).wait()
        return carry

    lax.fori_loop(0, 2 * blocks, end, 0)


def finish_grads(first, lefts, rights):
    rows, dim = lefts.shape[1:]
    block = min(TILE_ROWS, dim)
    blocks = dim // block
    shape = jax.ShapeDtypeStruct((dim, dim), F32)
    any_space = pl.BlockSpec(memory_space=pl.ANY)
    dma = pltpu.SemaphoreType.DMA
    return pl.pallas_call(
        finish_kernel,
        out_shape=(shape, shape),
        in_specs=[any_space] * 3,
        out_specs=(any_space, any_space),
        scratch_shapes=[
            pltpu.VMEM((2 * blocks, block, dim), F32),
            pltpu.VMEM((2, rows, dim), BF16),
            pltpu.VMEM((2, rows, dim), BF16),
            dma((2 * blocks,)),
            dma((2 * blocks,)),
            dma((2, 2, 2)),
        ],
        compiler_params=pltpu.CompilerParams(vmem_limit_bytes=62 * 1024 * 1024),
        cost_estimate=pl.CostEstimate(flops=4 * rows * dim * dim, bytes_accessed=16 * dim * dim, transcendentals=0),
        name="finish_kernel",
    )(first, lefts, rights)


def solution(mesh):
    n_stage = mesh.shape["stage"]
    n_model = mesh.shape["model"]

    def stage_step(inputs, targets, w_in, w_out):
        num_micro, num_tokens, model_dim = inputs.shape
        hid_dim = w_in.shape[3]
        rows = num_micro * num_tokens
        chunk = min(CHUNK_TOKENS, num_tokens)
        n_chunk = rows // chunk
        piece = min(PIECE_COLS, model_dim // 2)
        half_pieces = model_dim // 2 // piece
        grad_scale = 1.0 / (rows * model_dim)
        lead = [n_chunk] * (n_stage - 2) + [min(PREV_LEAD, n_chunk), min(LAST_LEAD, n_chunk)]
        idle = [FIRST_IDLE] + [NEXT_IDLE] * (n_stage - 3) + [0, 0]
        n_fore, n_relay = min(FORE_CHUNKS, n_chunk - 1), min(RELAY_CHUNKS, n_chunk - 1)
        n_grad = min(FIRST_GRADS, n_chunk // 2)
        rest = rows - n_grad * chunk
        tile_rows, tile_cols = min(TILE_ROWS, hid_dim), min(TILE_COLS, model_dim)
        kernel = functools.partial(
            stage_kernel, n_stage, n_model, n_chunk, half_pieces, piece, HOP_LAG, lead, idle, n_fore, n_relay, n_grad, grad_scale
        )
        any_space = pl.BlockSpec(memory_space=pl.ANY)
        dma = pltpu.SemaphoreType.DMA
        lefts, rights, first_grads, loss = pl.pallas_call(
            kernel,
            out_shape=(
                jax.ShapeDtypeStruct((2, rest, model_dim), BF16),
                jax.ShapeDtypeStruct((2, rest, model_dim), BF16),
                jax.ShapeDtypeStruct((2, hid_dim, model_dim), F32),
                jax.ShapeDtypeStruct((8, 128), F32),
            ),
            in_specs=[any_space] * 4,
            out_specs=(any_space, any_space, any_space, pl.BlockSpec(memory_space=pltpu.VMEM)),
            scratch_shapes=[
                pltpu.VMEM((4, model_dim, hid_dim), BF16),
                pltpu.VMEM((2, n_chunk, chunk, model_dim), BF16),
                pltpu.VMEM((2, n_chunk, chunk, hid_dim), BF16),
                pltpu.VMEM((2, 2, half_pieces, chunk, piece), F32),
                pltpu.VMEM((2, RECV_SLOTS, chunk, piece), F32),
                pltpu.VMEM((8, 128), F32),
                pltpu.VMEM((2, 8, 128), F32),
                dma((PARTS + 1,)),
                dma((n_chunk,)),
                dma,
                dma((2, 2)),
                dma((2, RECV_SLOTS)),
                dma((2, 2)),
                dma((2, n_chunk * half_pieces)),
                dma((2, 2)),
                dma((2, 2)),
                dma((2, (n_chunk + n_fore) * half_pieces)),
                dma((2, 2)),
                dma((4, n_chunk)),
                dma((n_stage * n_model,)),
                dma((2,)),
                pltpu.SemaphoreType.REGULAR((2,)),
                dma((2, 2)),
                dma((2, 2)),
                dma((2, n_relay * half_pieces)),
                dma((n_relay,)),
                pltpu.SemaphoreType.REGULAR((2,)),
                pltpu.SMEM((2 * n_chunk + max(idle) + 2 * MARGIN,), jnp.int32),
                pltpu.VMEM((2, tile_rows, tile_cols), F32),
                dma((2,)),
                pltpu.VMEM((2, 2, half_pieces, chunk, piece), BF16),
            ],
            compiler_params=pltpu.CompilerParams(collective_id=0, has_side_effects=True, vmem_limit_bytes=63 * 1024 * 1024),
            name="stage_kernel",
        )(
            inputs.reshape(n_chunk, chunk, model_dim),
            targets.reshape(n_chunk, chunk, model_dim),
            w_in.reshape(model_dim, hid_dim),
            w_out.reshape(hid_dim, model_dim),
        )

        grad_in, grad_out = finish_grads(first_grads, lefts, rights)
        return grad_in[None, None], grad_out[None, None], loss[0, :1]

    return jax.shard_map(
        stage_step,
        mesh=mesh,
        in_specs=(P("data", None, None), P("data", None, None), P("stage", None, None, "model"), P("stage", None, "model", None)),
        out_specs=(P(("data", "stage"), None, None, "model"), P(("data", "stage"), None, "model", None), P("data")),
        check_vma=False,
    )
```

```python
import functools

import jax
import jax.numpy as jnp
from jax import lax
from jax.experimental import pallas as pl
from jax.experimental.pallas import tpu as pltpu
from jax.sharding import PartitionSpec as P

GELU_COEF = 0.7978845608028654
CUBIC_COEF = 0.044715

CHUNK_TOKENS = 64
PIECE_COLS = 256
HIDDEN_COLS = 512
PARTS = 2
HOP_LAG = 2
RECV_SLOTS = 8
LAST_LEAD = 5
PREV_LEAD = 16
FIRST_IDLE = 12
NEXT_IDLE = 7
FORE_CHUNKS = 6
RELAY_CHUNKS = 18
RELAY_START = 0

FIRST_GRADS = 12
TILE_ROWS = 256
TILE_COLS = 1024
IN_FLIGHT = 8
FIRST_TILES = (32, 1)
NEXT_TILES = (16, 3)

SUM, BACK, GATHER, EARLY, TAKE, FWD, BWD = 256, 512, 1024, 2048, 4096, 8192, 16384
MARGIN = 8

BF16 = jnp.bfloat16
F32 = jnp.float32
MESH = pl.DeviceIdType.MESH


def gelu_tanh(values):
    inner_arg = GELU_COEF * (values + CUBIC_COEF * values * values * values)
    return 0.5 * values * (1.0 + jnp.tanh(inner_arg))


def gelu_slope(values):
    tanh_val = jnp.tanh(GELU_COEF * (values + CUBIC_COEF * values * values * values))
    return 0.5 * (1.0 + tanh_val) + 0.5 * values * (1.0 - tanh_val * tanh_val) * GELU_COEF * (1.0 + 3.0 * CUBIC_COEF * values * values)


def dot_nn(left, right):
    return jnp.dot(left, right, preferred_element_type=F32)


def dot_nt(left, right):
    return lax.dot_general(left, right, (((1,), (1,)), ((), ())), preferred_element_type=F32)


def stage_kernel(
    n_stage, n_model, n_chunk, half_pieces, piece, hop, lead, idle, n_fore, n_relay, n_grad, grad_scale,
    inputs_hbm, targets_hbm, w1_hbm, w2_hbm,
    left_out, right_out, grad_hbm, loss_out,
    wts, acts, hid, send_buf, recv_buf, loss_acc, loss_in,
    w_sem, in_sem, tgt_sem, sum_send, sum_recv, gat_send, gat_recv, over_send, back_send, take_recv, down_send, out_sem,
    loss_send, loss_recv, spent_sem, rel_send, rel_over, rel_recv, rel_in, free_sem, table, tile_buf, tile_sem, end_buf,
):
    pos = lax.axis_index("model")
    stage = lax.axis_index("stage")
    last_pos = n_model - 1
    last_stage = n_stage - 1
    fore_stage = n_stage - 2
    bits = half_pieces.bit_length() - 1
    total = n_chunk * half_pieces
    half = half_pieces * piece
    hid_dim = wts.shape[2]
    chunk_rows = acts.shape[2]
    hid_part = hid_dim // PARTS
    hid_cols = min(HIDDEN_COLS, hid_part)
    n_lead, n_idle = jnp.int32(n_chunk), jnp.int32(0)
    for at in range(n_stage):
        n_lead = jnp.where(stage == at, lead[at], n_lead)
        n_idle = jnp.where(stage == at, idle[at], n_idle)
    turns = 2 * n_chunk + n_idle
    n_steps = turns * half_pieces + jnp.where(stage == 0, 1 - hop, half_pieces + hop * last_pos + 1)
    early = half_pieces + 3 * hop + 1

    barrier = pltpu.get_barrier_semaphore()
    for to_stage in range(n_stage):
        for to_pos in range(n_model):

            @pl.when((to_stage != stage) | (to_pos != pos))
            def _():
                pl.semaphore_signal(barrier, inc=1, device_id={"stage": to_stage, "model": to_pos}, device_id_type=MESH)

    copy_w2 = pltpu.make_async_copy(w2_hbm, wts.at[1], w_sem.at[PARTS])

    def copy_w1(part):
        cols = pl.ds(part * hid_part, hid_part)
        return pltpu.make_async_copy(w1_hbm.at[:, cols], wts.at[0, :, cols], w_sem.at[part])


    def copy_in(chunk):
        return pltpu.make_async_copy(inputs_hbm.at[chunk], acts.at[0, chunk], in_sem.at[chunk])

    def grad_in(chunk):
        return pltpu.make_async_copy(inputs_hbm.at[chunk], acts.at[1, chunk], rel_in.at[chunk])

    def copy_targets(side):
        cols = pl.ds(side * half, half)
        return pltpu.make_async_copy(targets_hbm.at[:, :, cols], acts.at[1, :, :, cols], tgt_sem)

    def copy_out(kind, chunk):
        src = (acts.at[0], hid.at[0], hid.at[1], acts.at[1])[kind]
        dst = (left_out.at[0], left_out.at[1], right_out.at[0], right_out.at[1])[kind]
        rows = pl.ds(pl.multiple_of((chunk - n_grad) * chunk_rows, chunk_rows), chunk_rows)
        return pltpu.make_async_copy(src.at[chunk], dst.at[rows, :], out_sem.at[kind, chunk])

    @pl.when(stage == 0)
    def _():
        copy_in(0).start()

    for part in range(PARTS):
        copy_w1(part).start()
    copy_w2.start()

    @pl.when(stage == 0)
    def _():
        def start_in(chunk, carry):
            copy_in(chunk).start()
            return carry

        lax.fori_loop(1, n_chunk, start_in, 0)

    @pl.when((stage == last_stage) & (pos == last_pos))
    def _():
        copy_targets(0).start()

    @pl.when((stage == last_stage) & (pos == 0))
    def _():
        copy_targets(1).start()

    def transpose_weights():
        tile = min(256, hid_dim)
        count = hid_dim // tile

        def one(index, carry):
            rows = pl.ds(pl.multiple_of((index // count) * tile, tile), tile)
            cols = pl.ds(pl.multiple_of((index % count) * tile, tile), tile)
            wts[2, cols, rows] = jnp.swapaxes(wts[1, rows, cols], 0, 1)
            wts[3, cols, rows] = jnp.swapaxes(wts[0, rows, cols], 0, 1)
            return carry

        lax.fori_loop(0, count * count, one, 0)

    n_mixed = 2 * (n_chunk - n_lead)
    n_after = 2 * n_chunk - n_lead
    n_first = n_lead + n_idle

    def fill(entry, carry):
        turn = entry - MARGIN
        after = turn - n_first
        pair = (after + 1024) // 2 - 512
        odd = (after + 1024) % 2 == 1
        mixed = (after >= 0) & (after < n_mixed)
        leads = (turn >= 0) & (turn < n_lead)
        fwd = leads | (mixed & odd)
        bwd = (after >= 0) & (after < n_after) & jnp.logical_not(mixed & odd)
        chunk = jnp.where(leads, turn, jnp.where(odd, n_lead + pair, pair))
        chunk = jnp.where(bwd & (after >= n_mixed), after - (n_chunk - n_lead), chunk)
        early_one = fwd & (stage == fore_stage - 1) & (chunk < n_fore)
        back = bwd & (stage < last_stage) & ((stage < fore_stage) | (chunk >= n_relay))
        take = back | (fwd & (stage == fore_stage) & (chunk < n_fore))
        word = jnp.int32(0)
        for flag, bit in (
            (fwd | (bwd & (stage > 0)), SUM),
            (bwd, BACK),
            (fwd & jnp.logical_not(early_one), GATHER),
            (early_one, EARLY),
            (take, TAKE),
            (fwd, FWD),
            (bwd, BWD),
        ):
            word = word + jnp.where(flag, bit, 0)
        table[entry] = word
        return carry

    lax.fori_loop(0, table.shape[0], fill, 0)
    loss_acc[...] = jnp.zeros_like(loss_acc)
    copy_w1(0).wait()

    @pl.when(stage > 0)
    def _():
        for part in range(1, PARTS):
            copy_w1(part).wait()
        copy_w2.wait()
        transpose_weights()

    def meet():
        pl.semaphore_wait(barrier, n_stage * n_model - 1)

    @pl.when(stage == fore_stage)
    def _():
        meet()


    def turn_of(place):
        return lax.shift_right_logical(place + MARGIN * half_pieces, jnp.int32(bits))

    def piece_of(place):
        return lax.bitwise_and(place + MARGIN * half_pieces, jnp.int32(half_pieces - 1))

    def has(word, mask):
        return lax.bitwise_and(word, jnp.int32(mask)) != 0

    def fwd_chunk(turn):
        after = turn - (n_first + MARGIN)
        return jnp.where(turn < n_lead + MARGIN, turn - MARGIN, n_lead + lax.shift_right_arithmetic(after, jnp.int32(1)))

    def bwd_chunk(turn):
        after = turn - (n_first + MARGIN)
        return jnp.where(after < n_mixed, lax.shift_right_arithmetic(after, jnp.int32(1)), after - (n_chunk - n_lead))

    def back_of(turn):
        after = turn - (n_first + MARGIN)
        odd = lax.bitwise_and(after, jnp.int32(1)) == 1
        return ((after >= 0) & jnp.logical_not((after < n_mixed) & odd)).astype(jnp.int32)

    def chunk_of(turn, is_back):
        return jnp.clip(jnp.where(is_back == 1, bwd_chunk(turn), fwd_chunk(turn)), 0, n_chunk - 1)

    def piece_at(side, index):
        col = side * half + index * piece
        return pl.ds(pl.multiple_of(col, piece), piece)

    def remote(src, dst, send_sem, recv_sem, device):
        return pltpu.make_async_remote_copy(
            src_ref=src, dst_ref=dst, send_sem=send_sem, recv_sem=recv_sem, device_id=device, device_id_type=MESH
        )

    def left(send_sem, like):
        remote(like, like, send_sem, loss_recv.at[0], {"model": pos}).wait_send()

    turn_pieces = acts.at[0, 0, :, pl.ds(0, half)]
    turn_sums = send_buf.at[0, 0]

    def rank_of(side):
        return pos if side == 0 else last_pos - pos

    def up(side):
        return {"model": pos + 1 if side == 0 else pos - 1}

    def down(side):
        return {"model": pos - 1 if side == 0 else pos + 1}

    def first_product(step, part):
        place = step + PARTS - 1 - part
        turn = turn_of(place)
        word = table[turn]
        starts = piece_of(place) == 0

        @pl.when(starts & has(word, FWD))
        def _():
            chunk = fwd_chunk(turn)
            if part == 0:

                @pl.when((stage != fore_stage) | (chunk >= n_fore))
                def _():
                    copy_in(chunk).wait()

                @pl.when(chunk >= n_grad)
                def _():
                    copy_out(0, chunk).start()

            else:

                @pl.when((stage == 0) & (place == 0))
                def _():
                    copy_w1(part).wait()

            for col in range(part * hid_part, (part + 1) * hid_part, hid_cols):
                cols = pl.ds(col, hid_cols)
                pre = dot_nn(acts[0, chunk], wts[0, :, cols]).astype(BF16)
                hid[1, chunk, :, cols] = pre
                hid[0, chunk, :, cols] = gelu_tanh(pre.astype(F32)).astype(BF16)
            if part == PARTS - 1:

                @pl.when(chunk >= n_grad)
                def _():
                    copy_out(1, chunk).start()

                @pl.when((stage == 0) & (place == 0))
                def _():
                    copy_w2.wait()

        @pl.when(starts & has(word, BWD))
        def _():
            chunk = bwd_chunk(turn)
            if part == 0:

                @pl.when((stage == fore_stage) & (chunk < n_relay))
                def _():
                    grad_in(chunk).wait()

                @pl.when(chunk >= n_grad)
                def _():
                    copy_out(3, chunk).start()

            for col in range(part * hid_part, (part + 1) * hid_part, hid_cols):
                cols = pl.ds(col, hid_cols)
                grad_act = dot_nn(acts[1, chunk], wts[2, :, cols]).astype(BF16)
                slope = gelu_slope(hid[1, chunk, :, cols].astype(F32))
                hid[1, chunk, :, cols] = (slope * grad_act.astype(F32)).astype(BF16)
            if part == PARTS - 1:

                @pl.when(chunk >= n_grad)
                def _():
                    copy_out(2, chunk).start()

        if part == 0:

            @pl.when((stage == 0) & (place == n_lead * half_pieces))
            def _():
                transpose_weights()

    def loss_copy(side, to_stage, to_pos):
        return remote(
            loss_acc, loss_in.at[side], loss_send.at[to_stage * n_model + to_pos], loss_recv.at[side],
            {"stage": to_stage, "model": to_pos},
        )

    def send_loss(side):
        loss_in[side] = loss_acc[...]
        for to_stage in range(n_stage):
            for to_pos in range(n_model):

                @pl.when((to_stage != stage) | (to_pos != pos))
                def _():
                    loss_copy(side, to_stage, to_pos).start()

    def sum_steps(step):
        now = []
        for side in (0, 1):
            rank = rank_of(side)
            place = step - hop * rank
            turn = turn_of(place)
            word, old = table[turn], table[turn - 2]
            index = piece_of(place)
            half_turn = lax.bitwise_and(turn, jnp.int32(1))
            inn = lax.bitwise_and(place + MARGIN * half_pieces, jnp.int32(RECV_SLOTS - 1))
            sums = has(word, SUM)
            is_back = back_of(turn)
            now.append((rank, word, sums, is_back, chunk_of(turn, is_back), index, half_turn, inn, piece_at(side, index)))

            @pl.when((index == 0) & has(old, SUM))
            def _():
                @pl.when(rank < last_pos)
                def _():
                    left(sum_send.at[side, half_turn], turn_sums)

                @pl.when((rank == last_pos) & has(old, BACK))
                def _():
                    left(down_send.at[side, half_turn], turn_pieces)

        @pl.when(now[0][2] | now[1][2])
        def _():
            for side in (0, 1):
                _, _, _, is_back, chunk, index, half_turn, _, cols = now[side]
                send_buf[side, half_turn, index] = dot_nn(hid[is_back, chunk], wts[1 + 2 * is_back, :, cols])

        for side in (0, 1):
            rank, word, sums, is_back, chunk, out, half_turn, inn, cols = now[side]
            bwd = has(word, BACK)
            index = chunk * half_pieces + out
            mine = send_buf.at[side, half_turn, out]
            gone = down_send.at[side, half_turn]
            hand_on = remote(mine, recv_buf.at[side, inn], sum_send.at[side, half_turn], sum_recv.at[side, inn], up(side))

            @pl.when(sums & (rank > 0))
            def _():
                hand_on.wait_recv()
                mine[...] = mine[...] + recv_buf[side, inn]

            @pl.when(sums & (rank < last_pos))
            def _():
                hand_on.start()

            @pl.when(sums & (rank == last_pos))
            def _():
                whole = acts[is_back, chunk, :, cols].astype(F32) + mine[...]
                scored = has(word, FWD) & (stage == last_stage)

                @pl.when(scored)
                def _():
                    @pl.when(index == 0)
                    def _():
                        copy_targets(side).wait()

                    err = whole.astype(BF16).astype(F32) - acts[1, chunk, :, cols].astype(F32)
                    acts[1, chunk, :, cols] = (err * grad_scale).astype(BF16)
                    square = jnp.sum((err * err).reshape(err.shape[0] // 8, 8, piece), axis=0)
                    part = square[:, :128]
                    for lane in range(1, piece // 128):
                        part = part + square[:, lane * 128 : (lane + 1) * 128]
                    loss_acc[...] = loss_acc[...] + part

                    @pl.when(index == total - 1)
                    def _():
                        send_loss(side)

                @pl.when(has(word, FWD) & (stage < last_stage))
                def _():
                    acts[1, chunk, :, cols] = whole.astype(BF16)

                ended = end_buf.at[side, half_turn, out]

                @pl.when(bwd)
                def _():
                    ended[...] = whole.astype(BF16)

                @pl.when(bwd & (index == total - 2 * half_pieces))
                def _():
                    pl.semaphore_wait(spent_sem.at[side], 1)

                @pl.when(bwd & (stage == 1) & (index == (n_relay - 2) * half_pieces))
                def _():
                    pl.semaphore_wait(free_sem.at[side], 1)

                relayed = (stage == last_stage) & (chunk < n_relay)
                there = acts.at[1, chunk, :, cols]

                @pl.when(bwd & relayed)
                def _():
                    arrived = rel_recv.at[side, jnp.minimum(index, n_relay * half_pieces - 1)]
                    remote(ended, there, gone, arrived, {"stage": 0}).start()

                @pl.when(bwd & jnp.logical_not(relayed))
                def _():
                    arrived = take_recv.at[side, index]
                    remote(ended, there, gone, arrived, {"stage": stage - 1}).start()

    def gather_step(side, step):
        rank = rank_of(side)
        place = step - 1 - 3 * hop - hop * (last_pos - rank)
        turn = turn_of(place)
        word, old = table[turn], table[turn - 2]
        out = piece_of(place)
        half_turn = lax.bitwise_and(turn, jnp.int32(1))
        chunk = jnp.clip(fwd_chunk(turn), 0, n_chunk - 1)
        index = chunk * half_pieces + out
        cols = piece_at(side, out)
        here = acts.at[1, chunk, :, cols]
        gone = over_send.at[side, half_turn]

        @pl.when((out == 0) & has(old, GATHER | EARLY))
        def _():
            @pl.when(has(old, GATHER) & (rank > 0))
            def _():
                left(gat_send.at[side, half_turn], turn_pieces)

            @pl.when((stage < last_stage) & (has(old, GATHER) | (rank == last_pos)))
            def _():
                left(gone, turn_pieces)

                @pl.when((fwd_chunk(turn - 2) == n_chunk - 1) & (rank == last_pos))
                def _():
                    pl.semaphore_signal(spent_sem.at[side], inc=1, device_id={"stage": stage + 1}, device_id_type=MESH)

        @pl.when(has(word, GATHER))
        def _():
            hand_on = remote(here, here, gat_send.at[side, half_turn], gat_recv.at[side, index], down(side))

            @pl.when(rank < last_pos)
            def _():
                hand_on.wait_recv()

            @pl.when(rank > 0)
            def _():
                hand_on.start()

            @pl.when(stage < last_stage)
            def _():
                remote(here, acts.at[0, chunk, :, cols], gone, in_sem.at[chunk], {"stage": stage + 1}).start()

        @pl.when(has(word, EARLY) & (rank == last_pos))
        def _():
            arrived = take_recv.at[side, jnp.minimum(total + index, total + n_fore * half_pieces - 1)]
            remote(here, acts.at[0, chunk, :, cols], gone, arrived, {"stage": stage + 1}).start()

    def take_step(side, step):
        rank = rank_of(side)
        place = step + early - hop * (last_pos - rank)
        turn = turn_of(place)
        word, old = table[turn], table[turn - 2]
        out = piece_of(place)
        gone = back_send.at[side, lax.bitwise_and(turn, jnp.int32(1))]

        @pl.when((out == 0) & has(old, TAKE) & (rank > 0))
        def _():
            left(gone, turn_pieces)

        @pl.when(has(word, TAKE))
        def _():
            is_back = back_of(turn)
            chunk = chunk_of(turn, is_back)
            index = chunk * half_pieces + out + (1 - is_back) * total
            here = acts.at[is_back, chunk, :, piece_at(side, out)]
            hand_on = remote(here, here, gone, take_recv.at[side, index], down(side))
            hand_on.wait_recv()

            @pl.when(rank > 0)
            def _():
                hand_on.start()

    def relay_step(side, step):
        rank = rank_of(side)
        place = step - (n_chunk + RELAY_START) * half_pieces - hop * (last_pos - rank)
        turn = turn_of(place) - MARGIN
        out = piece_of(place)
        half_turn = lax.bitwise_and(turn, jnp.int32(1))
        chunk = jnp.clip(turn, 0, n_relay - 1)
        here = acts.at[1, chunk, :, piece_at(side, out)]
        gone = rel_over.at[side, half_turn]
        hand_on = remote(here, here, rel_send.at[side, half_turn], rel_recv.at[side, chunk * half_pieces + out], down(side))

        @pl.when((out == 0) & (turn >= 2) & (turn < n_relay + 2))
        def _():
            @pl.when(rank > 0)
            def _():
                left(rel_send.at[side, half_turn], turn_pieces)

            left(gone, turn_pieces)

            @pl.when((turn == n_relay + 1) & (rank == last_pos))
            def _():
                pl.semaphore_signal(free_sem.at[side], inc=1, device_id={"stage": 1}, device_id_type=MESH)

        @pl.when((turn >= 0) & (turn < n_relay))
        def _():
            hand_on.wait_recv()

            @pl.when(rank > 0)
            def _():
                hand_on.start()

            remote(here, here, gone, rel_in.at[chunk], {"stage": fore_stage}).start()

    tile_rows, tile_cols = tile_buf.shape[1], tile_buf.shape[2]
    per_row = wts.shape[1] // tile_cols
    n_tiles = hid_dim // tile_rows * per_row

    def copy_tile(which, index):
        rows = pl.ds(pl.multiple_of(index // per_row * tile_rows, tile_rows), tile_rows)
        cols = pl.ds(pl.multiple_of(index % per_row * tile_cols, tile_cols), tile_cols)
        return pltpu.make_async_copy(tile_buf.at[index % 2], grad_hbm.at[which, rows, cols], tile_sem.at[index % 2])

    def grad_tile(number):
        for which, index in ((1, number), (0, number - n_tiles)):

            @pl.when((index >= 0) & (index < n_tiles))
            def _():
                rows = pl.ds(pl.multiple_of(index // per_row * tile_rows, tile_rows), tile_rows)
                cols = pl.ds(pl.multiple_of(index % per_row * tile_cols, tile_cols), tile_cols)

                @pl.when(number >= 2)
                def _():
                    copy_tile(which, index).wait()

                inputs, grads = (acts.at[0], hid.at[1]) if which == 0 else (hid.at[0], acts.at[1])
                lefts = inputs[0:n_grad, :, rows].reshape(n_grad * chunk_rows, tile_rows)
                rights = grads[0:n_grad, :, cols].reshape(n_grad * chunk_rows, tile_cols)
                tile_buf[index % 2] = lax.dot_general(lefts, rights, (((0,), (0,)), ((), ())), preferred_element_type=F32)
                copy_tile(which, index).start()

    in_loop = jnp.where(stage == 0, FIRST_TILES[0], jnp.where(stage == 1, NEXT_TILES[0], 0))
    pitch = jnp.where(stage == 0, FIRST_TILES[1], NEXT_TILES[1])
    first_tile = (n_first + n_grad) * half_pieces

    def loop_step(step, carry):
        for part in range(PARTS):
            first_product(step, part)

        @pl.when((step == 0) & (stage != fore_stage))
        def _():
            meet()

        gather_step(0, step)
        gather_step(1, step)
        sum_steps(step)

        @pl.when((stage == 0) & (step >= n_chunk * half_pieces))
        def _():
            relay_step(0, step)
            relay_step(1, step)

        take_step(0, step)
        take_step(1, step)
        since = step - first_tile

        @pl.when((since >= 0) & (since < in_loop * pitch) & (since % pitch == 0))
        def _():
            grad_tile(since // pitch)

        return carry

    lax.fori_loop(jnp.where(stage == fore_stage, -early, 1 - PARTS), n_steps, loop_step, 0)

    def next_tile(number, carry):
        grad_tile(number)
        return carry

    lax.fori_loop(in_loop, 2 * n_tiles, next_tile, 0)

    for side, owner in ((0, last_pos), (1, 0)):
        owns = (stage == last_stage) & (pos == owner)

        @pl.when(jnp.logical_not(owns))
        def _():
            loss_copy(side, 0, 0).wait_recv()

        @pl.when(owns)
        def _():
            for to_stage in range(n_stage):
                for to_pos in range(n_model):

                    @pl.when((to_stage != stage) | (to_pos != pos))
                    def _():
                        loss_copy(side, to_stage, to_pos).wait_send()

    loss_out[...] = jnp.full(loss_out.shape, jnp.sum(loss_in[0] + loss_in[1]) * (0.5 * grad_scale), F32)

    for index in (0, 1):
        copy_tile(0, index).wait()

    def end_out(chunk, carry):
        for kind in range(4):
            copy_out(kind, chunk).wait()
        return carry

    lax.fori_loop(n_grad, n_chunk, end_out, 0)


def finish_kernel(
    first_hbm, lefts_hbm, rights_hbm, loss_hbm, grad_in, grad_out, loss_out, sums, lefts, rights, loss, sum_in, sum_out, operand_in, loss_sem
):
    block = sums.shape[1]
    blocks = grad_in.shape[0] // block
    half = lefts.shape[1] // 2

    def copy_operands(which):
        pairs = ((rights_hbm, rights, 0), (lefts_hbm, lefts, 1))
        return [
            pltpu.make_async_copy(
                src.at[which, pl.ds(part * half, half), :], dst.at[which, pl.ds(part * half, half), :], operand_in.at[which, kind, part]
            )
            for src, dst, kind in pairs
            for part in (0, 1)
        ]

    def rows_of(number):
        return pl.ds(pl.multiple_of(number % blocks * block, block), block)

    def copy_first(number):
        return pltpu.make_async_copy(first_hbm.at[number // blocks, rows_of(number), :], sums.at[number], sum_in.at[number])

    def copy_result(number, which):
        return pltpu.make_async_copy(sums.at[number], (grad_in, grad_out)[which].at[rows_of(number), :], sum_out.at[number])

    copy_loss = pltpu.make_async_copy(loss_hbm, loss, loss_sem)
    for copy in copy_operands(0):
        copy.start()
    for number in range(IN_FLIGHT):
        copy_first(number).start()
    copy_loss.start()

    def one(number, carry):
        for which in (0, 1):

            @pl.when(number == which * blocks)
            def _():
                for copy in copy_operands(which):
                    copy.wait()

        @pl.when(number == 1)
        def _():
            for copy in copy_operands(1):
                copy.start()

        copy_first(number).wait()

        @pl.when(number + IN_FLIGHT < 2 * blocks)
        def _():
            copy_first(number + IN_FLIGHT).start()

        which = number // blocks
        part = lax.dot_general(
            lefts[which, :, rows_of(number)], rights[which], (((0,), (0,)), ((), ())), preferred_element_type=F32
        )
        sums[number] = sums[number] + part

        for kind in (0, 1):

            @pl.when(which == kind)
            def _():
                copy_result(number, kind).start()

        return carry

    lax.fori_loop(0, 2 * blocks, one, 0)
    copy_loss.wait()
    loss_out[0] = loss[0, 0]

    def end(number, carry):
        copy_result(number, 0).wait()
        return carry

    lax.fori_loop(0, 2 * blocks, end, 0)


def finish_grads(first, lefts, rights, loss):
    rows, dim = lefts.shape[1:]
    block = min(TILE_ROWS, dim)
    blocks = dim // block
    shape = jax.ShapeDtypeStruct((dim, dim), F32)
    any_space = pl.BlockSpec(memory_space=pl.ANY)
    dma = pltpu.SemaphoreType.DMA
    return pl.pallas_call(
        finish_kernel,
        out_shape=(shape, shape, jax.ShapeDtypeStruct((1,), F32)),
        in_specs=[any_space] * 4,
        out_specs=(any_space, any_space, pl.BlockSpec(memory_space=pltpu.SMEM)),
        scratch_shapes=[
            pltpu.VMEM((2 * blocks, block, dim), F32),
            pltpu.VMEM((2, rows, dim), BF16),
            pltpu.VMEM((2, rows, dim), BF16),
            pltpu.VMEM(loss.shape, F32),
            dma((2 * blocks,)),
            dma((2 * blocks,)),
            dma((2, 2, 2)),
            dma,
        ],
        compiler_params=pltpu.CompilerParams(vmem_limit_bytes=62 * 1024 * 1024),
        cost_estimate=pl.CostEstimate(flops=4 * rows * dim * dim, bytes_accessed=16 * dim * dim, transcendentals=0),
        name="finish_kernel",
    )(first, lefts, rights, loss)


def solution(mesh):
    n_stage = mesh.shape["stage"]
    n_model = mesh.shape["model"]

    def stage_step(inputs, targets, w_in, w_out):
        num_micro, num_tokens, model_dim = inputs.shape
        hid_dim = w_in.shape[3]
        rows = num_micro * num_tokens
        chunk = min(CHUNK_TOKENS, num_tokens)
        n_chunk = rows // chunk
        piece = min(PIECE_COLS, model_dim // 2)
        half_pieces = model_dim // 2 // piece
        grad_scale = 1.0 / (rows * model_dim)
        lead = [n_chunk] * (n_stage - 2) + [min(PREV_LEAD, n_chunk), min(LAST_LEAD, n_chunk)]
        idle = [FIRST_IDLE] + [NEXT_IDLE] * (n_stage - 3) + [0, 0]
        n_fore, n_relay = min(FORE_CHUNKS, n_chunk - 1), min(RELAY_CHUNKS, n_chunk - 1)
        n_grad = min(FIRST_GRADS, n_chunk // 2)
        rest = rows - n_grad * chunk
        tile_rows, tile_cols = min(TILE_ROWS, hid_dim), min(TILE_COLS, model_dim)
        kernel = functools.partial(
            stage_kernel, n_stage, n_model, n_chunk, half_pieces, piece, HOP_LAG, lead, idle, n_fore, n_relay, n_grad, grad_scale
        )
        any_space = pl.BlockSpec(memory_space=pl.ANY)
        dma = pltpu.SemaphoreType.DMA
        lefts, rights, first_grads, loss = pl.pallas_call(
            kernel,
            out_shape=(
                jax.ShapeDtypeStruct((2, rest, model_dim), BF16),
                jax.ShapeDtypeStruct((2, rest, model_dim), BF16),
                jax.ShapeDtypeStruct((2, hid_dim, model_dim), F32),
                jax.ShapeDtypeStruct((8, 128), F32),
            ),
            in_specs=[any_space] * 4,
            out_specs=(any_space, any_space, any_space, pl.BlockSpec(memory_space=pltpu.VMEM)),
            scratch_shapes=[
                pltpu.VMEM((4, model_dim, hid_dim), BF16),
                pltpu.VMEM((2, n_chunk, chunk, model_dim), BF16),
                pltpu.VMEM((2, n_chunk, chunk, hid_dim), BF16),
                pltpu.VMEM((2, 2, half_pieces, chunk, piece), F32),
                pltpu.VMEM((2, RECV_SLOTS, chunk, piece), F32),
                pltpu.VMEM((8, 128), F32),
                pltpu.VMEM((2, 8, 128), F32),
                dma((PARTS + 1,)),
                dma((n_chunk,)),
                dma,
                dma((2, 2)),
                dma((2, RECV_SLOTS)),
                dma((2, 2)),
                dma((2, n_chunk * half_pieces)),
                dma((2, 2)),
                dma((2, 2)),
                dma((2, (n_chunk + n_fore) * half_pieces)),
                dma((2, 2)),
                dma((4, n_chunk)),
                dma((n_stage * n_model,)),
                dma((2,)),
                pltpu.SemaphoreType.REGULAR((2,)),
                dma((2, 2)),
                dma((2, 2)),
                dma((2, n_relay * half_pieces)),
                dma((n_relay,)),
                pltpu.SemaphoreType.REGULAR((2,)),
                pltpu.SMEM((2 * n_chunk + max(idle) + 2 * MARGIN,), jnp.int32),
                pltpu.VMEM((2, tile_rows, tile_cols), F32),
                dma((2,)),
                pltpu.VMEM((2, 2, half_pieces, chunk, piece), BF16),
            ],
            compiler_params=pltpu.CompilerParams(collective_id=0, has_side_effects=True, vmem_limit_bytes=63 * 1024 * 1024),
            name="stage_kernel",
        )(
            inputs.reshape(n_chunk, chunk, model_dim),
            targets.reshape(n_chunk, chunk, model_dim),
            w_in.reshape(model_dim, hid_dim),
            w_out.reshape(hid_dim, model_dim),
        )

        grad_in, grad_out, loss = finish_grads(first_grads, lefts, rights, loss)
        return grad_in[None, None], grad_out[None, None], loss

    return jax.shard_map(
        stage_step,
        mesh=mesh,
        in_specs=(P("data", None, None), P("data", None, None), P("stage", None, None, "model"), P("stage", None, "model", None)),
        out_specs=(P(("data", "stage"), None, None, "model"), P(("data", "stage"), None, "model", None), P("data")),
        check_vma=False,
    )
```

```python
import functools

import jax
import jax.numpy as jnp
from jax import lax
from jax.experimental import pallas as pl
from jax.experimental.pallas import tpu as pltpu
from jax.sharding import PartitionSpec as P

GELU_COEF = 0.7978845608028654
CUBIC_COEF = 0.044715

CHUNK_TOKENS = 64
PIECE_COLS = 256
HIDDEN_COLS = 512
PARTS = 2
HOP_LAG = 2
RECV_SLOTS = 8
LAST_LEAD = 5
PREV_LEAD = 16
FIRST_IDLE = 12
NEXT_IDLE = 7
FORE_CHUNKS = 6
RELAY_CHUNKS = 18
RELAY_START = 0

FIRST_GRADS = 12
TILE_ROWS = 256
TILE_COLS = 1024
IN_FLIGHT = 6
AT_START = 2
FIRST_TILES = (32, 1)
NEXT_TILES = (24, 2)

SUM, BACK, GATHER, EARLY, TAKE, FWD, BWD = 256, 512, 1024, 2048, 4096, 8192, 16384
MARGIN = 8

BF16 = jnp.bfloat16
F32 = jnp.float32
MESH = pl.DeviceIdType.MESH


def gelu_tanh(values):
    inner_arg = GELU_COEF * (values + CUBIC_COEF * values * values * values)
    return 0.5 * values * (1.0 + jnp.tanh(inner_arg))


def gelu_slope(values):
    tanh_val = jnp.tanh(GELU_COEF * (values + CUBIC_COEF * values * values * values))
    return 0.5 * (1.0 + tanh_val) + 0.5 * values * (1.0 - tanh_val * tanh_val) * GELU_COEF * (1.0 + 3.0 * CUBIC_COEF * values * values)


def dot_nn(left, right):
    return jnp.dot(left, right, preferred_element_type=F32)


def dot_nt(left, right):
    return lax.dot_general(left, right, (((1,), (1,)), ((), ())), preferred_element_type=F32)


def stage_kernel(
    n_stage, n_model, n_chunk, half_pieces, piece, hop, lead, idle, n_fore, n_relay, n_grad, grad_scale,
    inputs_hbm, targets_hbm, w1_hbm, w2_hbm,
    left_out, right_out, grad_hbm, loss_out,
    wts, acts, hid, send_buf, recv_buf, loss_acc, loss_in,
    w_sem, in_sem, tgt_sem, sum_send, sum_recv, gat_send, gat_recv, over_send, back_send, take_recv, down_send, out_sem,
    loss_send, loss_recv, spent_sem, rel_send, rel_over, rel_recv, rel_in, free_sem, table, tile_buf, tile_sem, end_buf,
):
    pos = lax.axis_index("model")
    stage = lax.axis_index("stage")
    last_pos = n_model - 1
    last_stage = n_stage - 1
    fore_stage = n_stage - 2
    bits = half_pieces.bit_length() - 1
    total = n_chunk * half_pieces
    half = half_pieces * piece
    hid_dim = wts.shape[2]
    chunk_rows = acts.shape[2]
    hid_part = hid_dim // PARTS
    hid_cols = min(HIDDEN_COLS, hid_part)
    n_lead, n_idle = jnp.int32(n_chunk), jnp.int32(0)
    for at in range(n_stage):
        n_lead = jnp.where(stage == at, lead[at], n_lead)
        n_idle = jnp.where(stage == at, idle[at], n_idle)
    turns = 2 * n_chunk + n_idle
    n_steps = turns * half_pieces + jnp.where(stage == 0, 1 - hop, half_pieces + hop * last_pos + 1)
    early = half_pieces + 3 * hop + 1

    barrier = pltpu.get_barrier_semaphore()
    for to_stage in range(n_stage):
        for to_pos in range(n_model):

            @pl.when((to_stage != stage) | (to_pos != pos))
            def _():
                pl.semaphore_signal(barrier, inc=1, device_id={"stage": to_stage, "model": to_pos}, device_id_type=MESH)

    copy_w2 = pltpu.make_async_copy(w2_hbm, wts.at[1], w_sem.at[PARTS])

    def copy_w1(part):
        cols = pl.ds(part * hid_part, hid_part)
        return pltpu.make_async_copy(w1_hbm.at[:, cols], wts.at[0, :, cols], w_sem.at[part])


    def copy_in(chunk):
        return pltpu.make_async_copy(inputs_hbm.at[chunk], acts.at[0, chunk], in_sem.at[chunk])

    def grad_in(chunk):
        return pltpu.make_async_copy(inputs_hbm.at[chunk], acts.at[1, chunk], rel_in.at[chunk])

    def copy_targets(side):
        cols = pl.ds(side * half, half)
        return pltpu.make_async_copy(targets_hbm.at[:, :, cols], acts.at[1, :, :, cols], tgt_sem)

    def copy_out(kind, chunk):
        src = (acts.at[0], hid.at[0], hid.at[1], acts.at[1])[kind]
        dst = (left_out.at[0], left_out.at[1], right_out.at[0], right_out.at[1])[kind]
        rows = pl.ds(pl.multiple_of((chunk - n_grad) * chunk_rows, chunk_rows), chunk_rows)
        return pltpu.make_async_copy(src.at[chunk], dst.at[rows, :], out_sem.at[kind, chunk])

    @pl.when(stage == 0)
    def _():
        copy_in(0).start()

    for part in range(PARTS):
        copy_w1(part).start()
    copy_w2.start()

    @pl.when(stage == 0)
    def _():
        def start_in(chunk, carry):
            copy_in(chunk).start()
            return carry

        lax.fori_loop(1, n_chunk, start_in, 0)

    @pl.when((stage == last_stage) & (pos == last_pos))
    def _():
        copy_targets(0).start()

    @pl.when((stage == last_stage) & (pos == 0))
    def _():
        copy_targets(1).start()

    def transpose_weights():
        tile = min(256, hid_dim)
        count = hid_dim // tile

        def one(index, carry):
            rows = pl.ds(pl.multiple_of((index // count) * tile, tile), tile)
            cols = pl.ds(pl.multiple_of((index % count) * tile, tile), tile)
            wts[2, cols, rows] = jnp.swapaxes(wts[1, rows, cols], 0, 1)
            wts[3, cols, rows] = jnp.swapaxes(wts[0, rows, cols], 0, 1)
            return carry

        lax.fori_loop(0, count * count, one, 0)

    n_mixed = 2 * (n_chunk - n_lead)
    n_after = 2 * n_chunk - n_lead
    n_first = n_lead + n_idle

    def fill(entry, carry):
        turn = entry - MARGIN
        after = turn - n_first
        pair = (after + 1024) // 2 - 512
        odd = (after + 1024) % 2 == 1
        mixed = (after >= 0) & (after < n_mixed)
        leads = (turn >= 0) & (turn < n_lead)
        fwd = leads | (mixed & odd)
        bwd = (after >= 0) & (after < n_after) & jnp.logical_not(mixed & odd)
        chunk = jnp.where(leads, turn, jnp.where(odd, n_lead + pair, pair))
        chunk = jnp.where(bwd & (after >= n_mixed), after - (n_chunk - n_lead), chunk)
        early_one = fwd & (stage == fore_stage - 1) & (chunk < n_fore)
        back = bwd & (stage < last_stage) & ((stage < fore_stage) | (chunk >= n_relay))
        take = back | (fwd & (stage == fore_stage) & (chunk < n_fore))
        word = jnp.int32(0)
        for flag, bit in (
            (fwd | (bwd & (stage > 0)), SUM),
            (bwd, BACK),
            (fwd & jnp.logical_not(early_one), GATHER),
            (early_one, EARLY),
            (take, TAKE),
            (fwd, FWD),
            (bwd, BWD),
        ):
            word = word + jnp.where(flag, bit, 0)
        table[entry] = word
        return carry

    lax.fori_loop(0, table.shape[0], fill, 0)
    loss_acc[...] = jnp.zeros_like(loss_acc)
    copy_w1(0).wait()

    @pl.when(stage > 0)
    def _():
        for part in range(1, PARTS):
            copy_w1(part).wait()
        copy_w2.wait()
        transpose_weights()

    def meet():
        pl.semaphore_wait(barrier, n_stage * n_model - 1)

    @pl.when(stage == fore_stage)
    def _():
        meet()


    def turn_of(place):
        return lax.shift_right_logical(place + MARGIN * half_pieces, jnp.int32(bits))

    def piece_of(place):
        return lax.bitwise_and(place + MARGIN * half_pieces, jnp.int32(half_pieces - 1))

    def has(word, mask):
        return lax.bitwise_and(word, jnp.int32(mask)) != 0

    def fwd_chunk(turn):
        after = turn - (n_first + MARGIN)
        return jnp.where(turn < n_lead + MARGIN, turn - MARGIN, n_lead + lax.shift_right_arithmetic(after, jnp.int32(1)))

    def bwd_chunk(turn):
        after = turn - (n_first + MARGIN)
        return jnp.where(after < n_mixed, lax.shift_right_arithmetic(after, jnp.int32(1)), after - (n_chunk - n_lead))

    def back_of(turn):
        after = turn - (n_first + MARGIN)
        odd = lax.bitwise_and(after, jnp.int32(1)) == 1
        return ((after >= 0) & jnp.logical_not((after < n_mixed) & odd)).astype(jnp.int32)

    def chunk_of(turn, is_back):
        return jnp.clip(jnp.where(is_back == 1, bwd_chunk(turn), fwd_chunk(turn)), 0, n_chunk - 1)

    def piece_at(side, index):
        col = side * half + index * piece
        return pl.ds(pl.multiple_of(col, piece), piece)

    def remote(src, dst, send_sem, recv_sem, device):
        return pltpu.make_async_remote_copy(
            src_ref=src, dst_ref=dst, send_sem=send_sem, recv_sem=recv_sem, device_id=device, device_id_type=MESH
        )

    def left(send_sem, like):
        remote(like, like, send_sem, loss_recv.at[0], {"model": pos}).wait_send()

    turn_pieces = acts.at[0, 0, :, pl.ds(0, half)]
    turn_sums = send_buf.at[0, 0]

    def rank_of(side):
        return pos if side == 0 else last_pos - pos

    def up(side):
        return {"model": pos + 1 if side == 0 else pos - 1}

    def down(side):
        return {"model": pos - 1 if side == 0 else pos + 1}

    def first_product(step, part):
        place = step + PARTS - 1 - part
        turn = turn_of(place)
        word = table[turn]
        starts = piece_of(place) == 0

        @pl.when(starts & has(word, FWD))
        def _():
            chunk = fwd_chunk(turn)
            if part == 0:

                @pl.when((stage != fore_stage) | (chunk >= n_fore))
                def _():
                    copy_in(chunk).wait()

                @pl.when(chunk >= n_grad)
                def _():
                    copy_out(0, chunk).start()

            else:

                @pl.when((stage == 0) & (place == 0))
                def _():
                    copy_w1(part).wait()

            for col in range(part * hid_part, (part + 1) * hid_part, hid_cols):
                cols = pl.ds(col, hid_cols)
                pre = dot_nn(acts[0, chunk], wts[0, :, cols]).astype(BF16)
                hid[1, chunk, :, cols] = pre
                hid[0, chunk, :, cols] = gelu_tanh(pre.astype(F32)).astype(BF16)
            if part == PARTS - 1:

                @pl.when(chunk >= n_grad)
                def _():
                    copy_out(1, chunk).start()

                @pl.when((stage == 0) & (place == 0))
                def _():
                    copy_w2.wait()

        @pl.when(starts & has(word, BWD))
        def _():
            chunk = bwd_chunk(turn)
            if part == 0:

                @pl.when((stage == fore_stage) & (chunk < n_relay))
                def _():
                    grad_in(chunk).wait()

                @pl.when(chunk >= n_grad)
                def _():
                    copy_out(3, chunk).start()

            for col in range(part * hid_part, (part + 1) * hid_part, hid_cols):
                cols = pl.ds(col, hid_cols)
                grad_act = dot_nn(acts[1, chunk], wts[2, :, cols]).astype(BF16)
                slope = gelu_slope(hid[1, chunk, :, cols].astype(F32))
                hid[1, chunk, :, cols] = (slope * grad_act.astype(F32)).astype(BF16)
            if part == PARTS - 1:

                @pl.when(chunk >= n_grad)
                def _():
                    copy_out(2, chunk).start()

        if part == 0:

            @pl.when((stage == 0) & (place == n_lead * half_pieces))
            def _():
                transpose_weights()

    def loss_copy(side, to_stage, to_pos):
        return remote(
            loss_acc, loss_in.at[side], loss_send.at[to_stage * n_model + to_pos], loss_recv.at[side],
            {"stage": to_stage, "model": to_pos},
        )

    def send_loss(side):
        loss_in[side] = loss_acc[...]
        for to_stage in range(n_stage):
            for to_pos in range(n_model):

                @pl.when((to_stage != stage) | (to_pos != pos))
                def _():
                    loss_copy(side, to_stage, to_pos).start()

    def sum_steps(step):
        now = []
        for side in (0, 1):
            rank = rank_of(side)
            place = step - hop * rank
            turn = turn_of(place)
            word, old = table[turn], table[turn - 2]
            index = piece_of(place)
            half_turn = lax.bitwise_and(turn, jnp.int32(1))
            inn = lax.bitwise_and(place + MARGIN * half_pieces, jnp.int32(RECV_SLOTS - 1))
            sums = has(word, SUM)
            is_back = back_of(turn)
            now.append((rank, word, sums, is_back, chunk_of(turn, is_back), index, half_turn, inn, piece_at(side, index)))

            @pl.when((index == 0) & has(old, SUM))
            def _():
                @pl.when(rank < last_pos)
                def _():
                    left(sum_send.at[side, half_turn], turn_sums)

                @pl.when((rank == last_pos) & has(old, BACK))
                def _():
                    left(down_send.at[side, half_turn], turn_pieces)

        @pl.when(now[0][2] | now[1][2])
        def _():
            for side in (0, 1):
                _, _, _, is_back, chunk, index, half_turn, _, cols = now[side]
                send_buf[side, half_turn, index] = dot_nn(hid[is_back, chunk], wts[1 + 2 * is_back, :, cols])

        for side in (0, 1):
            rank, word, sums, is_back, chunk, out, half_turn, inn, cols = now[side]
            bwd = has(word, BACK)
            index = chunk * half_pieces + out
            mine = send_buf.at[side, half_turn, out]
            gone = down_send.at[side, half_turn]
            hand_on = remote(mine, recv_buf.at[side, inn], sum_send.at[side, half_turn], sum_recv.at[side, inn], up(side))

            @pl.when(sums & (rank > 0))
            def _():
                hand_on.wait_recv()
                mine[...] = mine[...] + recv_buf[side, inn]

            @pl.when(sums & (rank < last_pos))
            def _():
                hand_on.start()

            @pl.when(sums & (rank == last_pos))
            def _():
                whole = acts[is_back, chunk, :, cols].astype(F32) + mine[...]
                scored = has(word, FWD) & (stage == last_stage)

                @pl.when(scored)
                def _():
                    @pl.when(index == 0)
                    def _():
                        copy_targets(side).wait()

                    err = whole.astype(BF16).astype(F32) - acts[1, chunk, :, cols].astype(F32)
                    acts[1, chunk, :, cols] = (err * grad_scale).astype(BF16)
                    square = jnp.sum((err * err).reshape(err.shape[0] // 8, 8, piece), axis=0)
                    part = square[:, :128]
                    for lane in range(1, piece // 128):
                        part = part + square[:, lane * 128 : (lane + 1) * 128]
                    loss_acc[...] = loss_acc[...] + part

                    @pl.when(index == total - 1)
                    def _():
                        send_loss(side)

                @pl.when(has(word, FWD) & (stage < last_stage))
                def _():
                    acts[1, chunk, :, cols] = whole.astype(BF16)

                ended = end_buf.at[side, half_turn, out]

                @pl.when(bwd)
                def _():
                    ended[...] = whole.astype(BF16)

                @pl.when(bwd & (index == total - 2 * half_pieces))
                def _():
                    pl.semaphore_wait(spent_sem.at[side], 1)

                @pl.when(bwd & (stage == 1) & (index == (n_relay - 2) * half_pieces))
                def _():
                    pl.semaphore_wait(free_sem.at[side], 1)

                relayed = (stage == last_stage) & (chunk < n_relay)
                there = acts.at[1, chunk, :, cols]

                @pl.when(bwd & relayed)
                def _():
                    arrived = rel_recv.at[side, jnp.minimum(index, n_relay * half_pieces - 1)]
                    remote(ended, there, gone, arrived, {"stage": 0}).start()

                @pl.when(bwd & jnp.logical_not(relayed))
                def _():
                    arrived = take_recv.at[side, index]
                    remote(ended, there, gone, arrived, {"stage": stage - 1}).start()

    def gather_step(side, step):
        rank = rank_of(side)
        place = step - 1 - 3 * hop - hop * (last_pos - rank)
        turn = turn_of(place)
        word, old = table[turn], table[turn - 2]
        out = piece_of(place)
        half_turn = lax.bitwise_and(turn, jnp.int32(1))
        chunk = jnp.clip(fwd_chunk(turn), 0, n_chunk - 1)
        index = chunk * half_pieces + out
        cols = piece_at(side, out)
        here = acts.at[1, chunk, :, cols]
        gone = over_send.at[side, half_turn]

        @pl.when((out == 0) & has(old, GATHER | EARLY))
        def _():
            @pl.when(has(old, GATHER) & (rank > 0))
            def _():
                left(gat_send.at[side, half_turn], turn_pieces)

            @pl.when((stage < last_stage) & (has(old, GATHER) | (rank == last_pos)))
            def _():
                left(gone, turn_pieces)

                @pl.when((fwd_chunk(turn - 2) == n_chunk - 1) & (rank == last_pos))
                def _():
                    pl.semaphore_signal(spent_sem.at[side], inc=1, device_id={"stage": stage + 1}, device_id_type=MESH)

        @pl.when(has(word, GATHER))
        def _():
            hand_on = remote(here, here, gat_send.at[side, half_turn], gat_recv.at[side, index], down(side))

            @pl.when(rank < last_pos)
            def _():
                hand_on.wait_recv()

            @pl.when(rank > 0)
            def _():
                hand_on.start()

            @pl.when(stage < last_stage)
            def _():
                remote(here, acts.at[0, chunk, :, cols], gone, in_sem.at[chunk], {"stage": stage + 1}).start()

        @pl.when(has(word, EARLY) & (rank == last_pos))
        def _():
            arrived = take_recv.at[side, jnp.minimum(total + index, total + n_fore * half_pieces - 1)]
            remote(here, acts.at[0, chunk, :, cols], gone, arrived, {"stage": stage + 1}).start()

    def take_step(side, step):
        rank = rank_of(side)
        place = step + early - hop * (last_pos - rank)
        turn = turn_of(place)
        word, old = table[turn], table[turn - 2]
        out = piece_of(place)
        gone = back_send.at[side, lax.bitwise_and(turn, jnp.int32(1))]

        @pl.when((out == 0) & has(old, TAKE) & (rank > 0))
        def _():
            left(gone, turn_pieces)

        @pl.when(has(word, TAKE))
        def _():
            is_back = back_of(turn)
            chunk = chunk_of(turn, is_back)
            index = chunk * half_pieces + out + (1 - is_back) * total
            here = acts.at[is_back, chunk, :, piece_at(side, out)]
            hand_on = remote(here, here, gone, take_recv.at[side, index], down(side))
            hand_on.wait_recv()

            @pl.when(rank > 0)
            def _():
                hand_on.start()

    def relay_step(side, step):
        rank = rank_of(side)
        place = step - (n_chunk + RELAY_START) * half_pieces - hop * (last_pos - rank)
        turn = turn_of(place) - MARGIN
        out = piece_of(place)
        half_turn = lax.bitwise_and(turn, jnp.int32(1))
        chunk = jnp.clip(turn, 0, n_relay - 1)
        here = acts.at[1, chunk, :, piece_at(side, out)]
        gone = rel_over.at[side, half_turn]
        hand_on = remote(here, here, rel_send.at[side, half_turn], rel_recv.at[side, chunk * half_pieces + out], down(side))

        @pl.when((out == 0) & (turn >= 2) & (turn < n_relay + 2))
        def _():
            @pl.when(rank > 0)
            def _():
                left(rel_send.at[side, half_turn], turn_pieces)

            left(gone, turn_pieces)

            @pl.when((turn == n_relay + 1) & (rank == last_pos))
            def _():
                pl.semaphore_signal(free_sem.at[side], inc=1, device_id={"stage": 1}, device_id_type=MESH)

        @pl.when((turn >= 0) & (turn < n_relay))
        def _():
            hand_on.wait_recv()

            @pl.when(rank > 0)
            def _():
                hand_on.start()

            remote(here, here, gone, rel_in.at[chunk], {"stage": fore_stage}).start()

    tile_rows, tile_cols = tile_buf.shape[1], tile_buf.shape[2]
    per_row = wts.shape[1] // tile_cols
    n_tiles = hid_dim // tile_rows * per_row

    def copy_tile(which, index):
        rows = pl.ds(pl.multiple_of(index // per_row * tile_rows, tile_rows), tile_rows)
        cols = pl.ds(pl.multiple_of(index % per_row * tile_cols, tile_cols), tile_cols)
        return pltpu.make_async_copy(tile_buf.at[index % 2], grad_hbm.at[which, rows, cols], tile_sem.at[index % 2])

    def grad_tile(number):
        for which, index in ((1, number), (0, number - n_tiles)):

            @pl.when((index >= 0) & (index < n_tiles))
            def _():
                rows = pl.ds(pl.multiple_of(index // per_row * tile_rows, tile_rows), tile_rows)
                cols = pl.ds(pl.multiple_of(index % per_row * tile_cols, tile_cols), tile_cols)

                @pl.when(number >= 2)
                def _():
                    copy_tile(which, index).wait()

                inputs, grads = (acts.at[0], hid.at[1]) if which == 0 else (hid.at[0], acts.at[1])
                lefts = inputs[0:n_grad, :, rows].reshape(n_grad * chunk_rows, tile_rows)
                rights = grads[0:n_grad, :, cols].reshape(n_grad * chunk_rows, tile_cols)
                tile_buf[index % 2] = lax.dot_general(lefts, rights, (((0,), (0,)), ((), ())), preferred_element_type=F32)
                copy_tile(which, index).start()

    in_loop = jnp.where(stage == 0, FIRST_TILES[0], jnp.where(stage == 1, NEXT_TILES[0], 0))
    pitch = jnp.where(stage == 0, FIRST_TILES[1], NEXT_TILES[1])
    first_tile = (n_first + n_grad) * half_pieces

    def loop_step(step, carry):
        for part in range(PARTS):
            first_product(step, part)

        @pl.when((step == 0) & (stage != fore_stage))
        def _():
            meet()

        gather_step(0, step)
        gather_step(1, step)
        sum_steps(step)

        @pl.when((stage == 0) & (step >= n_chunk * half_pieces))
        def _():
            relay_step(0, step)
            relay_step(1, step)

        take_step(0, step)
        take_step(1, step)
        since = step - first_tile

        @pl.when((since >= 0) & (since < in_loop * pitch) & (since % pitch == 0))
        def _():
            grad_tile(since // pitch)

        return carry

    lax.fori_loop(jnp.where(stage == fore_stage, -early, 1 - PARTS), n_steps, loop_step, 0)

    def next_tile(number, carry):
        grad_tile(number)
        return carry

    lax.fori_loop(in_loop, 2 * n_tiles, next_tile, 0)

    for side, owner in ((0, last_pos), (1, 0)):
        owns = (stage == last_stage) & (pos == owner)

        @pl.when(jnp.logical_not(owns))
        def _():
            loss_copy(side, 0, 0).wait_recv()

        @pl.when(owns)
        def _():
            for to_stage in range(n_stage):
                for to_pos in range(n_model):

                    @pl.when((to_stage != stage) | (to_pos != pos))
                    def _():
                        loss_copy(side, to_stage, to_pos).wait_send()

    loss_out[...] = jnp.full(loss_out.shape, jnp.sum(loss_in[0] + loss_in[1]) * (0.5 * grad_scale), F32)

    for index in (0, 1):
        copy_tile(0, index).wait()

    def end_out(chunk, carry):
        for kind in range(4):
            copy_out(kind, chunk).wait()
        return carry

    lax.fori_loop(n_grad, n_chunk, end_out, 0)


def finish_kernel(
    first_hbm, lefts_hbm, rights_hbm, loss_hbm, grad_in, grad_out, loss_out, sums, lefts, rights, loss, sum_in, sum_out, operand_in, loss_sem
):
    block = sums.shape[1]
    blocks = grad_in.shape[0] // block
    half = lefts.shape[1] // 2

    def copy_operands(which):
        pairs = ((rights_hbm, rights, 0), (lefts_hbm, lefts, 1))
        return [
            pltpu.make_async_copy(
                src.at[which, pl.ds(part * half, half), :], dst.at[which, pl.ds(part * half, half), :], operand_in.at[which, kind, part]
            )
            for src, dst, kind in pairs
            for part in (0, 1)
        ]

    def rows_of(number):
        return pl.ds(pl.multiple_of(number % blocks * block, block), block)

    def copy_first(number):
        return pltpu.make_async_copy(first_hbm.at[number // blocks, rows_of(number), :], sums.at[number], sum_in.at[number])

    def copy_result(number, which):
        return pltpu.make_async_copy(sums.at[number], (grad_in, grad_out)[which].at[rows_of(number), :], sum_out.at[number])

    copy_loss = pltpu.make_async_copy(loss_hbm, loss, loss_sem)
    for copy in copy_operands(0):
        copy.start()
    for number in range(AT_START):
        copy_first(number).start()
    copy_loss.start()

    def one(number, carry):
        for which in (0, 1):

            @pl.when(number == which * blocks)
            def _():
                for copy in copy_operands(which):
                    copy.wait()

        copy_first(number).wait()

        @pl.when(number == 0)
        def _():
            for ahead in range(AT_START, IN_FLIGHT):
                copy_first(ahead).start()

        @pl.when(number == 2)
        def _():
            for copy in copy_operands(1):
                copy.start()

        @pl.when(number + IN_FLIGHT < 2 * blocks)
        def _():
            copy_first(number + IN_FLIGHT).start()

        which = number // blocks
        part = lax.dot_general(
            lefts[which, :, rows_of(number)], rights[which], (((0,), (0,)), ((), ())), preferred_element_type=F32
        )
        sums[number] = sums[number] + part

        for kind in (0, 1):

            @pl.when(which == kind)
            def _():
                copy_result(number, kind).start()

        return carry

    lax.fori_loop(0, 2 * blocks, one, 0)
    copy_loss.wait()
    loss_out[0] = loss[0, 0]

    def end(number, carry):
        copy_result(number, 0).wait()
        return carry

    lax.fori_loop(0, 2 * blocks, end, 0)


def finish_grads(first, lefts, rights, loss):
    rows, dim = lefts.shape[1:]
    block = min(TILE_ROWS, dim)
    blocks = dim // block
    shape = jax.ShapeDtypeStruct((dim, dim), F32)
    any_space = pl.BlockSpec(memory_space=pl.ANY)
    dma = pltpu.SemaphoreType.DMA
    return pl.pallas_call(
        finish_kernel,
        out_shape=(shape, shape, jax.ShapeDtypeStruct((1,), F32)),
        in_specs=[any_space] * 4,
        out_specs=(any_space, any_space, pl.BlockSpec(memory_space=pltpu.SMEM)),
        scratch_shapes=[
            pltpu.VMEM((2 * blocks, block, dim), F32),
            pltpu.VMEM((2, rows, dim), BF16),
            pltpu.VMEM((2, rows, dim), BF16),
            pltpu.VMEM(loss.shape, F32),
            dma((2 * blocks,)),
            dma((2 * blocks,)),
            dma((2, 2, 2)),
            dma,
        ],
        compiler_params=pltpu.CompilerParams(vmem_limit_bytes=62 * 1024 * 1024),
        cost_estimate=pl.CostEstimate(flops=4 * rows * dim * dim, bytes_accessed=16 * dim * dim, transcendentals=0),
        name="finish_kernel",
    )(first, lefts, rights, loss)


def solution(mesh):
    n_stage = mesh.shape["stage"]
    n_model = mesh.shape["model"]

    def stage_step(inputs, targets, w_in, w_out):
        num_micro, num_tokens, model_dim = inputs.shape
        hid_dim = w_in.shape[3]
        rows = num_micro * num_tokens
        chunk = min(CHUNK_TOKENS, num_tokens)
        n_chunk = rows // chunk
        piece = min(PIECE_COLS, model_dim // 2)
        half_pieces = model_dim // 2 // piece
        grad_scale = 1.0 / (rows * model_dim)
        lead = [n_chunk] * (n_stage - 2) + [min(PREV_LEAD, n_chunk), min(LAST_LEAD, n_chunk)]
        idle = [FIRST_IDLE] + [NEXT_IDLE] * (n_stage - 3) + [0, 0]
        n_fore, n_relay = min(FORE_CHUNKS, n_chunk - 1), min(RELAY_CHUNKS, n_chunk - 1)
        n_grad = min(FIRST_GRADS, n_chunk // 2)
        rest = rows - n_grad * chunk
        tile_rows, tile_cols = min(TILE_ROWS, hid_dim), min(TILE_COLS, model_dim)
        kernel = functools.partial(
            stage_kernel, n_stage, n_model, n_chunk, half_pieces, piece, HOP_LAG, lead, idle, n_fore, n_relay, n_grad, grad_scale
        )
        any_space = pl.BlockSpec(memory_space=pl.ANY)
        dma = pltpu.SemaphoreType.DMA
        lefts, rights, first_grads, loss = pl.pallas_call(
            kernel,
            out_shape=(
                jax.ShapeDtypeStruct((2, rest, model_dim), BF16),
                jax.ShapeDtypeStruct((2, rest, model_dim), BF16),
                jax.ShapeDtypeStruct((2, hid_dim, model_dim), F32),
                jax.ShapeDtypeStruct((8, 128), F32),
            ),
            in_specs=[any_space] * 4,
            out_specs=(any_space, any_space, any_space, pl.BlockSpec(memory_space=pltpu.VMEM)),
            scratch_shapes=[
                pltpu.VMEM((4, model_dim, hid_dim), BF16),
                pltpu.VMEM((2, n_chunk, chunk, model_dim), BF16),
                pltpu.VMEM((2, n_chunk, chunk, hid_dim), BF16),
                pltpu.VMEM((2, 2, half_pieces, chunk, piece), F32),
                pltpu.VMEM((2, RECV_SLOTS, chunk, piece), F32),
                pltpu.VMEM((8, 128), F32),
                pltpu.VMEM((2, 8, 128), F32),
                dma((PARTS + 1,)),
                dma((n_chunk,)),
                dma,
                dma((2, 2)),
                dma((2, RECV_SLOTS)),
                dma((2, 2)),
                dma((2, n_chunk * half_pieces)),
                dma((2, 2)),
                dma((2, 2)),
                dma((2, (n_chunk + n_fore) * half_pieces)),
                dma((2, 2)),
                dma((4, n_chunk)),
                dma((n_stage * n_model,)),
                dma((2,)),
                pltpu.SemaphoreType.REGULAR((2,)),
                dma((2, 2)),
                dma((2, 2)),
                dma((2, n_relay * half_pieces)),
                dma((n_relay,)),
                pltpu.SemaphoreType.REGULAR((2,)),
                pltpu.SMEM((2 * n_chunk + max(idle) + 2 * MARGIN,), jnp.int32),
                pltpu.VMEM((2, tile_rows, tile_cols), F32),
                dma((2,)),
                pltpu.VMEM((2, 2, half_pieces, chunk, piece), BF16),
            ],
            compiler_params=pltpu.CompilerParams(collective_id=0, has_side_effects=True, vmem_limit_bytes=63 * 1024 * 1024),
            name="stage_kernel",
        )(
            inputs.reshape(n_chunk, chunk, model_dim),
            targets.reshape(n_chunk, chunk, model_dim),
            w_in.reshape(model_dim, hid_dim),
            w_out.reshape(hid_dim, model_dim),
        )

        grad_in, grad_out, loss = finish_grads(first_grads, lefts, rights, loss)
        return grad_in[None, None], grad_out[None, None], loss

    return jax.shard_map(
        stage_step,
        mesh=mesh,
        in_specs=(P("data", None, None), P("data", None, None), P("stage", None, None, "model"), P("stage", None, "model", None)),
        out_specs=(P(("data", "stage"), None, None, "model"), P(("data", "stage"), None, "model", None), P("data")),
        check_vma=False,
    )
```

```python
import functools

import jax
import jax.numpy as jnp
from jax import lax
from jax.experimental import pallas as pl
from jax.experimental.pallas import tpu as pltpu
from jax.sharding import PartitionSpec as P

GELU_COEF = 0.7978845608028654
CUBIC_COEF = 0.044715

CHUNK_TOKENS = 64
PIECE_COLS = 256
HIDDEN_COLS = 512
PARTS = 2
HOP_LAG = 2
RECV_SLOTS = 8
LAST_LEAD = 5
PREV_LEAD = 15
FIRST_IDLE = 12
NEXT_IDLE = 7
FORE_CHUNKS = 7
RELAY_CHUNKS = 19
RELAY_START = 0

FIRST_GRADS = 12
TILE_ROWS = 256
TILE_COLS = 1024
IN_FLIGHT = 8
FIRST_TILES = (32, 1)
NEXT_TILES = (16, 3)

SUM, BACK, GATHER, EARLY, TAKE, FWD, BWD = 256, 512, 1024, 2048, 4096, 8192, 16384
MARGIN = 8

BF16 = jnp.bfloat16
F32 = jnp.float32
MESH = pl.DeviceIdType.MESH


def gelu_tanh(values):
    inner_arg = GELU_COEF * (values + CUBIC_COEF * values * values * values)
    return 0.5 * values * (1.0 + jnp.tanh(inner_arg))


def gelu_slope(values):
    tanh_val = jnp.tanh(GELU_COEF * (values + CUBIC_COEF * values * values * values))
    return 0.5 * (1.0 + tanh_val) + 0.5 * values * (1.0 - tanh_val * tanh_val) * GELU_COEF * (1.0 + 3.0 * CUBIC_COEF * values * values)


def dot_nn(left, right):
    return jnp.dot(left, right, preferred_element_type=F32)


def dot_nt(left, right):
    return lax.dot_general(left, right, (((1,), (1,)), ((), ())), preferred_element_type=F32)


def stage_kernel(
    n_stage, n_model, n_chunk, half_pieces, piece, hop, lead, idle, n_fore, n_relay, n_grad, grad_scale,
    inputs_hbm, targets_hbm, w1_hbm, w2_hbm,
    left_out, right_out, grad_hbm, loss_out,
    wts, acts, hid, send_buf, recv_buf, loss_acc, loss_in,
    w_sem, in_sem, tgt_sem, sum_send, sum_recv, gat_send, gat_recv, over_send, back_send, take_recv, down_send, out_sem,
    loss_send, loss_recv, spent_sem, rel_send, rel_over, rel_recv, rel_in, free_sem, table, tile_buf, tile_sem, end_buf,
):
    pos = lax.axis_index("model")
    stage = lax.axis_index("stage")
    last_pos = n_model - 1
    last_stage = n_stage - 1
    fore_stage = n_stage - 2
    bits = half_pieces.bit_length() - 1
    total = n_chunk * half_pieces
    half = half_pieces * piece
    hid_dim = wts.shape[2]
    chunk_rows = acts.shape[2]
    hid_part = hid_dim // PARTS
    hid_cols = min(HIDDEN_COLS, hid_part)
    n_lead, n_idle = jnp.int32(n_chunk), jnp.int32(0)
    for at in range(n_stage):
        n_lead = jnp.where(stage == at, lead[at], n_lead)
        n_idle = jnp.where(stage == at, idle[at], n_idle)
    turns = 2 * n_chunk + n_idle
    n_steps = turns * half_pieces + jnp.where(stage == 0, 1 - hop, half_pieces + hop * last_pos + 1)
    early = half_pieces + 3 * hop + 1

    barrier = pltpu.get_barrier_semaphore()
    for to_stage in range(n_stage):
        for to_pos in range(n_model):

            @pl.when((to_stage != stage) | (to_pos != pos))
            def _():
                pl.semaphore_signal(barrier, inc=1, device_id={"stage": to_stage, "model": to_pos}, device_id_type=MESH)

    copy_w2 = pltpu.make_async_copy(w2_hbm, wts.at[1], w_sem.at[PARTS])

    def copy_w1(part):
        cols = pl.ds(part * hid_part, hid_part)
        return pltpu.make_async_copy(w1_hbm.at[:, cols], wts.at[0, :, cols], w_sem.at[part])


    def copy_in(chunk):
        return pltpu.make_async_copy(inputs_hbm.at[chunk], acts.at[0, chunk], in_sem.at[chunk])

    def grad_in(chunk):
        return pltpu.make_async_copy(inputs_hbm.at[chunk], acts.at[1, chunk], rel_in.at[chunk])

    def copy_targets(side):
        cols = pl.ds(side * half, half)
        return pltpu.make_async_copy(targets_hbm.at[:, :, cols], acts.at[1, :, :, cols], tgt_sem)

    def copy_out(kind, chunk):
        src = (acts.at[0], hid.at[0], hid.at[1], acts.at[1])[kind]
        dst = (left_out.at[0], left_out.at[1], right_out.at[0], right_out.at[1])[kind]
        rows = pl.ds(pl.multiple_of((chunk - n_grad) * chunk_rows, chunk_rows), chunk_rows)
        return pltpu.make_async_copy(src.at[chunk], dst.at[rows, :], out_sem.at[kind, chunk])

    @pl.when(stage == 0)
    def _():
        copy_in(0).start()

    for part in range(PARTS):
        copy_w1(part).start()
    copy_w2.start()

    @pl.when(stage == 0)
    def _():
        def start_in(chunk, carry):
            copy_in(chunk).start()
            return carry

        lax.fori_loop(1, n_chunk, start_in, 0)

    @pl.when((stage == last_stage) & (pos == last_pos))
    def _():
        copy_targets(0).start()

    @pl.when((stage == last_stage) & (pos == 0))
    def _():
        copy_targets(1).start()

    def transpose_weights():
        tile = min(256, hid_dim)
        count = hid_dim // tile

        def one(index, carry):
            rows = pl.ds(pl.multiple_of((index // count) * tile, tile), tile)
            cols = pl.ds(pl.multiple_of((index % count) * tile, tile), tile)
            wts[2, cols, rows] = jnp.swapaxes(wts[1, rows, cols], 0, 1)
            wts[3, cols, rows] = jnp.swapaxes(wts[0, rows, cols], 0, 1)
            return carry

        lax.fori_loop(0, count * count, one, 0)

    n_mixed = 2 * (n_chunk - n_lead)
    n_after = 2 * n_chunk - n_lead
    n_first = n_lead + n_idle

    def fill(entry, carry):
        turn = entry - MARGIN
        after = turn - n_first
        pair = (after + 1024) // 2 - 512
        odd = (after + 1024) % 2 == 1
        mixed = (after >= 0) & (after < n_mixed)
        leads = (turn >= 0) & (turn < n_lead)
        fwd = leads | (mixed & odd)
        bwd = (after >= 0) & (after < n_after) & jnp.logical_not(mixed & odd)
        chunk = jnp.where(leads, turn, jnp.where(odd, n_lead + pair, pair))
        chunk = jnp.where(bwd & (after >= n_mixed), after - (n_chunk - n_lead), chunk)
        early_one = fwd & (stage == fore_stage - 1) & (chunk < n_fore)
        back = bwd & (stage < last_stage) & ((stage < fore_stage) | (chunk >= n_relay))
        take = back | (fwd & (stage == fore_stage) & (chunk < n_fore))
        word = jnp.int32(0)
        for flag, bit in (
            (fwd | (bwd & (stage > 0)), SUM),
            (bwd, BACK),
            (fwd & jnp.logical_not(early_one), GATHER),
            (early_one, EARLY),
            (take, TAKE),
            (fwd, FWD),
            (bwd, BWD),
        ):
            word = word + jnp.where(flag, bit, 0)
        table[entry] = word
        return carry

    lax.fori_loop(0, table.shape[0], fill, 0)
    loss_acc[...] = jnp.zeros_like(loss_acc)
    copy_w1(0).wait()

    @pl.when(stage > 0)
    def _():
        for part in range(1, PARTS):
            copy_w1(part).wait()
        copy_w2.wait()
        transpose_weights()

    def meet():
        pl.semaphore_wait(barrier, n_stage * n_model - 1)

    @pl.when(stage == fore_stage)
    def _():
        meet()


    def turn_of(place):
        return lax.shift_right_logical(place + MARGIN * half_pieces, jnp.int32(bits))

    def piece_of(place):
        return lax.bitwise_and(place + MARGIN * half_pieces, jnp.int32(half_pieces - 1))

    def has(word, mask):
        return lax.bitwise_and(word, jnp.int32(mask)) != 0

    def fwd_chunk(turn):
        after = turn - (n_first + MARGIN)
        return jnp.where(turn < n_lead + MARGIN, turn - MARGIN, n_lead + lax.shift_right_arithmetic(after, jnp.int32(1)))

    def bwd_chunk(turn):
        after = turn - (n_first + MARGIN)
        return jnp.where(after < n_mixed, lax.shift_right_arithmetic(after, jnp.int32(1)), after - (n_chunk - n_lead))

    def back_of(turn):
        after = turn - (n_first + MARGIN)
        odd = lax.bitwise_and(after, jnp.int32(1)) == 1
        return ((after >= 0) & jnp.logical_not((after < n_mixed) & odd)).astype(jnp.int32)

    def chunk_of(turn, is_back):
        return jnp.clip(jnp.where(is_back == 1, bwd_chunk(turn), fwd_chunk(turn)), 0, n_chunk - 1)

    def piece_at(side, index):
        col = side * half + index * piece
        return pl.ds(pl.multiple_of(col, piece), piece)

    def remote(src, dst, send_sem, recv_sem, device):
        return pltpu.make_async_remote_copy(
            src_ref=src, dst_ref=dst, send_sem=send_sem, recv_sem=recv_sem, device_id=device, device_id_type=MESH
        )

    def left(send_sem, like):
        remote(like, like, send_sem, loss_recv.at[0], {"model": pos}).wait_send()

    turn_pieces = acts.at[0, 0, :, pl.ds(0, half)]
    turn_sums = send_buf.at[0, 0]

    def rank_of(side):
        return pos if side == 0 else last_pos - pos

    def up(side):
        return {"model": pos + 1 if side == 0 else pos - 1}

    def down(side):
        return {"model": pos - 1 if side == 0 else pos + 1}

    def first_product(step, part):
        place = step + PARTS - 1 - part
        turn = turn_of(place)
        word = table[turn]
        starts = piece_of(place) == 0

        @pl.when(starts & has(word, FWD))
        def _():
            chunk = fwd_chunk(turn)
            if part == 0:

                @pl.when((stage != fore_stage) | (chunk >= n_fore))
                def _():
                    copy_in(chunk).wait()

                @pl.when(chunk >= n_grad)
                def _():
                    copy_out(0, chunk).start()

            else:

                @pl.when((stage == 0) & (place == 0))
                def _():
                    copy_w1(part).wait()

            for col in range(part * hid_part, (part + 1) * hid_part, hid_cols):
                cols = pl.ds(col, hid_cols)
                pre = dot_nn(acts[0, chunk], wts[0, :, cols]).astype(BF16)
                hid[1, chunk, :, cols] = pre
                hid[0, chunk, :, cols] = gelu_tanh(pre.astype(F32)).astype(BF16)
            if part == PARTS - 1:

                @pl.when(chunk >= n_grad)
                def _():
                    copy_out(1, chunk).start()

                @pl.when((stage == 0) & (place == 0))
                def _():
                    copy_w2.wait()

        @pl.when(starts & has(word, BWD))
        def _():
            chunk = bwd_chunk(turn)
            if part == 0:

                @pl.when((stage == fore_stage) & (chunk < n_relay))
                def _():
                    grad_in(chunk).wait()

                @pl.when(chunk >= n_grad)
                def _():
                    copy_out(3, chunk).start()

            for col in range(part * hid_part, (part + 1) * hid_part, hid_cols):
                cols = pl.ds(col, hid_cols)
                grad_act = dot_nn(acts[1, chunk], wts[2, :, cols]).astype(BF16)
                slope = gelu_slope(hid[1, chunk, :, cols].astype(F32))
                hid[1, chunk, :, cols] = (slope * grad_act.astype(F32)).astype(BF16)
            if part == PARTS - 1:

                @pl.when(chunk >= n_grad)
                def _():
                    copy_out(2, chunk).start()

        if part == 0:

            @pl.when((stage == 0) & (place == n_lead * half_pieces))
            def _():
                transpose_weights()

    def loss_copy(side, to_stage, to_pos):
        return remote(
            loss_acc, loss_in.at[side], loss_send.at[to_stage * n_model + to_pos], loss_recv.at[side],
            {"stage": to_stage, "model": to_pos},
        )

    def send_loss(side):
        loss_in[side] = loss_acc[...]
        for to_stage in range(n_stage):
            for to_pos in range(n_model):

                @pl.when((to_stage != stage) | (to_pos != pos))
                def _():
                    loss_copy(side, to_stage, to_pos).start()

    def sum_steps(step):
        now = []
        for side in (0, 1):
            rank = rank_of(side)
            place = step - hop * rank
            turn = turn_of(place)
            word, old = table[turn], table[turn - 2]
            index = piece_of(place)
            half_turn = lax.bitwise_and(turn, jnp.int32(1))
            inn = lax.bitwise_and(place + MARGIN * half_pieces, jnp.int32(RECV_SLOTS - 1))
            sums = has(word, SUM)
            is_back = back_of(turn)
            now.append((rank, word, sums, is_back, chunk_of(turn, is_back), index, half_turn, inn, piece_at(side, index)))

            @pl.when((index == 0) & has(old, SUM))
            def _():
                @pl.when(rank < last_pos)
                def _():
                    left(sum_send.at[side, half_turn], turn_sums)

                @pl.when((rank == last_pos) & has(old, BACK))
                def _():
                    left(down_send.at[side, half_turn], turn_pieces)

        @pl.when(now[0][2] | now[1][2])
        def _():
            for side in (0, 1):
                _, _, _, is_back, chunk, index, half_turn, _, cols = now[side]
                send_buf[side, half_turn, index] = dot_nn(hid[is_back, chunk], wts[1 + 2 * is_back, :, cols])

        for side in (0, 1):
            rank, word, sums, is_back, chunk, out, half_turn, inn, cols = now[side]
            bwd = has(word, BACK)
            index = chunk * half_pieces + out
            mine = send_buf.at[side, half_turn, out]
            gone = down_send.at[side, half_turn]
            hand_on = remote(mine, recv_buf.at[side, inn], sum_send.at[side, half_turn], sum_recv.at[side, inn], up(side))

            @pl.when(sums & (rank > 0))
            def _():
                hand_on.wait_recv()
                mine[...] = mine[...] + recv_buf[side, inn]

            @pl.when(sums & (rank < last_pos))
            def _():
                hand_on.start()

            @pl.when(sums & (rank == last_pos))
            def _():
                whole = acts[is_back, chunk, :, cols].astype(F32) + mine[...]
                scored = has(word, FWD) & (stage == last_stage)

                @pl.when(scored)
                def _():
                    @pl.when(index == 0)
                    def _():
                        copy_targets(side).wait()

                    err = whole.astype(BF16).astype(F32) - acts[1, chunk, :, cols].astype(F32)
                    acts[1, chunk, :, cols] = (err * grad_scale).astype(BF16)
                    square = jnp.sum((err * err).reshape(err.shape[0] // 8, 8, piece), axis=0)
                    part = square[:, :128]
                    for lane in range(1, piece // 128):
                        part = part + square[:, lane * 128 : (lane + 1) * 128]
                    loss_acc[...] = loss_acc[...] + part

                    @pl.when(index == total - 1)
                    def _():
                        send_loss(side)

                @pl.when(has(word, FWD) & (stage < last_stage))
                def _():
                    acts[1, chunk, :, cols] = whole.astype(BF16)

                ended = end_buf.at[side, half_turn, out]

                @pl.when(bwd)
                def _():
                    ended[...] = whole.astype(BF16)

                @pl.when(bwd & (index == total - 2 * half_pieces))
                def _():
                    pl.semaphore_wait(spent_sem.at[side], 1)

                @pl.when(bwd & (stage == 1) & (index == (n_relay - 2) * half_pieces))
                def _():
                    pl.semaphore_wait(free_sem.at[side], 1)

                relayed = (stage == last_stage) & (chunk < n_relay)
                there = acts.at[1, chunk, :, cols]

                @pl.when(bwd & relayed)
                def _():
                    arrived = rel_recv.at[side, jnp.minimum(index, n_relay * half_pieces - 1)]
                    remote(ended, there, gone, arrived, {"stage": 0}).start()

                @pl.when(bwd & jnp.logical_not(relayed))
                def _():
                    arrived = take_recv.at[side, index]
                    remote(ended, there, gone, arrived, {"stage": stage - 1}).start()

    def gather_step(side, step):
        rank = rank_of(side)
        place = step - 1 - 3 * hop - hop * (last_pos - rank)
        turn = turn_of(place)
        word, old = table[turn], table[turn - 2]
        out = piece_of(place)
        half_turn = lax.bitwise_and(turn, jnp.int32(1))
        chunk = jnp.clip(fwd_chunk(turn), 0, n_chunk - 1)
        index = chunk * half_pieces + out
        cols = piece_at(side, out)
        here = acts.at[1, chunk, :, cols]
        gone = over_send.at[side, half_turn]

        @pl.when((out == 0) & has(old, GATHER | EARLY))
        def _():
            @pl.when(has(old, GATHER) & (rank > 0))
            def _():
                left(gat_send.at[side, half_turn], turn_pieces)

            @pl.when((stage < last_stage) & (has(old, GATHER) | (rank == last_pos)))
            def _():
                left(gone, turn_pieces)

                @pl.when((fwd_chunk(turn - 2) == n_chunk - 1) & (rank == last_pos))
                def _():
                    pl.semaphore_signal(spent_sem.at[side], inc=1, device_id={"stage": stage + 1}, device_id_type=MESH)

        @pl.when(has(word, GATHER))
        def _():
            hand_on = remote(here, here, gat_send.at[side, half_turn], gat_recv.at[side, index], down(side))

            @pl.when(rank < last_pos)
            def _():
                hand_on.wait_recv()

            @pl.when(rank > 0)
            def _():
                hand_on.start()

            @pl.when(stage < last_stage)
            def _():
                remote(here, acts.at[0, chunk, :, cols], gone, in_sem.at[chunk], {"stage": stage + 1}).start()

        @pl.when(has(word, EARLY) & (rank == last_pos))
        def _():
            arrived = take_recv.at[side, jnp.minimum(total + index, total + n_fore * half_pieces - 1)]
            remote(here, acts.at[0, chunk, :, cols], gone, arrived, {"stage": stage + 1}).start()

    def take_step(side, step):
        rank = rank_of(side)
        place = step + early - hop * (last_pos - rank)
        turn = turn_of(place)
        word, old = table[turn], table[turn - 2]
        out = piece_of(place)
        gone = back_send.at[side, lax.bitwise_and(turn, jnp.int32(1))]

        @pl.when((out == 0) & has(old, TAKE) & (rank > 0))
        def _():
            left(gone, turn_pieces)

        @pl.when(has(word, TAKE))
        def _():
            is_back = back_of(turn)
            chunk = chunk_of(turn, is_back)
            index = chunk * half_pieces + out + (1 - is_back) * total
            here = acts.at[is_back, chunk, :, piece_at(side, out)]
            hand_on = remote(here, here, gone, take_recv.at[side, index], down(side))
            hand_on.wait_recv()

            @pl.when(rank > 0)
            def _():
                hand_on.start()

    def relay_step(side, step):
        rank = rank_of(side)
        place = step - (n_chunk + RELAY_START) * half_pieces - hop * (last_pos - rank)
        turn = turn_of(place) - MARGIN
        out = piece_of(place)
        half_turn = lax.bitwise_and(turn, jnp.int32(1))
        chunk = jnp.clip(turn, 0, n_relay - 1)
        here = acts.at[1, chunk, :, piece_at(side, out)]
        gone = rel_over.at[side, half_turn]
        hand_on = remote(here, here, rel_send.at[side, half_turn], rel_recv.at[side, chunk * half_pieces + out], down(side))

        @pl.when((out == 0) & (turn >= 2) & (turn < n_relay + 2))
        def _():
            @pl.when(rank > 0)
            def _():
                left(rel_send.at[side, half_turn], turn_pieces)

            left(gone, turn_pieces)

            @pl.when((turn == n_relay + 1) & (rank == last_pos))
            def _():
                pl.semaphore_signal(free_sem.at[side], inc=1, device_id={"stage": 1}, device_id_type=MESH)

        @pl.when((turn >= 0) & (turn < n_relay))
        def _():
            hand_on.wait_recv()

            @pl.when(rank > 0)
            def _():
                hand_on.start()

            remote(here, here, gone, rel_in.at[chunk], {"stage": fore_stage}).start()

    tile_rows, tile_cols = tile_buf.shape[1], tile_buf.shape[2]
    per_row = wts.shape[1] // tile_cols
    n_tiles = hid_dim // tile_rows * per_row

    def copy_tile(which, index):
        rows = pl.ds(pl.multiple_of(index // per_row * tile_rows, tile_rows), tile_rows)
        cols = pl.ds(pl.multiple_of(index % per_row * tile_cols, tile_cols), tile_cols)
        return pltpu.make_async_copy(tile_buf.at[index % 2], grad_hbm.at[which, rows, cols], tile_sem.at[index % 2])

    def grad_tile(number):
        for which, index in ((1, number), (0, number - n_tiles)):

            @pl.when((index >= 0) & (index < n_tiles))
            def _():
                rows = pl.ds(pl.multiple_of(index // per_row * tile_rows, tile_rows), tile_rows)
                cols = pl.ds(pl.multiple_of(index % per_row * tile_cols, tile_cols), tile_cols)

                @pl.when(number >= 2)
                def _():
                    copy_tile(which, index).wait()

                inputs, grads = (acts.at[0], hid.at[1]) if which == 0 else (hid.at[0], acts.at[1])
                lefts = inputs[0:n_grad, :, rows].reshape(n_grad * chunk_rows, tile_rows)
                rights = grads[0:n_grad, :, cols].reshape(n_grad * chunk_rows, tile_cols)
                tile_buf[index % 2] = lax.dot_general(lefts, rights, (((0,), (0,)), ((), ())), preferred_element_type=F32)
                copy_tile(which, index).start()

    in_loop = jnp.where(stage == 0, FIRST_TILES[0], jnp.where(stage == 1, NEXT_TILES[0], 0))
    pitch = jnp.where(stage == 0, FIRST_TILES[1], NEXT_TILES[1])
    first_tile = (n_first + n_grad) * half_pieces

    def loop_step(step, carry):
        for part in range(PARTS):
            first_product(step, part)

        @pl.when((step == 0) & (stage != fore_stage))
        def _():
            meet()

        gather_step(0, step)
        gather_step(1, step)
        sum_steps(step)

        @pl.when((stage == 0) & (step >= n_chunk * half_pieces))
        def _():
            relay_step(0, step)
            relay_step(1, step)

        take_step(0, step)
        take_step(1, step)
        since = step - first_tile

        @pl.when((since >= 0) & (since < in_loop * pitch) & (since % pitch == 0))
        def _():
            grad_tile(since // pitch)

        return carry

    lax.fori_loop(jnp.where(stage == fore_stage, -early, 1 - PARTS), n_steps, loop_step, 0)

    def next_tile(number, carry):
        grad_tile(number)
        return carry

    lax.fori_loop(in_loop, 2 * n_tiles, next_tile, 0)

    for side, owner in ((0, last_pos), (1, 0)):
        owns = (stage == last_stage) & (pos == owner)

        @pl.when(jnp.logical_not(owns))
        def _():
            loss_copy(side, 0, 0).wait_recv()

        @pl.when(owns)
        def _():
            for to_stage in range(n_stage):
                for to_pos in range(n_model):

                    @pl.when((to_stage != stage) | (to_pos != pos))
                    def _():
                        loss_copy(side, to_stage, to_pos).wait_send()

    loss_out[...] = jnp.full(loss_out.shape, jnp.sum(loss_in[0] + loss_in[1]) * (0.5 * grad_scale), F32)

    for index in (0, 1):
        copy_tile(0, index).wait()

    def end_out(chunk, carry):
        for kind in range(4):
            copy_out(kind, chunk).wait()
        return carry

    lax.fori_loop(n_grad, n_chunk, end_out, 0)


def finish_kernel(
    first_hbm, lefts_hbm, rights_hbm, loss_hbm, grad_in, grad_out, loss_out, sums, lefts, rights, loss, sum_in, sum_out, operand_in, loss_sem
):
    block = sums.shape[1]
    blocks = grad_in.shape[0] // block
    half = lefts.shape[1] // 2

    def copy_operands(which):
        pairs = ((rights_hbm, rights, 0), (lefts_hbm, lefts, 1))
        return [
            pltpu.make_async_copy(
                src.at[which, pl.ds(part * half, half), :], dst.at[which, pl.ds(part * half, half), :], operand_in.at[which, kind, part]
            )
            for src, dst, kind in pairs
            for part in (0, 1)
        ]

    def rows_of(number):
        return pl.ds(pl.multiple_of(number % blocks * block, block), block)

    def copy_first(number):
        return pltpu.make_async_copy(first_hbm.at[number // blocks, rows_of(number), :], sums.at[number], sum_in.at[number])

    def copy_result(number, which):
        return pltpu.make_async_copy(sums.at[number], (grad_in, grad_out)[which].at[rows_of(number), :], sum_out.at[number])

    copy_loss = pltpu.make_async_copy(loss_hbm, loss, loss_sem)
    for copy in copy_operands(0):
        copy.start()
    for number in range(IN_FLIGHT):
        copy_first(number).start()
    copy_loss.start()

    def one(number, carry):
        for which in (0, 1):

            @pl.when(number == which * blocks)
            def _():
                for copy in copy_operands(which):
                    copy.wait()

        @pl.when(number == 1)
        def _():
            for copy in copy_operands(1):
                copy.start()

        copy_first(number).wait()

        @pl.when(number + IN_FLIGHT < 2 * blocks)
        def _():
            copy_first(number + IN_FLIGHT).start()

        which = number // blocks
        part = lax.dot_general(
            lefts[which, :, rows_of(number)], rights[which], (((0,), (0,)), ((), ())), preferred_element_type=F32
        )
        sums[number] = sums[number] + part

        for kind in (0, 1):

            @pl.when(which == kind)
            def _():
                copy_result(number, kind).start()

        return carry

    lax.fori_loop(0, 2 * blocks, one, 0)
    copy_loss.wait()
    loss_out[0] = loss[0, 0]

    def end(number, carry):
        copy_result(number, 0).wait()
        return carry

    lax.fori_loop(0, 2 * blocks, end, 0)


def finish_grads(first, lefts, rights, loss):
    rows, dim = lefts.shape[1:]
    block = min(TILE_ROWS, dim)
    blocks = dim // block
    shape = jax.ShapeDtypeStruct((dim, dim), F32)
    any_space = pl.BlockSpec(memory_space=pl.ANY)
    dma = pltpu.SemaphoreType.DMA
    return pl.pallas_call(
        finish_kernel,
        out_shape=(shape, shape, jax.ShapeDtypeStruct((1,), F32)),
        in_specs=[any_space] * 4,
        out_specs=(any_space, any_space, pl.BlockSpec(memory_space=pltpu.SMEM)),
        scratch_shapes=[
            pltpu.VMEM((2 * blocks, block, dim), F32),
            pltpu.VMEM((2, rows, dim), BF16),
            pltpu.VMEM((2, rows, dim), BF16),
            pltpu.VMEM(loss.shape, F32),
            dma((2 * blocks,)),
            dma((2 * blocks,)),
            dma((2, 2, 2)),
            dma,
        ],
        compiler_params=pltpu.CompilerParams(vmem_limit_bytes=62 * 1024 * 1024),
        cost_estimate=pl.CostEstimate(flops=4 * rows * dim * dim, bytes_accessed=16 * dim * dim, transcendentals=0),
        name="finish_kernel",
    )(first, lefts, rights, loss)


def solution(mesh):
    n_stage = mesh.shape["stage"]
    n_model = mesh.shape["model"]

    def stage_step(inputs, targets, w_in, w_out):
        num_micro, num_tokens, model_dim = inputs.shape
        hid_dim = w_in.shape[3]
        rows = num_micro * num_tokens
        chunk = min(CHUNK_TOKENS, num_tokens)
        n_chunk = rows // chunk
        piece = min(PIECE_COLS, model_dim // 2)
        half_pieces = model_dim // 2 // piece
        grad_scale = 1.0 / (rows * model_dim)
        lead = [n_chunk] * (n_stage - 2) + [min(PREV_LEAD, n_chunk), min(LAST_LEAD, n_chunk)]
        idle = [FIRST_IDLE] + [NEXT_IDLE] * (n_stage - 3) + [0, 0]
        n_fore, n_relay = min(FORE_CHUNKS, n_chunk - 1), min(RELAY_CHUNKS, n_chunk - 1)
        n_grad = min(FIRST_GRADS, n_chunk // 2)
        rest = rows - n_grad * chunk
        tile_rows, tile_cols = min(TILE_ROWS, hid_dim), min(TILE_COLS, model_dim)
        kernel = functools.partial(
            stage_kernel, n_stage, n_model, n_chunk, half_pieces, piece, HOP_LAG, lead, idle, n_fore, n_relay, n_grad, grad_scale
        )
        any_space = pl.BlockSpec(memory_space=pl.ANY)
        dma = pltpu.SemaphoreType.DMA
        lefts, rights, first_grads, loss = pl.pallas_call(
            kernel,
            out_shape=(
                jax.ShapeDtypeStruct((2, rest, model_dim), BF16),
                jax.ShapeDtypeStruct((2, rest, model_dim), BF16),
                jax.ShapeDtypeStruct((2, hid_dim, model_dim), F32),
                jax.ShapeDtypeStruct((8, 128), F32),
            ),
            in_specs=[any_space] * 4,
            out_specs=(any_space, any_space, any_space, pl.BlockSpec(memory_space=pltpu.VMEM)),
            scratch_shapes=[
                pltpu.VMEM((4, model_dim, hid_dim), BF16),
                pltpu.VMEM((2, n_chunk, chunk, model_dim), BF16),
                pltpu.VMEM((2, n_chunk, chunk, hid_dim), BF16),
                pltpu.VMEM((2, 2, half_pieces, chunk, piece), F32),
                pltpu.VMEM((2, RECV_SLOTS, chunk, piece), F32),
                pltpu.VMEM((8, 128), F32),
                pltpu.VMEM((2, 8, 128), F32),
                dma((PARTS + 1,)),
                dma((n_chunk,)),
                dma,
                dma((2, 2)),
                dma((2, RECV_SLOTS)),
                dma((2, 2)),
                dma((2, n_chunk * half_pieces)),
                dma((2, 2)),
                dma((2, 2)),
                dma((2, (n_chunk + n_fore) * half_pieces)),
                dma((2, 2)),
                dma((4, n_chunk)),
                dma((n_stage * n_model,)),
                dma((2,)),
                pltpu.SemaphoreType.REGULAR((2,)),
                dma((2, 2)),
                dma((2, 2)),
                dma((2, n_relay * half_pieces)),
                dma((n_relay,)),
                pltpu.SemaphoreType.REGULAR((2,)),
                pltpu.SMEM((2 * n_chunk + max(idle) + 2 * MARGIN,), jnp.int32),
                pltpu.VMEM((2, tile_rows, tile_cols), F32),
                dma((2,)),
                pltpu.VMEM((2, 2, half_pieces, chunk, piece), BF16),
            ],
            compiler_params=pltpu.CompilerParams(collective_id=0, has_side_effects=True, vmem_limit_bytes=63 * 1024 * 1024),
            name="stage_kernel",
        )(
            inputs.reshape(n_chunk, chunk, model_dim),
            targets.reshape(n_chunk, chunk, model_dim),
            w_in.reshape(model_dim, hid_dim),
            w_out.reshape(hid_dim, model_dim),
        )

        grad_in, grad_out, loss = finish_grads(first_grads, lefts, rights, loss)
        return grad_in[None, None], grad_out[None, None], loss

    return jax.shard_map(
        stage_step,
        mesh=mesh,
        in_specs=(P("data", None, None), P("data", None, None), P("stage", None, None, "model"), P("stage", None, "model", None)),
        out_specs=(P(("data", "stage"), None, None, "model"), P(("data", "stage"), None, "model", None), P("data")),
        check_vma=False,
    )
```

```python
import functools

import jax
import jax.numpy as jnp
from jax import lax
from jax.experimental import pallas as pl
from jax.experimental.pallas import tpu as pltpu
from jax.sharding import PartitionSpec as P

GELU_COEF = 0.7978845608028654
CUBIC_COEF = 0.044715

CHUNK_TOKENS = 64
PIECE_COLS = 256
HIDDEN_COLS = 512
PARTS = 2
HOP_LAG = 2
RECV_SLOTS = 8
LAST_LEAD = 5
PREV_LEAD = 15
FIRST_IDLE = 12
NEXT_IDLE = 7
FORE_CHUNKS = 7
RELAY_CHUNKS = 19
RELAY_START = 0

FIRST_GRADS = 14
TILE_ROWS = 256
TILE_COLS = 1024
IN_FLIGHT = 8
FIRST_TILES = (32, 1)
NEXT_TILES = (14, 2)

SUM, BACK, GATHER, EARLY, TAKE, FWD, BWD = 256, 512, 1024, 2048, 4096, 8192, 16384
MARGIN = 8

BF16 = jnp.bfloat16
F32 = jnp.float32
MESH = pl.DeviceIdType.MESH


def gelu_tanh(values):
    inner_arg = GELU_COEF * (values + CUBIC_COEF * values * values * values)
    return 0.5 * values * (1.0 + jnp.tanh(inner_arg))


def gelu_slope(values):
    tanh_val = jnp.tanh(GELU_COEF * (values + CUBIC_COEF * values * values * values))
    return 0.5 * (1.0 + tanh_val) + 0.5 * values * (1.0 - tanh_val * tanh_val) * GELU_COEF * (1.0 + 3.0 * CUBIC_COEF * values * values)


def dot_nn(left, right):
    return jnp.dot(left, right, preferred_element_type=F32)


def dot_nt(left, right):
    return lax.dot_general(left, right, (((1,), (1,)), ((), ())), preferred_element_type=F32)


def stage_kernel(
    n_stage, n_model, n_chunk, half_pieces, piece, hop, lead, idle, n_fore, n_relay, n_grad, grad_scale,
    inputs_hbm, targets_hbm, w1_hbm, w2_hbm,
    left_out, right_out, grad_hbm, loss_out,
    wts, acts, hid, send_buf, recv_buf, loss_acc, loss_in,
    w_sem, in_sem, tgt_sem, sum_send, sum_recv, gat_send, gat_recv, over_send, back_send, take_recv, down_send, out_sem,
    loss_send, loss_recv, spent_sem, rel_send, rel_over, rel_recv, rel_in, free_sem, table, tile_buf, tile_sem, end_buf,
):
    pos = lax.axis_index("model")
    stage = lax.axis_index("stage")
    last_pos = n_model - 1
    last_stage = n_stage - 1
    fore_stage = n_stage - 2
    bits = half_pieces.bit_length() - 1
    total = n_chunk * half_pieces
    half = half_pieces * piece
    hid_dim = wts.shape[2]
    chunk_rows = acts.shape[2]
    hid_part = hid_dim // PARTS
    hid_cols = min(HIDDEN_COLS, hid_part)
    n_lead, n_idle = jnp.int32(n_chunk), jnp.int32(0)
    for at in range(n_stage):
        n_lead = jnp.where(stage == at, lead[at], n_lead)
        n_idle = jnp.where(stage == at, idle[at], n_idle)
    turns = 2 * n_chunk + n_idle
    n_steps = turns * half_pieces + jnp.where(stage == 0, 1 - hop, half_pieces + hop * last_pos + 1)
    early = half_pieces + 3 * hop + 1

    barrier = pltpu.get_barrier_semaphore()
    for to_stage in range(n_stage):
        for to_pos in range(n_model):

            @pl.when((to_stage != stage) | (to_pos != pos))
            def _():
                pl.semaphore_signal(barrier, inc=1, device_id={"stage": to_stage, "model": to_pos}, device_id_type=MESH)

    copy_w2 = pltpu.make_async_copy(w2_hbm, wts.at[1], w_sem.at[PARTS])

    def copy_w1(part):
        cols = pl.ds(part * hid_part, hid_part)
        return pltpu.make_async_copy(w1_hbm.at[:, cols], wts.at[0, :, cols], w_sem.at[part])


    def copy_in(chunk):
        return pltpu.make_async_copy(inputs_hbm.at[chunk], acts.at[0, chunk], in_sem.at[chunk])

    def grad_in(chunk):
        return pltpu.make_async_copy(inputs_hbm.at[chunk], acts.at[1, chunk], rel_in.at[chunk])

    def copy_targets(side):
        cols = pl.ds(side * half, half)
        return pltpu.make_async_copy(targets_hbm.at[:, :, cols], acts.at[1, :, :, cols], tgt_sem)

    def copy_out(kind, chunk):
        src = (acts.at[0], hid.at[0], hid.at[1], acts.at[1])[kind]
        dst = (left_out.at[0], left_out.at[1], right_out.at[0], right_out.at[1])[kind]
        rows = pl.ds(pl.multiple_of((chunk - n_grad) * chunk_rows, chunk_rows), chunk_rows)
        return pltpu.make_async_copy(src.at[chunk], dst.at[rows, :], out_sem.at[kind, chunk])

    @pl.when(stage == 0)
    def _():
        copy_in(0).start()

    for part in range(PARTS):
        copy_w1(part).start()
    copy_w2.start()

    @pl.when(stage == 0)
    def _():
        def start_in(chunk, carry):
            copy_in(chunk).start()
            return carry

        lax.fori_loop(1, n_chunk, start_in, 0)

    @pl.when((stage == last_stage) & (pos == last_pos))
    def _():
        copy_targets(0).start()

    @pl.when((stage == last_stage) & (pos == 0))
    def _():
        copy_targets(1).start()

    def transpose_weights():
        tile = min(256, hid_dim)
        count = hid_dim // tile

        def one(index, carry):
            rows = pl.ds(pl.multiple_of((index // count) * tile, tile), tile)
            cols = pl.ds(pl.multiple_of((index % count) * tile, tile), tile)
            wts[2, cols, rows] = jnp.swapaxes(wts[1, rows, cols], 0, 1)
            wts[3, cols, rows] = jnp.swapaxes(wts[0, rows, cols], 0, 1)
            return carry

        lax.fori_loop(0, count * count, one, 0)

    n_mixed = 2 * (n_chunk - n_lead)
    n_after = 2 * n_chunk - n_lead
    n_first = n_lead + n_idle

    def fill(entry, carry):
        turn = entry - MARGIN
        after = turn - n_first
        pair = (after + 1024) // 2 - 512
        odd = (after + 1024) % 2 == 1
        mixed = (after >= 0) & (after < n_mixed)
        leads = (turn >= 0) & (turn < n_lead)
        fwd = leads | (mixed & odd)
        bwd = (after >= 0) & (after < n_after) & jnp.logical_not(mixed & odd)
        chunk = jnp.where(leads, turn, jnp.where(odd, n_lead + pair, pair))
        chunk = jnp.where(bwd & (after >= n_mixed), after - (n_chunk - n_lead), chunk)
        early_one = fwd & (stage == fore_stage - 1) & (chunk < n_fore)
        back = bwd & (stage < last_stage) & ((stage < fore_stage) | (chunk >= n_relay))
        take = back | (fwd & (stage == fore_stage) & (chunk < n_fore))
        word = jnp.int32(0)
        for flag, bit in (
            (fwd | (bwd & (stage > 0)), SUM),
            (bwd, BACK),
            (fwd & jnp.logical_not(early_one), GATHER),
            (early_one, EARLY),
            (take, TAKE),
            (fwd, FWD),
            (bwd, BWD),
        ):
            word = word + jnp.where(flag, bit, 0)
        table[entry] = word
        return carry

    lax.fori_loop(0, table.shape[0], fill, 0)
    loss_acc[...] = jnp.zeros_like(loss_acc)
    copy_w1(0).wait()

    @pl.when(stage > 0)
    def _():
        for part in range(1, PARTS):
            copy_w1(part).wait()
        copy_w2.wait()
        transpose_weights()

    def meet():
        pl.semaphore_wait(barrier, n_stage * n_model - 1)

    @pl.when(stage == fore_stage)
    def _():
        meet()


    def turn_of(place):
        return lax.shift_right_logical(place + MARGIN * half_pieces, jnp.int32(bits))

    def piece_of(place):
        return lax.bitwise_and(place + MARGIN * half_pieces, jnp.int32(half_pieces - 1))

    def has(word, mask):
        return lax.bitwise_and(word, jnp.int32(mask)) != 0

    def fwd_chunk(turn):
        after = turn - (n_first + MARGIN)
        return jnp.where(turn < n_lead + MARGIN, turn - MARGIN, n_lead + lax.shift_right_arithmetic(after, jnp.int32(1)))

    def bwd_chunk(turn):
        after = turn - (n_first + MARGIN)
        return jnp.where(after < n_mixed, lax.shift_right_arithmetic(after, jnp.int32(1)), after - (n_chunk - n_lead))

    def back_of(turn):
        after = turn - (n_first + MARGIN)
        odd = lax.bitwise_and(after, jnp.int32(1)) == 1
        return ((after >= 0) & jnp.logical_not((after < n_mixed) & odd)).astype(jnp.int32)

    def chunk_of(turn, is_back):
        return jnp.clip(jnp.where(is_back == 1, bwd_chunk(turn), fwd_chunk(turn)), 0, n_chunk - 1)

    def piece_at(side, index):
        col = side * half + index * piece
        return pl.ds(pl.multiple_of(col, piece), piece)

    def remote(src, dst, send_sem, recv_sem, device):
        return pltpu.make_async_remote_copy(
            src_ref=src, dst_ref=dst, send_sem=send_sem, recv_sem=recv_sem, device_id=device, device_id_type=MESH
        )

    def left(send_sem, like):
        remote(like, like, send_sem, loss_recv.at[0], {"model": pos}).wait_send()

    turn_pieces = acts.at[0, 0, :, pl.ds(0, half)]
    turn_sums = send_buf.at[0, 0]

    def rank_of(side):
        return pos if side == 0 else last_pos - pos

    def up(side):
        return {"model": pos + 1 if side == 0 else pos - 1}

    def down(side):
        return {"model": pos - 1 if side == 0 else pos + 1}

    def first_product(step, part):
        place = step + PARTS - 1 - part
        turn = turn_of(place)
        word = table[turn]
        starts = piece_of(place) == 0

        @pl.when(starts & has(word, FWD))
        def _():
            chunk = fwd_chunk(turn)
            if part == 0:

                @pl.when((stage != fore_stage) | (chunk >= n_fore))
                def _():
                    copy_in(chunk).wait()

                @pl.when(chunk >= n_grad)
                def _():
                    copy_out(0, chunk).start()

            else:

                @pl.when((stage == 0) & (place == 0))
                def _():
                    copy_w1(part).wait()

            for col in range(part * hid_part, (part + 1) * hid_part, hid_cols):
                cols = pl.ds(col, hid_cols)
                pre = dot_nn(acts[0, chunk], wts[0, :, cols]).astype(BF16)
                hid[1, chunk, :, cols] = pre
                hid[0, chunk, :, cols] = gelu_tanh(pre.astype(F32)).astype(BF16)
            if part == PARTS - 1:

                @pl.when(chunk >= n_grad)
                def _():
                    copy_out(1, chunk).start()

                @pl.when((stage == 0) & (place == 0))
                def _():
                    copy_w2.wait()

        @pl.when(starts & has(word, BWD))
        def _():
            chunk = bwd_chunk(turn)
            if part == 0:

                @pl.when((stage == fore_stage) & (chunk < n_relay))
                def _():
                    grad_in(chunk).wait()

                @pl.when(chunk >= n_grad)
                def _():
                    copy_out(3, chunk).start()

            for col in range(part * hid_part, (part + 1) * hid_part, hid_cols):
                cols = pl.ds(col, hid_cols)
                grad_act = dot_nn(acts[1, chunk], wts[2, :, cols]).astype(BF16)
                slope = gelu_slope(hid[1, chunk, :, cols].astype(F32))
                hid[1, chunk, :, cols] = (slope * grad_act.astype(F32)).astype(BF16)
            if part == PARTS - 1:

                @pl.when(chunk >= n_grad)
                def _():
                    copy_out(2, chunk).start()

        if part == 0:

            @pl.when((stage == 0) & (place == n_lead * half_pieces))
            def _():
                transpose_weights()

    def loss_copy(side, to_stage, to_pos):
        return remote(
            loss_acc, loss_in.at[side], loss_send.at[to_stage * n_model + to_pos], loss_recv.at[side],
            {"stage": to_stage, "model": to_pos},
        )

    def send_loss(side):
        loss_in[side] = loss_acc[...]
        for to_stage in range(n_stage):
            for to_pos in range(n_model):

                @pl.when((to_stage != stage) | (to_pos != pos))
                def _():
                    loss_copy(side, to_stage, to_pos).start()

    def sum_steps(step):
        now = []
        for side in (0, 1):
            rank = rank_of(side)
            place = step - hop * rank
            turn = turn_of(place)
            word, old = table[turn], table[turn - 2]
            index = piece_of(place)
            half_turn = lax.bitwise_and(turn, jnp.int32(1))
            inn = lax.bitwise_and(place + MARGIN * half_pieces, jnp.int32(RECV_SLOTS - 1))
            sums = has(word, SUM)
            is_back = back_of(turn)
            now.append((rank, word, sums, is_back, chunk_of(turn, is_back), index, half_turn, inn, piece_at(side, index)))

            @pl.when((index == 0) & has(old, SUM))
            def _():
                @pl.when(rank < last_pos)
                def _():
                    left(sum_send.at[side, half_turn], turn_sums)

                @pl.when((rank == last_pos) & has(old, BACK))
                def _():
                    left(down_send.at[side, half_turn], turn_pieces)

        @pl.when(now[0][2] | now[1][2])
        def _():
            for side in (0, 1):
                _, _, _, is_back, chunk, index, half_turn, _, cols = now[side]
                send_buf[side, half_turn, index] = dot_nn(hid[is_back, chunk], wts[1 + 2 * is_back, :, cols])

        for side in (0, 1):
            rank, word, sums, is_back, chunk, out, half_turn, inn, cols = now[side]
            bwd = has(word, BACK)
            index = chunk * half_pieces + out
            mine = send_buf.at[side, half_turn, out]
            gone = down_send.at[side, half_turn]
            hand_on = remote(mine, recv_buf.at[side, inn], sum_send.at[side, half_turn], sum_recv.at[side, inn], up(side))

            @pl.when(sums & (rank > 0))
            def _():
                hand_on.wait_recv()
                mine[...] = mine[...] + recv_buf[side, inn]

            @pl.when(sums & (rank < last_pos))
            def _():
                hand_on.start()

            @pl.when(sums & (rank == last_pos))
            def _():
                whole = acts[is_back, chunk, :, cols].astype(F32) + mine[...]
                scored = has(word, FWD) & (stage == last_stage)

                @pl.when(scored)
                def _():
                    @pl.when(index == 0)
                    def _():
                        copy_targets(side).wait()

                    err = whole.astype(BF16).astype(F32) - acts[1, chunk, :, cols].astype(F32)
                    acts[1, chunk, :, cols] = (err * grad_scale).astype(BF16)
                    square = jnp.sum((err * err).reshape(err.shape[0] // 8, 8, piece), axis=0)
                    part = square[:, :128]
                    for lane in range(1, piece // 128):
                        part = part + square[:, lane * 128 : (lane + 1) * 128]
                    loss_acc[...] = loss_acc[...] + part

                    @pl.when(index == total - 1)
                    def _():
                        send_loss(side)

                @pl.when(has(word, FWD) & (stage < last_stage))
                def _():
                    acts[1, chunk, :, cols] = whole.astype(BF16)

                ended = end_buf.at[side, half_turn, out]

                @pl.when(bwd)
                def _():
                    ended[...] = whole.astype(BF16)

                @pl.when(bwd & (index == total - 2 * half_pieces))
                def _():
                    pl.semaphore_wait(spent_sem.at[side], 1)

                @pl.when(bwd & (stage == 1) & (index == (n_relay - 2) * half_pieces))
                def _():
                    pl.semaphore_wait(free_sem.at[side], 1)

                relayed = (stage == last_stage) & (chunk < n_relay)
                there = acts.at[1, chunk, :, cols]

                @pl.when(bwd & relayed)
                def _():
                    arrived = rel_recv.at[side, jnp.minimum(index, n_relay * half_pieces - 1)]
                    remote(ended, there, gone, arrived, {"stage": 0}).start()

                @pl.when(bwd & jnp.logical_not(relayed))
                def _():
                    arrived = take_recv.at[side, index]
                    remote(ended, there, gone, arrived, {"stage": stage - 1}).start()

    def gather_step(side, step):
        rank = rank_of(side)
        place = step - 1 - 3 * hop - hop * (last_pos - rank)
        turn = turn_of(place)
        word, old = table[turn], table[turn - 2]
        out = piece_of(place)
        half_turn = lax.bitwise_and(turn, jnp.int32(1))
        chunk = jnp.clip(fwd_chunk(turn), 0, n_chunk - 1)
        index = chunk * half_pieces + out
        cols = piece_at(side, out)
        here = acts.at[1, chunk, :, cols]
        gone = over_send.at[side, half_turn]

        @pl.when((out == 0) & has(old, GATHER | EARLY))
        def _():
            @pl.when(has(old, GATHER) & (rank > 0))
            def _():
                left(gat_send.at[side, half_turn], turn_pieces)

            @pl.when((stage < last_stage) & (has(old, GATHER) | (rank == last_pos)))
            def _():
                left(gone, turn_pieces)

                @pl.when((fwd_chunk(turn - 2) == n_chunk - 1) & (rank == last_pos))
                def _():
                    pl.semaphore_signal(spent_sem.at[side], inc=1, device_id={"stage": stage + 1}, device_id_type=MESH)

        @pl.when(has(word, GATHER))
        def _():
            hand_on = remote(here, here, gat_send.at[side, half_turn], gat_recv.at[side, index], down(side))

            @pl.when(rank < last_pos)
            def _():
                hand_on.wait_recv()

            @pl.when(rank > 0)
            def _():
                hand_on.start()

            @pl.when(stage < last_stage)
            def _():
                remote(here, acts.at[0, chunk, :, cols], gone, in_sem.at[chunk], {"stage": stage + 1}).start()

        @pl.when(has(word, EARLY) & (rank == last_pos))
        def _():
            arrived = take_recv.at[side, jnp.minimum(total + index, total + n_fore * half_pieces - 1)]
            remote(here, acts.at[0, chunk, :, cols], gone, arrived, {"stage": stage + 1}).start()

    def take_step(side, step):
        rank = rank_of(side)
        place = step + early - hop * (last_pos - rank)
        turn = turn_of(place)
        word, old = table[turn], table[turn - 2]
        out = piece_of(place)
        gone = back_send.at[side, lax.bitwise_and(turn, jnp.int32(1))]

        @pl.when((out == 0) & has(old, TAKE) & (rank > 0))
        def _():
            left(gone, turn_pieces)

        @pl.when(has(word, TAKE))
        def _():
            is_back = back_of(turn)
            chunk = chunk_of(turn, is_back)
            index = chunk * half_pieces + out + (1 - is_back) * total
            here = acts.at[is_back, chunk, :, piece_at(side, out)]
            hand_on = remote(here, here, gone, take_recv.at[side, index], down(side))
            hand_on.wait_recv()

            @pl.when(rank > 0)
            def _():
                hand_on.start()

    def relay_step(side, step):
        rank = rank_of(side)
        place = step - (n_chunk + RELAY_START) * half_pieces - hop * (last_pos - rank)
        turn = turn_of(place) - MARGIN
        out = piece_of(place)
        half_turn = lax.bitwise_and(turn, jnp.int32(1))
        chunk = jnp.clip(turn, 0, n_relay - 1)
        here = acts.at[1, chunk, :, piece_at(side, out)]
        gone = rel_over.at[side, half_turn]
        hand_on = remote(here, here, rel_send.at[side, half_turn], rel_recv.at[side, chunk * half_pieces + out], down(side))

        @pl.when((out == 0) & (turn >= 2) & (turn < n_relay + 2))
        def _():
            @pl.when(rank > 0)
            def _():
                left(rel_send.at[side, half_turn], turn_pieces)

            left(gone, turn_pieces)

            @pl.when((turn == n_relay + 1) & (rank == last_pos))
            def _():
                pl.semaphore_signal(free_sem.at[side], inc=1, device_id={"stage": 1}, device_id_type=MESH)

        @pl.when((turn >= 0) & (turn < n_relay))
        def _():
            hand_on.wait_recv()

            @pl.when(rank > 0)
            def _():
                hand_on.start()

            remote(here, here, gone, rel_in.at[chunk], {"stage": fore_stage}).start()

    tile_rows, tile_cols = tile_buf.shape[1], tile_buf.shape[2]
    per_row = wts.shape[1] // tile_cols
    n_tiles = hid_dim // tile_rows * per_row

    def copy_tile(which, index):
        rows = pl.ds(pl.multiple_of(index // per_row * tile_rows, tile_rows), tile_rows)
        cols = pl.ds(pl.multiple_of(index % per_row * tile_cols, tile_cols), tile_cols)
        return pltpu.make_async_copy(tile_buf.at[index % 2], grad_hbm.at[which, rows, cols], tile_sem.at[index % 2])

    def grad_tile(number):
        for which, index in ((1, number), (0, number - n_tiles)):

            @pl.when((index >= 0) & (index < n_tiles))
            def _():
                rows = pl.ds(pl.multiple_of(index // per_row * tile_rows, tile_rows), tile_rows)
                cols = pl.ds(pl.multiple_of(index % per_row * tile_cols, tile_cols), tile_cols)

                @pl.when(number >= 2)
                def _():
                    copy_tile(which, index).wait()

                inputs, grads = (acts.at[0], hid.at[1]) if which == 0 else (hid.at[0], acts.at[1])
                lefts = inputs[0:n_grad, :, rows].reshape(n_grad * chunk_rows, tile_rows)
                rights = grads[0:n_grad, :, cols].reshape(n_grad * chunk_rows, tile_cols)
                tile_buf[index % 2] = lax.dot_general(lefts, rights, (((0,), (0,)), ((), ())), preferred_element_type=F32)
                copy_tile(which, index).start()

    in_loop = jnp.where(stage == 0, FIRST_TILES[0], jnp.where(stage == 1, NEXT_TILES[0], 0))
    pitch = jnp.where(stage == 0, FIRST_TILES[1], NEXT_TILES[1])
    first_tile = (n_first + n_grad) * half_pieces

    def loop_step(step, carry):
        for part in range(PARTS):
            first_product(step, part)

        @pl.when((step == 0) & (stage != fore_stage))
        def _():
            meet()

        gather_step(0, step)
        gather_step(1, step)
        sum_steps(step)

        @pl.when((stage == 0) & (step >= n_chunk * half_pieces))
        def _():
            relay_step(0, step)
            relay_step(1, step)

        take_step(0, step)
        take_step(1, step)
        since = step - first_tile

        @pl.when((since >= 0) & (since < in_loop * pitch) & (since % pitch == 0))
        def _():
            grad_tile(since // pitch)

        return carry

    lax.fori_loop(jnp.where(stage == fore_stage, -early, 1 - PARTS), n_steps, loop_step, 0)

    def next_tile(number, carry):
        grad_tile(number)
        return carry

    lax.fori_loop(in_loop, 2 * n_tiles, next_tile, 0)

    for side, owner in ((0, last_pos), (1, 0)):
        owns = (stage == last_stage) & (pos == owner)

        @pl.when(jnp.logical_not(owns))
        def _():
            loss_copy(side, 0, 0).wait_recv()

        @pl.when(owns)
        def _():
            for to_stage in range(n_stage):
                for to_pos in range(n_model):

                    @pl.when((to_stage != stage) | (to_pos != pos))
                    def _():
                        loss_copy(side, to_stage, to_pos).wait_send()

    loss_out[...] = jnp.full(loss_out.shape, jnp.sum(loss_in[0] + loss_in[1]) * (0.5 * grad_scale), F32)

    for index in (0, 1):
        copy_tile(0, index).wait()

    def end_out(chunk, carry):
        for kind in range(4):
            copy_out(kind, chunk).wait()
        return carry

    lax.fori_loop(n_grad, n_chunk, end_out, 0)


def finish_kernel(
    first_hbm, lefts_hbm, rights_hbm, loss_hbm, grad_in, grad_out, loss_out, sums, lefts, rights, loss, sum_in, sum_out, operand_in, loss_sem
):
    block = sums.shape[1]
    blocks = grad_in.shape[0] // block
    half = lefts.shape[1] // 2

    def copy_operands(which):
        pairs = ((rights_hbm, rights, 0), (lefts_hbm, lefts, 1))
        return [
            pltpu.make_async_copy(
                src.at[which, pl.ds(part * half, half), :], dst.at[which, pl.ds(part * half, half), :], operand_in.at[which, kind, part]
            )
            for src, dst, kind in pairs
            for part in (0, 1)
        ]

    def rows_of(number):
        return pl.ds(pl.multiple_of(number % blocks * block, block), block)

    def copy_first(number):
        return pltpu.make_async_copy(first_hbm.at[number // blocks, rows_of(number), :], sums.at[number], sum_in.at[number])

    def copy_result(number, which):
        return pltpu.make_async_copy(sums.at[number], (grad_in, grad_out)[which].at[rows_of(number), :], sum_out.at[number])

    copy_loss = pltpu.make_async_copy(loss_hbm, loss, loss_sem)
    for copy in copy_operands(0):
        copy.start()
    for number in range(IN_FLIGHT):
        copy_first(number).start()
    copy_loss.start()

    def one(number, carry):
        for which in (0, 1):

            @pl.when(number == which * blocks)
            def _():
                for copy in copy_operands(which):
                    copy.wait()

        @pl.when(number == 1)
        def _():
            for copy in copy_operands(1):
                copy.start()

        copy_first(number).wait()

        @pl.when(number + IN_FLIGHT < 2 * blocks)
        def _():
            copy_first(number + IN_FLIGHT).start()

        which = number // blocks
        part = lax.dot_general(
            lefts[which, :, rows_of(number)], rights[which], (((0,), (0,)), ((), ())), preferred_element_type=F32
        )
        sums[number] = sums[number] + part

        for kind in (0, 1):

            @pl.when(which == kind)
            def _():
                copy_result(number, kind).start()

        return carry

    lax.fori_loop(0, 2 * blocks, one, 0)
    copy_loss.wait()
    loss_out[0] = loss[0, 0]

    def end(number, carry):
        copy_result(number, 0).wait()
        return carry

    lax.fori_loop(0, 2 * blocks, end, 0)


def finish_grads(first, lefts, rights, loss):
    rows, dim = lefts.shape[1:]
    block = min(TILE_ROWS, dim)
    blocks = dim // block
    shape = jax.ShapeDtypeStruct((dim, dim), F32)
    any_space = pl.BlockSpec(memory_space=pl.ANY)
    dma = pltpu.SemaphoreType.DMA
    return pl.pallas_call(
        finish_kernel,
        out_shape=(shape, shape, jax.ShapeDtypeStruct((1,), F32)),
        in_specs=[any_space] * 4,
        out_specs=(any_space, any_space, pl.BlockSpec(memory_space=pltpu.SMEM)),
        scratch_shapes=[
            pltpu.VMEM((2 * blocks, block, dim), F32),
            pltpu.VMEM((2, rows, dim), BF16),
            pltpu.VMEM((2, rows, dim), BF16),
            pltpu.VMEM(loss.shape, F32),
            dma((2 * blocks,)),
            dma((2 * blocks,)),
            dma((2, 2, 2)),
            dma,
        ],
        compiler_params=pltpu.CompilerParams(vmem_limit_bytes=62 * 1024 * 1024),
        cost_estimate=pl.CostEstimate(flops=4 * rows * dim * dim, bytes_accessed=16 * dim * dim, transcendentals=0),
        name="finish_kernel",
    )(first, lefts, rights, loss)


def solution(mesh):
    n_stage = mesh.shape["stage"]
    n_model = mesh.shape["model"]

    def stage_step(inputs, targets, w_in, w_out):
        num_micro, num_tokens, model_dim = inputs.shape
        hid_dim = w_in.shape[3]
        rows = num_micro * num_tokens
        chunk = min(CHUNK_TOKENS, num_tokens)
        n_chunk = rows // chunk
        piece = min(PIECE_COLS, model_dim // 2)
        half_pieces = model_dim // 2 // piece
        grad_scale = 1.0 / (rows * model_dim)
        lead = [n_chunk] * (n_stage - 2) + [min(PREV_LEAD, n_chunk), min(LAST_LEAD, n_chunk)]
        idle = [FIRST_IDLE] + [NEXT_IDLE] * (n_stage - 3) + [0, 0]
        n_fore, n_relay = min(FORE_CHUNKS, n_chunk - 1), min(RELAY_CHUNKS, n_chunk - 1)
        n_grad = min(FIRST_GRADS, n_chunk // 2)
        rest = rows - n_grad * chunk
        tile_rows, tile_cols = min(TILE_ROWS, hid_dim), min(TILE_COLS, model_dim)
        kernel = functools.partial(
            stage_kernel, n_stage, n_model, n_chunk, half_pieces, piece, HOP_LAG, lead, idle, n_fore, n_relay, n_grad, grad_scale
        )
        any_space = pl.BlockSpec(memory_space=pl.ANY)
        dma = pltpu.SemaphoreType.DMA
        lefts, rights, first_grads, loss = pl.pallas_call(
            kernel,
            out_shape=(
                jax.ShapeDtypeStruct((2, rest, model_dim), BF16),
                jax.ShapeDtypeStruct((2, rest, model_dim), BF16),
                jax.ShapeDtypeStruct((2, hid_dim, model_dim), F32),
                jax.ShapeDtypeStruct((8, 128), F32),
            ),
            in_specs=[any_space] * 4,
            out_specs=(any_space, any_space, any_space, pl.BlockSpec(memory_space=pltpu.VMEM)),
            scratch_shapes=[
                pltpu.VMEM((4, model_dim, hid_dim), BF16),
                pltpu.VMEM((2, n_chunk, chunk, model_dim), BF16),
                pltpu.VMEM((2, n_chunk, chunk, hid_dim), BF16),
                pltpu.VMEM((2, 2, half_pieces, chunk, piece), F32),
                pltpu.VMEM((2, RECV_SLOTS, chunk, piece), F32),
                pltpu.VMEM((8, 128), F32),
                pltpu.VMEM((2, 8, 128), F32),
                dma((PARTS + 1,)),
                dma((n_chunk,)),
                dma,
                dma((2, 2)),
                dma((2, RECV_SLOTS)),
                dma((2, 2)),
                dma((2, n_chunk * half_pieces)),
                dma((2, 2)),
                dma((2, 2)),
                dma((2, (n_chunk + n_fore) * half_pieces)),
                dma((2, 2)),
                dma((4, n_chunk)),
                dma((n_stage * n_model,)),
                dma((2,)),
                pltpu.SemaphoreType.REGULAR((2,)),
                dma((2, 2)),
                dma((2, 2)),
                dma((2, n_relay * half_pieces)),
                dma((n_relay,)),
                pltpu.SemaphoreType.REGULAR((2,)),
                pltpu.SMEM((2 * n_chunk + max(idle) + 2 * MARGIN,), jnp.int32),
                pltpu.VMEM((2, tile_rows, tile_cols), F32),
                dma((2,)),
                pltpu.VMEM((2, 2, half_pieces, chunk, piece), BF16),
            ],
            compiler_params=pltpu.CompilerParams(collective_id=0, has_side_effects=True, vmem_limit_bytes=63 * 1024 * 1024),
            name="stage_kernel",
        )(
            inputs.reshape(n_chunk, chunk, model_dim),
            targets.reshape(n_chunk, chunk, model_dim),
            w_in.reshape(model_dim, hid_dim),
            w_out.reshape(hid_dim, model_dim),
        )

        grad_in, grad_out, loss = finish_grads(first_grads, lefts, rights, loss)
        return grad_in[None, None], grad_out[None, None], loss

    return jax.shard_map(
        stage_step,
        mesh=mesh,
        in_specs=(P("data", None, None), P("data", None, None), P("stage", None, None, "model"), P("stage", None, "model", None)),
        out_specs=(P(("data", "stage"), None, None, "model"), P(("data", "stage"), None, "model", None), P("data")),
        check_vma=False,
    )
```
